32 devices in a mesh: gy: 8 (over z, core), gz: 4 (over y, x).
Axes of the slice: x: 2, y: 2, z: 4, core: 2. Of those that a mesh axis runs over, the one named last changes fastest.
Arguments:
- measured: float32 [4, 1024, 1024], P('gz', 'gy'), may hold values from -20 to 20
- point_spread: float32 [1024, 1024], P('gy'), may hold values from -0.005859375 to 0.005859375
- stencil_weights: float32 [3, 3, 3], replicated, may hold values from -0.9 to 0.9
- upstream: float32 [4, 1024, 1024], P('gz', 'gy'), may hold values from -6 to 6
Outputs:
- grad_measured: float32 [4, 1024, 1024], P('gz', 'gy')
- grad_stencil: float32 [3, 3, 3], replicated
The draws below stay inside these ranges and needn't reach their ends.
All inputs are finite; a program needn't handle non-finite values.
Results may differ from the reference program's by a relative error of at most 0.00021.
Values sent between devices are 32-bit elements; how exact they have to be, the bound alone decides.
A program may use at most 64 MiB of HBM per device.

```python
import math
import jax
import jax.numpy as jnp

X = 1024
Y = 1024
ITERS = 2
Z = 4


def draw_measured(key, part):
    subkeys = jax.random.split(jax.random.fold_in(key, 11), 1)
    plane_index = jnp.arange(Z, dtype=jnp.float32)[:, None, None]
    attenuation = jnp.exp(-math.log(3.0) * plane_index / max(Z - 1, 1))
    return jnp.clip(jax.random.normal(subkeys[0], (Z, Y, X), jnp.float32), -6.0, 6.0) * attenuation


def block_levels(key, shape, cuts, smallest, largest):
    gain, own = 1.0, jax.random.fold_in(key, 6)
    for dim, blocks in cuts:
        heights = jnp.exp(jax.random.uniform(jax.random.fold_in(own, dim), (blocks,), jnp.float32, smallest / len(cuts), largest / len(cuts)))
        gain = gain * jnp.repeat(heights, shape[dim] // blocks).reshape([-1 if axis == dim else 1 for axis in range(len(shape))])
    return gain


def normal_values(own_key, extent, deviation, bound, pieces=(), kind=jnp.bfloat16):
    values = deviation * jax.random.normal(own_key, extent, jnp.float32)
    if pieces:
        values = values * block_levels(own_key, extent, pieces, -0.22, 0.18)
    return jnp.clip(values, -bound, bound).astype(kind)


def setup_inputs(seed: int = 0) -> dict:
    key_of = jax.random.split(jax.random.key(seed), 5)
    measured = draw_measured(jax.random.fold_in(key_of[4], 71), 0)
    point_spread = normal_values(key_of[1], (Y, X), (X * Y) ** -0.5, 0.005859375, ((0, 8),), jnp.float32)
    stencil_weights = normal_values(key_of[2], (3, 3, 3), 0.15, 0.9, (), jnp.float32)
    upstream = normal_values(key_of[3], (Z, Y, X), 1.0, 6.0, ((0, 4), (1, 8)), jnp.float32)
    return dict(measured=measured, point_spread=point_spread, stencil_weights=stencil_weights, upstream=upstream)


def apply_stencil(volume, kernel):
    planes, row_count, columns = volume.shape
    padded = jnp.pad(volume, 1)
    summed = jnp.zeros(volume.shape, jnp.float32)
    for shift_z in range(3):
        for shift_y in range(3):
            for shift_x in range(3):
                summed = summed + kernel[shift_z, shift_y, shift_x] * padded[shift_z:shift_z + planes, shift_y:shift_y + row_count, shift_x:shift_x + columns]
    return summed

def regularize(volume, kernel):
    mapped = apply_stencil(volume, kernel)
    return apply_stencil(mapped, kernel[::-1, ::-1, ::-1])

def filtered(volume, response):
    spectrum = jnp.fft.fft2(volume, axes=(1, 2))
    return jnp.real(jnp.fft.ifft2(spectrum * response, axes=(1, 2))).astype(jnp.float32)

def restore(measured, kernel, transfer):
    power_gain = jnp.real(transfer) ** 2 + jnp.imag(transfer) ** 2
    right_side = filtered(measured, jnp.conj(transfer))
    solution = jnp.zeros_like(right_side)
    residual = right_side
    direction = right_side
    norm_now = jnp.sum(residual * residual)
    for iteration in range(ITERS):
        applied = filtered(direction, power_gain) + regularize(direction, kernel)
        step_size = norm_now / jnp.sum(direction * applied)
        solution = solution + step_size * direction
        if iteration + 1 < ITERS:
            residual = residual - step_size * applied
            norm_next = jnp.sum(residual * residual)
            direction = residual + norm_next / norm_now * direction
            norm_now = norm_next
    return solution

def reference(measured, point_spread, stencil_weights, upstream):
    transfer = jnp.fft.fft2(point_spread)

    def forward(values, weights):
        return restore(values, weights, transfer)
    unused, pullback = jax.vjp(forward, measured, stencil_weights)
    grad_measured, grad_weights = pullback(upstream)
    return (grad_measured, grad_weights / math.sqrt(X * Y * Z))
```

```python
import math

import jax
import jax.numpy as jnp
import numpy as np
from jax import lax
from jax.experimental import pallas as pl
from jax.experimental.pallas import tpu as pltpu
from jax.sharding import PartitionSpec as P

MESH = pl.DeviceIdType.MESH
SIDES = [(dy, dz) for dy in (-1, 0, 1) for dz in (-1, 0, 1) if (dy, dz) != (0, 0)]
VMEM = pl.BlockSpec(memory_space=pltpu.VMEM)
SMEM = pl.BlockSpec(memory_space=pltpu.SMEM)


def moved(value, shift):
    if shift == 0:
        return value
    width = value.shape[1]
    lane = lax.broadcasted_iota(jnp.int32, value.shape, 1)
    edge = 0 if shift > 0 else width - 1
    return jnp.where(lane == edge, 0.0, pltpu.roll(value, shift % width, 1))


def regular_kernel(count_y, count_z, weights, volume, back, grown, mapped, shifted, send, receive):
    rows, columns = volume.shape
    y, z = (lax.axis_index("gy"), lax.axis_index("gz"))

    def there(dy, dz):
        return (y + dy >= 0) & (y + dy < count_y) & (z + dz >= 0) & (z + dz < count_z)

    barrier = pltpu.get_barrier_semaphore()
    for dy, dz in SIDES:

        @pl.when(there(dy, dz))
        def _():
            pl.semaphore_signal(barrier, inc=1, device_id=(y + dy, z + dz), device_id_type=MESH)

    def span(place, count):
        return 1 + jnp.where(place > 0, 1, 0) + jnp.where(place < count - 1, 1, 0)

    pl.semaphore_wait(barrier, span(y, count_y) * span(z, count_z) - 1)

    def copy(field, phase, number):
        dy, dz = SIDES[number]
        source = field.at[1, pl.ds(rows if dy > 0 else 8, 8 if dy else rows)]
        start = 8 if dy == 0 else 0 if dy > 0 else rows + 8
        return pltpu.make_async_remote_copy(
            src_ref=source,
            dst_ref=field.at[1 - dz, pl.ds(start, 8 if dy else rows)],
            send_sem=send.at[phase, number],
            recv_sem=receive.at[phase, number],
            device_id=(y + dy, z + dz),
            device_id_type=MESH,
        )

    def exchange(field, phase):
        for number, (dy, dz) in enumerate(SIDES):

            @pl.when(there(dy, dz))
            def _():
                copy(field, phase, number).start()

        for number, (dy, dz) in enumerate(SIDES):
            start = 8 if dy == 0 else 0 if dy > 0 else rows + 8

            @pl.when(jnp.logical_not(there(-dy, -dz)))
            def _():
                field[1 - dz, pl.ds(start, 8 if dy else rows)] = jnp.zeros(
                    (8 if dy else rows, columns), jnp.float32
                )

        for number, (dy, dz) in enumerate(SIDES):

            @pl.when(there(-dy, -dz))
            def _():
                copy(field, phase, number).wait_recv()

            @pl.when(there(dy, dz))
            def _():
                copy(field, phase, number).wait_send()

    def apply(field, flip, put):
        def weight(a, b, c):
            return weights[26 - (9 * a + 3 * b + c) if flip else 9 * a + 3 * b + c]

        @pl.loop(0, (rows + 16) // 8)
        def _(step):
            here = pl.ds(pl.multiple_of(step * 8, 8), 8)
            sums = [None] * 3
            for a in range(3):
                value = field[a, here]
                for c in range(3):
                    turned = moved(value, 1 - c)
                    for b in range(3):
                        term = weight(a, b, c) * turned
                        sums[b] = term if sums[b] is None else sums[b] + term
            for b in range(3):
                shifted[b, here] = sums[b]

        @pl.loop(0, rows // 8)
        def _(step):
            first = pl.multiple_of(step * 8, 8)
            around = pl.ds(first, 24)
            total = shifted[1, pl.ds(first + 8, 8)]
            total = total + shifted[0, around][7:15] + shifted[2, around][9:17]
            put(first, total)

    @pl.loop(0, rows // 8)
    def _(step):
        first = pl.multiple_of(step * 8, 8)
        grown[1, pl.ds(first + 8, 8)] = volume[pl.ds(first, 8)]

    exchange(grown, 0)

    def put_mapped(first, total):
        mapped[1, pl.ds(first + 8, 8)] = total

    apply(grown, False, put_mapped)
    exchange(mapped, 1)

    def put_back(first, total):
        back[pl.ds(first, 8)] = total

    apply(mapped, True, put_back)


def regular(volume, kernel):
    rows, columns = volume.shape[1:]
    count_y, count_z = (lax.axis_size("gy"), lax.axis_size("gz"))
    field = jax.ShapeDtypeStruct((3, rows + 16, columns), jnp.float32)

    def body(*refs):
        regular_kernel(count_y, count_z, *refs)

    back, grown, mapped = pl.pallas_call(
        body,
        out_shape=(jax.ShapeDtypeStruct((rows, columns), jnp.float32), field, field),
        in_specs=[SMEM, VMEM],
        out_specs=(VMEM, VMEM, VMEM),
        scratch_shapes=[
            pltpu.VMEM((3, rows + 16, columns), jnp.float32),
            pltpu.SemaphoreType.DMA((2, 8)),
            pltpu.SemaphoreType.DMA((2, 8)),
        ],
        cost_estimate=pl.CostEstimate(flops=120 * rows * columns, bytes_accessed=20 * rows * columns, transcendentals=0),
        compiler_params=pltpu.CompilerParams(collective_id=0, has_side_effects=True),
        name="regular",
    )(kernel.reshape(27), volume[0])
    return (back[None], grown, mapped)


def total_kernel(count_y, count_z, value, out, column, row, across, send, receive):
    y, z = (lax.axis_index("gy"), lax.axis_index("gz"))
    along_y = [(lax.rem(y + k, count_y), z) for k in range(1, count_y)]
    along_z = [(y, lax.rem(z + k, count_z)) for k in range(1, count_z)]
    barrier = pltpu.get_barrier_semaphore()
    for place in along_y + along_z:
        pl.semaphore_signal(barrier, inc=1, device_id=place, device_id_type=MESH)
    pl.semaphore_wait(barrier, count_y + count_z - 2)

    def gather(source, slots, places, base):
        copies = []
        for k, place in enumerate(places):
            copies.append(
                pltpu.make_async_remote_copy(
                    src_ref=source,
                    dst_ref=slots.at[k],
                    send_sem=send.at[base + k],
                    recv_sem=receive.at[base + k],
                    device_id=place,
                    device_id_type=MESH,
                )
            )
            copies[-1].start()
        for item in copies:
            item.wait()

    def ordered(own, slots, index, count):
        total = jnp.zeros_like(own)
        for j in range(count):
            term = own
            for k in range(1, count):
                term = jnp.where(lax.rem(index - j + count, count) == k, slots[k - 1], term)
            total = total + term
        return total

    gather(value, column, along_y, 0)
    across[...] = ordered(value[...], column, y, count_y)
    gather(across, row, along_z, count_y - 1)
    out[...] = ordered(across[...], row, z, count_z)


def total(values, collective):
    count_y, count_z = (lax.axis_size("gy"), lax.axis_size("gz"))
    count = values.shape[0]

    def body(*refs):
        total_kernel(count_y, count_z, *refs)

    block = jnp.broadcast_to(jnp.pad(values, (0, 128 - count))[None], (8, 128))
    copies = count_y + count_z - 2
    summed = pl.pallas_call(
        body,
        out_shape=jax.ShapeDtypeStruct((8, 128), jnp.float32),
        in_specs=[VMEM],
        out_specs=VMEM,
        scratch_shapes=[
            pltpu.VMEM((count_y - 1, 8, 128), jnp.float32),
            pltpu.VMEM((count_z - 1, 8, 128), jnp.float32),
            pltpu.VMEM((8, 128), jnp.float32),
            pltpu.SemaphoreType.DMA((copies,)),
            pltpu.SemaphoreType.DMA((copies,)),
        ],
        compiler_params=pltpu.CompilerParams(collective_id=collective, has_side_effects=True),
        name="total",
    )(block)
    return summed[0, :count]


def correlate_kernel(scalars, grown_0, grown_1, grown_2, grown_up, mapped_0, mapped_1, mapped_2, mapped_up, out):
    rows = grown_0.shape[1] - 16
    columns = grown_0.shape[2]
    c_up, c_zero, c_one, c_two, d_zero, d_one, s_zero, s_grad, s_direction = (scalars[k] for k in range(9))
    out[...] = jnp.zeros_like(out)

    @pl.loop(0, rows // 8)
    def _(step):
        first = pl.multiple_of(step * 8, 8)
        here = pl.ds(first + 8, 8)
        zero, one = (mapped_0[1, here], mapped_1[1, here])
        grad = c_up * mapped_up[1, here] + c_zero * zero + c_one * one + c_two * mapped_2[1, here]
        values = (
            s_zero * zero + s_grad * grad,
            s_grad * zero,
            s_direction * (d_zero * zero + d_one * one),
        )
        turned = [[moved(value, c - 1) for value in values] for c in range(3)]
        for a in range(3):
            around = pl.ds(first, 24)
            full_0, full_1 = (grown_0[a, around], grown_1[a, around])
            full_grad = c_up * grown_up[a, around] + c_zero * full_0 + c_one * full_1 + c_two * grown_2[a, around]
            full_direction = d_zero * full_0 + d_one * full_1
            for b in range(3):
                fields = [item[7 + b : 15 + b] for item in (full_0, full_grad, full_direction)]
                for c in range(3):
                    product = turned[c][0] * fields[0] + turned[c][1] * fields[1] + turned[c][2] * fields[2]
                    folded = product[:, :128]
                    for part in range(1, columns // 128):
                        folded = folded + product[:, 128 * part : 128 * part + 128]
                    out[9 * a + 3 * b + c] += folded


def correlate(scalars, *fields):
    return pl.pallas_call(
        correlate_kernel,
        out_shape=jax.ShapeDtypeStruct((27, 8, 128), jnp.float32),
        in_specs=[SMEM] + [VMEM] * 8,
        out_specs=VMEM,
        cost_estimate=pl.CostEstimate(flops=40000000, bytes_accessed=8000000, transcendentals=0),
        name="correlate",
    )(scalars, *fields).sum((1, 2))


def contract(form, left, right):
    return jnp.einsum(form, left, right, precision=lax.Precision.HIGH)


def wave_tables(length, groups):
    half = length // 2
    bins = half // groups
    pair = groups // 2
    shape = (half, pair, 2, bins)
    place = lax.broadcasted_iota(jnp.int32, shape, 0)
    part = lax.broadcasted_iota(jnp.int32, shape, 2)
    slot = lax.broadcasted_iota(jnp.int32, shape, 1) * bins + lax.broadcasted_iota(jnp.int32, shape, 3)
    tables = []
    for odd in range(2):
        frequency = 2 * slot + odd
        steps = place * frequency + part * (length // 4)
        if not odd:
            steps = jnp.where((slot == 0) & (part == 1), place * half, steps)
        angle = (steps % length).astype(jnp.float32) * (2.0 * math.pi / length)
        tables.append(jnp.cos(angle).reshape(half, pair, 2 * bins))
    return tables


def combine(raw, on_row, on_lane):
    even, odd = raw
    a, b, c, d = (
        jnp.concatenate([piece[:, part, :, :, side] for piece in (even, odd)], 0)
        for part, side in ((0, 0), (0, 1), (1, 0), (1, 1))
    )
    special = on_row | on_lane
    plus_real = jnp.where(special, a, a - d)
    plus_imaginary = jnp.where(on_row, b, jnp.where(on_lane, c, b + c))
    minus_real = jnp.where(on_row, c, jnp.where(on_lane, b, a + d))
    minus_imaginary = jnp.where(special, d, b - c)
    return (jnp.stack([plus_real, minus_real]), jnp.stack([plus_imaginary, minus_imaginary]))


def separate(spectrum, on_row, on_lane):
    (plus_real, minus_real), (plus_imaginary, minus_imaginary) = spectrum
    special = on_row | on_lane
    a = jnp.where(special, plus_real, plus_real + minus_real)
    d = jnp.where(special, minus_imaginary, minus_real - plus_real)
    b = jnp.where(on_row, plus_imaginary, jnp.where(on_lane, minus_real, plus_imaginary + minus_imaginary))
    c = jnp.where(on_row, minus_real, jnp.where(on_lane, plus_imaginary, plus_imaginary - minus_imaginary))
    scale = jnp.where(on_row & on_lane, 1.0, 2.0)
    a, b, c, d = (value * scale for value in (a, b, c, d))
    whole = jnp.stack([jnp.stack([a, b], 3), jnp.stack([c, d], 3)], 1)
    pair = whole.shape[0] // 2
    return (whole[:pair], whole[pair:])


def times(left, right, corner, conjugate=False):
    (a, b), (c, d) = (left, right)
    cross = b * d
    sign = -1.0 if conjugate else 1.0
    real = jnp.where(corner, a * c, a * c - sign * cross)
    imaginary = jnp.where(corner, cross, sign * a * d + b * c)
    return (real, imaginary)


def linear(*terms):
    total_real = total_imaginary = 0.0
    for scale, (real, imaginary) in terms:
        scale_real, scale_imaginary = scale if isinstance(scale, tuple) else (scale, scale)
        total_real = total_real + scale_real * real
        total_imaginary = total_imaginary + scale_imaginary * imaginary
    return (total_real, total_imaginary)


def local(measured, point_spread, stencil_weights, upstream):
    planes, row_count, columns = measured.shape
    groups = lax.axis_size("gy")
    rows = row_count * groups
    cells = planes * rows * columns * lax.axis_size("gz")
    bins = columns // 2 // groups
    even_x, odd_x = wave_tables(columns, groups)
    even_y, odd_y = (even_x, odd_x) if rows == columns else wave_tables(rows, groups)
    y_bins = rows // 2 // groups
    spectral = (groups, y_bins, 1, bins)
    on_row = (lax.broadcasted_iota(jnp.int32, spectral, 0) == 0) & (
        lax.broadcasted_iota(jnp.int32, spectral, 1) == 0
    )
    on_lane = (lax.broadcasted_iota(jnp.int32, spectral, 3) == 0) & (lax.axis_index("gy") == 0)
    corner = on_row & on_lane

    def forward(volumes):
        count = volumes.shape[0]
        low, high = (volumes[:, :, : columns // 2], volumes[:, :, columns // 2 :])
        sent = jnp.concatenate(
            [contract("vrj,jdl->drvl", low + high, even_x), contract("vrj,jdl->drvl", low - high, odd_x)], 0
        )
        arrived = lax.all_to_all(
            sent.reshape(groups, row_count, count * 2 * bins), "gy", split_axis=0, concat_axis=0, tiled=True
        )
        arrived = arrived.reshape(rows, count * 2 * bins)
        low, high = (arrived[: rows // 2], arrived[rows // 2 :])
        raw = [
            contract("jds,jl->dsl", table, value).reshape(groups // 2, 2, y_bins, count, 2, bins)
            for table, value in ((even_y, low + high), (odd_y, low - high))
        ]
        return combine(raw, on_row, on_lane)

    def inverse(spectrum):
        count = spectrum[0].shape[3]
        pieces = separate(spectrum, on_row, on_lane)
        one, two = (
            contract("jds,dsl->jl", table, piece.reshape(groups // 2, 2 * y_bins, count * 2 * bins))
            for table, piece in ((even_y, pieces[0]), (odd_y, pieces[1]))
        )
        sent = jnp.concatenate([one + two, one - two], 0).reshape(groups, row_count, count * 2 * bins)
        arrived = lax.all_to_all(sent, "gy", split_axis=0, concat_axis=0, tiled=True)
        arrived = arrived.reshape(groups, row_count, count, 2 * bins)
        one = contract("drvl,jdl->vrj", arrived[: groups // 2], even_x)
        two = contract("drvl,jdl->vrj", arrived[groups // 2 :], odd_x)
        return jnp.concatenate([one + two, one - two], 2) / float(rows * columns)

    def pick(spectrum, start, count):
        return tuple(lax.slice_in_dim(part, start, start + count, axis=3) for part in spectrum)

    def join(*spectra):
        return tuple(jnp.concatenate(parts, 3) for parts in zip(*spectra))

    spectra = forward(jnp.concatenate([point_spread[None], measured], 0))
    transfer = pick(spectra, 0, 1)
    squares = (transfer[0] ** 2, transfer[1] ** 2)
    gain = (
        jnp.where(corner, squares[0], squares[0] + squares[1]),
        jnp.where(corner, squares[1], squares[0] + squares[1]),
    )
    spectrum_0 = times(pick(spectra, 1, planes), transfer, corner, True)
    blurred_0 = linear((gain, spectrum_0))
    pair = inverse(join(spectrum_0, blurred_0))
    vector_0 = pair[:planes]
    back_0, grown_0, mapped_0 = regular(vector_0, stencil_weights)
    back_up, grown_up, mapped_up = regular(upstream, stencil_weights)
    vector_1 = pair[planes:] + back_0
    spectrum_1 = linear((1.0, blurred_0), (1.0, forward(back_0)))
    blurred_1 = linear((gain, spectrum_1))
    early = forward(jnp.concatenate([upstream, back_up], 0))
    back_1, grown_1, mapped_1 = regular(vector_1, stencil_weights)
    vector_2 = inverse(blurred_1) + back_1
    norm_0, curve_0, image_0, up_0, up_1 = total(
        jnp.stack(
            [
                jnp.sum(vector_0 * vector_0),
                jnp.sum(vector_0 * vector_1),
                jnp.sum(vector_1 * vector_1),
                jnp.sum(upstream * vector_0),
                jnp.sum(upstream * vector_1),
            ]
        ),
        1,
    )
    step_0 = norm_0 / curve_0
    residual = vector_0 - step_0 * vector_1
    residual_image = vector_1 - step_0 * vector_2
    norm_1, cross, inner, up_residual, image_cross = total(
        jnp.stack(
            [
                jnp.sum(residual * residual),
                jnp.sum(residual * vector_1),
                jnp.sum(residual * residual_image),
                jnp.sum(upstream * residual),
                jnp.sum(residual_image * vector_1),
            ]
        ),
        2,
    )
    back_2, grown_2, mapped_2 = regular(vector_2, stencil_weights)
    late = forward(jnp.concatenate([back_1, back_2], 0))
    ratio = norm_1 / norm_0
    curve_1 = inner + 2.0 * ratio * cross + ratio * ratio * curve_0
    step_1 = norm_1 / curve_1
    grad_step_1 = up_residual + ratio * up_0
    grad_curve_1 = -grad_step_1 * step_1 / curve_1
    grad_ratio = step_1 * up_0 + 2.0 * grad_curve_1 * (cross + ratio * curve_0)
    known_image = step_1 * up_1 + 2.0 * grad_curve_1 * (image_cross + ratio * image_0)
    grad_norm = grad_step_1 / curve_1 + grad_ratio / norm_0
    grad_step_0 = up_0 - known_image - 2.0 * grad_norm * cross
    grad_curve_0 = -grad_step_0 * step_0 / curve_0
    grad_norm_0 = -grad_ratio * ratio / norm_0 + grad_step_0 / curve_0

    spectrum_2 = linear((1.0, linear((gain, spectrum_1))), (1.0, pick(late, 0, planes)))
    spectrum_up = pick(early, 0, planes)
    residual_terms = ((1.0, spectrum_0), (-step_0, spectrum_1))
    direction_image = linear((1.0 + ratio, spectrum_1), (-step_0, spectrum_2))
    grad_direction = linear((step_1, spectrum_up), (2.0 * grad_curve_1, direction_image))
    grad_residual = linear((1.0, grad_direction), (2.0 * grad_norm, linear(*residual_terms)))
    grad_back = linear(
        (step_1, pick(early, planes, planes)),
        (2.0 * grad_curve_1 * (1.0 + ratio) - 2.0 * grad_norm * step_0, pick(late, 0, planes)),
        (-2.0 * grad_curve_1 * step_0, pick(late, planes, planes)),
        (2.0 * grad_norm, linear((1.0, spectrum_1), (-1.0, blurred_0))),
    )
    grad_right = linear(
        (step_0, spectrum_up),
        (ratio, grad_direction),
        (2.0 * grad_curve_0, spectrum_1),
        (2.0 * grad_norm_0, spectrum_0),
        (1.0, grad_residual),
        (-step_0, linear((gain, grad_residual), (1.0, grad_back))),
    )
    grad_measured = inverse(times(grad_right, transfer, corner))

    terms = correlate(
        jnp.stack(
            [
                step_1,
                2.0 * grad_norm,
                2.0 * grad_curve_1 * (1.0 + ratio) - 2.0 * grad_norm * step_0,
                -2.0 * grad_curve_1 * step_0,
                1.0 + ratio,
                -step_0,
                2.0 * grad_curve_0,
                -step_0,
                2.0 * grad_curve_1,
            ]
        ),
        grown_0, grown_1, grown_2, grown_up, mapped_0, mapped_1, mapped_2, mapped_up,
    )
    grad_stencil = total(terms, 3).reshape(3, 3, 3) / math.sqrt(cells)
    return (grad_measured, grad_stencil)


def spectral_fits(mesh_y, mesh_z, planes, row_count, columns):
    devices, rows, depth = (mesh_y * mesh_z, row_count * mesh_y, planes * mesh_z)
    if columns % (16 * devices) or row_count % 128 or rows % 512 or planes != 1 or mesh_z % 2:
        return False
    tiles = 4 * depth // 8 * (rows // 128)
    return depth < 8 and depth % 2 == 0 and devices % tiles == 0


def wave_rows(length):
    half, quarter = (length // 2, length // 4)
    place = np.arange(half)[None, :]
    tables = []
    for odd in range(2):
        frequency = 2 * np.arange(quarter)[:, None] + odd
        angle = (place * frequency % length) * (2.0 * np.pi / length)
        cosine, sine = (np.cos(angle), np.sin(angle))
        if not odd:
            sine[0] = np.cos(np.pi * place[0])
        tables += [cosine, sine]
    table = np.stack(tables)
    high = table.astype(jnp.bfloat16)
    low = (table - high.astype(np.float64)).astype(jnp.bfloat16)
    return (high, low)


def basis(length, place):
    half = length // 2
    frequency = np.concatenate([np.arange(0, half, 2), np.arange(1, half, 2)])
    angle = frequency * place % length * (2.0 * np.pi / length)
    cosine, sine = (np.cos(angle), np.sin(angle))
    sine[0] = np.cos(np.pi * place)
    return (cosine, sine)


def axis_values(length):
    cosine, sine = basis(length, 1)
    pure = sine.copy()
    pure[0] = 0.0
    other = cosine.copy()
    other[0] = -1.0
    weight = np.full(length // 2, 2.0)
    weight[0] = 1.0
    values = [(cosine, other), (pure, pure), basis(length, 0), basis(length, length - 1), (weight, weight)]
    for place in (0, 1, length - 2, length - 1):
        values.append(tuple(weight * part / length for part in basis(length, place)))
    return np.stack([np.stack(pair) for pair in values]).astype(np.float32)


COS, SIN, FIRST, LAST, WEIGHT, AT = range(6)


def split(value):
    high = value.astype(jnp.bfloat16)
    return (high, (value - high.astype(jnp.float32)).astype(jnp.bfloat16))


def product(left, right, contracting):
    numbers = (contracting, ((), ()))

    def one(a, b):
        return lax.dot_general(a, b, numbers, preferred_element_type=jnp.float32)

    return one(left[0], right[0]) + (one(left[0], right[1]) + one(left[1], right[0]))


class Spectral:
    def __init__(self, count_y, count_z, planes, row_count, columns):
        self.ny, self.nz = (count_y, count_z)
        self.nd = count_y * count_z
        self.depth = planes * count_z
        self.row_count = row_count
        self.rows = row_count * count_y
        self.columns = columns
        self.bins = columns // 2 // self.nd
        self.half = self.rows // 2
        self.steps = self.half // 128
        self.tiers = self.bins // 8
        self.lanes = self.rows // 128
        self.tiles = 4 * self.depth // 8 * self.lanes
        self.stride = self.nd // self.tiles

    def place_of(self, index):
        return (lax.rem(index, self.ny), lax.div(index, self.ny))

    def scratch(self):
        Z, bins, half, nd = (self.depth, self.bins, self.half, self.nd)
        packed = (Z, 2, bins, self.rows)
        field = (Z, 4, bins, half)
        edge = (2, Z, 2, bins, 128)
        F = jnp.float32
        D = pltpu.SemaphoreType.DMA
        names = dict(
            sent_m=pltpu.VMEM((nd, 2, bins, 128 * (self.row_count // 128)), F),
            sent_u=pltpu.VMEM((nd, 2, bins, self.row_count), F),
            sent_p=pltpu.VMEM((self.ny, 2, bins, self.row_count), F),
            got_m=pltpu.VMEM(packed, F),
            got_u=pltpu.VMEM(packed, F),
            got_p=pltpu.VMEM((2, bins, self.rows), F),
            wave=pltpu.VMEM(packed, F),
            wave_p=pltpu.VMEM((2, bins, self.rows), F),
            v0=pltpu.VMEM(field, F),
            v1=pltpu.VMEM(field, F),
            v2=pltpu.VMEM(field, F),
            up=pltpu.VMEM(field, F),
            w3=pltpu.VMEM(field, F),
            m0=pltpu.VMEM(field, F),
            m1=pltpu.VMEM(field, F),
            mw=pltpu.VMEM(field, F),
            stencil=pltpu.VMEM((3, 2, 3, bins, half), F),
            blur=pltpu.VMEM((2, 3, bins, half), F),
            gain=pltpu.VMEM((2, 2, bins, half), F),
            across=pltpu.VMEM((9, 2, bins, 128), F),
            rows_v0=pltpu.VMEM(edge, F),
            rows_v1=pltpu.VMEM(edge, F),
            rows_v2=pltpu.VMEM(edge, F),
            rows_up=pltpu.VMEM(edge, F),
            rows_w3=pltpu.VMEM(edge, F),
            rows_m0=pltpu.VMEM(edge, F),
            rows_m1=pltpu.VMEM(edge, F),
            rows_mw=pltpu.VMEM(edge, F),
            edge_rows=pltpu.VMEM(edge, F),
            cols_v0=pltpu.VMEM((4, 8, self.rows), F),
            cols_v1=pltpu.VMEM((4, 8, self.rows), F),
            cols_v2=pltpu.VMEM((4, 8, self.rows), F),
            cols_up=pltpu.VMEM((4, 8, self.rows), F),
            cols_w3=pltpu.VMEM((4, 8, self.rows), F),
            cols_m0=pltpu.VMEM((2, 8, self.rows), F),
            cols_m1=pltpu.VMEM((2, 8, self.rows), F),
            cols_mw=pltpu.VMEM((2, 8, self.rows), F),
            edge_cols=pltpu.VMEM((2, 8, self.rows), F),
            part=pltpu.VMEM((3, 3, self.tiles, 8, 128), F),
            slots=pltpu.VMEM((3, 3, nd, 8, 128), F),
            sums=pltpu.VMEM((3, 3, 8, 128), F),
            full=pltpu.VMEM((3, 3, self.tiles, 8, 128), F),
            acc=pltpu.VMEM((8, 8, 128), F),
            total=pltpu.VMEM((2, 8, 8, 128), F),
            taps=pltpu.VMEM((27, 8, 128), F),
            tap_part=pltpu.VMEM((8, 128), F),
            tap_slots=pltpu.VMEM((nd, 8, 128), F),
            sent_o=pltpu.VMEM(packed, F),
            got_o=pltpu.VMEM((nd, 2, bins, self.row_count), F),
            send_big=D((2, nd)),
            recv_big=D((2, nd)),
            send_p=D((self.ny,)),
            recv_p=D((self.ny,)),
            send_part=D((2, 3, self.tiles)),
            recv_part=D((2, 3, nd)),
            send_full=D((2, 3, nd)),
            recv_full=D((2, 3, self.tiles)),
            send_tap=D((nd,)),
            recv_tap=D((nd,)),
        )
        return names


    def remote(self, source, target, send, receive, peer):
        return pltpu.make_async_remote_copy(
            src_ref=source, dst_ref=target, send_sem=send, recv_sem=receive,
            device_id=self.place_of(peer), device_id_type=MESH,
        )

    def spread_copy(self, r, sent, got, lot, peer, source):
        y, z = self.place_of(source)
        lanes = pl.ds(pl.multiple_of(y * self.row_count, 128), self.row_count)
        return self.remote(
            sent.at[peer], got.at[z, :, :, lanes], r.send_big.at[lot, peer], r.recv_big.at[lot, source], peer
        )

    def spread_start(self, r, sent, got, lot):
        @pl.loop(1, self.nd)
        def _(k):
            peer = lax.rem(self.me + k, self.nd)
            self.spread_copy(r, sent, got, lot, peer, self.me).start()

        y, z = self.place_of(self.me)
        lanes = pl.ds(pl.multiple_of(y * self.row_count, 128), self.row_count)
        got[z, :, :, lanes] = sent[self.me]

    def spread_wait(self, r, sent, got, lot):
        @pl.loop(1, self.nd)
        def _(k):
            peer = lax.rem(self.me + k, self.nd)
            copy = self.spread_copy(r, sent, got, lot, peer, peer)
            copy.wait_recv()

        @pl.loop(1, self.nd)
        def _(k):
            peer = lax.rem(self.me + k, self.nd)
            self.spread_copy(r, sent, got, lot, peer, self.me).wait_send()

    def point_copy(self, r, peer_y, source_y):
        lanes = pl.ds(pl.multiple_of(source_y * self.row_count, 128), self.row_count)
        return self.remote(
            r.sent_p.at[peer_y], r.got_p.at[:, :, lanes], r.send_p.at[peer_y], r.recv_p.at[source_y],
            self.z * self.ny + peer_y,
        )

    def point_start(self, r):
        @pl.loop(1, self.ny)
        def _(k):
            self.point_copy(r, lax.rem(self.y + k, self.ny), self.y).start()

        lanes = pl.ds(pl.multiple_of(self.y * self.row_count, 128), self.row_count)
        r.got_p[:, :, lanes] = r.sent_p[self.y]

    def point_wait(self, r):
        @pl.loop(1, self.ny)
        def _(k):
            peer = lax.rem(self.y + k, self.ny)
            self.point_copy(r, peer, peer).wait_recv()

        @pl.loop(1, self.ny)
        def _(k):
            peer = lax.rem(self.y + k, self.ny)
            self.point_copy(r, peer, self.y).wait_send()

    def return_copy(self, r, peer, source):
        y, z = self.place_of(peer)
        lanes = pl.ds(pl.multiple_of(y * self.row_count, 128), self.row_count)
        return self.remote(
            r.sent_o.at[z, :, :, lanes], r.got_o.at[source], r.send_big.at[0, peer], r.recv_big.at[0, source], peer
        )

    def owner(self, kind, tile):
        if kind == 0:
            return tile * self.stride
        if kind == 1:
            return tile * self.stride + self.stride - 1
        return self.nd - 1

    def owned(self, kind):
        if kind == 0:
            return lax.rem(self.me, self.stride) == 0
        if kind == 1:
            return lax.rem(self.me, self.stride) == self.stride - 1
        return self.me == self.nd - 1

    def counts(self, kind):
        return 1 if kind == 2 else self.tiles

    def mine(self, kind):
        return 0 if kind == 2 else lax.div(self.me, self.stride)

    def reduce_start(self, r, turn, kinds):
        lot = turn % 2
        for kind in kinds:

            @pl.loop(0, self.counts(kind))
            def _(tile):
                owner = self.owner(kind, tile)

                @pl.when(owner != self.me)
                def _():
                    self.remote(
                        r.part.at[turn, kind, tile], r.slots.at[turn, kind, self.me],
                        r.send_part.at[lot, kind, tile], r.recv_part.at[lot, kind, self.me], owner,
                    ).start()

    def reduce_finish(self, r, turn, kinds):
        lot = turn % 2
        for kind in kinds:

            @pl.when(self.owned(kind))
            def _():
                tile = self.mine(kind)
                r.slots[turn, kind, self.me] = r.part[turn, kind, tile]

                @pl.loop(1, self.nd)
                def _(k):
                    peer = lax.rem(self.me + k, self.nd)
                    self.remote(
                        r.part.at[turn, kind, tile], r.slots.at[turn, kind, peer],
                        r.send_part.at[lot, kind, tile], r.recv_part.at[lot, kind, peer], peer,
                    ).wait_recv()

                lots = [r.slots[turn, kind, k] for k in range(self.nd)]
                while len(lots) > 1:
                    lots = [lots[k] + lots[k + 1] for k in range(0, len(lots) - 1, 2)] + lots[len(lots) // 2 * 2 :]
                r.sums[turn, kind] = lots[0]

                @pl.loop(1, self.nd)
                def _(k):
                    peer = lax.rem(self.me + k, self.nd)
                    self.remote(
                        r.sums.at[turn, kind], r.full.at[turn, kind, tile],
                        r.send_full.at[lot, kind, peer], r.recv_full.at[lot, kind, tile], peer,
                    ).start()

                r.full[turn, kind, tile] = r.sums[turn, kind]

        for kind in kinds:

            @pl.loop(0, self.counts(kind))
            def _(tile):
                owner = self.owner(kind, tile)

                @pl.when(owner != self.me)
                def _():
                    self.remote(
                        r.sums.at[turn, kind], r.full.at[turn, kind, tile],
                        r.send_full.at[lot, kind, owner], r.recv_full.at[lot, kind, tile], owner,
                    ).wait_recv()
                    self.remote(
                        r.part.at[turn, kind, tile], r.slots.at[turn, kind, self.me],
                        r.send_part.at[lot, kind, tile], r.recv_part.at[lot, kind, self.me], owner,
                    ).wait_send()

            @pl.when(self.owned(kind))
            def _():
                tile = self.mine(kind)

                @pl.loop(1, self.nd)
                def _(k):
                    peer = lax.rem(self.me + k, self.nd)
                    self.remote(
                        r.sums.at[turn, kind], r.full.at[turn, kind, tile],
                        r.send_full.at[lot, kind, peer], r.recv_full.at[lot, kind, tile], peer,
                    ).wait_send()


    def row_spectra(self, r, source, sent):
        half = self.columns // 2
        low, high = (source[:, :half], source[:, half:])
        per = self.nd // 2
        for odd, value in enumerate((low + high, low - high)):
            value = split(value)
            for part in range(2):
                table = (r.tab_x[0][2 * odd + part], r.tab_x[1][2 * odd + part])
                sent[pl.ds(odd * per, per), part] = product(table, value, ((1,), (1,))).reshape(
                    per, self.bins, self.row_count
                )

    def point_spectra(self, r, source):
        half = self.columns // 2
        low, high = (source[:, :half], source[:, half:])
        odd = lax.div(2 * self.z, self.nz)
        sign = 1.0 - 2.0 * odd.astype(jnp.float32)
        value = split(low + sign * high)
        block = self.ny * self.bins
        start = pl.multiple_of(lax.rem(self.z, self.nz // 2) * block, block)
        for part in range(2):
            table = tuple(half_table[2 * odd + part, pl.ds(start, block)] for half_table in r.tab_x)
            r.sent_p[:, part] = product(table, value, ((1,), (1,))).reshape(self.ny, self.bins, self.row_count)

    def column_spectra(self, r, got, wave):
        count = math.prod(got.shape[:-1])
        value = got[...].reshape(count, self.rows)
        low, high = (value[:, : self.half], value[:, self.half :])
        quarter = self.half // 2
        for odd, value in enumerate((low + high, low - high)):
            value = split(value)
            for part in range(2):
                table = (r.tab_y[0][2 * odd + part], r.tab_y[1][2 * odd + part])
                wave[..., pl.ds(part * self.half + odd * quarter, quarter)] = product(
                    value, table, ((1,), (1,))
                ).reshape(got.shape[:-1] + (quarter,))

    def column_values(self, r, wave, target):
        count = math.prod(wave.shape[:-1])
        value = wave[...].reshape(count, self.rows)
        quarter = self.half // 2
        even, odd = (
            sum(
                product(
                    split(value[:, part * self.half + k * quarter : part * self.half + (k + 1) * quarter]),
                    (r.tab_y[0][2 * k + part], r.tab_y[1][2 * k + part]),
                    ((1,), (0,)),
                )
                for part in range(2)
            )
            for k in range(2)
        )
        shape = wave.shape[:-1] + (self.half,)
        target[..., : self.half] = (even + odd).reshape(shape)
        target[..., self.half :] = (even - odd).reshape(shape)

    def row_values(self, r, got, out):
        per = self.nd // 2
        sides = []
        for k in range(2):
            side = 0.0
            for part in range(2):
                value = got[pl.ds(k * per, per), part].reshape(per * self.bins, self.row_count)
                side = side + product(
                    split(value.T), (r.tab_x[0][2 * k + part], r.tab_x[1][2 * k + part]), ((1,), (0,))
                )
            sides.append(side)
        half = self.columns // 2
        out[0, :, :half] = sides[0] + sides[1]
        out[0, :, half:] = sides[0] - sides[1]


    def masks(self, tier, step):
        shape = (8, 128)
        row = (lax.broadcasted_iota(jnp.int32, shape, 0) == 0) & (self.me == 0)
        lane = lax.broadcasted_iota(jnp.int32, shape, 1) + 128 * step == 0
        if tier:
            row = row & False
        return (row, lane, row & lane, row | lane)

    def combine(self, masks, ac, as_, bc, bs):
        row, lane, corner, special = masks
        pr = jnp.where(special, ac, ac - bs)
        pi = jnp.where(corner, as_, jnp.where(row, -as_, jnp.where(lane, -bc, -(as_ + bc))))
        mr = jnp.where(row, bc, jnp.where(lane, as_, ac + bs))
        mi = jnp.where(corner, bs, jnp.where(special, -bs, as_ - bc))
        return [pr, pi, mr, mi]

    def separate(self, masks, field):
        row, lane, corner, special = masks
        pr, pi, mr, mi = field
        ac = jnp.where(special, pr, 0.5 * (pr + mr))
        as_ = jnp.where(corner, pi, jnp.where(row, -pi, jnp.where(lane, mr, 0.5 * (mi - pi))))
        bc = jnp.where(row, mr, jnp.where(lane, -pi, -0.5 * (pi + mi)))
        bs = jnp.where(corner, mi, jnp.where(special, -mi, 0.5 * (mr - pr)))
        return (ac, as_, bc, bs)

    def lane_slice(self, step, part=0):
        return pl.ds(pl.multiple_of(part * self.half + step * 128, 128), 128)

    def along(self, r, which, step, part):
        return r.along[which, :, self.lane_slice(step, part)]

    def beside(self, r, which, part, tier):
        return r.across[which, part, pl.ds(8 * tier, 8)]

    def load(self, field, z, tier, step):
        return [field[z, k, pl.ds(8 * tier, 8), self.lane_slice(step)] for k in range(4)]

    def keep(self, field, z, tier, step, values):
        for k in range(4):
            field[z, k, pl.ds(8 * tier, 8), self.lane_slice(step)] = values[k]

    def load_wave(self, wave, z, tier, step):
        return [
            wave[z, part, pl.ds(8 * tier, 8), self.lane_slice(step, side)]
            for part in range(2)
            for side in range(2)
        ]

    def times(self, factor, value, conjugate=False):
        out = []
        for side in range(2):
            real, other, cross = factor[side]
            a, b = (value[2 * side], value[2 * side + 1])
            if conjugate:
                out += [real * a + cross * b, other * b - cross * a]
            else:
                out += [real * a - cross * b, other * b + cross * a]
        return out

    def factor(self, array, tier, step):
        where = (pl.ds(8 * tier, 8), self.lane_slice(step))
        return [[array[(side, k) + where] for k in range(3)] for side in range(2)]

    def sweep(self, body):
        @pl.loop(0, self.steps)
        def _(step):
            columns = {}
            for tier in range(self.tiers):
                body(tier, step, self.masks(tier, step), columns)

    def frames(self, r, masks, tier, step, z, value, rows, columns=None):
        ac, as_, bc, bs = self.separate(masks, value)
        here = pl.ds(8 * tier, 8)
        for k, which in enumerate((AT, AT + 3)):
            c, s = (self.along(r, which, step, 0), self.along(r, which, step, 1))
            rows[k, z, 0, here] += ac * c + as_ * s
            rows[k, z, 1, here] += bc * c + bs * s
        if columns is None:
            return
        for x in range(4):
            a, b = (self.beside(r, AT + x, 0, tier), self.beside(r, AT + x, 1, tier))
            for side, (p, q) in enumerate(((ac, bc), (as_, bs))):
                term = a * p + b * q
                key = (x, z, side)
                columns[key] = term if key not in columns else columns[key] + term

    def put_columns(self, part, tier, step, columns):
        if tier < self.tiers - 1:
            return
        for (x, z, side), value in columns.items():
            index = x * self.depth + z
            tile = index // 8 * self.lanes + side * self.steps + step
            part[tile, pl.ds(index % 8, 1)] = jnp.sum(value, 0, keepdims=True)

    def clear(self, *refs):
        for ref in refs:
            ref[...] = jnp.zeros(ref.shape, jnp.float32)

    def settle(self, rows):
        for k in range(2):
            rows[k] = jnp.broadcast_to(jnp.sum(rows[k], -1, keepdims=True), rows.shape[1:])

    def unpack(self, full, cols):
        Z = self.depth
        cols[...] = jnp.zeros(cols.shape, jnp.float32)
        for x in range(4):
            first = x * Z
            for lane in range(self.lanes):
                cols[x, pl.ds(0, Z), pl.ds(lane * 128, 128)] = full[
                    first // 8 * self.lanes + lane, pl.ds(first % 8, Z)
                ]

    def shifted(self, value, by):
        if by == 0:
            return value
        value = pltpu.roll(value, 7 if by > 0 else 1, 0)
        sub = lax.broadcasted_iota(jnp.int32, value.shape, 0)
        return jnp.where(sub < self.depth, value, 0.0)

    def corners(self, r, col):
        out = []
        for which in (AT, AT + 3):
            weight = jnp.concatenate([r.along[which, :, :]], 0)
            out.append(jnp.broadcast_to(jnp.sum(col * weight, -1, keepdims=True), (8, 128)))
        return out

    def edges(self, r, w, rows, col_first, col_last, inner=None, mapped=None):
        Z = self.depth
        k_first, k_last = (self.corners(r, col_first[...]), self.corners(r, col_last[...]))
        total = lambda terms: sum(terms[1:], terms[0])
        q = {}
        for name, b, c, value in ((0, 0, 0, k_last[1]), (1, 0, 2, k_first[1]), (2, 2, 0, k_last[0]), (3, 2, 2, k_first[0])):
            q[name] = total([w(a, b, c) * self.shifted(value, a - 1) for a in range(3)])
        if inner is not None:
            near, far = inner
            k_near, k_far = (self.corners(r, near[...]), self.corners(r, far[...]))
            fix = []
            for (c0, v0), (c1, v1) in (((1, k_first), (2, k_near)), ((0, k_far), (1, k_last))):
                fix.append(
                    [
                        total(
                            [
                                w(a, b, c0) * self.shifted(v0[y], a - 1) + w(a, b, c1) * self.shifted(v1[y], a - 1)
                                for a in range(3)
                            ]
                        )
                        for b, y in ((0, 1), (2, 0))
                    ]
                )

        @pl.loop(0, self.steps)
        def _(step):
            c = [self.along(r, COS, step, part) for part in range(2)]
            s = self.along(r, SIN, step, 0)
            first = [self.along(r, FIRST, step, part) for part in range(2)]
            last = [self.along(r, LAST, step, part) for part in range(2)]

            def get(col):
                return [col[:, self.lane_slice(step, part)] for part in range(2)]

            def line(a, c_index, col):
                w0, w1, w2 = (w(a, b, c_index) for b in range(3))
                turn = (w2 - w0) * s
                return [
                    (w1 + (w0 + w2) * c[0]) * col[0] + turn * col[1],
                    (w1 + (w0 + w2) * c[1]) * col[1] - turn * col[0],
                ]

            def stacked(pieces):
                out = None
                for a in range(3):
                    for c_index, col in pieces:
                        term = [self.shifted(part, a - 1) for part in line(a, c_index, col)]
                        out = term if out is None else [p + t for p, t in zip(out, term)]
                return out

            f, l = (get(col_first), get(col_last))
            for k, (pieces, upper, lower) in enumerate((([(0, l)], q[0], q[2]), ([(2, f)], q[1], q[3]))):
                value = stacked(pieces)
                for part in range(2):
                    r.edge_cols[k, :, self.lane_slice(step, part)] = (
                        value[part] - upper * first[part] - lower * last[part]
                    )
            if inner is not None:
                n, g = (get(near), get(far))
                for k, pieces in enumerate(([(1, f), (2, n)], [(0, g), (1, l)])):
                    value = stacked(pieces)
                    for part in range(2):
                        mapped[k, :, self.lane_slice(step, part)] = (
                            value[part] - fix[k][0] * first[part] - fix[k][1] * last[part]
                        )

        for tier in range(self.tiers):
            here = pl.ds(8 * tier, 8)
            c = [self.beside(r, COS, part, tier) for part in range(2)]
            s = self.beside(r, SIN, 0, tier)
            for k, (b, source) in enumerate(((0, 1), (2, 0))):
                for z in range(Z):
                    out = None
                    for a in range(3):
                        if not 0 <= z + a - 1 < Z:
                            continue
                        w0, w1, w2 = (w(a, b, c_index) for c_index in range(3))
                        turn = (w2 - w0) * s
                        p, t = (rows[source, z + a - 1, part, here] for part in range(2))
                        term = [
                            (w1 + (w0 + w2) * c[0]) * p + turn * t,
                            (w1 + (w0 + w2) * c[1]) * t - turn * p,
                        ]
                        out = term if out is None else [x + v for x, v in zip(out, term)]
                    for part in range(2):
                        r.edge_rows[k, z, part, here] = out[part]

    def edge_field(self, r, masks, tier, step, z):
        here = pl.ds(8 * tier, 8)
        out = []
        for part in range(2):
            e0, e1 = (r.edge_rows[k, z, part, here] for k in range(2))
            x0, x1 = (self.beside(r, which, part, tier) for which in (FIRST, LAST))
            for side in range(2):
                y0, y1 = (self.along(r, which, step, side) for which in (FIRST, LAST))
                c0, c1 = (r.edge_cols[k, pl.ds(z, 1), self.lane_slice(step, side)] for k in range(2))
                out.append(e0 * y0 + e1 * y1 + x0 * c0 + x1 * c1)
        return self.combine(masks, *out)

    def stencil_field(self, r, masks, tier, step, field, flip):
        Z = self.depth
        value = [self.load(field, z, tier, step) for z in range(Z)]
        out = [[-e for e in self.edge_field(r, masks, tier, step, z)] for z in range(Z)]
        for a in range(3):
            where = (pl.ds(8 * tier, 8), self.lane_slice(step))
            factor = [[r.stencil[(a, side, k) + where] for k in range(3)] for side in range(2)]
            for z in range(Z):
                other = z + (1 - a if flip else a - 1)
                if 0 <= other < Z:
                    term = self.times(factor, value[other], flip)
                    out[z] = [o + t for o, t in zip(out[z], term)]
        return out

    def build_stencil(self, r, w):
        def body(tier, step, masks, columns):
            row, lane, corner, special = masks
            here = pl.ds(8 * tier, 8)
            sx = self.beside(r, SIN, 0, tier)
            ys = self.along(r, SIN, step, 0)
            for side in range(2):
                cx = self.beside(r, COS, side, tier)
                cy = self.along(r, COS, step, 0)
                sy = jnp.broadcast_to(ys, (8, 128))
                cy = jnp.broadcast_to(cy, (8, 128))
                if side:
                    cy = jnp.where(row, cy, self.along(r, COS, step, 1))
                    sy = jnp.where(row, sy, -sy)
                for a in range(3):
                    real, imag = ([], [])
                    for b in range(3):
                        real.append(w(a, b, 1) + (w(a, b, 0) + w(a, b, 2)) * cx)
                        imag.append((w(a, b, 2) - w(a, b, 0)) * sx)
                    value = real[1] + (real[0] + real[2]) * cy - (imag[2] - imag[0]) * sy
                    cross = imag[1] + (imag[0] + imag[2]) * cy + (real[2] - real[0]) * sy
                    other = jnp.where(corner, real[1] - (real[0] + real[2]), value)
                    for k, item in enumerate((value, other, cross)):
                        r.stencil[a, side, k, here, self.lane_slice(step)] = item

        self.sweep(body)

    def build_blur(self, r):
        def body(tier, step, masks, columns):
            row, lane, corner, special = masks
            here = pl.ds(8 * tier, 8)
            wave = [
                r.wave_p[part, here, self.lane_slice(step, side)] for part in range(2) for side in range(2)
            ]
            value = self.combine(masks, wave[0], wave[1], wave[2], wave[3])
            for side in range(2):
                real, imag = (value[2 * side], value[2 * side + 1])
                other = jnp.where(corner, imag, real)
                cross = jnp.where(corner, 0.0, imag)
                for k, item in enumerate((real, other, cross)):
                    r.blur[side, k, here, self.lane_slice(step)] = item
                square = cross * cross
                r.gain[side, 0, here, self.lane_slice(step)] = real * real + square
                r.gain[side, 1, here, self.lane_slice(step)] = other * other + square

        self.sweep(body)

    def gained(self, r, tier, step, value):
        where = (pl.ds(8 * tier, 8), self.lane_slice(step))
        return [r.gain[(k // 2, k % 2) + where] * value[k] for k in range(4)]

    def dot(self, masks, left, right):
        corner = masks[2]
        total = sum(a * b for a, b in zip(left, right))
        return jnp.where(corner, 0.5 * total, total)


    def stencil_twice(self, r, w, field, rows, cols, mapped, rows_m, cols_m, finish, after=None):
        def flipped(a, b, c):
            return w(2 - a, 2 - b, 2 - c)

        self.edges(r, w, rows, cols.at[0], cols.at[3], (cols.at[1], cols.at[2]), cols_m)
        self.clear(rows_m)

        def forward(tier, step, masks, columns):
            out = self.stencil_field(r, masks, tier, step, field, False)
            for z in range(self.depth):
                self.keep(mapped, z, tier, step, out[z])
                self.frames(r, masks, tier, step, z, out[z], rows_m)

        self.sweep(forward)
        self.settle(rows_m)
        self.edges(r, flipped, rows_m, cols_m.at[0], cols_m.at[1])

        def back(tier, step, masks, columns):
            finish(tier, step, masks, columns, self.stencil_field(r, masks, tier, step, mapped, True))

        self.sweep(back)

    def scalars_out(self, r, turn, count):
        for k in range(count):
            r.part[turn, 2, 0, pl.ds(k, 1)] = jnp.sum(r.acc[k], 0, keepdims=True)
        for k in range(count, 8):
            r.part[turn, 2, 0, pl.ds(k, 1)] = jnp.zeros((1, 128), jnp.float32)

    def scalars_in(self, r, turn, count):
        value = jnp.sum(r.full[turn, 2, 0], -1, keepdims=True)
        return [jnp.broadcast_to(value[k : k + 1], (8, 128)) for k in range(count)]

    def run(self, r):
        Z = self.depth
        self.y, self.z = (lax.axis_index("gy"), lax.axis_index("gz"))
        self.me = self.z * self.ny + self.y

        def w(a, b, c):
            return r.weights[9 * a + 3 * b + c]

        barrier = pltpu.get_barrier_semaphore()

        @pl.loop(1, self.nd)
        def _(k):
            pl.semaphore_signal(
                barrier, inc=1, device_id=self.place_of(lax.rem(self.me + k, self.nd)), device_id_type=MESH
            )

        own = r.frequencies[self.me]
        for which in range(9):
            for part in range(2):
                r.across[which, part] = jnp.broadcast_to(
                    own[part * self.bins : (part + 1) * self.bins, which : which + 1], (self.bins, 128)
                )
        self.point_spectra(r, r.point_spread[...])
        self.row_spectra(r, r.measured[0], r.sent_m)
        pl.semaphore_wait(barrier, self.nd - 1)
        self.point_start(r)
        self.spread_start(r, r.sent_m, r.got_m, 0)
        self.row_spectra(r, r.upstream[0], r.sent_u)
        self.spread_start(r, r.sent_u, r.got_u, 1)
        self.build_stencil(r, w)
        self.clear(r.rows_v0, r.rows_v1, r.rows_v2, r.rows_up, r.acc, r.taps)

        self.point_wait(r)
        self.column_spectra(r, r.got_p, r.wave_p)
        self.build_blur(r)
        self.spread_wait(r, r.sent_m, r.got_m, 0)
        self.column_spectra(r, r.got_m, r.wave)

        def start(tier, step, masks, columns):
            factor = self.factor(r.blur, tier, step)
            for z in range(Z):
                value = self.combine(masks, *self.load_wave(r.wave, z, tier, step))
                value = self.times(factor, value, True)
                self.keep(r.v0, z, tier, step, value)
                self.frames(r, masks, tier, step, z, value, r.rows_v0, columns)
            self.put_columns(r.part.at[0, 0], tier, step, columns)

        self.sweep(start)
        self.reduce_start(r, 0, [0])
        self.settle(r.rows_v0)
        self.reduce_finish(r, 0, [0])
        self.unpack(r.full.at[0, 0], r.cols_v0)

        def first(tier, step, masks, columns, back):
            for z in range(Z):
                before = self.load(r.v0, z, tier, step)
                value = [g + b for g, b in zip(self.gained(r, tier, step, before), back[z])]
                self.keep(r.v1, z, tier, step, value)
                self.frames(r, masks, tier, step, z, value, r.rows_v1, columns)
                r.acc[0] += self.dot(masks, before, before)
                r.acc[1] += self.dot(masks, before, value)
                r.acc[2] += self.dot(masks, value, value)
            self.put_columns(r.part.at[1, 0], tier, step, columns)

        self.stencil_twice(r, w, r.v0, r.rows_v0, r.cols_v0, r.m0, r.rows_m0, r.cols_m0, first)
        self.scalars_out(r, 1, 3)
        self.reduce_start(r, 1, [0, 2])
        self.settle(r.rows_v1)
        self.spread_wait(r, r.sent_u, r.got_u, 1)
        self.column_spectra(r, r.got_u, r.wave)

        def upper(tier, step, masks, columns):
            for z in range(Z):
                value = self.combine(masks, *self.load_wave(r.wave, z, tier, step))
                self.keep(r.up, z, tier, step, value)
                self.frames(r, masks, tier, step, z, value, r.rows_up, columns)
            self.put_columns(r.part.at[2, 1], tier, step, columns)

        self.sweep(upper)
        self.settle(r.rows_up)
        self.clear(r.acc)
        self.reduce_finish(r, 1, [0, 2])
        self.reduce_start(r, 2, [1])
        self.unpack(r.full.at[1, 0], r.cols_v1)
        norm_0, curve_0, image_0 = self.scalars_in(r, 1, 3)
        step_0 = norm_0 / curve_0

        def second(tier, step, masks, columns, back):
            for z in range(Z):
                before, value = (self.load(f, z, tier, step) for f in (r.v0, r.v1))
                up = self.load(r.up, z, tier, step)
                after = [g + b for g, b in zip(self.gained(r, tier, step, value), back[z])]
                self.keep(r.v2, z, tier, step, after)
                self.frames(r, masks, tier, step, z, after, r.rows_v2, columns)
                residual = [p - step_0 * q for p, q in zip(before, value)]
                image = [p - step_0 * q for p, q in zip(value, after)]
                for k, (p, q) in enumerate(
                    ((residual, residual), (residual, value), (residual, image), (image, value), (up, residual), (up, before), (up, value))
                ):
                    r.acc[k] += self.dot(masks, p, q)
            self.put_columns(r.part.at[2, 0], tier, step, columns)

        self.stencil_twice(r, w, r.v1, r.rows_v1, r.cols_v1, r.m1, r.rows_m1, r.cols_m1, second)
        self.scalars_out(r, 2, 7)
        self.reduce_start(r, 2, [0, 2])
        self.settle(r.rows_v2)
        self.reduce_finish(r, 2, [0, 1, 2])
        self.unpack(r.full.at[2, 0], r.cols_v2)
        self.unpack(r.full.at[2, 1], r.cols_up)

        norm_1, cross, inner, image_cross, up_residual, up_0, up_1 = self.scalars_in(r, 2, 7)
        ratio = norm_1 / norm_0
        curve_1 = inner + 2.0 * ratio * cross + ratio * ratio * curve_0
        step_1 = norm_1 / curve_1
        grad_step_1 = up_residual + ratio * up_0
        grad_curve_1 = -grad_step_1 * step_1 / curve_1
        grad_ratio = step_1 * up_0 + 2.0 * grad_curve_1 * (cross + ratio * curve_0)
        grad_norm = grad_step_1 / curve_1 + grad_ratio / norm_0
        grad_step_0 = (
            up_0 - step_1 * up_1 - 2.0 * grad_curve_1 * (image_cross + ratio * image_0) - 2.0 * grad_norm * cross
        )
        more = 1.0 + ratio
        g0 = grad_norm - grad_ratio * ratio / norm_0 + grad_step_0 / curve_0
        g1 = grad_curve_1 * more * more - 2.0 * grad_norm * step_0 - grad_step_0 * step_0 / curve_0
        g2 = -2.0 * grad_curve_1 * step_0 * more + grad_norm * step_0 * step_0
        g3 = grad_curve_1 * step_0 * step_0
        q0 = step_0 + step_1 * more
        q1 = -step_1 * step_0
        mix = (g1, 2.0 * g2, 2.0 * g3, q1)

        def mixed(*values):
            return mix[0] * values[0] + mix[1] * values[1] + mix[2] * values[2] + mix[3] * values[3]

        for x in range(4):

            @pl.loop(0, self.lanes)
            def _(lane):
                here = (x, slice(None), pl.ds(pl.multiple_of(lane * 128, 128), 128))
                r.cols_w3[here] = mixed(*(f[here] for f in (r.cols_v0, r.cols_v1, r.cols_v2, r.cols_up)))

        for k in range(2):
            for part in range(2):
                for tier in range(self.tiers):

                    @pl.loop(0, Z)
                    def _(z):
                        here = (k, z, part, pl.ds(8 * tier, 8))
                        r.rows_w3[here] = mixed(*(f[here] for f in (r.rows_v0, r.rows_v1, r.rows_v2, r.rows_up)))

        def blend(tier, step, masks, columns):
            for z in range(Z):
                values = [self.load(f, z, tier, step) for f in (r.v0, r.v1, r.v2, r.up)]
                self.keep(r.w3, z, tier, step, [mixed(*parts) for parts in zip(*values)])

        self.sweep(blend)
        scale = 1.0 / (self.rows * self.columns)

        def last(tier, step, masks, columns, back):
            factor = self.factor(r.blur, tier, step)
            here = pl.ds(8 * tier, 8)
            for z in range(Z):
                v0, v1, w3, up = (self.load(f, z, tier, step) for f in (r.v0, r.v1, r.w3, r.up))
                value = [
                    b + d + 2.0 * g0 * p + g1 * q + q0 * u
                    for b, d, p, q, u in zip(back[z], self.gained(r, tier, step, w3), v0, v1, up)
                ]
                value = self.separate(masks, self.times(factor, value))
                for part in range(2):
                    heavy = scale * self.beside(r, WEIGHT, part, tier)
                    for side in range(2):
                        r.wave[z, part, here, self.lane_slice(step, side)] = (
                            value[2 * part + side] * heavy * self.along(r, WEIGHT, step, side)
                        )

        self.stencil_twice(r, w, r.w3, r.rows_w3, r.cols_w3, r.mw, r.rows_mw, r.cols_mw, last)
        self.column_values(r, r.wave, r.sent_o)

        @pl.loop(1, self.nd)
        def _(k):
            self.return_copy(r, lax.rem(self.me + k, self.nd), self.me).start()

        lanes = pl.ds(pl.multiple_of(self.y * self.row_count, 128), self.row_count)
        r.got_o[self.me] = r.sent_o[self.z, :, :, lanes]

        self.tap_sums(r, 2.0 * g3)

        @pl.loop(1, self.nd)
        def _(k):
            peer = lax.rem(self.me + k, self.nd)
            self.remote(
                r.tap_part, r.tap_slots.at[self.me], r.send_tap.at[peer], r.recv_tap.at[self.me], peer
            ).start()

        r.tap_slots[self.me] = r.tap_part[...]

        @pl.loop(1, self.nd)
        def _(k):
            peer = lax.rem(self.me + k, self.nd)
            self.return_copy(r, peer, peer).wait_recv()

        self.row_values(r, r.got_o, r.out)

        @pl.loop(1, self.nd)
        def _(k):
            peer = lax.rem(self.me + k, self.nd)
            self.return_copy(r, peer, self.me).wait_send()
            self.remote(
                r.tap_part, r.tap_slots.at[peer], r.send_tap.at[peer], r.recv_tap.at[peer], peer
            ).wait()

        lots = [r.tap_slots[k] for k in range(self.nd)]
        while len(lots) > 1:
            lots = [lots[k] + lots[k + 1] for k in range(0, len(lots) - 1, 2)] + lots[len(lots) // 2 * 2 :]
        r.tap_out[...] = lots[0] / math.sqrt(self.depth * self.rows * self.columns)

    def tap_sums(self, r, weight):
        Z = self.depth
        pairs = ((r.v0, r.mw, None), (r.w3, r.m0, None), (r.v1, r.m1, weight))

        def body(tier, step, masks, columns):
            corner = masks[2]
            sx = self.beside(r, SIN, 0, tier)
            gamma = [[None, None, None, None] for a in range(3)]
            for left, right, scale in pairs:
                x = [self.load(left, z, tier, step) for z in range(Z)]
                if scale is not None:
                    x = [[scale * item for item in value] for value in x]
                for z in range(Z):
                    m = self.load(right, z, tier, step)
                    for a in range(3):
                        if not 0 <= z + a - 1 < Z:
                            continue
                        v = x[z + a - 1]
                        for side in range(2):
                            vr, vi, mr, mi = (v[2 * side], v[2 * side + 1], m[2 * side], m[2 * side + 1])
                            p, q = (vr * mr, vi * mi)
                            terms = (jnp.where(corner, 0.5 * (p + q), p + q), jnp.where(corner, 0.5 * (p - q), p + q), vi * mr - vr * mi)
                            old = gamma[a][side]
                            gamma[a][side] = terms if old is None else [o + t for o, t in zip(old, terms)]
            for a in range(3):
                sums = [0.0] * 9
                for side in range(2):
                    cx = self.beside(r, COS, side, tier)
                    cy = jnp.broadcast_to(self.along(r, COS, step, 0), (8, 128))
                    sy = jnp.broadcast_to(self.along(r, SIN, step, 0), (8, 128))
                    if side:
                        cy = jnp.where(masks[0], cy, self.along(r, COS, step, 1))
                        sy = jnp.where(masks[0], sy, -sy)
                    near, far, turn = gamma[a][side]
                    items = (
                        near, near * cx, far * cy, far * cy * cx, near * sx * sy,
                        turn * sx, turn * sy, turn * cx * sy, turn * sx * cy,
                    )
                    sums = [s + item for s, item in zip(sums, items)]
                for k in range(9):
                    r.taps[9 * a + k] += sums[k]

        self.sweep(body)

        sides = (
            (r.rows_v0, r.cols_v0, r.rows_mw, r.cols_mw, None),
            (r.rows_w3, r.cols_w3, r.rows_m0, r.cols_m0, None),
            (r.rows_v1, r.cols_v1, r.rows_m1, r.cols_m1, weight),
        )
        zero = jnp.zeros((8, 128), jnp.float32)
        by_row = [[[zero] * 3 for k in range(2)] for a in range(3)]
        by_col = [[[zero] * 3 for k in range(2)] for a in range(3)]
        by_corner = [[[zero] * 2 for k in range(2)] for a in range(3)]
        for rows_x, cols_x, rows_m, cols_m, scale in sides:
            extra = 1.0 if scale is None else scale
            for tier in range(self.tiers):
                here = pl.ds(8 * tier, 8)
                heavy = self.beside(r, WEIGHT, 0, tier) * extra
                ca, cb = (self.beside(r, COS, part, tier) for part in range(2))
                s = self.beside(r, SIN, 0, tier)
                for k in range(2):
                    for z in range(Z):
                        ma, mb = (rows_m[k, z, part, here] for part in range(2))
                        for a in range(3):
                            if not 0 <= z + a - 1 < Z:
                                continue
                            xa, xb = (rows_x[1 - k, z + a - 1, part, here] for part in range(2))
                            p, q = (heavy * xa * ma, heavy * xb * mb)
                            terms = (p + q, p * ca + q * cb, heavy * s * (xa * mb - xb * ma))
                            by_row[a][k] = [o + t for o, t in zip(by_row[a][k], terms)]
            for k in range(2):
                col_x, col_m = (cols_x.at[0 if k else 3], cols_m.at[k])
                for step in range(self.steps):
                    (xc, xs), (mc, ms) = (
                        [ref[:, pl.ds(part * self.half + 128 * step, 128)] * (extra if ref is col_x else 1.0) for part in range(2)]
                        for ref in (col_x, col_m)
                    )
                    heavy = self.along(r, WEIGHT, step, 0)
                    cc, cs = (self.along(r, COS, step, part) for part in range(2))
                    s = self.along(r, SIN, step, 0)
                    for a in range(3):
                        xc_a, xs_a = (self.shifted(item, a - 1) for item in (xc, xs))
                        p, q = (heavy * xc_a * mc, heavy * xs_a * ms)
                        terms = (p + q, p * cc + q * cs, heavy * s * (xc_a * ms - xs_a * mc))
                        by_col[a][k] = [o + t for o, t in zip(by_col[a][k], terms)]
                at_x, at_m = (self.corners(r, ref[...]) for ref in (col_x, col_m))
                for a in range(3):
                    for edge in range(2):
                        term = extra * self.shifted(at_x[1 - edge], a - 1) * at_m[edge]
                        by_corner[a][edge][k] = by_corner[a][edge][k] + term

        lane = lax.broadcasted_iota(jnp.int32, (8, 128), 1)
        lots = []
        for a in range(3):
            s = [r.taps[9 * a + k] for k in range(9)]
            for b in range(3):
                for c in range(3):
                    beta, gamma = (float(b - 1), float(c - 1))
                    if b == 1 and c == 1:
                        value = s[0]
                    elif b == 1:
                        value = s[1] - gamma * s[5]
                    elif c == 1:
                        value = s[2] - beta * s[6]
                    else:
                        value = s[3] - beta * gamma * s[4] - beta * s[7] - gamma * s[8]
                    value = value * (2.0 / (self.rows * self.columns))
                    if b != 1:
                        one, two, three = by_row[a][b // 2]
                        value = value - (one if c == 1 else two - gamma * three) * (1.0 / (128 * self.columns))
                    if c != 1:
                        one, two, three = by_col[a][c // 2]
                        value = value - (one if b == 1 else two - beta * three) * (1.0 / (self.rows * self.nd))
                    if b != 1 and c != 1:
                        value = value + by_corner[a][b // 2][c // 2] * (1.0 / (128 * self.nd))
                    lots.append(value)
        tile = jnp.zeros((8, 128), jnp.float32)
        sub = lax.broadcasted_iota(jnp.int32, (8, 128), 0)
        for k, value in enumerate(lots):
            whole = jnp.sum(jnp.sum(value, 0, keepdims=True), -1, keepdims=True)
            tile = jnp.where((sub == k % 8) & (lane == k // 8), whole, tile)
        r.tap_part[...] = tile


class Refs:
    def __init__(self, names, refs):
        for name, ref in zip(names, refs):
            setattr(self, name, ref)


def spectral(measured, point_spread, stencil_weights, upstream):
    planes, row_count, columns = measured.shape
    plan = Spectral(lax.axis_size("gy"), lax.axis_size("gz"), planes, row_count, columns)
    waves = [jnp.asarray(part) for part in wave_rows(columns)]
    if plan.rows != columns:
        waves += [jnp.asarray(part) for part in wave_rows(plan.rows)]
    along = jnp.asarray(axis_values(plan.rows).reshape(9, 1, plan.rows))
    across = axis_values(columns).reshape(9, 2, plan.nd, plan.bins).transpose(2, 1, 3, 0)
    frequencies = np.zeros((plan.nd, 2 * plan.bins, 128), np.float32)
    frequencies[:, :, :9] = across.reshape(plan.nd, 2 * plan.bins, 9)
    scratch = plan.scratch()
    inputs = ["weights", "measured", "point_spread", "upstream", "along", "frequencies"]
    names = inputs + ["wave_%d" % k for k in range(len(waves))] + ["out", "tap_out"] + list(scratch)

    def body(*refs):
        r = Refs(names, refs)
        r.tab_x = (r.wave_0, r.wave_1)
        r.tab_y = (r.wave_2, r.wave_3) if len(waves) > 2 else r.tab_x
        plan.run(r)

    out, taps = pl.pallas_call(
        body,
        out_shape=(
            jax.ShapeDtypeStruct(measured.shape, jnp.float32),
            jax.ShapeDtypeStruct((8, 128), jnp.float32),
        ),
        in_specs=[SMEM] + [VMEM] * (5 + len(waves)),
        out_specs=(VMEM, VMEM),
        scratch_shapes=list(scratch.values()),
        compiler_params=pltpu.CompilerParams(
            collective_id=0, has_side_effects=True, vmem_limit_bytes=60 * 1024 * 1024
        ),
        name="spectral",
    )(
        stencil_weights.reshape(27), measured, point_spread, upstream, along, jnp.asarray(frequencies), *waves
    )
    taps = taps[:, :4].T.reshape(32)[:27].reshape(3, 3, 3)
    return (out, taps)


def solution(mesh):
    def program(measured, point_spread, stencil_weights, upstream):
        planes, row_count, columns = measured.shape
        fits = spectral_fits(mesh.shape["gy"], mesh.shape["gz"], planes, row_count, columns)
        chosen = spectral if fits else local
        return chosen(measured, point_spread, stencil_weights, upstream)

    return jax.shard_map(
        program,
        mesh=mesh,
        in_specs=(P("gz", "gy", None), P("gy", None), P(), P("gz", "gy", None)),
        out_specs=(P("gz", "gy", None), P()),
        check_vma=False,
    )
```

```python
import math

import jax
import jax.numpy as jnp
import numpy as np
from jax import lax
from jax.experimental import pallas as pl
from jax.experimental.pallas import tpu as pltpu
from jax.sharding import PartitionSpec as P

MESH = pl.DeviceIdType.MESH
SIDES = [(dy, dz) for dy in (-1, 0, 1) for dz in (-1, 0, 1) if (dy, dz) != (0, 0)]
VMEM = pl.BlockSpec(memory_space=pltpu.VMEM)
SMEM = pl.BlockSpec(memory_space=pltpu.SMEM)
HBM = pl.BlockSpec(memory_space=pltpu.HBM)


def moved(value, shift):
    if shift == 0:
        return value
    width = value.shape[1]
    lane = lax.broadcasted_iota(jnp.int32, value.shape, 1)
    edge = 0 if shift > 0 else width - 1
    return jnp.where(lane == edge, 0.0, pltpu.roll(value, shift % width, 1))


def regular_kernel(count_y, count_z, weights, volume, back, grown, mapped, shifted, send, receive):
    rows, columns = volume.shape
    y, z = (lax.axis_index("gy"), lax.axis_index("gz"))

    def there(dy, dz):
        return (y + dy >= 0) & (y + dy < count_y) & (z + dz >= 0) & (z + dz < count_z)

    barrier = pltpu.get_barrier_semaphore()
    for dy, dz in SIDES:

        @pl.when(there(dy, dz))
        def _():
            pl.semaphore_signal(barrier, inc=1, device_id=(y + dy, z + dz), device_id_type=MESH)

    def span(place, count):
        return 1 + jnp.where(place > 0, 1, 0) + jnp.where(place < count - 1, 1, 0)

    pl.semaphore_wait(barrier, span(y, count_y) * span(z, count_z) - 1)

    def copy(field, phase, number):
        dy, dz = SIDES[number]
        source = field.at[1, pl.ds(rows if dy > 0 else 8, 8 if dy else rows)]
        start = 8 if dy == 0 else 0 if dy > 0 else rows + 8
        return pltpu.make_async_remote_copy(
            src_ref=source,
            dst_ref=field.at[1 - dz, pl.ds(start, 8 if dy else rows)],
            send_sem=send.at[phase, number],
            recv_sem=receive.at[phase, number],
            device_id=(y + dy, z + dz),
            device_id_type=MESH,
        )

    def exchange(field, phase):
        for number, (dy, dz) in enumerate(SIDES):

            @pl.when(there(dy, dz))
            def _():
                copy(field, phase, number).start()

        for number, (dy, dz) in enumerate(SIDES):
            start = 8 if dy == 0 else 0 if dy > 0 else rows + 8

            @pl.when(jnp.logical_not(there(-dy, -dz)))
            def _():
                field[1 - dz, pl.ds(start, 8 if dy else rows)] = jnp.zeros(
                    (8 if dy else rows, columns), jnp.float32
                )

        for number, (dy, dz) in enumerate(SIDES):

            @pl.when(there(-dy, -dz))
            def _():
                copy(field, phase, number).wait_recv()

            @pl.when(there(dy, dz))
            def _():
                copy(field, phase, number).wait_send()

    def apply(field, flip, put):
        def weight(a, b, c):
            return weights[26 - (9 * a + 3 * b + c) if flip else 9 * a + 3 * b + c]

        @pl.loop(0, (rows + 16) // 8)
        def _(step):
            here = pl.ds(pl.multiple_of(step * 8, 8), 8)
            sums = [None] * 3
            for a in range(3):
                value = field[a, here]
                for c in range(3):
                    turned = moved(value, 1 - c)
                    for b in range(3):
                        term = weight(a, b, c) * turned
                        sums[b] = term if sums[b] is None else sums[b] + term
            for b in range(3):
                shifted[b, here] = sums[b]

        @pl.loop(0, rows // 8)
        def _(step):
            first = pl.multiple_of(step * 8, 8)
            around = pl.ds(first, 24)
            total = shifted[1, pl.ds(first + 8, 8)]
            total = total + shifted[0, around][7:15] + shifted[2, around][9:17]
            put(first, total)

    @pl.loop(0, rows // 8)
    def _(step):
        first = pl.multiple_of(step * 8, 8)
        grown[1, pl.ds(first + 8, 8)] = volume[pl.ds(first, 8)]

    exchange(grown, 0)

    def put_mapped(first, total):
        mapped[1, pl.ds(first + 8, 8)] = total

    apply(grown, False, put_mapped)
    exchange(mapped, 1)

    def put_back(first, total):
        back[pl.ds(first, 8)] = total

    apply(mapped, True, put_back)


def regular(volume, kernel):
    rows, columns = volume.shape[1:]
    count_y, count_z = (lax.axis_size("gy"), lax.axis_size("gz"))
    field = jax.ShapeDtypeStruct((3, rows + 16, columns), jnp.float32)

    def body(*refs):
        regular_kernel(count_y, count_z, *refs)

    back, grown, mapped = pl.pallas_call(
        body,
        out_shape=(jax.ShapeDtypeStruct((rows, columns), jnp.float32), field, field),
        in_specs=[SMEM, VMEM],
        out_specs=(VMEM, VMEM, VMEM),
        scratch_shapes=[
            pltpu.VMEM((3, rows + 16, columns), jnp.float32),
            pltpu.SemaphoreType.DMA((2, 8)),
            pltpu.SemaphoreType.DMA((2, 8)),
        ],
        cost_estimate=pl.CostEstimate(flops=120 * rows * columns, bytes_accessed=20 * rows * columns, transcendentals=0),
        compiler_params=pltpu.CompilerParams(collective_id=0, has_side_effects=True),
        name="regular",
    )(kernel.reshape(27), volume[0])
    return (back[None], grown, mapped)


def total_kernel(count_y, count_z, value, out, column, row, across, send, receive):
    y, z = (lax.axis_index("gy"), lax.axis_index("gz"))
    along_y = [(lax.rem(y + k, count_y), z) for k in range(1, count_y)]
    along_z = [(y, lax.rem(z + k, count_z)) for k in range(1, count_z)]
    barrier = pltpu.get_barrier_semaphore()
    for place in along_y + along_z:
        pl.semaphore_signal(barrier, inc=1, device_id=place, device_id_type=MESH)
    pl.semaphore_wait(barrier, count_y + count_z - 2)

    def gather(source, slots, places, base):
        copies = []
        for k, place in enumerate(places):
            copies.append(
                pltpu.make_async_remote_copy(
                    src_ref=source,
                    dst_ref=slots.at[k],
                    send_sem=send.at[base + k],
                    recv_sem=receive.at[base + k],
                    device_id=place,
                    device_id_type=MESH,
                )
            )
            copies[-1].start()
        for item in copies:
            item.wait()

    def ordered(own, slots, index, count):
        total = jnp.zeros_like(own)
        for j in range(count):
            term = own
            for k in range(1, count):
                term = jnp.where(lax.rem(index - j + count, count) == k, slots[k - 1], term)
            total = total + term
        return total

    gather(value, column, along_y, 0)
    across[...] = ordered(value[...], column, y, count_y)
    gather(across, row, along_z, count_y - 1)
    out[...] = ordered(across[...], row, z, count_z)


def total(values, collective):
    count_y, count_z = (lax.axis_size("gy"), lax.axis_size("gz"))
    count = values.shape[0]

    def body(*refs):
        total_kernel(count_y, count_z, *refs)

    block = jnp.broadcast_to(jnp.pad(values, (0, 128 - count))[None], (8, 128))
    copies = count_y + count_z - 2
    summed = pl.pallas_call(
        body,
        out_shape=jax.ShapeDtypeStruct((8, 128), jnp.float32),
        in_specs=[VMEM],
        out_specs=VMEM,
        scratch_shapes=[
            pltpu.VMEM((count_y - 1, 8, 128), jnp.float32),
            pltpu.VMEM((count_z - 1, 8, 128), jnp.float32),
            pltpu.VMEM((8, 128), jnp.float32),
            pltpu.SemaphoreType.DMA((copies,)),
            pltpu.SemaphoreType.DMA((copies,)),
        ],
        compiler_params=pltpu.CompilerParams(collective_id=collective, has_side_effects=True),
        name="total",
    )(block)
    return summed[0, :count]


def correlate_kernel(scalars, grown_0, grown_1, grown_2, grown_up, mapped_0, mapped_1, mapped_2, mapped_up, out):
    rows = grown_0.shape[1] - 16
    columns = grown_0.shape[2]
    c_up, c_zero, c_one, c_two, d_zero, d_one, s_zero, s_grad, s_direction = (scalars[k] for k in range(9))
    out[...] = jnp.zeros_like(out)

    @pl.loop(0, rows // 8)
    def _(step):
        first = pl.multiple_of(step * 8, 8)
        here = pl.ds(first + 8, 8)
        zero, one = (mapped_0[1, here], mapped_1[1, here])
        grad = c_up * mapped_up[1, here] + c_zero * zero + c_one * one + c_two * mapped_2[1, here]
        values = (
            s_zero * zero + s_grad * grad,
            s_grad * zero,
            s_direction * (d_zero * zero + d_one * one),
        )
        turned = [[moved(value, c - 1) for value in values] for c in range(3)]
        for a in range(3):
            around = pl.ds(first, 24)
            full_0, full_1 = (grown_0[a, around], grown_1[a, around])
            full_grad = c_up * grown_up[a, around] + c_zero * full_0 + c_one * full_1 + c_two * grown_2[a, around]
            full_direction = d_zero * full_0 + d_one * full_1
            for b in range(3):
                fields = [item[7 + b : 15 + b] for item in (full_0, full_grad, full_direction)]
                for c in range(3):
                    product = turned[c][0] * fields[0] + turned[c][1] * fields[1] + turned[c][2] * fields[2]
                    folded = product[:, :128]
                    for part in range(1, columns // 128):
                        folded = folded + product[:, 128 * part : 128 * part + 128]
                    out[9 * a + 3 * b + c] += folded


def correlate(scalars, *fields):
    return pl.pallas_call(
        correlate_kernel,
        out_shape=jax.ShapeDtypeStruct((27, 8, 128), jnp.float32),
        in_specs=[SMEM] + [VMEM] * 8,
        out_specs=VMEM,
        cost_estimate=pl.CostEstimate(flops=40000000, bytes_accessed=8000000, transcendentals=0),
        name="correlate",
    )(scalars, *fields).sum((1, 2))


def contract(form, left, right):
    return jnp.einsum(form, left, right, precision=lax.Precision.HIGH)


def wave_tables(length, groups):
    half = length // 2
    bins = half // groups
    pair = groups // 2
    shape = (half, pair, 2, bins)
    place = lax.broadcasted_iota(jnp.int32, shape, 0)
    part = lax.broadcasted_iota(jnp.int32, shape, 2)
    slot = lax.broadcasted_iota(jnp.int32, shape, 1) * bins + lax.broadcasted_iota(jnp.int32, shape, 3)
    tables = []
    for odd in range(2):
        frequency = 2 * slot + odd
        steps = place * frequency + part * (length // 4)
        if not odd:
            steps = jnp.where((slot == 0) & (part == 1), place * half, steps)
        angle = (steps % length).astype(jnp.float32) * (2.0 * math.pi / length)
        tables.append(jnp.cos(angle).reshape(half, pair, 2 * bins))
    return tables


def combine(raw, on_row, on_lane):
    even, odd = raw
    a, b, c, d = (
        jnp.concatenate([piece[:, part, :, :, side] for piece in (even, odd)], 0)
        for part, side in ((0, 0), (0, 1), (1, 0), (1, 1))
    )
    special = on_row | on_lane
    plus_real = jnp.where(special, a, a - d)
    plus_imaginary = jnp.where(on_row, b, jnp.where(on_lane, c, b + c))
    minus_real = jnp.where(on_row, c, jnp.where(on_lane, b, a + d))
    minus_imaginary = jnp.where(special, d, b - c)
    return (jnp.stack([plus_real, minus_real]), jnp.stack([plus_imaginary, minus_imaginary]))


def separate(spectrum, on_row, on_lane):
    (plus_real, minus_real), (plus_imaginary, minus_imaginary) = spectrum
    special = on_row | on_lane
    a = jnp.where(special, plus_real, plus_real + minus_real)
    d = jnp.where(special, minus_imaginary, minus_real - plus_real)
    b = jnp.where(on_row, plus_imaginary, jnp.where(on_lane, minus_real, plus_imaginary + minus_imaginary))
    c = jnp.where(on_row, minus_real, jnp.where(on_lane, plus_imaginary, plus_imaginary - minus_imaginary))
    scale = jnp.where(on_row & on_lane, 1.0, 2.0)
    a, b, c, d = (value * scale for value in (a, b, c, d))
    whole = jnp.stack([jnp.stack([a, b], 3), jnp.stack([c, d], 3)], 1)
    pair = whole.shape[0] // 2
    return (whole[:pair], whole[pair:])


def times(left, right, corner, conjugate=False):
    (a, b), (c, d) = (left, right)
    cross = b * d
    sign = -1.0 if conjugate else 1.0
    real = jnp.where(corner, a * c, a * c - sign * cross)
    imaginary = jnp.where(corner, cross, sign * a * d + b * c)
    return (real, imaginary)


def linear(*terms):
    total_real = total_imaginary = 0.0
    for scale, (real, imaginary) in terms:
        scale_real, scale_imaginary = scale if isinstance(scale, tuple) else (scale, scale)
        total_real = total_real + scale_real * real
        total_imaginary = total_imaginary + scale_imaginary * imaginary
    return (total_real, total_imaginary)


def local(measured, point_spread, stencil_weights, upstream):
    planes, row_count, columns = measured.shape
    groups = lax.axis_size("gy")
    rows = row_count * groups
    cells = planes * rows * columns * lax.axis_size("gz")
    bins = columns // 2 // groups
    even_x, odd_x = wave_tables(columns, groups)
    even_y, odd_y = (even_x, odd_x) if rows == columns else wave_tables(rows, groups)
    y_bins = rows // 2 // groups
    spectral = (groups, y_bins, 1, bins)
    on_row = (lax.broadcasted_iota(jnp.int32, spectral, 0) == 0) & (
        lax.broadcasted_iota(jnp.int32, spectral, 1) == 0
    )
    on_lane = (lax.broadcasted_iota(jnp.int32, spectral, 3) == 0) & (lax.axis_index("gy") == 0)
    corner = on_row & on_lane

    def forward(volumes):
        count = volumes.shape[0]
        low, high = (volumes[:, :, : columns // 2], volumes[:, :, columns // 2 :])
        sent = jnp.concatenate(
            [contract("vrj,jdl->drvl", low + high, even_x), contract("vrj,jdl->drvl", low - high, odd_x)], 0
        )
        arrived = lax.all_to_all(
            sent.reshape(groups, row_count, count * 2 * bins), "gy", split_axis=0, concat_axis=0, tiled=True
        )
        arrived = arrived.reshape(rows, count * 2 * bins)
        low, high = (arrived[: rows // 2], arrived[rows // 2 :])
        raw = [
            contract("jds,jl->dsl", table, value).reshape(groups // 2, 2, y_bins, count, 2, bins)
            for table, value in ((even_y, low + high), (odd_y, low - high))
        ]
        return combine(raw, on_row, on_lane)

    def inverse(spectrum):
        count = spectrum[0].shape[3]
        pieces = separate(spectrum, on_row, on_lane)
        one, two = (
            contract("jds,dsl->jl", table, piece.reshape(groups // 2, 2 * y_bins, count * 2 * bins))
            for table, piece in ((even_y, pieces[0]), (odd_y, pieces[1]))
        )
        sent = jnp.concatenate([one + two, one - two], 0).reshape(groups, row_count, count * 2 * bins)
        arrived = lax.all_to_all(sent, "gy", split_axis=0, concat_axis=0, tiled=True)
        arrived = arrived.reshape(groups, row_count, count, 2 * bins)
        one = contract("drvl,jdl->vrj", arrived[: groups // 2], even_x)
        two = contract("drvl,jdl->vrj", arrived[groups // 2 :], odd_x)
        return jnp.concatenate([one + two, one - two], 2) / float(rows * columns)

    def pick(spectrum, start, count):
        return tuple(lax.slice_in_dim(part, start, start + count, axis=3) for part in spectrum)

    def join(*spectra):
        return tuple(jnp.concatenate(parts, 3) for parts in zip(*spectra))

    spectra = forward(jnp.concatenate([point_spread[None], measured], 0))
    transfer = pick(spectra, 0, 1)
    squares = (transfer[0] ** 2, transfer[1] ** 2)
    gain = (
        jnp.where(corner, squares[0], squares[0] + squares[1]),
        jnp.where(corner, squares[1], squares[0] + squares[1]),
    )
    spectrum_0 = times(pick(spectra, 1, planes), transfer, corner, True)
    blurred_0 = linear((gain, spectrum_0))
    pair = inverse(join(spectrum_0, blurred_0))
    vector_0 = pair[:planes]
    back_0, grown_0, mapped_0 = regular(vector_0, stencil_weights)
    back_up, grown_up, mapped_up = regular(upstream, stencil_weights)
    vector_1 = pair[planes:] + back_0
    spectrum_1 = linear((1.0, blurred_0), (1.0, forward(back_0)))
    blurred_1 = linear((gain, spectrum_1))
    early = forward(jnp.concatenate([upstream, back_up], 0))
    back_1, grown_1, mapped_1 = regular(vector_1, stencil_weights)
    vector_2 = inverse(blurred_1) + back_1
    norm_0, curve_0, image_0, up_0, up_1 = total(
        jnp.stack(
            [
                jnp.sum(vector_0 * vector_0),
                jnp.sum(vector_0 * vector_1),
                jnp.sum(vector_1 * vector_1),
                jnp.sum(upstream * vector_0),
                jnp.sum(upstream * vector_1),
            ]
        ),
        1,
    )
    step_0 = norm_0 / curve_0
    residual = vector_0 - step_0 * vector_1
    residual_image = vector_1 - step_0 * vector_2
    norm_1, cross, inner, up_residual, image_cross = total(
        jnp.stack(
            [
                jnp.sum(residual * residual),
                jnp.sum(residual * vector_1),
                jnp.sum(residual * residual_image),
                jnp.sum(upstream * residual),
                jnp.sum(residual_image * vector_1),
            ]
        ),
        2,
    )
    back_2, grown_2, mapped_2 = regular(vector_2, stencil_weights)
    late = forward(jnp.concatenate([back_1, back_2], 0))
    ratio = norm_1 / norm_0
    curve_1 = inner + 2.0 * ratio * cross + ratio * ratio * curve_0
    step_1 = norm_1 / curve_1
    grad_step_1 = up_residual + ratio * up_0
    grad_curve_1 = -grad_step_1 * step_1 / curve_1
    grad_ratio = step_1 * up_0 + 2.0 * grad_curve_1 * (cross + ratio * curve_0)
    known_image = step_1 * up_1 + 2.0 * grad_curve_1 * (image_cross + ratio * image_0)
    grad_norm = grad_step_1 / curve_1 + grad_ratio / norm_0
    grad_step_0 = up_0 - known_image - 2.0 * grad_norm * cross
    grad_curve_0 = -grad_step_0 * step_0 / curve_0
    grad_norm_0 = -grad_ratio * ratio / norm_0 + grad_step_0 / curve_0

    spectrum_2 = linear((1.0, linear((gain, spectrum_1))), (1.0, pick(late, 0, planes)))
    spectrum_up = pick(early, 0, planes)
    residual_terms = ((1.0, spectrum_0), (-step_0, spectrum_1))
    direction_image = linear((1.0 + ratio, spectrum_1), (-step_0, spectrum_2))
    grad_direction = linear((step_1, spectrum_up), (2.0 * grad_curve_1, direction_image))
    grad_residual = linear((1.0, grad_direction), (2.0 * grad_norm, linear(*residual_terms)))
    grad_back = linear(
        (step_1, pick(early, planes, planes)),
        (2.0 * grad_curve_1 * (1.0 + ratio) - 2.0 * grad_norm * step_0, pick(late, 0, planes)),
        (-2.0 * grad_curve_1 * step_0, pick(late, planes, planes)),
        (2.0 * grad_norm, linear((1.0, spectrum_1), (-1.0, blurred_0))),
    )
    grad_right = linear(
        (step_0, spectrum_up),
        (ratio, grad_direction),
        (2.0 * grad_curve_0, spectrum_1),
        (2.0 * grad_norm_0, spectrum_0),
        (1.0, grad_residual),
        (-step_0, linear((gain, grad_residual), (1.0, grad_back))),
    )
    grad_measured = inverse(times(grad_right, transfer, corner))

    terms = correlate(
        jnp.stack(
            [
                step_1,
                2.0 * grad_norm,
                2.0 * grad_curve_1 * (1.0 + ratio) - 2.0 * grad_norm * step_0,
                -2.0 * grad_curve_1 * step_0,
                1.0 + ratio,
                -step_0,
                2.0 * grad_curve_0,
                -step_0,
                2.0 * grad_curve_1,
            ]
        ),
        grown_0, grown_1, grown_2, grown_up, mapped_0, mapped_1, mapped_2, mapped_up,
    )
    grad_stencil = total(terms, 3).reshape(3, 3, 3) / math.sqrt(cells)
    return (grad_measured, grad_stencil)


def spectral_fits(mesh_y, mesh_z, planes, row_count, columns):
    devices, rows, depth = (mesh_y * mesh_z, row_count * mesh_y, planes * mesh_z)
    if columns % (16 * devices) or row_count % 128 or rows % 512 or planes != 1 or mesh_z % 2:
        return False
    tiles = 4 * depth // 8 * (rows // 128)
    return depth < 8 and depth % 2 == 0 and mesh_y % 4 == 0 and tiles % (2 * mesh_z) == 0


def wave_rows(length):
    half, quarter = (length // 2, length // 4)
    place = np.arange(half)[None, :]
    tables = []
    for odd in range(2):
        frequency = 2 * np.arange(quarter)[:, None] + odd
        angle = (place * frequency % length) * (2.0 * np.pi / length)
        cosine, sine = (np.cos(angle), np.sin(angle))
        if not odd:
            sine[0] = np.cos(np.pi * place[0])
        tables += [cosine, sine]
    table = np.stack(tables)
    high = table.astype(jnp.bfloat16)
    low = (table - high.astype(np.float64)).astype(jnp.bfloat16)
    return (high, low)


def basis(length, place):
    half = length // 2
    frequency = np.concatenate([np.arange(0, half, 2), np.arange(1, half, 2)])
    angle = frequency * place % length * (2.0 * np.pi / length)
    cosine, sine = (np.cos(angle), np.sin(angle))
    sine[0] = np.cos(np.pi * place)
    return (cosine, sine)


def axis_values(length):
    cosine, sine = basis(length, 1)
    pure = sine.copy()
    pure[0] = 0.0
    other = cosine.copy()
    other[0] = -1.0
    weight = np.full(length // 2, 2.0)
    weight[0] = 1.0
    values = [(cosine, other), (pure, pure), basis(length, 0), basis(length, length - 1), (weight, weight)]
    for place in (0, 1, length - 2, length - 1):
        values.append(tuple(weight * part / length for part in basis(length, place)))
    return np.stack([np.stack(pair) for pair in values]).astype(np.float32)


COS, SIN, FIRST, LAST, WEIGHT, AT = range(6)


def split(value):
    high = value.astype(jnp.bfloat16)
    return (high, (value - high.astype(jnp.float32)).astype(jnp.bfloat16))


def product(left, right, contracting):
    numbers = (contracting, ((), ()))

    def one(a, b):
        return lax.dot_general(a, b, numbers, preferred_element_type=jnp.float32)

    return one(left[0], right[0]) + (one(left[0], right[1]) + one(left[1], right[0]))


class Spectral:
    def __init__(self, count_y, count_z, planes, row_count, columns):
        self.ny, self.nz = (count_y, count_z)
        self.nd = count_y * count_z
        self.depth = planes * count_z
        self.row_count = row_count
        self.rows = row_count * count_y
        self.columns = columns
        self.bins = columns // 2 // self.nd
        self.half = self.rows // 2
        self.steps = self.half // 128
        self.tiers = self.bins // 8
        self.lanes = self.rows // 128
        self.tiles = 4 * self.depth // 8 * self.lanes
        self.share = self.tiles // (2 * self.nz)

    def place_of(self, index):
        return (lax.rem(index, self.ny), lax.div(index, self.ny))

    def scratch(self):
        Z, bins, half, nd = (self.depth, self.bins, self.half, self.nd)
        packed = (Z, 2, bins, self.rows)
        field = (Z, 4, bins, half)
        edge = (2, Z, 2, bins, 128)
        F = jnp.float32
        D = pltpu.SemaphoreType.DMA
        names = dict(
            sent_m=pltpu.VMEM((nd, 2, bins, 128 * (self.row_count // 128)), F),
            sent_u=pltpu.VMEM((nd, 2, bins, self.row_count), F),
            sent_p=pltpu.VMEM((self.ny, 2, bins, self.row_count), F),
            got_m=pltpu.VMEM(packed, F),
            got_u=pltpu.VMEM(packed, F),
            got_p=pltpu.VMEM((2, bins, self.rows), F),
            wave=pltpu.VMEM(packed, F),
            wave_p=pltpu.VMEM((2, bins, self.rows), F),
            v0=pltpu.VMEM(field, F),
            v1=pltpu.VMEM(field, F),
            v2=pltpu.VMEM(field, F),
            up=pltpu.VMEM(field, F),
            w3=pltpu.VMEM(field, F),
            m0=pltpu.VMEM(field, F),
            m1=pltpu.VMEM(field, F),
            mw=pltpu.VMEM(field, F),
            stencil=pltpu.VMEM((3, 2, 3, bins, half), F),
            blur=pltpu.VMEM((2, 3, bins, half), F),
            gain=pltpu.VMEM((2, 2, bins, half), F),
            across=pltpu.VMEM((9, 2, bins, 128), F),
            rows_v0=pltpu.VMEM(edge, F),
            rows_v1=pltpu.VMEM(edge, F),
            rows_v2=pltpu.VMEM(edge, F),
            rows_up=pltpu.VMEM(edge, F),
            rows_w3=pltpu.VMEM(edge, F),
            rows_m0=pltpu.VMEM(edge, F),
            rows_m1=pltpu.VMEM(edge, F),
            rows_mw=pltpu.VMEM(edge, F),
            edge_rows=pltpu.VMEM(edge, F),
            cols_v0=pltpu.VMEM((4, 8, self.rows), F),
            cols_v1=pltpu.VMEM((4, 8, self.rows), F),
            cols_v2=pltpu.VMEM((4, 8, self.rows), F),
            cols_up=pltpu.VMEM((4, 8, self.rows), F),
            cols_w3=pltpu.VMEM((4, 8, self.rows), F),
            cols_m0=pltpu.VMEM((2, 8, self.rows), F),
            cols_m1=pltpu.VMEM((2, 8, self.rows), F),
            cols_mw=pltpu.VMEM((2, 8, self.rows), F),
            edge_cols=pltpu.VMEM((2, 8, self.rows), F),
            part=pltpu.VMEM((3, 3, self.tiles, 8, 128), F),
            slots=pltpu.VMEM((3, 3, nd, self.share, 8, 128), F),
            sums=pltpu.VMEM((3, 3, self.share, 8, 128), F),
            full=pltpu.VMEM((3, 3, self.tiles, 8, 128), F),
            acc=pltpu.VMEM((8, 8, 128), F),
            taps=pltpu.VMEM((27, 8, 128), F),
            tap_part=pltpu.VMEM((1, 128), F),
            tap_slots=pltpu.VMEM((nd, 1, 128), F),
            sent_o=pltpu.VMEM(packed, F),
            got_o=pltpu.VMEM((nd, 2, bins, self.row_count), F),
            send_big=D((2, nd)),
            recv_big=D((2, nd)),
            send_p=D((self.ny,)),
            recv_p=D((self.ny,)),
            send_part=D((2, 3, 2 * self.nz)),
            recv_part=D((2, 3, nd)),
            send_full=D((2, 3, nd)),
            recv_full=D((2, 3, 2 * self.nz)),
            send_tap=D((nd,)),
            recv_tap=D((nd,)),
        )
        return names


    def remote(self, source, target, send, receive, peer):
        return pltpu.make_async_remote_copy(
            src_ref=source, dst_ref=target, send_sem=send, recv_sem=receive,
            device_id=self.place_of(peer), device_id_type=MESH,
        )

    def spread_copy(self, r, sent, got, lot, peer, source):
        y, z = self.place_of(source)
        lanes = pl.ds(pl.multiple_of(y * self.row_count, 128), self.row_count)
        return self.remote(
            sent.at[peer], got.at[z, :, :, lanes], r.send_big.at[lot, peer], r.recv_big.at[lot, source], peer
        )

    def spread_start(self, r, sent, got, lot, quarter=None):
        first, end = (1, self.nd)
        if quarter is not None:
            first, end = (max(1, quarter * self.nd // 4), (quarter + 1) * self.nd // 4)

        @pl.loop(first, end)
        def _(k):
            peer = lax.rem(self.me + k, self.nd)
            self.spread_copy(r, sent, got, lot, peer, self.me).start()

        if quarter:
            return
        y, z = self.place_of(self.me)
        lanes = pl.ds(pl.multiple_of(y * self.row_count, 128), self.row_count)
        got[z, :, :, lanes] = sent[self.me]

    def spread_wait(self, r, sent, got, lot):
        @pl.loop(1, self.nd)
        def _(k):
            peer = lax.rem(self.me + k, self.nd)
            copy = self.spread_copy(r, sent, got, lot, peer, peer)
            copy.wait_recv()

        @pl.loop(1, self.nd)
        def _(k):
            peer = lax.rem(self.me + k, self.nd)
            self.spread_copy(r, sent, got, lot, peer, self.me).wait_send()

    def point_copy(self, r, peer_y, source_y):
        lanes = pl.ds(pl.multiple_of(source_y * self.row_count, 128), self.row_count)
        return self.remote(
            r.sent_p.at[peer_y], r.got_p.at[:, :, lanes], r.send_p.at[peer_y], r.recv_p.at[source_y],
            self.z * self.ny + peer_y,
        )

    def point_start(self, r):
        @pl.loop(1, self.ny)
        def _(k):
            self.point_copy(r, lax.rem(self.y + k, self.ny), self.y).start()

        lanes = pl.ds(pl.multiple_of(self.y * self.row_count, 128), self.row_count)
        r.got_p[:, :, lanes] = r.sent_p[self.y]

    def point_wait(self, r):
        @pl.loop(1, self.ny)
        def _(k):
            peer = lax.rem(self.y + k, self.ny)
            self.point_copy(r, peer, peer).wait_recv()

        @pl.loop(1, self.ny)
        def _(k):
            peer = lax.rem(self.y + k, self.ny)
            self.point_copy(r, peer, self.y).wait_send()

    def return_copy(self, r, peer, source):
        y, z = self.place_of(peer)
        lanes = pl.ds(pl.multiple_of(y * self.row_count, 128), self.row_count)
        return self.remote(
            r.sent_o.at[z, :, :, lanes], r.got_o.at[source], r.send_big.at[0, peer], r.recv_big.at[0, source], peer
        )

    def owner(self, kind, number):
        if kind == 2:
            number = self.nz
        return lax.rem(number, self.nz) * self.ny + self.ny // 2 - 1 + 2 * lax.div(number, self.nz)

    def owned(self, kind):
        low = self.ny // 2 - 1
        if kind == 2:
            return self.me == self.owner(2, 0)
        return (self.y == low) | (self.y == low + 2)

    def owners(self, kind):
        return 1 if kind == 2 else 2 * self.nz

    def mine(self, kind):
        return 0 if kind == 2 else jnp.where(self.y == self.ny // 2 - 1, 0, self.nz) + self.z

    def lot(self, ref, turn, kind, number):
        count = 1 if kind == 2 else self.share
        return ref.at[turn, kind, pl.ds(number * count, count)]

    def slot(self, r, turn, kind, source):
        return r.slots.at[turn, kind, source, pl.ds(0, 1 if kind == 2 else self.share)]

    def part_copy(self, r, turn, kind, number, source, peer):
        return self.remote(
            self.lot(r.part, turn, kind, number), self.slot(r, turn, kind, source),
            r.send_part.at[turn % 2, kind, number], r.recv_part.at[turn % 2, kind, source], peer,
        )

    def full_copy(self, r, turn, kind, number, peer):
        return self.remote(
            r.sums.at[turn, kind, pl.ds(0, 1 if kind == 2 else self.share)], self.lot(r.full, turn, kind, number),
            r.send_full.at[turn % 2, kind, peer], r.recv_full.at[turn % 2, kind, number], peer,
        )

    def reduce_start(self, r, turn, kinds):
        for kind in kinds:

            @pl.loop(0, self.owners(kind))
            def _(number):
                owner = self.owner(kind, number)

                @pl.when(owner != self.me)
                def _():
                    self.part_copy(r, turn, kind, number, self.me, owner).start()

    def reduce_middle(self, r, turn, kinds):
        for kind in kinds:

            @pl.when(self.owned(kind))
            def _():
                number = self.mine(kind)
                self.slot(r, turn, kind, self.me)[...] = self.lot(r.part, turn, kind, number)[...]

                @pl.loop(1, self.nd)
                def _(k):
                    peer = lax.rem(self.me + k, self.nd)
                    self.part_copy(r, turn, kind, number, peer, peer).wait_recv()

                lots = [self.slot(r, turn, kind, k)[...] for k in range(self.nd)]
                while len(lots) > 1:
                    lots = [lots[k] + lots[k + 1] for k in range(0, len(lots) - 1, 2)] + lots[len(lots) // 2 * 2 :]
                r.sums[turn, kind, pl.ds(0, 1 if kind == 2 else self.share)] = lots[0]

                @pl.loop(1, self.nd)
                def _(k):
                    self.full_copy(r, turn, kind, number, lax.rem(self.me + k, self.nd)).start()

                self.lot(r.full, turn, kind, number)[...] = lots[0]

    def reduce_end(self, r, turn, kinds):
        for kind in kinds:

            @pl.loop(0, self.owners(kind))
            def _(number):
                owner = self.owner(kind, number)

                @pl.when(owner != self.me)
                def _():
                    self.full_copy(r, turn, kind, number, owner).wait_recv()
                    self.part_copy(r, turn, kind, number, self.me, owner).wait_send()

            @pl.when(self.owned(kind))
            def _():
                @pl.loop(1, self.nd)
                def _(k):
                    self.full_copy(r, turn, kind, self.mine(kind), lax.rem(self.me + k, self.nd)).wait_send()


    def row_spectra(self, r, source, sent):
        half = self.columns // 2
        low, high = (source[:, :half], source[:, half:])
        per = self.nd // 2
        for odd, value in enumerate((low + high, low - high)):
            value = split(value)
            for part in range(2):
                table = (r.tab_x[0][2 * odd + part], r.tab_x[1][2 * odd + part])
                sent[pl.ds(odd * per, per), part] = product(table, value, ((1,), (1,))).reshape(
                    per, self.bins, self.row_count
                )

    def point_spectra(self, r, source):
        half = self.columns // 2
        low, high = (source[:, :half], source[:, half:])
        odd = lax.div(2 * self.z, self.nz)
        sign = 1.0 - 2.0 * odd.astype(jnp.float32)
        value = split(low + sign * high)
        block = self.ny * self.bins
        start = pl.multiple_of(lax.rem(self.z, self.nz // 2) * block, block)
        for part in range(2):
            table = tuple(half_table[2 * odd + part, pl.ds(start, block)] for half_table in r.tab_x)
            r.sent_p[:, part] = product(table, value, ((1,), (1,))).reshape(self.ny, self.bins, self.row_count)

    def column_spectra(self, r, got, wave):
        count = math.prod(got.shape[:-1])
        value = got[...].reshape(count, self.rows)
        low, high = (value[:, : self.half], value[:, self.half :])
        quarter = self.half // 2
        for odd, value in enumerate((low + high, low - high)):
            value = split(value)
            for part in range(2):
                table = (r.tab_y[0][2 * odd + part], r.tab_y[1][2 * odd + part])
                wave[..., pl.ds(part * self.half + odd * quarter, quarter)] = product(
                    value, table, ((1,), (1,))
                ).reshape(got.shape[:-1] + (quarter,))

    def column_values(self, r, wave, target):
        count = math.prod(wave.shape[:-1])
        value = wave[...].reshape(count, self.rows)
        quarter = self.half // 2
        even, odd = (
            sum(
                product(
                    split(value[:, part * self.half + k * quarter : part * self.half + (k + 1) * quarter]),
                    (r.tab_y[0][2 * k + part], r.tab_y[1][2 * k + part]),
                    ((1,), (0,)),
                )
                for part in range(2)
            )
            for k in range(2)
        )
        shape = wave.shape[:-1] + (self.half,)
        target[..., : self.half] = (even + odd).reshape(shape)
        target[..., self.half :] = (even - odd).reshape(shape)

    def row_values(self, r, got, out):
        per = self.nd // 2
        sides = []
        for k in range(2):
            side = 0.0
            for part in range(2):
                value = got[pl.ds(k * per, per), part].reshape(per * self.bins, self.row_count)
                side = side + product(
                    split(value.T), (r.tab_x[0][2 * k + part], r.tab_x[1][2 * k + part]), ((1,), (0,))
                )
            sides.append(side)
        half = self.columns // 2
        out[0, :, :half] = sides[0] + sides[1]
        out[0, :, half:] = sides[0] - sides[1]


    def masks(self, tier, step):
        shape = (8, 128)
        row = (lax.broadcasted_iota(jnp.int32, shape, 0) == 0) & (self.me == 0)
        lane = lax.broadcasted_iota(jnp.int32, shape, 1) + 128 * step == 0
        if tier:
            row = row & False
        return (row, lane, row & lane, row | lane)

    def combine(self, masks, ac, as_, bc, bs):
        row, lane, corner, special = masks
        pr = jnp.where(special, ac, ac - bs)
        pi = jnp.where(corner, as_, jnp.where(row, -as_, jnp.where(lane, -bc, -(as_ + bc))))
        mr = jnp.where(row, bc, jnp.where(lane, as_, ac + bs))
        mi = jnp.where(corner, bs, jnp.where(special, -bs, as_ - bc))
        return [pr, pi, mr, mi]

    def separate(self, masks, field):
        row, lane, corner, special = masks
        pr, pi, mr, mi = field
        ac = jnp.where(special, pr, 0.5 * (pr + mr))
        as_ = jnp.where(corner, pi, jnp.where(row, -pi, jnp.where(lane, mr, 0.5 * (mi - pi))))
        bc = jnp.where(row, mr, jnp.where(lane, -pi, -0.5 * (pi + mi)))
        bs = jnp.where(corner, mi, jnp.where(special, -mi, 0.5 * (mr - pr)))
        return (ac, as_, bc, bs)

    def lane_slice(self, step, part=0):
        return pl.ds(pl.multiple_of(part * self.half + step * 128, 128), 128)

    def along(self, r, which, step, part):
        return r.along[which, :, self.lane_slice(step, part)]

    def beside(self, r, which, part, tier):
        return r.across[which, part, pl.ds(8 * tier, 8)]

    def load(self, field, z, tier, step):
        return [field[z, k, pl.ds(8 * tier, 8), self.lane_slice(step)] for k in range(4)]

    def keep(self, field, z, tier, step, values):
        for k in range(4):
            field[z, k, pl.ds(8 * tier, 8), self.lane_slice(step)] = values[k]

    def load_wave(self, wave, z, tier, step):
        return [
            wave[z, part, pl.ds(8 * tier, 8), self.lane_slice(step, side)]
            for part in range(2)
            for side in range(2)
        ]

    def times(self, factor, value, conjugate=False):
        out = []
        for side in range(2):
            real, other, cross = factor[side]
            a, b = (value[2 * side], value[2 * side + 1])
            if conjugate:
                out += [real * a + cross * b, other * b - cross * a]
            else:
                out += [real * a - cross * b, other * b + cross * a]
        return out

    def factor(self, array, tier, step):
        where = (pl.ds(8 * tier, 8), self.lane_slice(step))
        return [[array[(side, k) + where] for k in range(3)] for side in range(2)]

    def sweep(self, body):
        @pl.loop(0, self.steps)
        def _(step):
            columns = {}
            for tier in range(self.tiers):
                body(tier, step, self.masks(tier, step), columns)

    def frames(self, r, masks, tier, step, z, value, rows, columns=None):
        ac, as_, bc, bs = self.separate(masks, value)
        here = pl.ds(8 * tier, 8)
        for k, which in enumerate((AT, AT + 3)):
            c, s = (self.along(r, which, step, 0), self.along(r, which, step, 1))
            rows[k, z, 0, here] += ac * c + as_ * s
            rows[k, z, 1, here] += bc * c + bs * s
        if columns is None:
            return
        for x in range(4):
            a, b = (self.beside(r, AT + x, 0, tier), self.beside(r, AT + x, 1, tier))
            for side, (p, q) in enumerate(((ac, bc), (as_, bs))):
                term = a * p + b * q
                key = (x, z, side)
                columns[key] = term if key not in columns else columns[key] + term

    def put_columns(self, part, tier, step, columns):
        if tier < self.tiers - 1:
            return
        for (x, z, side), value in columns.items():
            index = x * self.depth + z
            tile = index // 8 * self.lanes + side * self.steps + step
            part[tile, pl.ds(index % 8, 1)] = jnp.sum(value, 0, keepdims=True)

    def clear(self, *refs):
        for ref in refs:
            ref[...] = jnp.zeros(ref.shape, jnp.float32)

    def settle(self, rows):
        for k in range(2):
            rows[k] = jnp.broadcast_to(jnp.sum(rows[k], -1, keepdims=True), rows.shape[1:])

    def unpack(self, full, cols):
        Z = self.depth
        cols[...] = jnp.zeros(cols.shape, jnp.float32)
        for x in range(4):
            first = x * Z
            for lane in range(self.lanes):
                cols[x, pl.ds(0, Z), pl.ds(lane * 128, 128)] = full[
                    first // 8 * self.lanes + lane, pl.ds(first % 8, Z)
                ]

    def shifted(self, value, by):
        if by == 0:
            return value
        value = pltpu.roll(value, 7 if by > 0 else 1, 0)
        sub = lax.broadcasted_iota(jnp.int32, value.shape, 0)
        return jnp.where(sub < self.depth, value, 0.0)

    def corners(self, r, col):
        out = []
        for which in (AT, AT + 3):
            weight = jnp.concatenate([r.along[which, :, :]], 0)
            out.append(jnp.broadcast_to(jnp.sum(col * weight, -1, keepdims=True), (8, 128)))
        return out

    def edges(self, r, w, rows, col_first, col_last, inner=None, mapped=None):
        Z = self.depth
        k_first, k_last = (self.corners(r, col_first[...]), self.corners(r, col_last[...]))
        total = lambda terms: sum(terms[1:], terms[0])
        q = {}
        for name, b, c, value in ((0, 0, 0, k_last[1]), (1, 0, 2, k_first[1]), (2, 2, 0, k_last[0]), (3, 2, 2, k_first[0])):
            q[name] = total([w(a, b, c) * self.shifted(value, a - 1) for a in range(3)])
        if inner is not None:
            near, far = inner
            k_near, k_far = (self.corners(r, near[...]), self.corners(r, far[...]))
            fix = []
            for (c0, v0), (c1, v1) in (((1, k_first), (2, k_near)), ((0, k_far), (1, k_last))):
                fix.append(
                    [
                        total(
                            [
                                w(a, b, c0) * self.shifted(v0[y], a - 1) + w(a, b, c1) * self.shifted(v1[y], a - 1)
                                for a in range(3)
                            ]
                        )
                        for b, y in ((0, 1), (2, 0))
                    ]
                )

        @pl.loop(0, self.steps)
        def _(step):
            c = [self.along(r, COS, step, part) for part in range(2)]
            s = self.along(r, SIN, step, 0)
            first = [self.along(r, FIRST, step, part) for part in range(2)]
            last = [self.along(r, LAST, step, part) for part in range(2)]

            def get(col):
                return [col[:, self.lane_slice(step, part)] for part in range(2)]

            def line(a, c_index, col):
                w0, w1, w2 = (w(a, b, c_index) for b in range(3))
                turn = (w2 - w0) * s
                return [
                    (w1 + (w0 + w2) * c[0]) * col[0] + turn * col[1],
                    (w1 + (w0 + w2) * c[1]) * col[1] - turn * col[0],
                ]

            def stacked(pieces):
                out = None
                for a in range(3):
                    for c_index, col in pieces:
                        term = [self.shifted(part, a - 1) for part in line(a, c_index, col)]
                        out = term if out is None else [p + t for p, t in zip(out, term)]
                return out

            f, l = (get(col_first), get(col_last))
            for k, (pieces, upper, lower) in enumerate((([(0, l)], q[0], q[2]), ([(2, f)], q[1], q[3]))):
                value = stacked(pieces)
                for part in range(2):
                    r.edge_cols[k, :, self.lane_slice(step, part)] = (
                        value[part] - upper * first[part] - lower * last[part]
                    )
            if inner is not None:
                n, g = (get(near), get(far))
                for k, pieces in enumerate(([(1, f), (2, n)], [(0, g), (1, l)])):
                    value = stacked(pieces)
                    for part in range(2):
                        mapped[k, :, self.lane_slice(step, part)] = (
                            value[part] - fix[k][0] * first[part] - fix[k][1] * last[part]
                        )

        for tier in range(self.tiers):
            here = pl.ds(8 * tier, 8)
            c = [self.beside(r, COS, part, tier) for part in range(2)]
            s = self.beside(r, SIN, 0, tier)
            for k, (b, source) in enumerate(((0, 1), (2, 0))):
                for z in range(Z):
                    out = None
                    for a in range(3):
                        if not 0 <= z + a - 1 < Z:
                            continue
                        w0, w1, w2 = (w(a, b, c_index) for c_index in range(3))
                        turn = (w2 - w0) * s
                        p, t = (rows[source, z + a - 1, part, here] for part in range(2))
                        term = [
                            (w1 + (w0 + w2) * c[0]) * p + turn * t,
                            (w1 + (w0 + w2) * c[1]) * t - turn * p,
                        ]
                        out = term if out is None else [x + v for x, v in zip(out, term)]
                    for part in range(2):
                        r.edge_rows[k, z, part, here] = out[part]

    def edge_field(self, r, masks, tier, step, z):
        here = pl.ds(8 * tier, 8)
        out = []
        for part in range(2):
            e0, e1 = (r.edge_rows[k, z, part, here] for k in range(2))
            x0, x1 = (self.beside(r, which, part, tier) for which in (FIRST, LAST))
            for side in range(2):
                y0, y1 = (self.along(r, which, step, side) for which in (FIRST, LAST))
                c0, c1 = (r.edge_cols[k, pl.ds(z, 1), self.lane_slice(step, side)] for k in range(2))
                out.append(e0 * y0 + e1 * y1 + x0 * c0 + x1 * c1)
        return self.combine(masks, *out)

    def stencil_field(self, r, masks, tier, step, field, flip):
        Z = self.depth
        value = [self.load(field, z, tier, step) for z in range(Z)]
        out = [[-e for e in self.edge_field(r, masks, tier, step, z)] for z in range(Z)]
        for a in range(3):
            where = (pl.ds(8 * tier, 8), self.lane_slice(step))
            factor = [[r.stencil[(a, side, k) + where] for k in range(3)] for side in range(2)]
            for z in range(Z):
                other = z + (1 - a if flip else a - 1)
                if 0 <= other < Z:
                    term = self.times(factor, value[other], flip)
                    out[z] = [o + t for o, t in zip(out[z], term)]
        return out

    def build_stencil(self, r, w):
        def body(tier, step, masks, columns):
            row, lane, corner, special = masks
            here = pl.ds(8 * tier, 8)
            sx = self.beside(r, SIN, 0, tier)
            ys = self.along(r, SIN, step, 0)
            for side in range(2):
                cx = self.beside(r, COS, side, tier)
                cy = self.along(r, COS, step, 0)
                sy = jnp.broadcast_to(ys, (8, 128))
                cy = jnp.broadcast_to(cy, (8, 128))
                if side:
                    cy = jnp.where(row, cy, self.along(r, COS, step, 1))
                    sy = jnp.where(row, sy, -sy)
                for a in range(3):
                    real, imag = ([], [])
                    for b in range(3):
                        real.append(w(a, b, 1) + (w(a, b, 0) + w(a, b, 2)) * cx)
                        imag.append((w(a, b, 2) - w(a, b, 0)) * sx)
                    value = real[1] + (real[0] + real[2]) * cy - (imag[2] - imag[0]) * sy
                    cross = imag[1] + (imag[0] + imag[2]) * cy + (real[2] - real[0]) * sy
                    other = jnp.where(corner, real[1] - (real[0] + real[2]), value)
                    for k, item in enumerate((value, other, cross)):
                        r.stencil[a, side, k, here, self.lane_slice(step)] = item

        self.sweep(body)

    def build_blur(self, r):
        def body(tier, step, masks, columns):
            row, lane, corner, special = masks
            here = pl.ds(8 * tier, 8)
            wave = [
                r.wave_p[part, here, self.lane_slice(step, side)] for part in range(2) for side in range(2)
            ]
            value = self.combine(masks, wave[0], wave[1], wave[2], wave[3])
            for side in range(2):
                real, imag = (value[2 * side], value[2 * side + 1])
                other = jnp.where(corner, imag, real)
                cross = jnp.where(corner, 0.0, imag)
                for k, item in enumerate((real, other, cross)):
                    r.blur[side, k, here, self.lane_slice(step)] = item
                square = cross * cross
                r.gain[side, 0, here, self.lane_slice(step)] = real * real + square
                r.gain[side, 1, here, self.lane_slice(step)] = other * other + square

        self.sweep(body)

    def gained(self, r, tier, step, value):
        where = (pl.ds(8 * tier, 8), self.lane_slice(step))
        return [r.gain[(k // 2, k % 2) + where] * value[k] for k in range(4)]

    def dot(self, masks, left, right):
        corner = masks[2]
        total = sum(a * b for a, b in zip(left, right))
        return jnp.where(corner, 0.5 * total, total)


    def stencil_twice(self, r, w, field, rows, cols, mapped, rows_m, cols_m, finish, after=None):
        def flipped(a, b, c):
            return w(2 - a, 2 - b, 2 - c)

        self.edges(r, w, rows, cols.at[0], cols.at[3], (cols.at[1], cols.at[2]), cols_m)
        self.clear(rows_m)

        def forward(tier, step, masks, columns):
            out = self.stencil_field(r, masks, tier, step, field, False)
            for z in range(self.depth):
                self.keep(mapped, z, tier, step, out[z])
                self.frames(r, masks, tier, step, z, out[z], rows_m)

        self.sweep(forward)
        self.settle(rows_m)
        self.edges(r, flipped, rows_m, cols_m.at[0], cols_m.at[1])

        def back(tier, step, masks, columns):
            finish(tier, step, masks, columns, self.stencil_field(r, masks, tier, step, mapped, True))

        self.sweep(back)

    def scalars_out(self, r, turn, count):
        for k in range(count):
            r.part[turn, 2, 0, pl.ds(k, 1)] = jnp.sum(r.acc[k], 0, keepdims=True)
        for k in range(count, 8):
            r.part[turn, 2, 0, pl.ds(k, 1)] = jnp.zeros((1, 128), jnp.float32)

    def scalars_in(self, r, turn, count):
        value = jnp.sum(r.full[turn, 2, 0], -1, keepdims=True)
        return [jnp.broadcast_to(value[k : k + 1], (8, 128)) for k in range(count)]

    def run(self, r):
        Z = self.depth
        self.y, self.z = (lax.axis_index("gy"), lax.axis_index("gz"))
        self.me = self.z * self.ny + self.y

        def w(a, b, c):
            return r.weights[a, b, c]

        barrier = pltpu.get_barrier_semaphore()

        @pl.loop(1, self.nd)
        def _(k):
            pl.semaphore_signal(
                barrier, inc=1, device_id=self.place_of(lax.rem(self.me + k, self.nd)), device_id_type=MESH
            )

        def load(name):
            far = getattr(r, "far_" + name)
            far = far.at[self.me] if name == "frequencies" else far
            return pltpu.make_async_copy(far, getattr(r, name), r.loaded.at[r.inputs.index(name)])

        tables = [name for name in r.inputs if name.startswith("wave")]
        order = ["frequencies", "weights", "along", "point_spread"] + tables + ["measured", "upstream"]
        for name in order:
            load(name).start()
        load("frequencies").wait()
        for which in range(9):
            for part in range(2):
                r.across[which, part] = jnp.broadcast_to(
                    r.frequencies[part * self.bins : (part + 1) * self.bins, which : which + 1], (self.bins, 128)
                )
        load("along").wait()
        load("weights").wait()
        self.build_stencil(r, w)
        load("point_spread").wait()
        for name in tables:
            load(name).wait()
        self.point_spectra(r, r.point_spread[...])
        load("measured").wait()
        self.row_spectra(r, r.measured[0], r.sent_m)
        pl.semaphore_wait(barrier, self.nd - 1)
        self.point_start(r)
        self.spread_start(r, r.sent_m, r.got_m, 0)
        load("upstream").wait()
        self.row_spectra(r, r.upstream[0], r.sent_u)
        self.clear(r.rows_v0, r.rows_v1, r.rows_v2, r.rows_up, r.acc, r.taps)

        self.point_wait(r)
        self.column_spectra(r, r.got_p, r.wave_p)
        self.build_blur(r)
        self.spread_wait(r, r.sent_m, r.got_m, 0)
        self.spread_start(r, r.sent_u, r.got_u, 1, 0)
        self.column_spectra(r, r.got_m, r.wave)

        def start(tier, step, masks, columns):
            factor = self.factor(r.blur, tier, step)
            for z in range(Z):
                value = self.combine(masks, *self.load_wave(r.wave, z, tier, step))
                value = self.times(factor, value, True)
                self.keep(r.v0, z, tier, step, value)
                self.frames(r, masks, tier, step, z, value, r.rows_v0, columns)
            self.put_columns(r.part.at[0, 0], tier, step, columns)

        self.sweep(start)
        self.reduce_start(r, 0, [0])
        self.spread_start(r, r.sent_u, r.got_u, 1, 1)
        self.settle(r.rows_v0)
        self.reduce_middle(r, 0, [0])
        self.reduce_end(r, 0, [0])
        self.spread_start(r, r.sent_u, r.got_u, 1, 2)
        self.unpack(r.full.at[0, 0], r.cols_v0)

        def first(tier, step, masks, columns, back):
            for z in range(Z):
                before = self.load(r.v0, z, tier, step)
                value = [g + b for g, b in zip(self.gained(r, tier, step, before), back[z])]
                self.keep(r.v1, z, tier, step, value)
                self.frames(r, masks, tier, step, z, value, r.rows_v1, columns)
                r.acc[0] += self.dot(masks, before, before)
                r.acc[1] += self.dot(masks, before, value)
                r.acc[2] += self.dot(masks, value, value)
            self.put_columns(r.part.at[1, 0], tier, step, columns)

        self.stencil_twice(r, w, r.v0, r.rows_v0, r.cols_v0, r.m0, r.rows_m0, r.cols_m0, first)
        self.scalars_out(r, 1, 3)
        self.reduce_start(r, 1, [0, 2])
        self.spread_start(r, r.sent_u, r.got_u, 1, 3)
        self.settle(r.rows_v1)
        self.reduce_middle(r, 1, [0, 2])
        self.spread_wait(r, r.sent_u, r.got_u, 1)
        self.column_spectra(r, r.got_u, r.wave)

        def upper(tier, step, masks, columns):
            for z in range(Z):
                value = self.combine(masks, *self.load_wave(r.wave, z, tier, step))
                self.keep(r.up, z, tier, step, value)
                self.frames(r, masks, tier, step, z, value, r.rows_up, columns)
            self.put_columns(r.part.at[2, 1], tier, step, columns)

        self.sweep(upper)
        self.settle(r.rows_up)
        self.clear(r.acc)
        self.reduce_end(r, 1, [0, 2])
        self.reduce_start(r, 2, [1])
        self.unpack(r.full.at[1, 0], r.cols_v1)
        norm_0, curve_0, image_0 = self.scalars_in(r, 1, 3)
        step_0 = norm_0 / curve_0

        def second(tier, step, masks, columns, back):
            for z in range(Z):
                before, value = (self.load(f, z, tier, step) for f in (r.v0, r.v1))
                up = self.load(r.up, z, tier, step)
                after = [g + b for g, b in zip(self.gained(r, tier, step, value), back[z])]
                self.keep(r.v2, z, tier, step, after)
                self.frames(r, masks, tier, step, z, after, r.rows_v2, columns)
                residual = [p - step_0 * q for p, q in zip(before, value)]
                image = [p - step_0 * q for p, q in zip(value, after)]
                for k, (p, q) in enumerate(
                    ((residual, residual), (residual, value), (residual, image), (image, value), (up, residual), (up, before), (up, value))
                ):
                    r.acc[k] += self.dot(masks, p, q)
            self.put_columns(r.part.at[2, 0], tier, step, columns)

        self.stencil_twice(r, w, r.v1, r.rows_v1, r.cols_v1, r.m1, r.rows_m1, r.cols_m1, second)
        self.scalars_out(r, 2, 7)
        self.reduce_start(r, 2, [0, 2])
        self.settle(r.rows_v2)
        self.reduce_middle(r, 2, [1, 0, 2])
        self.reduce_end(r, 2, [1, 0, 2])
        self.unpack(r.full.at[2, 0], r.cols_v2)
        self.unpack(r.full.at[2, 1], r.cols_up)

        norm_1, cross, inner, image_cross, up_residual, up_0, up_1 = self.scalars_in(r, 2, 7)
        ratio = norm_1 / norm_0
        curve_1 = inner + 2.0 * ratio * cross + ratio * ratio * curve_0
        step_1 = norm_1 / curve_1
        grad_step_1 = up_residual + ratio * up_0
        grad_curve_1 = -grad_step_1 * step_1 / curve_1
        grad_ratio = step_1 * up_0 + 2.0 * grad_curve_1 * (cross + ratio * curve_0)
        grad_norm = grad_step_1 / curve_1 + grad_ratio / norm_0
        grad_step_0 = (
            up_0 - step_1 * up_1 - 2.0 * grad_curve_1 * (image_cross + ratio * image_0) - 2.0 * grad_norm * cross
        )
        more = 1.0 + ratio
        g0 = grad_norm - grad_ratio * ratio / norm_0 + grad_step_0 / curve_0
        g1 = grad_curve_1 * more * more - 2.0 * grad_norm * step_0 - grad_step_0 * step_0 / curve_0
        g2 = -2.0 * grad_curve_1 * step_0 * more + grad_norm * step_0 * step_0
        g3 = grad_curve_1 * step_0 * step_0
        q0 = step_0 + step_1 * more
        q1 = -step_1 * step_0
        mix = (g1, 2.0 * g2, 2.0 * g3, q1)

        def mixed(*values):
            return mix[0] * values[0] + mix[1] * values[1] + mix[2] * values[2] + mix[3] * values[3]

        for x in range(4):

            @pl.loop(0, self.lanes)
            def _(lane):
                here = (x, slice(None), pl.ds(pl.multiple_of(lane * 128, 128), 128))
                r.cols_w3[here] = mixed(*(f[here] for f in (r.cols_v0, r.cols_v1, r.cols_v2, r.cols_up)))

        for k in range(2):
            for part in range(2):
                for tier in range(self.tiers):

                    @pl.loop(0, Z)
                    def _(z):
                        here = (k, z, part, pl.ds(8 * tier, 8))
                        r.rows_w3[here] = mixed(*(f[here] for f in (r.rows_v0, r.rows_v1, r.rows_v2, r.rows_up)))

        def blend(tier, step, masks, columns):
            for z in range(Z):
                values = [self.load(f, z, tier, step) for f in (r.v0, r.v1, r.v2, r.up)]
                self.keep(r.w3, z, tier, step, [mixed(*parts) for parts in zip(*values)])

        self.sweep(blend)
        scale = 1.0 / (self.rows * self.columns)

        def last(tier, step, masks, columns, back):
            factor = self.factor(r.blur, tier, step)
            here = pl.ds(8 * tier, 8)
            for z in range(Z):
                v0, v1, w3, up = (self.load(f, z, tier, step) for f in (r.v0, r.v1, r.w3, r.up))
                value = [
                    b + d + 2.0 * g0 * p + g1 * q + q0 * u
                    for b, d, p, q, u in zip(back[z], self.gained(r, tier, step, w3), v0, v1, up)
                ]
                value = self.separate(masks, self.times(factor, value))
                for part in range(2):
                    heavy = scale * self.beside(r, WEIGHT, part, tier)
                    for side in range(2):
                        r.wave[z, part, here, self.lane_slice(step, side)] = (
                            value[2 * part + side] * heavy * self.along(r, WEIGHT, step, side)
                        )

        self.stencil_twice(r, w, r.w3, r.rows_w3, r.cols_w3, r.mw, r.rows_mw, r.cols_mw, last)
        self.column_values(r, r.wave, r.sent_o)

        @pl.loop(1, self.nd)
        def _(k):
            self.return_copy(r, lax.rem(self.me + k, self.nd), self.me).start()

        lanes = pl.ds(pl.multiple_of(self.y * self.row_count, 128), self.row_count)
        r.got_o[self.me] = r.sent_o[self.z, :, :, lanes]

        self.tap_sums(r, 2.0 * g3)

        @pl.loop(1, self.nd)
        def _(k):
            peer = lax.rem(self.me + k, self.nd)
            self.remote(
                r.tap_part, r.tap_slots.at[self.me], r.send_tap.at[peer], r.recv_tap.at[self.me], peer
            ).start()

        r.tap_slots[self.me] = r.tap_part[...]

        @pl.loop(1, self.nd)
        def _(k):
            peer = lax.rem(self.me + k, self.nd)
            self.return_copy(r, peer, peer).wait_recv()

        self.row_values(r, r.got_o, r.out)

        @pl.loop(1, self.nd)
        def _(k):
            peer = lax.rem(self.me + k, self.nd)
            self.return_copy(r, peer, self.me).wait_send()
            self.remote(
                r.tap_part, r.tap_slots.at[peer], r.send_tap.at[peer], r.recv_tap.at[peer], peer
            ).wait()

        lots = [r.tap_slots[k] for k in range(self.nd)]
        while len(lots) > 1:
            lots = [lots[k] + lots[k + 1] for k in range(0, len(lots) - 1, 2)] + lots[len(lots) // 2 * 2 :]
        line = jnp.broadcast_to(lots[0] / math.sqrt(self.depth * self.rows * self.columns), (8, 128))
        for a in range(3):
            for b in range(3):
                first = 9 * a + 3 * b
                turned = pltpu.roll(line, 128 - first, 1) if first else line
                r.tap_out[a, pl.ds(b, 1)] = turned[:1, :3]

    def tap_sums(self, r, weight):
        Z = self.depth
        pairs = ((r.v0, r.mw, None), (r.w3, r.m0, None), (r.v1, r.m1, weight))

        def body(tier, step, masks, columns):
            corner = masks[2]
            sx = self.beside(r, SIN, 0, tier)
            gamma = [[None, None, None, None] for a in range(3)]
            for left, right, scale in pairs:
                x = [self.load(left, z, tier, step) for z in range(Z)]
                if scale is not None:
                    x = [[scale * item for item in value] for value in x]
                for z in range(Z):
                    m = self.load(right, z, tier, step)
                    for a in range(3):
                        if not 0 <= z + a - 1 < Z:
                            continue
                        v = x[z + a - 1]
                        for side in range(2):
                            vr, vi, mr, mi = (v[2 * side], v[2 * side + 1], m[2 * side], m[2 * side + 1])
                            p, q = (vr * mr, vi * mi)
                            terms = (jnp.where(corner, 0.5 * (p + q), p + q), jnp.where(corner, 0.5 * (p - q), p + q), vi * mr - vr * mi)
                            old = gamma[a][side]
                            gamma[a][side] = terms if old is None else [o + t for o, t in zip(old, terms)]
            for a in range(3):
                sums = [0.0] * 9
                for side in range(2):
                    cx = self.beside(r, COS, side, tier)
                    cy = jnp.broadcast_to(self.along(r, COS, step, 0), (8, 128))
                    sy = jnp.broadcast_to(self.along(r, SIN, step, 0), (8, 128))
                    if side:
                        cy = jnp.where(masks[0], cy, self.along(r, COS, step, 1))
                        sy = jnp.where(masks[0], sy, -sy)
                    near, far, turn = gamma[a][side]
                    items = (
                        near, near * cx, far * cy, far * cy * cx, near * sx * sy,
                        turn * sx, turn * sy, turn * cx * sy, turn * sx * cy,
                    )
                    sums = [s + item for s, item in zip(sums, items)]
                for k in range(9):
                    r.taps[9 * a + k] += sums[k]

        self.sweep(body)

        sides = (
            (r.rows_v0, r.cols_v0, r.rows_mw, r.cols_mw, None),
            (r.rows_w3, r.cols_w3, r.rows_m0, r.cols_m0, None),
            (r.rows_v1, r.cols_v1, r.rows_m1, r.cols_m1, weight),
        )
        zero = jnp.zeros((8, 128), jnp.float32)
        by_row = [[[zero] * 3 for k in range(2)] for a in range(3)]
        by_col = [[[zero] * 3 for k in range(2)] for a in range(3)]
        by_corner = [[[zero] * 2 for k in range(2)] for a in range(3)]
        for rows_x, cols_x, rows_m, cols_m, scale in sides:
            extra = 1.0 if scale is None else scale
            for tier in range(self.tiers):
                here = pl.ds(8 * tier, 8)
                heavy = self.beside(r, WEIGHT, 0, tier) * extra
                ca, cb = (self.beside(r, COS, part, tier) for part in range(2))
                s = self.beside(r, SIN, 0, tier)
                for k in range(2):
                    for z in range(Z):
                        ma, mb = (rows_m[k, z, part, here] for part in range(2))
                        for a in range(3):
                            if not 0 <= z + a - 1 < Z:
                                continue
                            xa, xb = (rows_x[1 - k, z + a - 1, part, here] for part in range(2))
                            p, q = (heavy * xa * ma, heavy * xb * mb)
                            terms = (p + q, p * ca + q * cb, heavy * s * (xa * mb - xb * ma))
                            by_row[a][k] = [o + t for o, t in zip(by_row[a][k], terms)]
            for k in range(2):
                col_x, col_m = (cols_x.at[0 if k else 3], cols_m.at[k])
                for step in range(self.steps):
                    (xc, xs), (mc, ms) = (
                        [ref[:, pl.ds(part * self.half + 128 * step, 128)] * (extra if ref is col_x else 1.0) for part in range(2)]
                        for ref in (col_x, col_m)
                    )
                    heavy = self.along(r, WEIGHT, step, 0)
                    cc, cs = (self.along(r, COS, step, part) for part in range(2))
                    s = self.along(r, SIN, step, 0)
                    for a in range(3):
                        xc_a, xs_a = (self.shifted(item, a - 1) for item in (xc, xs))
                        p, q = (heavy * xc_a * mc, heavy * xs_a * ms)
                        terms = (p + q, p * cc + q * cs, heavy * s * (xc_a * ms - xs_a * mc))
                        by_col[a][k] = [o + t for o, t in zip(by_col[a][k], terms)]
                at_x, at_m = (self.corners(r, ref[...]) for ref in (col_x, col_m))
                for a in range(3):
                    for edge in range(2):
                        term = extra * self.shifted(at_x[1 - edge], a - 1) * at_m[edge]
                        by_corner[a][edge][k] = by_corner[a][edge][k] + term

        lots = []
        for a in range(3):
            s = [r.taps[9 * a + k] for k in range(9)]
            for b in range(3):
                for c in range(3):
                    beta, gamma = (float(b - 1), float(c - 1))
                    if b == 1 and c == 1:
                        value = s[0]
                    elif b == 1:
                        value = s[1] - gamma * s[5]
                    elif c == 1:
                        value = s[2] - beta * s[6]
                    else:
                        value = s[3] - beta * gamma * s[4] - beta * s[7] - gamma * s[8]
                    value = value * (2.0 / (self.rows * self.columns))
                    if b != 1:
                        one, two, three = by_row[a][b // 2]
                        value = value - (one if c == 1 else two - gamma * three) * (1.0 / (128 * self.columns))
                    if c != 1:
                        one, two, three = by_col[a][c // 2]
                        value = value - (one if b == 1 else two - beta * three) * (1.0 / (self.rows * self.nd))
                    if b != 1 and c != 1:
                        value = value + by_corner[a][b // 2][c // 2] * (1.0 / (128 * self.nd))
                    lots.append(value)
        lane = lax.broadcasted_iota(jnp.int32, (1, 128), 1)
        line = jnp.zeros((1, 128), jnp.float32)
        for k, value in enumerate(lots):
            whole = jnp.sum(jnp.sum(value, 0, keepdims=True), -1, keepdims=True)
            line = jnp.where(lane == k, whole, line)
        r.tap_part[...] = line


class Refs:
    def __init__(self, names, refs):
        for name, ref in zip(names, refs):
            setattr(self, name, ref)


def spectral(measured, point_spread, stencil_weights, upstream):
    planes, row_count, columns = measured.shape
    plan = Spectral(lax.axis_size("gy"), lax.axis_size("gz"), planes, row_count, columns)
    waves = [jnp.asarray(part) for part in wave_rows(columns)]
    if plan.rows != columns:
        waves += [jnp.asarray(part) for part in wave_rows(plan.rows)]
    along = jnp.asarray(axis_values(plan.rows).reshape(9, 1, plan.rows))
    across = axis_values(columns).reshape(9, 2, plan.nd, plan.bins).transpose(2, 1, 3, 0)
    frequencies = np.zeros((plan.nd, 2 * plan.bins, 128), np.float32)
    frequencies[:, :, :9] = across.reshape(plan.nd, 2 * plan.bins, 9)
    scratch = plan.scratch()
    arrays = dict(weights=stencil_weights, measured=measured, point_spread=point_spread, upstream=upstream, along=along)
    arrays.update({"wave_%d" % k: part for k, part in enumerate(waves)})
    arrays["frequencies"] = jnp.asarray(frequencies)
    for name, array in arrays.items():
        shape = array.shape[1:] if name == "frequencies" else array.shape
        space = pltpu.SMEM if name == "weights" else pltpu.VMEM
        scratch[name] = space(shape, array.dtype)
    scratch["loaded"] = pltpu.SemaphoreType.DMA((len(arrays),))
    names = ["far_" + name for name in arrays] + ["out", "tap_out"] + list(scratch)

    def body(*refs):
        r = Refs(names, refs)
        r.tab_x = (r.wave_0, r.wave_1)
        r.tab_y = (r.wave_2, r.wave_3) if len(waves) > 2 else r.tab_x
        r.inputs = list(arrays)
        plan.run(r)

    out, taps = pl.pallas_call(
        body,
        out_shape=(
            jax.ShapeDtypeStruct(measured.shape, jnp.float32),
            jax.ShapeDtypeStruct((3, 3, 3), jnp.float32),
        ),
        in_specs=[HBM] * len(arrays),
        out_specs=(VMEM, VMEM),
        scratch_shapes=list(scratch.values()),
        compiler_params=pltpu.CompilerParams(
            collective_id=0, has_side_effects=True, vmem_limit_bytes=32 * 1024 * 1024
        ),
        name="spectral",
    )(
        *(pltpu.with_memory_space_constraint(array, pltpu.HBM) for array in arrays.values())
    )
    return (out, taps)


def solution(mesh):
    def program(measured, point_spread, stencil_weights, upstream):
        planes, row_count, columns = measured.shape
        fits = spectral_fits(mesh.shape["gy"], mesh.shape["gz"], planes, row_count, columns)
        chosen = spectral if fits else local
        return chosen(measured, point_spread, stencil_weights, upstream)

    return jax.shard_map(
        program,
        mesh=mesh,
        in_specs=(P("gz", "gy", None), P("gy", None), P(), P("gz", "gy", None)),
        out_specs=(P("gz", "gy", None), P()),
        check_vma=False,
    )
```

```python
import math

import jax
import jax.numpy as jnp
import numpy as np
from jax import lax
from jax.experimental import pallas as pl
from jax.experimental.pallas import tpu as pltpu
from jax.sharding import PartitionSpec as P

MESH = pl.DeviceIdType.MESH
SIDES = [(dy, dz) for dy in (-1, 0, 1) for dz in (-1, 0, 1) if (dy, dz) != (0, 0)]
VMEM = pl.BlockSpec(memory_space=pltpu.VMEM)
SMEM = pl.BlockSpec(memory_space=pltpu.SMEM)
HBM = pl.BlockSpec(memory_space=pltpu.HBM)


def moved(value, shift):
    if shift == 0:
        return value
    width = value.shape[1]
    lane = lax.broadcasted_iota(jnp.int32, value.shape, 1)
    edge = 0 if shift > 0 else width - 1
    return jnp.where(lane == edge, 0.0, pltpu.roll(value, shift % width, 1))


def regular_kernel(count_y, count_z, weights, volume, back, grown, mapped, shifted, send, receive):
    rows, columns = volume.shape
    y, z = (lax.axis_index("gy"), lax.axis_index("gz"))

    def there(dy, dz):
        return (y + dy >= 0) & (y + dy < count_y) & (z + dz >= 0) & (z + dz < count_z)

    barrier = pltpu.get_barrier_semaphore()
    for dy, dz in SIDES:

        @pl.when(there(dy, dz))
        def _():
            pl.semaphore_signal(barrier, inc=1, device_id=(y + dy, z + dz), device_id_type=MESH)

    def span(place, count):
        return 1 + jnp.where(place > 0, 1, 0) + jnp.where(place < count - 1, 1, 0)

    pl.semaphore_wait(barrier, span(y, count_y) * span(z, count_z) - 1)

    def copy(field, phase, number):
        dy, dz = SIDES[number]
        source = field.at[1, pl.ds(rows if dy > 0 else 8, 8 if dy else rows)]
        start = 8 if dy == 0 else 0 if dy > 0 else rows + 8
        return pltpu.make_async_remote_copy(
            src_ref=source,
            dst_ref=field.at[1 - dz, pl.ds(start, 8 if dy else rows)],
            send_sem=send.at[phase, number],
            recv_sem=receive.at[phase, number],
            device_id=(y + dy, z + dz),
            device_id_type=MESH,
        )

    def exchange(field, phase):
        for number, (dy, dz) in enumerate(SIDES):

            @pl.when(there(dy, dz))
            def _():
                copy(field, phase, number).start()

        for number, (dy, dz) in enumerate(SIDES):
            start = 8 if dy == 0 else 0 if dy > 0 else rows + 8

            @pl.when(jnp.logical_not(there(-dy, -dz)))
            def _():
                field[1 - dz, pl.ds(start, 8 if dy else rows)] = jnp.zeros(
                    (8 if dy else rows, columns), jnp.float32
                )

        for number, (dy, dz) in enumerate(SIDES):

            @pl.when(there(-dy, -dz))
            def _():
                copy(field, phase, number).wait_recv()

            @pl.when(there(dy, dz))
            def _():
                copy(field, phase, number).wait_send()

    def apply(field, flip, put):
        def weight(a, b, c):
            return weights[26 - (9 * a + 3 * b + c) if flip else 9 * a + 3 * b + c]

        @pl.loop(0, (rows + 16) // 8)
        def _(step):
            here = pl.ds(pl.multiple_of(step * 8, 8), 8)
            sums = [None] * 3
            for a in range(3):
                value = field[a, here]
                for c in range(3):
                    turned = moved(value, 1 - c)
                    for b in range(3):
                        term = weight(a, b, c) * turned
                        sums[b] = term if sums[b] is None else sums[b] + term
            for b in range(3):
                shifted[b, here] = sums[b]

        @pl.loop(0, rows // 8)
        def _(step):
            first = pl.multiple_of(step * 8, 8)
            around = pl.ds(first, 24)
            total = shifted[1, pl.ds(first + 8, 8)]
            total = total + shifted[0, around][7:15] + shifted[2, around][9:17]
            put(first, total)

    @pl.loop(0, rows // 8)
    def _(step):
        first = pl.multiple_of(step * 8, 8)
        grown[1, pl.ds(first + 8, 8)] = volume[pl.ds(first, 8)]

    exchange(grown, 0)

    def put_mapped(first, total):
        mapped[1, pl.ds(first + 8, 8)] = total

    apply(grown, False, put_mapped)
    exchange(mapped, 1)

    def put_back(first, total):
        back[pl.ds(first, 8)] = total

    apply(mapped, True, put_back)


def regular(volume, kernel):
    rows, columns = volume.shape[1:]
    count_y, count_z = (lax.axis_size("gy"), lax.axis_size("gz"))
    field = jax.ShapeDtypeStruct((3, rows + 16, columns), jnp.float32)

    def body(*refs):
        regular_kernel(count_y, count_z, *refs)

    back, grown, mapped = pl.pallas_call(
        body,
        out_shape=(jax.ShapeDtypeStruct((rows, columns), jnp.float32), field, field),
        in_specs=[SMEM, VMEM],
        out_specs=(VMEM, VMEM, VMEM),
        scratch_shapes=[
            pltpu.VMEM((3, rows + 16, columns), jnp.float32),
            pltpu.SemaphoreType.DMA((2, 8)),
            pltpu.SemaphoreType.DMA((2, 8)),
        ],
        cost_estimate=pl.CostEstimate(flops=120 * rows * columns, bytes_accessed=20 * rows * columns, transcendentals=0),
        compiler_params=pltpu.CompilerParams(collective_id=0, has_side_effects=True),
        name="regular",
    )(kernel.reshape(27), volume[0])
    return (back[None], grown, mapped)


def total_kernel(count_y, count_z, value, out, column, row, across, send, receive):
    y, z = (lax.axis_index("gy"), lax.axis_index("gz"))
    along_y = [(lax.rem(y + k, count_y), z) for k in range(1, count_y)]
    along_z = [(y, lax.rem(z + k, count_z)) for k in range(1, count_z)]
    barrier = pltpu.get_barrier_semaphore()
    for place in along_y + along_z:
        pl.semaphore_signal(barrier, inc=1, device_id=place, device_id_type=MESH)
    pl.semaphore_wait(barrier, count_y + count_z - 2)

    def gather(source, slots, places, base):
        copies = []
        for k, place in enumerate(places):
            copies.append(
                pltpu.make_async_remote_copy(
                    src_ref=source,
                    dst_ref=slots.at[k],
                    send_sem=send.at[base + k],
                    recv_sem=receive.at[base + k],
                    device_id=place,
                    device_id_type=MESH,
                )
            )
            copies[-1].start()
        for item in copies:
            item.wait()

    def ordered(own, slots, index, count):
        total = jnp.zeros_like(own)
        for j in range(count):
            term = own
            for k in range(1, count):
                term = jnp.where(lax.rem(index - j + count, count) == k, slots[k - 1], term)
            total = total + term
        return total

    gather(value, column, along_y, 0)
    across[...] = ordered(value[...], column, y, count_y)
    gather(across, row, along_z, count_y - 1)
    out[...] = ordered(across[...], row, z, count_z)


def total(values, collective):
    count_y, count_z = (lax.axis_size("gy"), lax.axis_size("gz"))
    count = values.shape[0]

    def body(*refs):
        total_kernel(count_y, count_z, *refs)

    block = jnp.broadcast_to(jnp.pad(values, (0, 128 - count))[None], (8, 128))
    copies = count_y + count_z - 2
    summed = pl.pallas_call(
        body,
        out_shape=jax.ShapeDtypeStruct((8, 128), jnp.float32),
        in_specs=[VMEM],
        out_specs=VMEM,
        scratch_shapes=[
            pltpu.VMEM((count_y - 1, 8, 128), jnp.float32),
            pltpu.VMEM((count_z - 1, 8, 128), jnp.float32),
            pltpu.VMEM((8, 128), jnp.float32),
            pltpu.SemaphoreType.DMA((copies,)),
            pltpu.SemaphoreType.DMA((copies,)),
        ],
        compiler_params=pltpu.CompilerParams(collective_id=collective, has_side_effects=True),
        name="total",
    )(block)
    return summed[0, :count]


def correlate_kernel(scalars, grown_0, grown_1, grown_2, grown_up, mapped_0, mapped_1, mapped_2, mapped_up, out):
    rows = grown_0.shape[1] - 16
    columns = grown_0.shape[2]
    c_up, c_zero, c_one, c_two, d_zero, d_one, s_zero, s_grad, s_direction = (scalars[k] for k in range(9))
    out[...] = jnp.zeros_like(out)

    @pl.loop(0, rows // 8)
    def _(step):
        first = pl.multiple_of(step * 8, 8)
        here = pl.ds(first + 8, 8)
        zero, one = (mapped_0[1, here], mapped_1[1, here])
        grad = c_up * mapped_up[1, here] + c_zero * zero + c_one * one + c_two * mapped_2[1, here]
        values = (
            s_zero * zero + s_grad * grad,
            s_grad * zero,
            s_direction * (d_zero * zero + d_one * one),
        )
        turned = [[moved(value, c - 1) for value in values] for c in range(3)]
        for a in range(3):
            around = pl.ds(first, 24)
            full_0, full_1 = (grown_0[a, around], grown_1[a, around])
            full_grad = c_up * grown_up[a, around] + c_zero * full_0 + c_one * full_1 + c_two * grown_2[a, around]
            full_direction = d_zero * full_0 + d_one * full_1
            for b in range(3):
                fields = [item[7 + b : 15 + b] for item in (full_0, full_grad, full_direction)]
                for c in range(3):
                    product = turned[c][0] * fields[0] + turned[c][1] * fields[1] + turned[c][2] * fields[2]
                    folded = product[:, :128]
                    for part in range(1, columns // 128):
                        folded = folded + product[:, 128 * part : 128 * part + 128]
                    out[9 * a + 3 * b + c] += folded


def correlate(scalars, *fields):
    return pl.pallas_call(
        correlate_kernel,
        out_shape=jax.ShapeDtypeStruct((27, 8, 128), jnp.float32),
        in_specs=[SMEM] + [VMEM] * 8,
        out_specs=VMEM,
        cost_estimate=pl.CostEstimate(flops=40000000, bytes_accessed=8000000, transcendentals=0),
        name="correlate",
    )(scalars, *fields).sum((1, 2))


def contract(form, left, right):
    return jnp.einsum(form, left, right, precision=lax.Precision.HIGH)


def wave_tables(length, groups):
    half = length // 2
    bins = half // groups
    pair = groups // 2
    shape = (half, pair, 2, bins)
    place = lax.broadcasted_iota(jnp.int32, shape, 0)
    part = lax.broadcasted_iota(jnp.int32, shape, 2)
    slot = lax.broadcasted_iota(jnp.int32, shape, 1) * bins + lax.broadcasted_iota(jnp.int32, shape, 3)
    tables = []
    for odd in range(2):
        frequency = 2 * slot + odd
        steps = place * frequency + part * (length // 4)
        if not odd:
            steps = jnp.where((slot == 0) & (part == 1), place * half, steps)
        angle = (steps % length).astype(jnp.float32) * (2.0 * math.pi / length)
        tables.append(jnp.cos(angle).reshape(half, pair, 2 * bins))
    return tables


def combine(raw, on_row, on_lane):
    even, odd = raw
    a, b, c, d = (
        jnp.concatenate([piece[:, part, :, :, side] for piece in (even, odd)], 0)
        for part, side in ((0, 0), (0, 1), (1, 0), (1, 1))
    )
    special = on_row | on_lane
    plus_real = jnp.where(special, a, a - d)
    plus_imaginary = jnp.where(on_row, b, jnp.where(on_lane, c, b + c))
    minus_real = jnp.where(on_row, c, jnp.where(on_lane, b, a + d))
    minus_imaginary = jnp.where(special, d, b - c)
    return (jnp.stack([plus_real, minus_real]), jnp.stack([plus_imaginary, minus_imaginary]))


def separate(spectrum, on_row, on_lane):
    (plus_real, minus_real), (plus_imaginary, minus_imaginary) = spectrum
    special = on_row | on_lane
    a = jnp.where(special, plus_real, plus_real + minus_real)
    d = jnp.where(special, minus_imaginary, minus_real - plus_real)
    b = jnp.where(on_row, plus_imaginary, jnp.where(on_lane, minus_real, plus_imaginary + minus_imaginary))
    c = jnp.where(on_row, minus_real, jnp.where(on_lane, plus_imaginary, plus_imaginary - minus_imaginary))
    scale = jnp.where(on_row & on_lane, 1.0, 2.0)
    a, b, c, d = (value * scale for value in (a, b, c, d))
    whole = jnp.stack([jnp.stack([a, b], 3), jnp.stack([c, d], 3)], 1)
    pair = whole.shape[0] // 2
    return (whole[:pair], whole[pair:])


def times(left, right, corner, conjugate=False):
    (a, b), (c, d) = (left, right)
    cross = b * d
    sign = -1.0 if conjugate else 1.0
    real = jnp.where(corner, a * c, a * c - sign * cross)
    imaginary = jnp.where(corner, cross, sign * a * d + b * c)
    return (real, imaginary)


def linear(*terms):
    total_real = total_imaginary = 0.0
    for scale, (real, imaginary) in terms:
        scale_real, scale_imaginary = scale if isinstance(scale, tuple) else (scale, scale)
        total_real = total_real + scale_real * real
        total_imaginary = total_imaginary + scale_imaginary * imaginary
    return (total_real, total_imaginary)


def local(measured, point_spread, stencil_weights, upstream):
    planes, row_count, columns = measured.shape
    groups = lax.axis_size("gy")
    rows = row_count * groups
    cells = planes * rows * columns * lax.axis_size("gz")
    bins = columns // 2 // groups
    even_x, odd_x = wave_tables(columns, groups)
    even_y, odd_y = (even_x, odd_x) if rows == columns else wave_tables(rows, groups)
    y_bins = rows // 2 // groups
    spectral = (groups, y_bins, 1, bins)
    on_row = (lax.broadcasted_iota(jnp.int32, spectral, 0) == 0) & (
        lax.broadcasted_iota(jnp.int32, spectral, 1) == 0
    )
    on_lane = (lax.broadcasted_iota(jnp.int32, spectral, 3) == 0) & (lax.axis_index("gy") == 0)
    corner = on_row & on_lane

    def forward(volumes):
        count = volumes.shape[0]
        low, high = (volumes[:, :, : columns // 2], volumes[:, :, columns // 2 :])
        sent = jnp.concatenate(
            [contract("vrj,jdl->drvl", low + high, even_x), contract("vrj,jdl->drvl", low - high, odd_x)], 0
        )
        arrived = lax.all_to_all(
            sent.reshape(groups, row_count, count * 2 * bins), "gy", split_axis=0, concat_axis=0, tiled=True
        )
        arrived = arrived.reshape(rows, count * 2 * bins)
        low, high = (arrived[: rows // 2], arrived[rows // 2 :])
        raw = [
            contract("jds,jl->dsl", table, value).reshape(groups // 2, 2, y_bins, count, 2, bins)
            for table, value in ((even_y, low + high), (odd_y, low - high))
        ]
        return combine(raw, on_row, on_lane)

    def inverse(spectrum):
        count = spectrum[0].shape[3]
        pieces = separate(spectrum, on_row, on_lane)
        one, two = (
            contract("jds,dsl->jl", table, piece.reshape(groups // 2, 2 * y_bins, count * 2 * bins))
            for table, piece in ((even_y, pieces[0]), (odd_y, pieces[1]))
        )
        sent = jnp.concatenate([one + two, one - two], 0).reshape(groups, row_count, count * 2 * bins)
        arrived = lax.all_to_all(sent, "gy", split_axis=0, concat_axis=0, tiled=True)
        arrived = arrived.reshape(groups, row_count, count, 2 * bins)
        one = contract("drvl,jdl->vrj", arrived[: groups // 2], even_x)
        two = contract("drvl,jdl->vrj", arrived[groups // 2 :], odd_x)
        return jnp.concatenate([one + two, one - two], 2) / float(rows * columns)

    def pick(spectrum, start, count):
        return tuple(lax.slice_in_dim(part, start, start + count, axis=3) for part in spectrum)

    def join(*spectra):
        return tuple(jnp.concatenate(parts, 3) for parts in zip(*spectra))

    spectra = forward(jnp.concatenate([point_spread[None], measured], 0))
    transfer = pick(spectra, 0, 1)
    squares = (transfer[0] ** 2, transfer[1] ** 2)
    gain = (
        jnp.where(corner, squares[0], squares[0] + squares[1]),
        jnp.where(corner, squares[1], squares[0] + squares[1]),
    )
    spectrum_0 = times(pick(spectra, 1, planes), transfer, corner, True)
    blurred_0 = linear((gain, spectrum_0))
    pair = inverse(join(spectrum_0, blurred_0))
    vector_0 = pair[:planes]
    back_0, grown_0, mapped_0 = regular(vector_0, stencil_weights)
    back_up, grown_up, mapped_up = regular(upstream, stencil_weights)
    vector_1 = pair[planes:] + back_0
    spectrum_1 = linear((1.0, blurred_0), (1.0, forward(back_0)))
    blurred_1 = linear((gain, spectrum_1))
    early = forward(jnp.concatenate([upstream, back_up], 0))
    back_1, grown_1, mapped_1 = regular(vector_1, stencil_weights)
    vector_2 = inverse(blurred_1) + back_1
    norm_0, curve_0, image_0, up_0, up_1 = total(
        jnp.stack(
            [
                jnp.sum(vector_0 * vector_0),
                jnp.sum(vector_0 * vector_1),
                jnp.sum(vector_1 * vector_1),
                jnp.sum(upstream * vector_0),
                jnp.sum(upstream * vector_1),
            ]
        ),
        1,
    )
    step_0 = norm_0 / curve_0
    residual = vector_0 - step_0 * vector_1
    residual_image = vector_1 - step_0 * vector_2
    norm_1, cross, inner, up_residual, image_cross = total(
        jnp.stack(
            [
                jnp.sum(residual * residual),
                jnp.sum(residual * vector_1),
                jnp.sum(residual * residual_image),
                jnp.sum(upstream * residual),
                jnp.sum(residual_image * vector_1),
            ]
        ),
        2,
    )
    back_2, grown_2, mapped_2 = regular(vector_2, stencil_weights)
    late = forward(jnp.concatenate([back_1, back_2], 0))
    ratio = norm_1 / norm_0
    curve_1 = inner + 2.0 * ratio * cross + ratio * ratio * curve_0
    step_1 = norm_1 / curve_1
    grad_step_1 = up_residual + ratio * up_0
    grad_curve_1 = -grad_step_1 * step_1 / curve_1
    grad_ratio = step_1 * up_0 + 2.0 * grad_curve_1 * (cross + ratio * curve_0)
    known_image = step_1 * up_1 + 2.0 * grad_curve_1 * (image_cross + ratio * image_0)
    grad_norm = grad_step_1 / curve_1 + grad_ratio / norm_0
    grad_step_0 = up_0 - known_image - 2.0 * grad_norm * cross
    grad_curve_0 = -grad_step_0 * step_0 / curve_0
    grad_norm_0 = -grad_ratio * ratio / norm_0 + grad_step_0 / curve_0

    spectrum_2 = linear((1.0, linear((gain, spectrum_1))), (1.0, pick(late, 0, planes)))
    spectrum_up = pick(early, 0, planes)
    residual_terms = ((1.0, spectrum_0), (-step_0, spectrum_1))
    direction_image = linear((1.0 + ratio, spectrum_1), (-step_0, spectrum_2))
    grad_direction = linear((step_1, spectrum_up), (2.0 * grad_curve_1, direction_image))
    grad_residual = linear((1.0, grad_direction), (2.0 * grad_norm, linear(*residual_terms)))
    grad_back = linear(
        (step_1, pick(early, planes, planes)),
        (2.0 * grad_curve_1 * (1.0 + ratio) - 2.0 * grad_norm * step_0, pick(late, 0, planes)),
        (-2.0 * grad_curve_1 * step_0, pick(late, planes, planes)),
        (2.0 * grad_norm, linear((1.0, spectrum_1), (-1.0, blurred_0))),
    )
    grad_right = linear(
        (step_0, spectrum_up),
        (ratio, grad_direction),
        (2.0 * grad_curve_0, spectrum_1),
        (2.0 * grad_norm_0, spectrum_0),
        (1.0, grad_residual),
        (-step_0, linear((gain, grad_residual), (1.0, grad_back))),
    )
    grad_measured = inverse(times(grad_right, transfer, corner))

    terms = correlate(
        jnp.stack(
            [
                step_1,
                2.0 * grad_norm,
                2.0 * grad_curve_1 * (1.0 + ratio) - 2.0 * grad_norm * step_0,
                -2.0 * grad_curve_1 * step_0,
                1.0 + ratio,
                -step_0,
                2.0 * grad_curve_0,
                -step_0,
                2.0 * grad_curve_1,
            ]
        ),
        grown_0, grown_1, grown_2, grown_up, mapped_0, mapped_1, mapped_2, mapped_up,
    )
    grad_stencil = total(terms, 3).reshape(3, 3, 3) / math.sqrt(cells)
    return (grad_measured, grad_stencil)


def spectral_fits(mesh_y, mesh_z, planes, row_count, columns):
    devices, rows, depth = (mesh_y * mesh_z, row_count * mesh_y, planes * mesh_z)
    if columns % (16 * devices) or row_count % 128 or rows % 512 or planes != 1 or mesh_z % 2:
        return False
    tiles = 4 * depth // 8 * (rows // 128)
    return depth < 8 and depth % 2 == 0 and mesh_y % 4 == 0 and tiles % (2 * mesh_z) == 0


def wave_rows(length):
    half, quarter = (length // 2, length // 4)
    place = np.arange(half)[None, :]
    tables = []
    for odd in range(2):
        frequency = 2 * np.arange(quarter)[:, None] + odd
        angle = (place * frequency % length) * (2.0 * np.pi / length)
        cosine, sine = (np.cos(angle), np.sin(angle))
        if not odd:
            sine[0] = np.cos(np.pi * place[0])
        tables += [cosine, sine]
    table = np.stack(tables)
    high = table.astype(jnp.bfloat16)
    low = (table - high.astype(np.float64)).astype(jnp.bfloat16)
    return (high, low)


def basis(length, place):
    half = length // 2
    frequency = np.concatenate([np.arange(0, half, 2), np.arange(1, half, 2)])
    angle = frequency * place % length * (2.0 * np.pi / length)
    cosine, sine = (np.cos(angle), np.sin(angle))
    sine[0] = np.cos(np.pi * place)
    return (cosine, sine)


def axis_values(length):
    cosine, sine = basis(length, 1)
    pure = sine.copy()
    pure[0] = 0.0
    other = cosine.copy()
    other[0] = -1.0
    weight = np.full(length // 2, 2.0)
    weight[0] = 1.0
    values = [(cosine, other), (pure, pure), basis(length, 0), basis(length, length - 1), (weight, weight)]
    for place in (0, 1, length - 2, length - 1):
        values.append(tuple(weight * part / length for part in basis(length, place)))
    return np.stack([np.stack(pair) for pair in values]).astype(np.float32)


COS, SIN, FIRST, LAST, WEIGHT, AT = range(6)


def split(value):
    high = value.astype(jnp.bfloat16)
    return (high, (value - high.astype(jnp.float32)).astype(jnp.bfloat16))


def product(left, right, contracting):
    numbers = (contracting, ((), ()))

    def one(a, b):
        return lax.dot_general(a, b, numbers, preferred_element_type=jnp.float32)

    return one(left[0], right[0]) + (one(left[0], right[1]) + one(left[1], right[0]))


class Spectral:
    def __init__(self, count_y, count_z, planes, row_count, columns):
        self.ny, self.nz = (count_y, count_z)
        self.nd = count_y * count_z
        self.depth = planes * count_z
        self.row_count = row_count
        self.rows = row_count * count_y
        self.columns = columns
        self.bins = columns // 2 // self.nd
        self.half = self.rows // 2
        self.steps = self.half // 128
        self.tiers = self.bins // 8
        self.lanes = self.rows // 128
        self.tiles = 4 * self.depth // 8 * self.lanes
        self.share = self.tiles // (2 * self.nz)

    def place_of(self, index):
        return (lax.rem(index, self.ny), lax.div(index, self.ny))

    def scratch(self):
        Z, bins, half, nd = (self.depth, self.bins, self.half, self.nd)
        packed = (Z, 2, bins, self.rows)
        field = (Z, 4, bins, half)
        edge = (2, Z, 2, bins, 128)
        F = jnp.float32
        D = pltpu.SemaphoreType.DMA
        others = nd - 1
        names = dict(
            sent_m=pltpu.VMEM((nd, 2, bins, 128 * (self.row_count // 128)), F),
            sent_u=pltpu.VMEM((nd, 2, bins, self.row_count), F),
            sent_p=pltpu.VMEM((self.ny, 2, bins, self.row_count), F),
            got_m=pltpu.VMEM(packed, F),
            got_u=pltpu.VMEM(packed, F),
            got_p=pltpu.VMEM((2, bins, self.rows), F),
            wave=pltpu.VMEM(packed, F),
            wave_p=pltpu.VMEM((2, bins, self.rows), F),
            v0=pltpu.VMEM(field, F),
            v1=pltpu.VMEM(field, F),
            v2=pltpu.VMEM(field, F),
            up=pltpu.VMEM(field, F),
            w3=pltpu.VMEM(field, F),
            m0=pltpu.VMEM(field, F),
            m1=pltpu.VMEM(field, F),
            mw=pltpu.VMEM(field, F),
            stencil=pltpu.VMEM((3, 2, 3, bins, half), F),
            blur=pltpu.VMEM((2, 3, bins, half), F),
            gain=pltpu.VMEM((2, 2, bins, half), F),
            across=pltpu.VMEM((9, 2, bins, 128), F),
            rows_v0=pltpu.VMEM(edge, F),
            rows_v1=pltpu.VMEM(edge, F),
            rows_v2=pltpu.VMEM(edge, F),
            rows_up=pltpu.VMEM(edge, F),
            rows_w3=pltpu.VMEM(edge, F),
            rows_m0=pltpu.VMEM(edge, F),
            rows_m1=pltpu.VMEM(edge, F),
            rows_mw=pltpu.VMEM(edge, F),
            edge_rows=pltpu.VMEM(edge, F),
            cols_v0=pltpu.VMEM((4, 8, self.rows), F),
            cols_v1=pltpu.VMEM((4, 8, self.rows), F),
            cols_v2=pltpu.VMEM((4, 8, self.rows), F),
            cols_up=pltpu.VMEM((4, 8, self.rows), F),
            cols_w3=pltpu.VMEM((4, 8, self.rows), F),
            cols_m0=pltpu.VMEM((2, 8, self.rows), F),
            cols_m1=pltpu.VMEM((2, 8, self.rows), F),
            cols_mw=pltpu.VMEM((2, 8, self.rows), F),
            edge_cols=pltpu.VMEM((2, 8, self.rows), F),
            part=pltpu.VMEM((3, 3, self.tiles, 8, 128), F),
            slots=pltpu.VMEM((3, 3, others, self.share, 8, 128), F),
            sums=pltpu.VMEM((3, 3, self.share, 8, 128), F),
            full=pltpu.VMEM((3, 3, self.tiles, 8, 128), F),
            acc=pltpu.VMEM((8, 8, 128), F),
            taps=pltpu.VMEM((27, 8, 128), F),
            tap_part=pltpu.VMEM((1, 128), F),
            tap_slots=pltpu.VMEM((nd, 1, 128), F),
            sent_o=pltpu.VMEM(packed, F),
            got_o=pltpu.VMEM((nd, 2, bins, self.row_count), F),
            send_big=D((3,)),
            recv_big=D((3,)),
            send_p=D,
            recv_p=D,
            send_part=D((2, 3)),
            recv_part=D((2, 3)),
            send_full=D((2, 3)),
            recv_full=D((2, 3)),
            send_tap=D,
            recv_tap=D,
        )
        return names


    def remote(self, source, target, send, receive, peer):
        return pltpu.make_async_remote_copy(
            src_ref=source, dst_ref=target, send_sem=send, recv_sem=receive,
            device_id=self.place_of(peer), device_id_type=MESH,
        )

    def arrived(self, shape, semaphore):
        self.remote(shape, shape, semaphore, semaphore, self.me).wait_recv()

    def row_lanes(self, y):
        return pl.ds(pl.multiple_of(y * self.row_count, 128), self.row_count)

    def spread_start(self, r, sent, got, lot, quarter=None):
        first, end = (1, self.nd)
        if quarter is not None:
            first, end = (max(1, quarter * self.nd // 4), (quarter + 1) * self.nd // 4)
        here = got.at[self.z, :, :, self.row_lanes(self.y)]

        @pl.loop(first, end)
        def _(k):
            peer = lax.rem(self.me + k, self.nd)
            self.remote(sent.at[peer], here, r.send_big.at[lot], r.recv_big.at[lot], peer).start()

        if not quarter:
            here[...] = sent[self.me]

    def spread_wait(self, r, sent, lot):
        others = sent.at[pl.ds(0, self.nd - 1)]
        self.arrived(others, r.recv_big.at[lot])
        self.arrived(others, r.send_big.at[lot])

    def point_start(self, r):
        here = r.got_p.at[:, :, self.row_lanes(self.y)]

        @pl.loop(1, self.ny)
        def _(k):
            peer = lax.rem(self.y + k, self.ny)
            self.remote(r.sent_p.at[peer], here, r.send_p, r.recv_p, self.z * self.ny + peer).start()

        here[...] = r.sent_p[self.y]

    def point_wait(self, r):
        others = r.sent_p.at[pl.ds(0, self.ny - 1)]
        self.arrived(others, r.recv_p)
        self.arrived(others, r.send_p)

    def return_start(self, r):
        @pl.loop(1, self.nd)
        def _(k):
            peer = lax.rem(self.me + k, self.nd)
            y, z = self.place_of(peer)
            self.remote(
                r.sent_o.at[z, :, :, self.row_lanes(y)], r.got_o.at[self.me], r.send_big.at[2], r.recv_big.at[2], peer
            ).start()

        r.got_o[self.me] = r.sent_o[self.z, :, :, self.row_lanes(self.y)]

    def owner(self, kind, number):
        if kind == 2:
            number = self.nz
        return lax.rem(number, self.nz) * self.ny + self.ny // 2 - 1 + 2 * lax.div(number, self.nz)

    def owned(self, kind):
        low = self.ny // 2 - 1
        if kind == 2:
            return self.me == self.owner(2, 0)
        return (self.y == low) | (self.y == low + 2)

    def owners(self, kind):
        return 1 if kind == 2 else 2 * self.nz

    def mine(self, kind):
        return 0 if kind == 2 else jnp.where(self.y == self.ny // 2 - 1, 0, self.nz) + self.z

    def width(self, kind):
        return 1 if kind == 2 else self.share

    def lot(self, ref, turn, kind, number, count=1):
        count = count * self.width(kind)
        return ref.at[turn, kind, pl.ds(number * self.width(kind), count)]

    def slot(self, r, turn, kind, first, count=1):
        return r.slots.at[turn, kind, pl.ds(first, count), pl.ds(0, self.width(kind))]

    def reduce_start(self, r, turn, kinds):
        for kind in kinds:
            send, receive = (r.send_part.at[turn % 2, kind], r.recv_part.at[turn % 2, kind])

            @pl.loop(0, self.owners(kind))
            def _(number):
                owner = self.owner(kind, number)

                @pl.when(owner != self.me)
                def _():
                    place = lax.rem(self.me - owner + self.nd, self.nd) - 1
                    self.remote(
                        self.lot(r.part, turn, kind, number), self.slot(r, turn, kind, place).at[0], send, receive, owner
                    ).start()

    def reduce_middle(self, r, turn, kinds):
        others = self.nd - 1
        for kind in kinds:
            send, receive = (r.send_full.at[turn % 2, kind], r.recv_full.at[turn % 2, kind])

            @pl.when(self.owned(kind))
            def _():
                number = self.mine(kind)
                self.arrived(self.slot(r, turn, kind, 0, others), r.recv_part.at[turn % 2, kind])
                lots = [self.lot(r.part, turn, kind, number)[...]]
                lots += [self.slot(r, turn, kind, k)[0] for k in range(others)]
                while len(lots) > 1:
                    lots = [lots[k] + lots[k + 1] for k in range(0, len(lots) - 1, 2)] + lots[len(lots) // 2 * 2 :]
                sums = r.sums.at[turn, kind, pl.ds(0, self.width(kind))]
                sums[...] = lots[0]

                @pl.loop(1, self.nd)
                def _(k):
                    self.remote(
                        sums, self.lot(r.full, turn, kind, number), send, receive, lax.rem(self.me + k, self.nd)
                    ).start()

                self.lot(r.full, turn, kind, number)[...] = lots[0]

    def reduce_end(self, r, turn, kinds):
        for kind in kinds:
            count = self.owners(kind)

            def finish(count):
                if count:
                    self.arrived(self.lot(r.full, turn, kind, 0, count), r.recv_full.at[turn % 2, kind])
                    self.arrived(self.lot(r.part, turn, kind, 0, count), r.send_part.at[turn % 2, kind])

            @pl.when(self.owned(kind))
            def _():
                finish(count - 1)
                self.arrived(self.slot(r, turn, kind, 0, self.nd - 1), r.send_full.at[turn % 2, kind])

            @pl.when(jnp.logical_not(self.owned(kind)))
            def _():
                finish(count)


    def row_spectra(self, r, source, sent):
        half = self.columns // 2
        low, high = (source[:, :half], source[:, half:])
        per = self.nd // 2
        for odd, value in enumerate((low + high, low - high)):
            value = split(value)
            for part in range(2):
                table = (r.tab_x[0][2 * odd + part], r.tab_x[1][2 * odd + part])
                sent[pl.ds(odd * per, per), part] = product(table, value, ((1,), (1,))).reshape(
                    per, self.bins, self.row_count
                )

    def point_spectra(self, r, source):
        half = self.columns // 2
        low, high = (source[:, :half], source[:, half:])
        odd = lax.div(2 * self.z, self.nz)
        sign = 1.0 - 2.0 * odd.astype(jnp.float32)
        value = split(low + sign * high)
        block = self.ny * self.bins
        start = pl.multiple_of(lax.rem(self.z, self.nz // 2) * block, block)
        for part in range(2):
            table = tuple(half_table[2 * odd + part, pl.ds(start, block)] for half_table in r.tab_x)
            r.sent_p[:, part] = product(table, value, ((1,), (1,))).reshape(self.ny, self.bins, self.row_count)

    def column_spectra(self, r, got, wave):
        count = math.prod(got.shape[:-1])
        value = got[...].reshape(count, self.rows)
        low, high = (value[:, : self.half], value[:, self.half :])
        quarter = self.half // 2
        for odd, value in enumerate((low + high, low - high)):
            value = split(value)
            for part in range(2):
                table = (r.tab_y[0][2 * odd + part], r.tab_y[1][2 * odd + part])
                wave[..., pl.ds(part * self.half + odd * quarter, quarter)] = product(
                    value, table, ((1,), (1,))
                ).reshape(got.shape[:-1] + (quarter,))

    def column_values(self, r, wave, target):
        count = math.prod(wave.shape[:-1])
        value = wave[...].reshape(count, self.rows)
        quarter = self.half // 2
        even, odd = (
            sum(
                product(
                    split(value[:, part * self.half + k * quarter : part * self.half + (k + 1) * quarter]),
                    (r.tab_y[0][2 * k + part], r.tab_y[1][2 * k + part]),
                    ((1,), (0,)),
                )
                for part in range(2)
            )
            for k in range(2)
        )
        shape = wave.shape[:-1] + (self.half,)
        target[..., : self.half] = (even + odd).reshape(shape)
        target[..., self.half :] = (even - odd).reshape(shape)

    def row_values(self, r, got, out):
        per = self.nd // 2
        sides = []
        for k in range(2):
            side = 0.0
            for part in range(2):
                value = got[pl.ds(k * per, per), part].reshape(per * self.bins, self.row_count)
                side = side + product(
                    split(value.T), (r.tab_x[0][2 * k + part], r.tab_x[1][2 * k + part]), ((1,), (0,))
                )
            sides.append(side)
        half = self.columns // 2
        out[0, :, :half] = sides[0] + sides[1]
        out[0, :, half:] = sides[0] - sides[1]


    def masks(self, tier, step):
        shape = (8, 128)
        row = (lax.broadcasted_iota(jnp.int32, shape, 0) == 0) & (self.me == 0)
        lane = lax.broadcasted_iota(jnp.int32, shape, 1) + 128 * step == 0
        if tier:
            row = row & False
        return (row, lane, row & lane, row | lane)

    def combine(self, masks, ac, as_, bc, bs):
        row, lane, corner, special = masks
        pr = jnp.where(special, ac, ac - bs)
        pi = jnp.where(corner, as_, jnp.where(row, -as_, jnp.where(lane, -bc, -(as_ + bc))))
        mr = jnp.where(row, bc, jnp.where(lane, as_, ac + bs))
        mi = jnp.where(corner, bs, jnp.where(special, -bs, as_ - bc))
        return [pr, pi, mr, mi]

    def separate(self, masks, field):
        row, lane, corner, special = masks
        pr, pi, mr, mi = field
        ac = jnp.where(special, pr, 0.5 * (pr + mr))
        as_ = jnp.where(corner, pi, jnp.where(row, -pi, jnp.where(lane, mr, 0.5 * (mi - pi))))
        bc = jnp.where(row, mr, jnp.where(lane, -pi, -0.5 * (pi + mi)))
        bs = jnp.where(corner, mi, jnp.where(special, -mi, 0.5 * (mr - pr)))
        return (ac, as_, bc, bs)

    def lane_slice(self, step, part=0):
        return pl.ds(pl.multiple_of(part * self.half + step * 128, 128), 128)

    def along(self, r, which, step, part):
        return r.along[which, :, self.lane_slice(step, part)]

    def beside(self, r, which, part, tier):
        return r.across[which, part, pl.ds(8 * tier, 8)]

    def load(self, field, z, tier, step):
        return [field[z, k, pl.ds(8 * tier, 8), self.lane_slice(step)] for k in range(4)]

    def keep(self, field, z, tier, step, values):
        for k in range(4):
            field[z, k, pl.ds(8 * tier, 8), self.lane_slice(step)] = values[k]

    def load_wave(self, wave, z, tier, step):
        return [
            wave[z, part, pl.ds(8 * tier, 8), self.lane_slice(step, side)]
            for part in range(2)
            for side in range(2)
        ]

    def times(self, factor, value, conjugate=False):
        out = []
        for side in range(2):
            real, other, cross = factor[side]
            a, b = (value[2 * side], value[2 * side + 1])
            if conjugate:
                out += [real * a + cross * b, other * b - cross * a]
            else:
                out += [real * a - cross * b, other * b + cross * a]
        return out

    def factor(self, array, tier, step):
        where = (pl.ds(8 * tier, 8), self.lane_slice(step))
        return [[array[(side, k) + where] for k in range(3)] for side in range(2)]

    def sweep(self, body):
        @pl.loop(0, self.steps)
        def _(step):
            columns = {}
            for tier in range(self.tiers):
                body(tier, step, self.masks(tier, step), columns)

    def frames(self, r, masks, tier, step, z, value, rows, columns=None):
        ac, as_, bc, bs = self.separate(masks, value)
        here = pl.ds(8 * tier, 8)
        for k, which in enumerate((AT, AT + 3)):
            c, s = (self.along(r, which, step, 0), self.along(r, which, step, 1))
            rows[k, z, 0, here] += ac * c + as_ * s
            rows[k, z, 1, here] += bc * c + bs * s
        if columns is None:
            return
        for x in range(4):
            a, b = (self.beside(r, AT + x, 0, tier), self.beside(r, AT + x, 1, tier))
            for side, (p, q) in enumerate(((ac, bc), (as_, bs))):
                term = a * p + b * q
                key = (x, z, side)
                columns[key] = term if key not in columns else columns[key] + term

    def put_columns(self, part, tier, step, columns):
        if tier < self.tiers - 1:
            return
        for (x, z, side), value in columns.items():
            index = x * self.depth + z
            tile = index // 8 * self.lanes + side * self.steps + step
            part[tile, pl.ds(index % 8, 1)] = jnp.sum(value, 0, keepdims=True)

    def clear(self, *refs):
        for ref in refs:
            ref[...] = jnp.zeros(ref.shape, jnp.float32)

    def settle(self, rows):
        for k in range(2):
            rows[k] = jnp.broadcast_to(jnp.sum(rows[k], -1, keepdims=True), rows.shape[1:])

    def unpack(self, full, cols):
        Z = self.depth
        cols[...] = jnp.zeros(cols.shape, jnp.float32)
        for x in range(4):
            first = x * Z
            for lane in range(self.lanes):
                cols[x, pl.ds(0, Z), pl.ds(lane * 128, 128)] = full[
                    first // 8 * self.lanes + lane, pl.ds(first % 8, Z)
                ]

    def shifted(self, value, by):
        if by == 0:
            return value
        value = pltpu.roll(value, 7 if by > 0 else 1, 0)
        sub = lax.broadcasted_iota(jnp.int32, value.shape, 0)
        return jnp.where(sub < self.depth, value, 0.0)

    def corners(self, r, col):
        out = []
        for which in (AT, AT + 3):
            weight = jnp.concatenate([r.along[which, :, :]], 0)
            out.append(jnp.broadcast_to(jnp.sum(col * weight, -1, keepdims=True), (8, 128)))
        return out

    def edges(self, r, w, rows, col_first, col_last, inner=None, mapped=None):
        Z = self.depth
        k_first, k_last = (self.corners(r, col_first[...]), self.corners(r, col_last[...]))
        total = lambda terms: sum(terms[1:], terms[0])
        q = {}
        for name, b, c, value in ((0, 0, 0, k_last[1]), (1, 0, 2, k_first[1]), (2, 2, 0, k_last[0]), (3, 2, 2, k_first[0])):
            q[name] = total([w(a, b, c) * self.shifted(value, a - 1) for a in range(3)])
        if inner is not None:
            near, far = inner
            k_near, k_far = (self.corners(r, near[...]), self.corners(r, far[...]))
            fix = []
            for (c0, v0), (c1, v1) in (((1, k_first), (2, k_near)), ((0, k_far), (1, k_last))):
                fix.append(
                    [
                        total(
                            [
                                w(a, b, c0) * self.shifted(v0[y], a - 1) + w(a, b, c1) * self.shifted(v1[y], a - 1)
                                for a in range(3)
                            ]
                        )
                        for b, y in ((0, 1), (2, 0))
                    ]
                )

        @pl.loop(0, self.steps)
        def _(step):
            c = [self.along(r, COS, step, part) for part in range(2)]
            s = self.along(r, SIN, step, 0)
            first = [self.along(r, FIRST, step, part) for part in range(2)]
            last = [self.along(r, LAST, step, part) for part in range(2)]

            def get(col):
                return [col[:, self.lane_slice(step, part)] for part in range(2)]

            def line(a, c_index, col):
                w0, w1, w2 = (w(a, b, c_index) for b in range(3))
                turn = (w2 - w0) * s
                return [
                    (w1 + (w0 + w2) * c[0]) * col[0] + turn * col[1],
                    (w1 + (w0 + w2) * c[1]) * col[1] - turn * col[0],
                ]

            def stacked(pieces):
                out = None
                for a in range(3):
                    for c_index, col in pieces:
                        term = [self.shifted(part, a - 1) for part in line(a, c_index, col)]
                        out = term if out is None else [p + t for p, t in zip(out, term)]
                return out

            f, l = (get(col_first), get(col_last))
            for k, (pieces, upper, lower) in enumerate((([(0, l)], q[0], q[2]), ([(2, f)], q[1], q[3]))):
                value = stacked(pieces)
                for part in range(2):
                    r.edge_cols[k, :, self.lane_slice(step, part)] = (
                        value[part] - upper * first[part] - lower * last[part]
                    )
            if inner is not None:
                n, g = (get(near), get(far))
                for k, pieces in enumerate(([(1, f), (2, n)], [(0, g), (1, l)])):
                    value = stacked(pieces)
                    for part in range(2):
                        mapped[k, :, self.lane_slice(step, part)] = (
                            value[part] - fix[k][0] * first[part] - fix[k][1] * last[part]
                        )

        for tier in range(self.tiers):
            here = pl.ds(8 * tier, 8)
            c = [self.beside(r, COS, part, tier) for part in range(2)]
            s = self.beside(r, SIN, 0, tier)
            for k, (b, source) in enumerate(((0, 1), (2, 0))):
                for z in range(Z):
                    out = None
                    for a in range(3):
                        if not 0 <= z + a - 1 < Z:
                            continue
                        w0, w1, w2 = (w(a, b, c_index) for c_index in range(3))
                        turn = (w2 - w0) * s
                        p, t = (rows[source, z + a - 1, part, here] for part in range(2))
                        term = [
                            (w1 + (w0 + w2) * c[0]) * p + turn * t,
                            (w1 + (w0 + w2) * c[1]) * t - turn * p,
                        ]
                        out = term if out is None else [x + v for x, v in zip(out, term)]
                    for part in range(2):
                        r.edge_rows[k, z, part, here] = out[part]

    def edge_field(self, r, masks, tier, step, z):
        here = pl.ds(8 * tier, 8)
        out = []
        for part in range(2):
            e0, e1 = (r.edge_rows[k, z, part, here] for k in range(2))
            x0, x1 = (self.beside(r, which, part, tier) for which in (FIRST, LAST))
            for side in range(2):
                y0, y1 = (self.along(r, which, step, side) for which in (FIRST, LAST))
                c0, c1 = (r.edge_cols[k, pl.ds(z, 1), self.lane_slice(step, side)] for k in range(2))
                out.append(e0 * y0 + e1 * y1 + x0 * c0 + x1 * c1)
        return self.combine(masks, *out)

    def stencil_field(self, r, masks, tier, step, field, flip):
        Z = self.depth
        value = [self.load(field, z, tier, step) for z in range(Z)]
        out = [[-e for e in self.edge_field(r, masks, tier, step, z)] for z in range(Z)]
        for a in range(3):
            where = (pl.ds(8 * tier, 8), self.lane_slice(step))
            factor = [[r.stencil[(a, side, k) + where] for k in range(3)] for side in range(2)]
            for z in range(Z):
                other = z + (1 - a if flip else a - 1)
                if 0 <= other < Z:
                    term = self.times(factor, value[other], flip)
                    out[z] = [o + t for o, t in zip(out[z], term)]
        return out

    def build_stencil(self, r, w):
        def body(tier, step, masks, columns):
            row, lane, corner, special = masks
            here = pl.ds(8 * tier, 8)
            sx = self.beside(r, SIN, 0, tier)
            ys = self.along(r, SIN, step, 0)
            for side in range(2):
                cx = self.beside(r, COS, side, tier)
                cy = self.along(r, COS, step, 0)
                sy = jnp.broadcast_to(ys, (8, 128))
                cy = jnp.broadcast_to(cy, (8, 128))
                if side:
                    cy = jnp.where(row, cy, self.along(r, COS, step, 1))
                    sy = jnp.where(row, sy, -sy)
                for a in range(3):
                    real, imag = ([], [])
                    for b in range(3):
                        real.append(w(a, b, 1) + (w(a, b, 0) + w(a, b, 2)) * cx)
                        imag.append((w(a, b, 2) - w(a, b, 0)) * sx)
                    value = real[1] + (real[0] + real[2]) * cy - (imag[2] - imag[0]) * sy
                    cross = imag[1] + (imag[0] + imag[2]) * cy + (real[2] - real[0]) * sy
                    other = jnp.where(corner, real[1] - (real[0] + real[2]), value)
                    for k, item in enumerate((value, other, cross)):
                        r.stencil[a, side, k, here, self.lane_slice(step)] = item

        self.sweep(body)

    def build_blur(self, r):
        def body(tier, step, masks, columns):
            row, lane, corner, special = masks
            here = pl.ds(8 * tier, 8)
            wave = [
                r.wave_p[part, here, self.lane_slice(step, side)] for part in range(2) for side in range(2)
            ]
            value = self.combine(masks, wave[0], wave[1], wave[2], wave[3])
            for side in range(2):
                real, imag = (value[2 * side], value[2 * side + 1])
                other = jnp.where(corner, imag, real)
                cross = jnp.where(corner, 0.0, imag)
                for k, item in enumerate((real, other, cross)):
                    r.blur[side, k, here, self.lane_slice(step)] = item
                square = cross * cross
                r.gain[side, 0, here, self.lane_slice(step)] = real * real + square
                r.gain[side, 1, here, self.lane_slice(step)] = other * other + square

        self.sweep(body)

    def gained(self, r, tier, step, value):
        where = (pl.ds(8 * tier, 8), self.lane_slice(step))
        return [r.gain[(k // 2, k % 2) + where] * value[k] for k in range(4)]

    def dot(self, masks, left, right):
        corner = masks[2]
        total = sum(a * b for a, b in zip(left, right))
        return jnp.where(corner, 0.5 * total, total)


    def stencil_twice(self, r, w, field, rows, cols, mapped, rows_m, cols_m, finish, after=None):
        def flipped(a, b, c):
            return w(2 - a, 2 - b, 2 - c)

        self.edges(r, w, rows, cols.at[0], cols.at[3], (cols.at[1], cols.at[2]), cols_m)
        self.clear(rows_m)

        def forward(tier, step, masks, columns):
            out = self.stencil_field(r, masks, tier, step, field, False)
            for z in range(self.depth):
                self.keep(mapped, z, tier, step, out[z])
                self.frames(r, masks, tier, step, z, out[z], rows_m)

        self.sweep(forward)
        self.settle(rows_m)
        self.edges(r, flipped, rows_m, cols_m.at[0], cols_m.at[1])

        def back(tier, step, masks, columns):
            finish(tier, step, masks, columns, self.stencil_field(r, masks, tier, step, mapped, True))

        self.sweep(back)

    def scalars_out(self, r, turn, count):
        for k in range(count):
            r.part[turn, 2, 0, pl.ds(k, 1)] = jnp.sum(r.acc[k], 0, keepdims=True)
        for k in range(count, 8):
            r.part[turn, 2, 0, pl.ds(k, 1)] = jnp.zeros((1, 128), jnp.float32)

    def scalars_in(self, r, turn, count):
        value = jnp.sum(r.full[turn, 2, 0], -1, keepdims=True)
        return [jnp.broadcast_to(value[k : k + 1], (8, 128)) for k in range(count)]

    def run(self, r):
        Z = self.depth
        self.y, self.z = (lax.axis_index("gy"), lax.axis_index("gz"))
        self.me = self.z * self.ny + self.y

        def w(a, b, c):
            return r.weights[a, b, c]

        barrier = pltpu.get_barrier_semaphore()

        @pl.loop(1, self.nd)
        def _(k):
            pl.semaphore_signal(
                barrier, inc=1, device_id=self.place_of(lax.rem(self.me + k, self.nd)), device_id_type=MESH
            )

        def load(name):
            far = getattr(r, "far_" + name)
            far = far.at[self.me] if name == "frequencies" else far
            return pltpu.make_async_copy(far, getattr(r, name), r.loaded.at[r.inputs.index(name)])

        tables = [name for name in r.inputs if name.startswith("wave")]
        order = ["frequencies", "weights", "along", "point_spread"] + tables + ["measured", "upstream"]
        for name in order:
            load(name).start()
        load("frequencies").wait()
        for which in range(9):
            for part in range(2):
                r.across[which, part] = jnp.broadcast_to(
                    r.frequencies[part * self.bins : (part + 1) * self.bins, which : which + 1], (self.bins, 128)
                )
        load("along").wait()
        load("weights").wait()
        self.build_stencil(r, w)
        load("point_spread").wait()
        for name in tables:
            load(name).wait()
        self.point_spectra(r, r.point_spread[...])
        load("measured").wait()
        self.row_spectra(r, r.measured[0], r.sent_m)
        pl.semaphore_wait(barrier, self.nd - 1)
        self.point_start(r)
        self.spread_start(r, r.sent_m, r.got_m, 0)
        load("upstream").wait()
        self.row_spectra(r, r.upstream[0], r.sent_u)
        self.clear(r.rows_v0, r.rows_v1, r.rows_v2, r.rows_up, r.acc, r.taps)

        self.point_wait(r)
        self.column_spectra(r, r.got_p, r.wave_p)
        self.build_blur(r)
        self.spread_wait(r, r.sent_m, 0)
        self.spread_start(r, r.sent_u, r.got_u, 1, 0)
        self.column_spectra(r, r.got_m, r.wave)

        def start(tier, step, masks, columns):
            factor = self.factor(r.blur, tier, step)
            for z in range(Z):
                value = self.combine(masks, *self.load_wave(r.wave, z, tier, step))
                value = self.times(factor, value, True)
                self.keep(r.v0, z, tier, step, value)
                self.frames(r, masks, tier, step, z, value, r.rows_v0, columns)
            self.put_columns(r.part.at[0, 0], tier, step, columns)

        self.sweep(start)
        self.reduce_start(r, 0, [0])
        self.spread_start(r, r.sent_u, r.got_u, 1, 1)
        self.settle(r.rows_v0)
        self.reduce_middle(r, 0, [0])
        self.reduce_end(r, 0, [0])
        self.spread_start(r, r.sent_u, r.got_u, 1, 2)
        self.unpack(r.full.at[0, 0], r.cols_v0)

        def first(tier, step, masks, columns, back):
            for z in range(Z):
                before = self.load(r.v0, z, tier, step)
                value = [g + b for g, b in zip(self.gained(r, tier, step, before), back[z])]
                self.keep(r.v1, z, tier, step, value)
                self.frames(r, masks, tier, step, z, value, r.rows_v1, columns)
                r.acc[0] += self.dot(masks, before, before)
                r.acc[1] += self.dot(masks, before, value)
                r.acc[2] += self.dot(masks, value, value)
            self.put_columns(r.part.at[1, 0], tier, step, columns)

        self.stencil_twice(r, w, r.v0, r.rows_v0, r.cols_v0, r.m0, r.rows_m0, r.cols_m0, first)
        self.scalars_out(r, 1, 3)
        self.reduce_start(r, 1, [0, 2])
        self.spread_start(r, r.sent_u, r.got_u, 1, 3)
        self.settle(r.rows_v1)
        self.reduce_middle(r, 1, [0, 2])
        self.spread_wait(r, r.sent_u, 1)
        self.column_spectra(r, r.got_u, r.wave)

        def upper(tier, step, masks, columns):
            for z in range(Z):
                value = self.combine(masks, *self.load_wave(r.wave, z, tier, step))
                self.keep(r.up, z, tier, step, value)
                self.frames(r, masks, tier, step, z, value, r.rows_up, columns)
            self.put_columns(r.part.at[2, 1], tier, step, columns)

        self.sweep(upper)
        self.settle(r.rows_up)
        self.clear(r.acc)
        self.reduce_end(r, 1, [0, 2])
        self.reduce_start(r, 2, [1])
        self.unpack(r.full.at[1, 0], r.cols_v1)
        norm_0, curve_0, image_0 = self.scalars_in(r, 1, 3)
        step_0 = norm_0 / curve_0

        def second(tier, step, masks, columns, back):
            for z in range(Z):
                before, value = (self.load(f, z, tier, step) for f in (r.v0, r.v1))
                up = self.load(r.up, z, tier, step)
                after = [g + b for g, b in zip(self.gained(r, tier, step, value), back[z])]
                self.keep(r.v2, z, tier, step, after)
                self.frames(r, masks, tier, step, z, after, r.rows_v2, columns)
                residual = [p - step_0 * q for p, q in zip(before, value)]
                image = [p - step_0 * q for p, q in zip(value, after)]
                for k, (p, q) in enumerate(
                    ((residual, residual), (residual, value), (residual, image), (image, value), (up, residual), (up, before), (up, value))
                ):
                    r.acc[k] += self.dot(masks, p, q)
            self.put_columns(r.part.at[2, 0], tier, step, columns)

        self.stencil_twice(r, w, r.v1, r.rows_v1, r.cols_v1, r.m1, r.rows_m1, r.cols_m1, second)
        self.scalars_out(r, 2, 7)
        self.reduce_start(r, 2, [0, 2])
        self.settle(r.rows_v2)
        self.reduce_middle(r, 2, [1, 0, 2])
        self.reduce_end(r, 2, [1, 0, 2])
        self.unpack(r.full.at[2, 0], r.cols_v2)
        self.unpack(r.full.at[2, 1], r.cols_up)

        norm_1, cross, inner, image_cross, up_residual, up_0, up_1 = self.scalars_in(r, 2, 7)
        ratio = norm_1 / norm_0
        curve_1 = inner + 2.0 * ratio * cross + ratio * ratio * curve_0
        step_1 = norm_1 / curve_1
        grad_step_1 = up_residual + ratio * up_0
        grad_curve_1 = -grad_step_1 * step_1 / curve_1
        grad_ratio = step_1 * up_0 + 2.0 * grad_curve_1 * (cross + ratio * curve_0)
        grad_norm = grad_step_1 / curve_1 + grad_ratio / norm_0
        grad_step_0 = (
            up_0 - step_1 * up_1 - 2.0 * grad_curve_1 * (image_cross + ratio * image_0) - 2.0 * grad_norm * cross
        )
        more = 1.0 + ratio
        g0 = grad_norm - grad_ratio * ratio / norm_0 + grad_step_0 / curve_0
        g1 = grad_curve_1 * more * more - 2.0 * grad_norm * step_0 - grad_step_0 * step_0 / curve_0
        g2 = -2.0 * grad_curve_1 * step_0 * more + grad_norm * step_0 * step_0
        g3 = grad_curve_1 * step_0 * step_0
        q0 = step_0 + step_1 * more
        q1 = -step_1 * step_0
        mix = (g1, 2.0 * g2, 2.0 * g3, q1)

        def mixed(*values):
            return mix[0] * values[0] + mix[1] * values[1] + mix[2] * values[2] + mix[3] * values[3]

        for x in range(4):

            @pl.loop(0, self.lanes)
            def _(lane):
                here = (x, slice(None), pl.ds(pl.multiple_of(lane * 128, 128), 128))
                r.cols_w3[here] = mixed(*(f[here] for f in (r.cols_v0, r.cols_v1, r.cols_v2, r.cols_up)))

        for k in range(2):
            for part in range(2):
                for tier in range(self.tiers):

                    @pl.loop(0, Z)
                    def _(z):
                        here = (k, z, part, pl.ds(8 * tier, 8))
                        r.rows_w3[here] = mixed(*(f[here] for f in (r.rows_v0, r.rows_v1, r.rows_v2, r.rows_up)))

        def blend(tier, step, masks, columns):
            for z in range(Z):
                values = [self.load(f, z, tier, step) for f in (r.v0, r.v1, r.v2, r.up)]
                self.keep(r.w3, z, tier, step, [mixed(*parts) for parts in zip(*values)])

        self.sweep(blend)
        scale = 1.0 / (self.rows * self.columns)

        def last(tier, step, masks, columns, back):
            factor = self.factor(r.blur, tier, step)
            here = pl.ds(8 * tier, 8)
            for z in range(Z):
                v0, v1, w3, up = (self.load(f, z, tier, step) for f in (r.v0, r.v1, r.w3, r.up))
                value = [
                    b + d + 2.0 * g0 * p + g1 * q + q0 * u
                    for b, d, p, q, u in zip(back[z], self.gained(r, tier, step, w3), v0, v1, up)
                ]
                value = self.separate(masks, self.times(factor, value))
                for part in range(2):
                    heavy = scale * self.beside(r, WEIGHT, part, tier)
                    for side in range(2):
                        r.wave[z, part, here, self.lane_slice(step, side)] = (
                            value[2 * part + side] * heavy * self.along(r, WEIGHT, step, side)
                        )

        self.stencil_twice(r, w, r.w3, r.rows_w3, r.cols_w3, r.mw, r.rows_mw, r.cols_mw, last)
        self.column_values(r, r.wave, r.sent_o)

        self.return_start(r)
        self.tap_sums(r, 2.0 * g3)

        @pl.loop(1, self.nd)
        def _(k):
            peer = lax.rem(self.me + k, self.nd)
            self.remote(r.tap_part, r.tap_slots.at[self.me], r.send_tap, r.recv_tap, peer).start()

        r.tap_slots[self.me] = r.tap_part[...]
        others = pl.ds(0, self.nd - 1)
        self.arrived(r.got_o.at[others], r.recv_big.at[2])
        self.row_values(r, r.got_o, r.out)
        self.arrived(r.got_o.at[others], r.send_big.at[2])
        self.arrived(r.tap_slots.at[others], r.recv_tap)
        self.arrived(r.tap_slots.at[others], r.send_tap)
        lots = [r.tap_slots[k] for k in range(self.nd)]
        while len(lots) > 1:
            lots = [lots[k] + lots[k + 1] for k in range(0, len(lots) - 1, 2)] + lots[len(lots) // 2 * 2 :]
        line = jnp.broadcast_to(lots[0] / math.sqrt(self.depth * self.rows * self.columns), (8, 128))
        for a in range(3):
            for b in range(3):
                first = 9 * a + 3 * b
                turned = pltpu.roll(line, 128 - first, 1) if first else line
                r.tap_out[a, pl.ds(b, 1)] = turned[:1, :3]

    def tap_sums(self, r, weight):
        Z = self.depth
        pairs = ((r.v0, r.mw, None), (r.w3, r.m0, None), (r.v1, r.m1, weight))

        def body(tier, step, masks, columns):
            corner = masks[2]
            sx = self.beside(r, SIN, 0, tier)
            gamma = [[None, None, None, None] for a in range(3)]
            for left, right, scale in pairs:
                x = [self.load(left, z, tier, step) for z in range(Z)]
                if scale is not None:
                    x = [[scale * item for item in value] for value in x]
                for z in range(Z):
                    m = self.load(right, z, tier, step)
                    for a in range(3):
                        if not 0 <= z + a - 1 < Z:
                            continue
                        v = x[z + a - 1]
                        for side in range(2):
                            vr, vi, mr, mi = (v[2 * side], v[2 * side + 1], m[2 * side], m[2 * side + 1])
                            p, q = (vr * mr, vi * mi)
                            terms = (jnp.where(corner, 0.5 * (p + q), p + q), jnp.where(corner, 0.5 * (p - q), p + q), vi * mr - vr * mi)
                            old = gamma[a][side]
                            gamma[a][side] = terms if old is None else [o + t for o, t in zip(old, terms)]
            for a in range(3):
                sums = [0.0] * 9
                for side in range(2):
                    cx = self.beside(r, COS, side, tier)
                    cy = jnp.broadcast_to(self.along(r, COS, step, 0), (8, 128))
                    sy = jnp.broadcast_to(self.along(r, SIN, step, 0), (8, 128))
                    if side:
                        cy = jnp.where(masks[0], cy, self.along(r, COS, step, 1))
                        sy = jnp.where(masks[0], sy, -sy)
                    near, far, turn = gamma[a][side]
                    items = (
                        near, near * cx, far * cy, far * cy * cx, near * sx * sy,
                        turn * sx, turn * sy, turn * cx * sy, turn * sx * cy,
                    )
                    sums = [s + item for s, item in zip(sums, items)]
                for k in range(9):
                    r.taps[9 * a + k] += sums[k]

        self.sweep(body)

        sides = (
            (r.rows_v0, r.cols_v0, r.rows_mw, r.cols_mw, None),
            (r.rows_w3, r.cols_w3, r.rows_m0, r.cols_m0, None),
            (r.rows_v1, r.cols_v1, r.rows_m1, r.cols_m1, weight),
        )
        zero = jnp.zeros((8, 128), jnp.float32)
        by_row = [[[zero] * 3 for k in range(2)] for a in range(3)]
        by_col = [[[zero] * 3 for k in range(2)] for a in range(3)]
        by_corner = [[[zero] * 2 for k in range(2)] for a in range(3)]
        for rows_x, cols_x, rows_m, cols_m, scale in sides:
            extra = 1.0 if scale is None else scale
            for tier in range(self.tiers):
                here = pl.ds(8 * tier, 8)
                heavy = self.beside(r, WEIGHT, 0, tier) * extra
                ca, cb = (self.beside(r, COS, part, tier) for part in range(2))
                s = self.beside(r, SIN, 0, tier)
                for k in range(2):
                    for z in range(Z):
                        ma, mb = (rows_m[k, z, part, here] for part in range(2))
                        for a in range(3):
                            if not 0 <= z + a - 1 < Z:
                                continue
                            xa, xb = (rows_x[1 - k, z + a - 1, part, here] for part in range(2))
                            p, q = (heavy * xa * ma, heavy * xb * mb)
                            terms = (p + q, p * ca + q * cb, heavy * s * (xa * mb - xb * ma))
                            by_row[a][k] = [o + t for o, t in zip(by_row[a][k], terms)]
            for k in range(2):
                col_x, col_m = (cols_x.at[0 if k else 3], cols_m.at[k])
                for step in range(self.steps):
                    (xc, xs), (mc, ms) = (
                        [ref[:, pl.ds(part * self.half + 128 * step, 128)] * (extra if ref is col_x else 1.0) for part in range(2)]
                        for ref in (col_x, col_m)
                    )
                    heavy = self.along(r, WEIGHT, step, 0)
                    cc, cs = (self.along(r, COS, step, part) for part in range(2))
                    s = self.along(r, SIN, step, 0)
                    for a in range(3):
                        xc_a, xs_a = (self.shifted(item, a - 1) for item in (xc, xs))
                        p, q = (heavy * xc_a * mc, heavy * xs_a * ms)
                        terms = (p + q, p * cc + q * cs, heavy * s * (xc_a * ms - xs_a * mc))
                        by_col[a][k] = [o + t for o, t in zip(by_col[a][k], terms)]
                at_x, at_m = (self.corners(r, ref[...]) for ref in (col_x, col_m))
                for a in range(3):
                    for edge in range(2):
                        term = extra * self.shifted(at_x[1 - edge], a - 1) * at_m[edge]
                        by_corner[a][edge][k] = by_corner[a][edge][k] + term

        lots = []
        for a in range(3):
            s = [r.taps[9 * a + k] for k in range(9)]
            for b in range(3):
                for c in range(3):
                    beta, gamma = (float(b - 1), float(c - 1))
                    if b == 1 and c == 1:
                        value = s[0]
                    elif b == 1:
                        value = s[1] - gamma * s[5]
                    elif c == 1:
                        value = s[2] - beta * s[6]
                    else:
                        value = s[3] - beta * gamma * s[4] - beta * s[7] - gamma * s[8]
                    value = value * (2.0 / (self.rows * self.columns))
                    if b != 1:
                        one, two, three = by_row[a][b // 2]
                        value = value - (one if c == 1 else two - gamma * three) * (1.0 / (128 * self.columns))
                    if c != 1:
                        one, two, three = by_col[a][c // 2]
                        value = value - (one if b == 1 else two - beta * three) * (1.0 / (self.rows * self.nd))
                    if b != 1 and c != 1:
                        value = value + by_corner[a][b // 2][c // 2] * (1.0 / (128 * self.nd))
                    lots.append(value)
        lane = lax.broadcasted_iota(jnp.int32, (1, 128), 1)
        line = jnp.zeros((1, 128), jnp.float32)
        for k, value in enumerate(lots):
            whole = jnp.sum(jnp.sum(value, 0, keepdims=True), -1, keepdims=True)
            line = jnp.where(lane == k, whole, line)
        r.tap_part[...] = line


class Refs:
    def __init__(self, names, refs):
        for name, ref in zip(names, refs):
            setattr(self, name, ref)


def spectral(measured, point_spread, stencil_weights, upstream):
    planes, row_count, columns = measured.shape
    plan = Spectral(lax.axis_size("gy"), lax.axis_size("gz"), planes, row_count, columns)
    waves = [jnp.asarray(part) for part in wave_rows(columns)]
    if plan.rows != columns:
        waves += [jnp.asarray(part) for part in wave_rows(plan.rows)]
    along = jnp.asarray(axis_values(plan.rows).reshape(9, 1, plan.rows))
    across = axis_values(columns).reshape(9, 2, plan.nd, plan.bins).transpose(2, 1, 3, 0)
    frequencies = np.zeros((plan.nd, 2 * plan.bins, 128), np.float32)
    frequencies[:, :, :9] = across.reshape(plan.nd, 2 * plan.bins, 9)
    scratch = plan.scratch()
    arrays = dict(weights=stencil_weights, measured=measured, point_spread=point_spread, upstream=upstream, along=along)
    arrays.update({"wave_%d" % k: part for k, part in enumerate(waves)})
    arrays["frequencies"] = jnp.asarray(frequencies)
    for name, array in arrays.items():
        shape = array.shape[1:] if name == "frequencies" else array.shape
        space = pltpu.SMEM if name == "weights" else pltpu.VMEM
        scratch[name] = space(shape, array.dtype)
    scratch["loaded"] = pltpu.SemaphoreType.DMA((len(arrays),))
    names = ["far_" + name for name in arrays] + ["out", "tap_out"] + list(scratch)

    def body(*refs):
        r = Refs(names, refs)
        r.tab_x = (r.wave_0, r.wave_1)
        r.tab_y = (r.wave_2, r.wave_3) if len(waves) > 2 else r.tab_x
        r.inputs = list(arrays)
        plan.run(r)

    out, taps = pl.pallas_call(
        body,
        out_shape=(
            jax.ShapeDtypeStruct(measured.shape, jnp.float32),
            jax.ShapeDtypeStruct((3, 3, 3), jnp.float32),
        ),
        in_specs=[HBM] * len(arrays),
        out_specs=(VMEM, VMEM),
        scratch_shapes=list(scratch.values()),
        compiler_params=pltpu.CompilerParams(
            collective_id=0, has_side_effects=True, vmem_limit_bytes=32 * 1024 * 1024
        ),
        name="spectral",
    )(
        *(pltpu.with_memory_space_constraint(array, pltpu.HBM) for array in arrays.values())
    )
    return (out, taps)


def solution(mesh):
    def program(measured, point_spread, stencil_weights, upstream):
        planes, row_count, columns = measured.shape
        fits = spectral_fits(mesh.shape["gy"], mesh.shape["gz"], planes, row_count, columns)
        chosen = spectral if fits else local
        return chosen(measured, point_spread, stencil_weights, upstream)

    return jax.shard_map(
        program,
        mesh=mesh,
        in_specs=(P("gz", "gy", None), P("gy", None), P(), P("gz", "gy", None)),
        out_specs=(P("gz", "gy", None), P()),
        check_vma=False,
    )
```

```python
import math

import jax
import jax.numpy as jnp
import numpy as np
from jax import lax
from jax.experimental import pallas as pl
from jax.experimental.pallas import tpu as pltpu
from jax.sharding import PartitionSpec as P

MESH = pl.DeviceIdType.MESH
SIDES = [(dy, dz) for dy in (-1, 0, 1) for dz in (-1, 0, 1) if (dy, dz) != (0, 0)]
VMEM = pl.BlockSpec(memory_space=pltpu.VMEM)
SMEM = pl.BlockSpec(memory_space=pltpu.SMEM)
HBM = pl.BlockSpec(memory_space=pltpu.HBM)


def moved(value, shift):
    if shift == 0:
        return value
    width = value.shape[1]
    lane = lax.broadcasted_iota(jnp.int32, value.shape, 1)
    edge = 0 if shift > 0 else width - 1
    return jnp.where(lane == edge, 0.0, pltpu.roll(value, shift % width, 1))


def regular_kernel(count_y, count_z, weights, volume, back, grown, mapped, shifted, send, receive):
    rows, columns = volume.shape
    y, z = (lax.axis_index("gy"), lax.axis_index("gz"))

    def there(dy, dz):
        return (y + dy >= 0) & (y + dy < count_y) & (z + dz >= 0) & (z + dz < count_z)

    barrier = pltpu.get_barrier_semaphore()
    for dy, dz in SIDES:

        @pl.when(there(dy, dz))
        def _():
            pl.semaphore_signal(barrier, inc=1, device_id=(y + dy, z + dz), device_id_type=MESH)

    def span(place, count):
        return 1 + jnp.where(place > 0, 1, 0) + jnp.where(place < count - 1, 1, 0)

    pl.semaphore_wait(barrier, span(y, count_y) * span(z, count_z) - 1)

    def copy(field, phase, number):
        dy, dz = SIDES[number]
        source = field.at[1, pl.ds(rows if dy > 0 else 8, 8 if dy else rows)]
        start = 8 if dy == 0 else 0 if dy > 0 else rows + 8
        return pltpu.make_async_remote_copy(
            src_ref=source,
            dst_ref=field.at[1 - dz, pl.ds(start, 8 if dy else rows)],
            send_sem=send.at[phase, number],
            recv_sem=receive.at[phase, number],
            device_id=(y + dy, z + dz),
            device_id_type=MESH,
        )

    def exchange(field, phase):
        for number, (dy, dz) in enumerate(SIDES):

            @pl.when(there(dy, dz))
            def _():
                copy(field, phase, number).start()

        for number, (dy, dz) in enumerate(SIDES):
            start = 8 if dy == 0 else 0 if dy > 0 else rows + 8

            @pl.when(jnp.logical_not(there(-dy, -dz)))
            def _():
                field[1 - dz, pl.ds(start, 8 if dy else rows)] = jnp.zeros(
                    (8 if dy else rows, columns), jnp.float32
                )

        for number, (dy, dz) in enumerate(SIDES):

            @pl.when(there(-dy, -dz))
            def _():
                copy(field, phase, number).wait_recv()

            @pl.when(there(dy, dz))
            def _():
                copy(field, phase, number).wait_send()

    def apply(field, flip, put):
        def weight(a, b, c):
            return weights[26 - (9 * a + 3 * b + c) if flip else 9 * a + 3 * b + c]

        @pl.loop(0, (rows + 16) // 8)
        def _(step):
            here = pl.ds(pl.multiple_of(step * 8, 8), 8)
            sums = [None] * 3
            for a in range(3):
                value = field[a, here]
                for c in range(3):
                    turned = moved(value, 1 - c)
                    for b in range(3):
                        term = weight(a, b, c) * turned
                        sums[b] = term if sums[b] is None else sums[b] + term
            for b in range(3):
                shifted[b, here] = sums[b]

        @pl.loop(0, rows // 8)
        def _(step):
            first = pl.multiple_of(step * 8, 8)
            around = pl.ds(first, 24)
            total = shifted[1, pl.ds(first + 8, 8)]
            total = total + shifted[0, around][7:15] + shifted[2, around][9:17]
            put(first, total)

    @pl.loop(0, rows // 8)
    def _(step):
        first = pl.multiple_of(step * 8, 8)
        grown[1, pl.ds(first + 8, 8)] = volume[pl.ds(first, 8)]

    exchange(grown, 0)

    def put_mapped(first, total):
        mapped[1, pl.ds(first + 8, 8)] = total

    apply(grown, False, put_mapped)
    exchange(mapped, 1)

    def put_back(first, total):
        back[pl.ds(first, 8)] = total

    apply(mapped, True, put_back)


def regular(volume, kernel):
    rows, columns = volume.shape[1:]
    count_y, count_z = (lax.axis_size("gy"), lax.axis_size("gz"))
    field = jax.ShapeDtypeStruct((3, rows + 16, columns), jnp.float32)

    def body(*refs):
        regular_kernel(count_y, count_z, *refs)

    back, grown, mapped = pl.pallas_call(
        body,
        out_shape=(jax.ShapeDtypeStruct((rows, columns), jnp.float32), field, field),
        in_specs=[SMEM, VMEM],
        out_specs=(VMEM, VMEM, VMEM),
        scratch_shapes=[
            pltpu.VMEM((3, rows + 16, columns), jnp.float32),
            pltpu.SemaphoreType.DMA((2, 8)),
            pltpu.SemaphoreType.DMA((2, 8)),
        ],
        cost_estimate=pl.CostEstimate(flops=120 * rows * columns, bytes_accessed=20 * rows * columns, transcendentals=0),
        compiler_params=pltpu.CompilerParams(collective_id=0, has_side_effects=True),
        name="regular",
    )(kernel.reshape(27), volume[0])
    return (back[None], grown, mapped)


def total_kernel(count_y, count_z, value, out, column, row, across, send, receive):
    y, z = (lax.axis_index("gy"), lax.axis_index("gz"))
    along_y = [(lax.rem(y + k, count_y), z) for k in range(1, count_y)]
    along_z = [(y, lax.rem(z + k, count_z)) for k in range(1, count_z)]
    barrier = pltpu.get_barrier_semaphore()
    for place in along_y + along_z:
        pl.semaphore_signal(barrier, inc=1, device_id=place, device_id_type=MESH)
    pl.semaphore_wait(barrier, count_y + count_z - 2)

    def gather(source, slots, places, base):
        copies = []
        for k, place in enumerate(places):
            copies.append(
                pltpu.make_async_remote_copy(
                    src_ref=source,
                    dst_ref=slots.at[k],
                    send_sem=send.at[base + k],
                    recv_sem=receive.at[base + k],
                    device_id=place,
                    device_id_type=MESH,
                )
            )
            copies[-1].start()
        for item in copies:
            item.wait()

    def ordered(own, slots, index, count):
        total = jnp.zeros_like(own)
        for j in range(count):
            term = own
            for k in range(1, count):
                term = jnp.where(lax.rem(index - j + count, count) == k, slots[k - 1], term)
            total = total + term
        return total

    gather(value, column, along_y, 0)
    across[...] = ordered(value[...], column, y, count_y)
    gather(across, row, along_z, count_y - 1)
    out[...] = ordered(across[...], row, z, count_z)


def total(values, collective):
    count_y, count_z = (lax.axis_size("gy"), lax.axis_size("gz"))
    count = values.shape[0]

    def body(*refs):
        total_kernel(count_y, count_z, *refs)

    block = jnp.broadcast_to(jnp.pad(values, (0, 128 - count))[None], (8, 128))
    copies = count_y + count_z - 2
    summed = pl.pallas_call(
        body,
        out_shape=jax.ShapeDtypeStruct((8, 128), jnp.float32),
        in_specs=[VMEM],
        out_specs=VMEM,
        scratch_shapes=[
            pltpu.VMEM((count_y - 1, 8, 128), jnp.float32),
            pltpu.VMEM((count_z - 1, 8, 128), jnp.float32),
            pltpu.VMEM((8, 128), jnp.float32),
            pltpu.SemaphoreType.DMA((copies,)),
            pltpu.SemaphoreType.DMA((copies,)),
        ],
        compiler_params=pltpu.CompilerParams(collective_id=collective, has_side_effects=True),
        name="total",
    )(block)
    return summed[0, :count]


def correlate_kernel(scalars, grown_0, grown_1, grown_2, grown_up, mapped_0, mapped_1, mapped_2, mapped_up, out):
    rows = grown_0.shape[1] - 16
    columns = grown_0.shape[2]
    c_up, c_zero, c_one, c_two, d_zero, d_one, s_zero, s_grad, s_direction = (scalars[k] for k in range(9))
    out[...] = jnp.zeros_like(out)

    @pl.loop(0, rows // 8)
    def _(step):
        first = pl.multiple_of(step * 8, 8)
        here = pl.ds(first + 8, 8)
        zero, one = (mapped_0[1, here], mapped_1[1, here])
        grad = c_up * mapped_up[1, here] + c_zero * zero + c_one * one + c_two * mapped_2[1, here]
        values = (
            s_zero * zero + s_grad * grad,
            s_grad * zero,
            s_direction * (d_zero * zero + d_one * one),
        )
        turned = [[moved(value, c - 1) for value in values] for c in range(3)]
        for a in range(3):
            around = pl.ds(first, 24)
            full_0, full_1 = (grown_0[a, around], grown_1[a, around])
            full_grad = c_up * grown_up[a, around] + c_zero * full_0 + c_one * full_1 + c_two * grown_2[a, around]
            full_direction = d_zero * full_0 + d_one * full_1
            for b in range(3):
                fields = [item[7 + b : 15 + b] for item in (full_0, full_grad, full_direction)]
                for c in range(3):
                    product = turned[c][0] * fields[0] + turned[c][1] * fields[1] + turned[c][2] * fields[2]
                    folded = product[:, :128]
                    for part in range(1, columns // 128):
                        folded = folded + product[:, 128 * part : 128 * part + 128]
                    out[9 * a + 3 * b + c] += folded


def correlate(scalars, *fields):
    return pl.pallas_call(
        correlate_kernel,
        out_shape=jax.ShapeDtypeStruct((27, 8, 128), jnp.float32),
        in_specs=[SMEM] + [VMEM] * 8,
        out_specs=VMEM,
        cost_estimate=pl.CostEstimate(flops=40000000, bytes_accessed=8000000, transcendentals=0),
        name="correlate",
    )(scalars, *fields).sum((1, 2))


def contract(form, left, right):
    return jnp.einsum(form, left, right, precision=lax.Precision.HIGH)


def wave_tables(length, groups):
    half = length // 2
    bins = half // groups
    pair = groups // 2
    shape = (half, pair, 2, bins)
    place = lax.broadcasted_iota(jnp.int32, shape, 0)
    part = lax.broadcasted_iota(jnp.int32, shape, 2)
    slot = lax.broadcasted_iota(jnp.int32, shape, 1) * bins + lax.broadcasted_iota(jnp.int32, shape, 3)
    tables = []
    for odd in range(2):
        frequency = 2 * slot + odd
        steps = place * frequency + part * (length // 4)
        if not odd:
            steps = jnp.where((slot == 0) & (part == 1), place * half, steps)
        angle = (steps % length).astype(jnp.float32) * (2.0 * math.pi / length)
        tables.append(jnp.cos(angle).reshape(half, pair, 2 * bins))
    return tables


def combine(raw, on_row, on_lane):
    even, odd = raw
    a, b, c, d = (
        jnp.concatenate([piece[:, part, :, :, side] for piece in (even, odd)], 0)
        for part, side in ((0, 0), (0, 1), (1, 0), (1, 1))
    )
    special = on_row | on_lane
    plus_real = jnp.where(special, a, a - d)
    plus_imaginary = jnp.where(on_row, b, jnp.where(on_lane, c, b + c))
    minus_real = jnp.where(on_row, c, jnp.where(on_lane, b, a + d))
    minus_imaginary = jnp.where(special, d, b - c)
    return (jnp.stack([plus_real, minus_real]), jnp.stack([plus_imaginary, minus_imaginary]))


def separate(spectrum, on_row, on_lane):
    (plus_real, minus_real), (plus_imaginary, minus_imaginary) = spectrum
    special = on_row | on_lane
    a = jnp.where(special, plus_real, plus_real + minus_real)
    d = jnp.where(special, minus_imaginary, minus_real - plus_real)
    b = jnp.where(on_row, plus_imaginary, jnp.where(on_lane, minus_real, plus_imaginary + minus_imaginary))
    c = jnp.where(on_row, minus_real, jnp.where(on_lane, plus_imaginary, plus_imaginary - minus_imaginary))
    scale = jnp.where(on_row & on_lane, 1.0, 2.0)
    a, b, c, d = (value * scale for value in (a, b, c, d))
    whole = jnp.stack([jnp.stack([a, b], 3), jnp.stack([c, d], 3)], 1)
    pair = whole.shape[0] // 2
    return (whole[:pair], whole[pair:])


def times(left, right, corner, conjugate=False):
    (a, b), (c, d) = (left, right)
    cross = b * d
    sign = -1.0 if conjugate else 1.0
    real = jnp.where(corner, a * c, a * c - sign * cross)
    imaginary = jnp.where(corner, cross, sign * a * d + b * c)
    return (real, imaginary)


def linear(*terms):
    total_real = total_imaginary = 0.0
    for scale, (real, imaginary) in terms:
        scale_real, scale_imaginary = scale if isinstance(scale, tuple) else (scale, scale)
        total_real = total_real + scale_real * real
        total_imaginary = total_imaginary + scale_imaginary * imaginary
    return (total_real, total_imaginary)


def local(measured, point_spread, stencil_weights, upstream):
    planes, row_count, columns = measured.shape
    groups = lax.axis_size("gy")
    rows = row_count * groups
    cells = planes * rows * columns * lax.axis_size("gz")
    bins = columns // 2 // groups
    even_x, odd_x = wave_tables(columns, groups)
    even_y, odd_y = (even_x, odd_x) if rows == columns else wave_tables(rows, groups)
    y_bins = rows // 2 // groups
    spectral = (groups, y_bins, 1, bins)
    on_row = (lax.broadcasted_iota(jnp.int32, spectral, 0) == 0) & (
        lax.broadcasted_iota(jnp.int32, spectral, 1) == 0
    )
    on_lane = (lax.broadcasted_iota(jnp.int32, spectral, 3) == 0) & (lax.axis_index("gy") == 0)
    corner = on_row & on_lane

    def forward(volumes):
        count = volumes.shape[0]
        low, high = (volumes[:, :, : columns // 2], volumes[:, :, columns // 2 :])
        sent = jnp.concatenate(
            [contract("vrj,jdl->drvl", low + high, even_x), contract("vrj,jdl->drvl", low - high, odd_x)], 0
        )
        arrived = lax.all_to_all(
            sent.reshape(groups, row_count, count * 2 * bins), "gy", split_axis=0, concat_axis=0, tiled=True
        )
        arrived = arrived.reshape(rows, count * 2 * bins)
        low, high = (arrived[: rows // 2], arrived[rows // 2 :])
        raw = [
            contract("jds,jl->dsl", table, value).reshape(groups // 2, 2, y_bins, count, 2, bins)
            for table, value in ((even_y, low + high), (odd_y, low - high))
        ]
        return combine(raw, on_row, on_lane)

    def inverse(spectrum):
        count = spectrum[0].shape[3]
        pieces = separate(spectrum, on_row, on_lane)
        one, two = (
            contract("jds,dsl->jl", table, piece.reshape(groups // 2, 2 * y_bins, count * 2 * bins))
            for table, piece in ((even_y, pieces[0]), (odd_y, pieces[1]))
        )
        sent = jnp.concatenate([one + two, one - two], 0).reshape(groups, row_count, count * 2 * bins)
        arrived = lax.all_to_all(sent, "gy", split_axis=0, concat_axis=0, tiled=True)
        arrived = arrived.reshape(groups, row_count, count, 2 * bins)
        one = contract("drvl,jdl->vrj", arrived[: groups // 2], even_x)
        two = contract("drvl,jdl->vrj", arrived[groups // 2 :], odd_x)
        return jnp.concatenate([one + two, one - two], 2) / float(rows * columns)

    def pick(spectrum, start, count):
        return tuple(lax.slice_in_dim(part, start, start + count, axis=3) for part in spectrum)

    def join(*spectra):
        return tuple(jnp.concatenate(parts, 3) for parts in zip(*spectra))

    spectra = forward(jnp.concatenate([point_spread[None], measured], 0))
    transfer = pick(spectra, 0, 1)
    squares = (transfer[0] ** 2, transfer[1] ** 2)
    gain = (
        jnp.where(corner, squares[0], squares[0] + squares[1]),
        jnp.where(corner, squares[1], squares[0] + squares[1]),
    )
    spectrum_0 = times(pick(spectra, 1, planes), transfer, corner, True)
    blurred_0 = linear((gain, spectrum_0))
    pair = inverse(join(spectrum_0, blurred_0))
    vector_0 = pair[:planes]
    back_0, grown_0, mapped_0 = regular(vector_0, stencil_weights)
    back_up, grown_up, mapped_up = regular(upstream, stencil_weights)
    vector_1 = pair[planes:] + back_0
    spectrum_1 = linear((1.0, blurred_0), (1.0, forward(back_0)))
    blurred_1 = linear((gain, spectrum_1))
    early = forward(jnp.concatenate([upstream, back_up], 0))
    back_1, grown_1, mapped_1 = regular(vector_1, stencil_weights)
    vector_2 = inverse(blurred_1) + back_1
    norm_0, curve_0, image_0, up_0, up_1 = total(
        jnp.stack(
            [
                jnp.sum(vector_0 * vector_0),
                jnp.sum(vector_0 * vector_1),
                jnp.sum(vector_1 * vector_1),
                jnp.sum(upstream * vector_0),
                jnp.sum(upstream * vector_1),
            ]
        ),
        1,
    )
    step_0 = norm_0 / curve_0
    residual = vector_0 - step_0 * vector_1
    residual_image = vector_1 - step_0 * vector_2
    norm_1, cross, inner, up_residual, image_cross = total(
        jnp.stack(
            [
                jnp.sum(residual * residual),
                jnp.sum(residual * vector_1),
                jnp.sum(residual * residual_image),
                jnp.sum(upstream * residual),
                jnp.sum(residual_image * vector_1),
            ]
        ),
        2,
    )
    back_2, grown_2, mapped_2 = regular(vector_2, stencil_weights)
    late = forward(jnp.concatenate([back_1, back_2], 0))
    ratio = norm_1 / norm_0
    curve_1 = inner + 2.0 * ratio * cross + ratio * ratio * curve_0
    step_1 = norm_1 / curve_1
    grad_step_1 = up_residual + ratio * up_0
    grad_curve_1 = -grad_step_1 * step_1 / curve_1
    grad_ratio = step_1 * up_0 + 2.0 * grad_curve_1 * (cross + ratio * curve_0)
    known_image = step_1 * up_1 + 2.0 * grad_curve_1 * (image_cross + ratio * image_0)
    grad_norm = grad_step_1 / curve_1 + grad_ratio / norm_0
    grad_step_0 = up_0 - known_image - 2.0 * grad_norm * cross
    grad_curve_0 = -grad_step_0 * step_0 / curve_0
    grad_norm_0 = -grad_ratio * ratio / norm_0 + grad_step_0 / curve_0

    spectrum_2 = linear((1.0, linear((gain, spectrum_1))), (1.0, pick(late, 0, planes)))
    spectrum_up = pick(early, 0, planes)
    residual_terms = ((1.0, spectrum_0), (-step_0, spectrum_1))
    direction_image = linear((1.0 + ratio, spectrum_1), (-step_0, spectrum_2))
    grad_direction = linear((step_1, spectrum_up), (2.0 * grad_curve_1, direction_image))
    grad_residual = linear((1.0, grad_direction), (2.0 * grad_norm, linear(*residual_terms)))
    grad_back = linear(
        (step_1, pick(early, planes, planes)),
        (2.0 * grad_curve_1 * (1.0 + ratio) - 2.0 * grad_norm * step_0, pick(late, 0, planes)),
        (-2.0 * grad_curve_1 * step_0, pick(late, planes, planes)),
        (2.0 * grad_norm, linear((1.0, spectrum_1), (-1.0, blurred_0))),
    )
    grad_right = linear(
        (step_0, spectrum_up),
        (ratio, grad_direction),
        (2.0 * grad_curve_0, spectrum_1),
        (2.0 * grad_norm_0, spectrum_0),
        (1.0, grad_residual),
        (-step_0, linear((gain, grad_residual), (1.0, grad_back))),
    )
    grad_measured = inverse(times(grad_right, transfer, corner))

    terms = correlate(
        jnp.stack(
            [
                step_1,
                2.0 * grad_norm,
                2.0 * grad_curve_1 * (1.0 + ratio) - 2.0 * grad_norm * step_0,
                -2.0 * grad_curve_1 * step_0,
                1.0 + ratio,
                -step_0,
                2.0 * grad_curve_0,
                -step_0,
                2.0 * grad_curve_1,
            ]
        ),
        grown_0, grown_1, grown_2, grown_up, mapped_0, mapped_1, mapped_2, mapped_up,
    )
    grad_stencil = total(terms, 3).reshape(3, 3, 3) / math.sqrt(cells)
    return (grad_measured, grad_stencil)


def spectral_fits(mesh_y, mesh_z, planes, row_count, columns):
    devices, rows, depth = (mesh_y * mesh_z, row_count * mesh_y, planes * mesh_z)
    if columns % (16 * devices) or row_count % 128 or rows % 512 or planes != 1 or mesh_z % 2:
        return False
    tiles = 2 * depth // 8 * (rows // 128)
    return depth == 4 and mesh_y % 4 == 0 and tiles % (2 * mesh_z) == 0


def wave_rows(length):
    half, quarter = (length // 2, length // 4)
    place = np.arange(half)[None, :]
    tables = []
    for odd in range(2):
        frequency = 2 * np.arange(quarter)[:, None] + odd
        angle = (place * frequency % length) * (2.0 * np.pi / length)
        cosine, sine = (np.cos(angle), np.sin(angle))
        if not odd:
            sine[0] = np.cos(np.pi * place[0])
        tables += [cosine, sine]
    table = np.stack(tables)
    high = table.astype(jnp.bfloat16)
    low = (table - high.astype(np.float64)).astype(jnp.bfloat16)
    return (high, low)


def basis(length, place):
    half = length // 2
    frequency = np.concatenate([np.arange(0, half, 2), np.arange(1, half, 2)])
    angle = frequency * place % length * (2.0 * np.pi / length)
    cosine, sine = (np.cos(angle), np.sin(angle))
    sine[0] = np.cos(np.pi * place)
    return (cosine, sine)


def axis_values(length):
    cosine, sine = basis(length, 1)
    pure = sine.copy()
    pure[0] = 0.0
    other = cosine.copy()
    other[0] = -1.0
    weight = np.full(length // 2, 2.0)
    weight[0] = 1.0
    values = [(cosine, other), (pure, pure), basis(length, 0), basis(length, length - 1), (weight, weight)]
    for place in (0, 1, length - 2, length - 1):
        values.append(tuple(weight * part / length for part in basis(length, place)))
    return np.stack([np.stack(pair) for pair in values]).astype(np.float32)


COS, SIN, FIRST, LAST, WEIGHT, AT = range(6)


def split(value):
    high = value.astype(jnp.bfloat16)
    return (high, (value - high.astype(jnp.float32)).astype(jnp.bfloat16))


def product(left, right, contracting):
    numbers = (contracting, ((), ()))

    def one(a, b):
        return lax.dot_general(a, b, numbers, preferred_element_type=jnp.float32)

    return one(left[0], right[0]) + (one(left[0], right[1]) + one(left[1], right[0]))


class Spectral:
    def __init__(self, count_y, count_z, planes, row_count, columns):
        self.ny, self.nz = (count_y, count_z)
        self.nd = count_y * count_z
        self.depth = planes * count_z
        self.row_count = row_count
        self.rows = row_count * count_y
        self.columns = columns
        self.bins = columns // 2 // self.nd
        self.half = self.rows // 2
        self.steps = self.half // 128
        self.tiers = self.bins // 8
        self.lanes = self.rows // 128
        self.tiles = 2 * self.depth // 8 * self.lanes
        self.share = self.tiles // (2 * self.nz)

    def place_of(self, index):
        return (lax.rem(index, self.ny), lax.div(index, self.ny))

    def find_place(self):
        self.y, self.z = (lax.axis_index("gy"), lax.axis_index("gz"))
        self.me = self.z * self.ny + self.y

        def turned(place, count):
            moved = [place + k for k in range(count)]
            return [jnp.where(item >= count, item - count, item) for item in moved]

        ys, zs = (turned(self.y, self.ny), turned(self.z, self.nz))
        far = sorted(range(self.ny), key=lambda k: -min(k, self.ny - k))
        self.cuts = (self.nd // 16, self.nd // 2, self.nd * 7 // 8)
        self.peers = [(ys[a], zs[b]) for a in far for b in reversed(range(self.nz)) if a or b]

    def remote_to(self, source, target, send, receive, place):
        return pltpu.make_async_remote_copy(
            src_ref=source, dst_ref=target, send_sem=send, recv_sem=receive, device_id=place, device_id_type=MESH
        )

    def scratch(self):
        Z, bins, half, nd = (self.depth, self.bins, self.half, self.nd)
        packed = (Z, 2, bins, self.rows)
        field = (Z, 4, bins, half)
        edge = (2, Z, 2, bins, 128)
        F = jnp.float32
        D = pltpu.SemaphoreType.DMA
        others = nd - 1
        names = dict(
            sent_m=pltpu.VMEM((nd, 2, bins, 128 * (self.row_count // 128)), F),
            sent_u=pltpu.VMEM((nd, 2, bins, self.row_count), F),
            sent_p=pltpu.VMEM((self.ny, 2, bins, self.row_count), F),
            got_m=pltpu.VMEM(packed, F),
            got_u=pltpu.VMEM(packed, F),
            got_p=pltpu.VMEM((2, bins, self.rows), F),
            wave=pltpu.VMEM(packed, F),
            wave_p=pltpu.VMEM((2, bins, self.rows), F),
            v0=pltpu.VMEM(field, F),
            v1=pltpu.VMEM(field, F),
            v2=pltpu.VMEM(field, F),
            up=pltpu.VMEM(field, F),
            w3=pltpu.VMEM(field, F),
            m0=pltpu.VMEM(field, F),
            m1=pltpu.VMEM(field, F),
            mw=pltpu.VMEM(field, F),
            stencil=pltpu.VMEM((3, 2, 3, bins, half), F),
            blur=pltpu.VMEM((2, 3, bins, half), F),
            gain=pltpu.VMEM((2, 2, bins, half), F),
            across=pltpu.VMEM((9, 2, bins, 128), F),
            rows_v0=pltpu.VMEM(edge, F),
            rows_v1=pltpu.VMEM(edge, F),
            rows_v2=pltpu.VMEM(edge, F),
            rows_up=pltpu.VMEM(edge, F),
            rows_w3=pltpu.VMEM(edge, F),
            rows_m0=pltpu.VMEM(edge, F),
            rows_m1=pltpu.VMEM(edge, F),
            rows_mw=pltpu.VMEM(edge, F),
            edge_rows=pltpu.VMEM(edge, F),
            cols_v0=pltpu.VMEM((4, 8, self.rows), F),
            cols_v1=pltpu.VMEM((4, 8, self.rows), F),
            cols_v2=pltpu.VMEM((4, 8, self.rows), F),
            cols_up=pltpu.VMEM((4, 8, self.rows), F),
            cols_w3=pltpu.VMEM((4, 8, self.rows), F),
            cols_m0=pltpu.VMEM((2, 8, self.rows), F),
            cols_m1=pltpu.VMEM((2, 8, self.rows), F),
            cols_mw=pltpu.VMEM((2, 8, self.rows), F),
            edge_cols=pltpu.VMEM((2, 8, self.rows), F),
            part=pltpu.VMEM((3, 5, self.tiles, 8, 128), F),
            slots=pltpu.VMEM((3, 5, others, self.share, 8, 128), F),
            sums=pltpu.VMEM((3, 5, self.share, 8, 128), F),
            full=pltpu.VMEM((3, 5, self.tiles, 8, 128), F),
            line_part=pltpu.VMEM((3, 1, 128), F),
            line_slots=pltpu.VMEM((3, others, 1, 128), F),
            line_sums=pltpu.VMEM((3, 1, 128), F),
            line_full=pltpu.VMEM((3, 1, 128), F),
            around=pltpu.VMEM(field, F),
            acc=pltpu.VMEM((8, 8, 128), F),
            taps=pltpu.VMEM((27, 8, 128), F),
            tap_part=pltpu.VMEM((1, 128), F),
            tap_slots=pltpu.VMEM((nd, 1, 128), F),
            sent_o=pltpu.VMEM(packed, F),
            got_o=pltpu.VMEM((nd, 2, bins, self.row_count), F),
            send_big=D((4,)),
            recv_big=D((4,)),
            send_p=D,
            recv_p=D,
            send_part=D((2, 5)),
            recv_part=D((2, 5)),
            send_full=D((2, 5)),
            recv_full=D((2, 5)),
            send_tap=D,
            recv_tap=D,
        )
        return names


    def remote(self, source, target, send, receive, peer):
        return pltpu.make_async_remote_copy(
            src_ref=source, dst_ref=target, send_sem=send, recv_sem=receive,
            device_id=self.place_of(peer), device_id_type=MESH,
        )

    def arrived(self, shape, semaphore):
        self.remote(shape, shape, semaphore, semaphore, self.me).wait_recv()

    def row_lanes(self, y):
        return pl.ds(pl.multiple_of(y * self.row_count, 128), self.row_count)

    def spread_start(self, r, sent, got, lot, first=0, end=None):
        here = got.at[self.z, :, :, self.row_lanes(self.y)]
        for y, z in self.peers[first:end]:
            self.remote_to(sent.at[z * self.ny + y], here, r.send_big.at[lot], r.recv_big.at[lot], (y, z)).start()
        if first == 0:
            here[...] = sent[self.me]

    def spread_wait(self, r, sent, lot):
        others = sent.at[pl.ds(0, self.nd - 1)]
        self.arrived(others, r.recv_big.at[lot])
        self.arrived(others, r.send_big.at[lot])

    def point_start(self, r):
        here = r.got_p.at[:, :, self.row_lanes(self.y)]

        @pl.loop(1, self.ny)
        def _(k):
            peer = lax.rem(self.y + k, self.ny)
            self.remote(r.sent_p.at[peer], here, r.send_p, r.recv_p, self.z * self.ny + peer).start()

        here[...] = r.sent_p[self.y]

    def point_wait(self, r):
        others = r.sent_p.at[pl.ds(0, self.ny - 1)]
        self.arrived(others, r.recv_p)
        self.arrived(others, r.send_p)

    def return_start(self, r, first, end):
        for y, z in self.peers[first:end]:
            self.remote_to(
                r.sent_o.at[z, :, :, self.row_lanes(y)], r.got_o.at[self.me], r.send_big.at[2], r.recv_big.at[2], (y, z)
            ).start()

    def owner(self, kind, number):
        if kind == 2:
            number = self.nz
        return lax.rem(number, self.nz) * self.ny + self.ny // 2 - 1 + 2 * lax.div(number, self.nz)

    def owned(self, kind):
        low = self.ny // 2 - 1
        if kind == 2:
            return self.me == self.owner(2, 0)
        return (self.y == low) | (self.y == low + 2)

    def owners(self, kind):
        return 1 if kind == 2 else 2 * self.nz

    def mine(self, kind):
        return 0 if kind == 2 else jnp.where(self.y == self.ny // 2 - 1, 0, self.nz) + self.z

    def width(self, kind):
        return 1 if kind == 2 else self.share

    def lot(self, r, name, turn, kind, number, count=1):
        if kind == 2:
            return getattr(r, "line_" + name).at[turn]
        return getattr(r, name).at[turn, kind, pl.ds(number * self.share, count * self.share)]

    def slot(self, r, turn, kind, first, count=1):
        if kind == 2:
            return r.line_slots.at[turn, pl.ds(first, count)]
        return r.slots.at[turn, kind, pl.ds(first, count)]

    def reduce_start(self, r, turn, kinds):
        for kind in kinds:
            send, receive = (r.send_part.at[turn % 2, kind], r.recv_part.at[turn % 2, kind])

            @pl.loop(0, self.owners(kind))
            def _(number):
                owner = self.owner(kind, number)

                @pl.when(owner != self.me)
                def _():
                    place = lax.rem(self.me - owner + self.nd, self.nd) - 1
                    self.remote(
                        self.lot(r, "part", turn, kind, number), self.slot(r, turn, kind, place).at[0], send, receive, owner
                    ).start()

    def reduce_middle(self, r, turn, kinds):
        others = self.nd - 1
        for kind in kinds:
            send, receive = (r.send_full.at[turn % 2, kind], r.recv_full.at[turn % 2, kind])

            @pl.when(self.owned(kind))
            def _():
                number = self.mine(kind)
                self.arrived(self.slot(r, turn, kind, 0, others), r.recv_part.at[turn % 2, kind])
                lots = [self.lot(r, "part", turn, kind, number)[...]]
                lots += [self.slot(r, turn, kind, k)[0] for k in range(others)]
                while len(lots) > 1:
                    lots = [lots[k] + lots[k + 1] for k in range(0, len(lots) - 1, 2)] + lots[len(lots) // 2 * 2 :]
                sums = self.lot(r, "sums", turn, kind, 0)
                sums[...] = lots[0]
                full = self.lot(r, "full", turn, kind, number)
                for place in self.peers:
                    self.remote_to(sums, full, send, receive, place).start()
                full[...] = lots[0]

    def reduce_end(self, r, turn, kinds):
        for kind in kinds:
            count = self.owners(kind)

            def finish(count):
                if count:
                    self.arrived(self.lot(r, "full", turn, kind, 0, count), r.recv_full.at[turn % 2, kind])
                    self.arrived(self.lot(r, "part", turn, kind, 0, count), r.send_part.at[turn % 2, kind])

            @pl.when(self.owned(kind))
            def _():
                finish(count - 1)
                self.arrived(self.slot(r, turn, kind, 0, self.nd - 1), r.send_full.at[turn % 2, kind])

            @pl.when(jnp.logical_not(self.owned(kind)))
            def _():
                finish(count)


    def row_spectra(self, r, source, sent):
        half = self.columns // 2
        low, high = (source[:, :half], source[:, half:])
        per = self.nd // 2
        for odd, value in enumerate((low + high, low - high)):
            value = split(value)
            for part in range(2):
                table = (r.tab_x[0][2 * odd + part], r.tab_x[1][2 * odd + part])
                sent[pl.ds(odd * per, per), part] = product(table, value, ((1,), (1,))).reshape(
                    per, self.bins, self.row_count
                )

    def point_spectra(self, r, source):
        half = self.columns // 2
        low, high = (source[:, :half], source[:, half:])
        odd = lax.div(2 * self.z, self.nz)
        sign = 1.0 - 2.0 * odd.astype(jnp.float32)
        value = split(low + sign * high)
        block = self.ny * self.bins
        start = pl.multiple_of(lax.rem(self.z, self.nz // 2) * block, block)
        for part in range(2):
            table = tuple(half_table[2 * odd + part, pl.ds(start, block)] for half_table in r.tab_x)
            r.sent_p[:, part] = product(table, value, ((1,), (1,))).reshape(self.ny, self.bins, self.row_count)

    def column_spectra(self, r, got, wave):
        count = math.prod(got.shape[:-1])
        value = got[...].reshape(count, self.rows)
        low, high = (value[:, : self.half], value[:, self.half :])
        quarter = self.half // 2
        for odd, value in enumerate((low + high, low - high)):
            value = split(value)
            for part in range(2):
                table = (r.tab_y[0][2 * odd + part], r.tab_y[1][2 * odd + part])
                wave[..., pl.ds(part * self.half + odd * quarter, quarter)] = product(
                    value, table, ((1,), (1,))
                ).reshape(got.shape[:-1] + (quarter,))

    def column_values(self, r, wave, target):
        count = math.prod(wave.shape[:-1])
        value = wave[...].reshape(count, self.rows)
        quarter = self.half // 2
        even, odd = (
            sum(
                product(
                    split(value[:, part * self.half + k * quarter : part * self.half + (k + 1) * quarter]),
                    (r.tab_y[0][2 * k + part], r.tab_y[1][2 * k + part]),
                    ((1,), (0,)),
                )
                for part in range(2)
            )
            for k in range(2)
        )
        shape = wave.shape[:-1] + (self.half,)
        target[..., : self.half] = (even + odd).reshape(shape)
        target[..., self.half :] = (even - odd).reshape(shape)

    def row_values(self, r, got, out):
        per = self.nd // 2
        sides = []
        for k in range(2):
            side = 0.0
            for part in range(2):
                value = got[pl.ds(k * per, per), part].reshape(per * self.bins, self.row_count)
                side = side + product(
                    split(value.T), (r.tab_x[0][2 * k + part], r.tab_x[1][2 * k + part]), ((1,), (0,))
                )
            sides.append(side)
        half = self.columns // 2
        out[0, :, :half] = sides[0] + sides[1]
        out[0, :, half:] = sides[0] - sides[1]


    def masks(self, tier, step):
        shape = (8, 128)
        row = (lax.broadcasted_iota(jnp.int32, shape, 0) == 0) & (self.me == 0)
        lane = lax.broadcasted_iota(jnp.int32, shape, 1) + 128 * step == 0
        if tier:
            row = row & False
        return (row, lane, row & lane, row | lane)

    def combine(self, masks, ac, as_, bc, bs):
        row, lane, corner, special = masks
        pr = jnp.where(special, ac, ac - bs)
        pi = jnp.where(corner, as_, jnp.where(row, -as_, jnp.where(lane, -bc, -(as_ + bc))))
        mr = jnp.where(row, bc, jnp.where(lane, as_, ac + bs))
        mi = jnp.where(corner, bs, jnp.where(special, -bs, as_ - bc))
        return [pr, pi, mr, mi]

    def separate(self, masks, field):
        row, lane, corner, special = masks
        pr, pi, mr, mi = field
        ac = jnp.where(special, pr, 0.5 * (pr + mr))
        as_ = jnp.where(corner, pi, jnp.where(row, -pi, jnp.where(lane, mr, 0.5 * (mi - pi))))
        bc = jnp.where(row, mr, jnp.where(lane, -pi, -0.5 * (pi + mi)))
        bs = jnp.where(corner, mi, jnp.where(special, -mi, 0.5 * (mr - pr)))
        return (ac, as_, bc, bs)

    def lane_slice(self, step, part=0):
        return pl.ds(pl.multiple_of(part * self.half + step * 128, 128), 128)

    def along(self, r, which, step, part):
        return r.along[which, :, self.lane_slice(step, part)]

    def beside(self, r, which, part, tier):
        return r.across[which, part, pl.ds(8 * tier, 8)]

    def load(self, field, z, tier, step):
        return [field[z, k, pl.ds(8 * tier, 8), self.lane_slice(step)] for k in range(4)]

    def keep(self, field, z, tier, step, values):
        for k in range(4):
            field[z, k, pl.ds(8 * tier, 8), self.lane_slice(step)] = values[k]

    def load_wave(self, wave, z, tier, step):
        return [
            wave[z, part, pl.ds(8 * tier, 8), self.lane_slice(step, side)]
            for part in range(2)
            for side in range(2)
        ]

    def times(self, factor, value, conjugate=False):
        out = []
        for side in range(2):
            real, other, cross = factor[side]
            a, b = (value[2 * side], value[2 * side + 1])
            if conjugate:
                out += [real * a + cross * b, other * b - cross * a]
            else:
                out += [real * a - cross * b, other * b + cross * a]
        return out

    def factor(self, array, tier, step):
        where = (pl.ds(8 * tier, 8), self.lane_slice(step))
        return [[array[(side, k) + where] for k in range(3)] for side in range(2)]

    def sweep(self, body):
        @pl.loop(0, self.steps)
        def _(step):
            columns = {}
            for tier in range(self.tiers):
                body(tier, step, self.masks(tier, step), columns)

    def frames(self, r, masks, tier, step, z, value, rows, columns=None):
        ac, as_, bc, bs = self.separate(masks, value)
        here = pl.ds(8 * tier, 8)
        for k, which in enumerate((AT, AT + 3)):
            c, s = (self.along(r, which, step, 0), self.along(r, which, step, 1))
            rows[k, z, 0, here] += ac * c + as_ * s
            rows[k, z, 1, here] += bc * c + bs * s
        if columns is None:
            return
        for x in range(4):
            a, b = (self.beside(r, AT + x, 0, tier), self.beside(r, AT + x, 1, tier))
            for side, (p, q) in enumerate(((ac, bc), (as_, bs))):
                term = a * p + b * q
                key = (x, z, side)
                columns[key] = term if key not in columns else columns[key] + term

    def put_columns(self, r, turn, kinds, tier, step, columns):
        if tier < self.tiers - 1:
            return
        for (x, z, side), value in columns.items():
            index = x // 2 * self.depth + z
            kind = kinds[0] if x in (0, 3) else kinds[1]
            tile = index // 8 * self.lanes + side * self.steps + step
            r.part[turn, kind, tile, pl.ds(index % 8, 1)] = jnp.sum(value, 0, keepdims=True)

    def clear(self, *refs):
        for ref in refs:
            ref[...] = jnp.zeros(ref.shape, jnp.float32)

    def settle(self, rows):
        for k in range(2):
            rows[k] = jnp.broadcast_to(jnp.sum(rows[k], -1, keepdims=True), rows.shape[1:])

    def unpack(self, r, turn, kind, cols, inner):
        Z = self.depth
        for x in (1, 2) if inner else (0, 3):
            first = x // 2 * Z
            for lane in range(self.lanes):
                cols[x, pl.ds(0, Z), pl.ds(lane * 128, 128)] = r.full[
                    turn, kind, first // 8 * self.lanes + lane, pl.ds(first % 8, Z)
                ]

    def shifted(self, value, by):
        if by == 0:
            return value
        value = pltpu.roll(value, 7 if by > 0 else 1, 0)
        sub = lax.broadcasted_iota(jnp.int32, value.shape, 0)
        return jnp.where(sub < self.depth, value, 0.0)

    def corners(self, r, col):
        out = []
        for which in (AT, AT + 3):
            weight = jnp.concatenate([r.along[which, :, :]], 0)
            out.append(jnp.broadcast_to(jnp.sum(col * weight, -1, keepdims=True), (8, 128)))
        return out

    def column_tools(self, r, w, step):
        c = [self.along(r, COS, step, part) for part in range(2)]
        s = self.along(r, SIN, step, 0)
        first = [self.along(r, FIRST, step, part) for part in range(2)]
        last = [self.along(r, LAST, step, part) for part in range(2)]

        def get(col):
            return [col[:, self.lane_slice(step, part)] for part in range(2)]

        def line(a, c_index, col):
            w0, w1, w2 = (w(a, b, c_index) for b in range(3))
            turn = (w2 - w0) * s
            return [
                (w1 + (w0 + w2) * c[0]) * col[0] + turn * col[1],
                (w1 + (w0 + w2) * c[1]) * col[1] - turn * col[0],
            ]

        def stacked(pieces):
            out = None
            for a in range(3):
                for c_index, col in pieces:
                    term = [self.shifted(part, a - 1) for part in line(a, c_index, col)]
                    out = term if out is None else [p + t for p, t in zip(out, term)]
            return out

        return (first, last, get, stacked)

    def edges(self, r, w, col_first, col_last):
        Z = self.depth
        k_first, k_last = (self.corners(r, col_first[...]), self.corners(r, col_last[...]))
        total = lambda terms: sum(terms[1:], terms[0])
        q = {}
        for name, b, c, value in ((0, 0, 0, k_last[1]), (1, 0, 2, k_first[1]), (2, 2, 0, k_last[0]), (3, 2, 2, k_first[0])):
            q[name] = total([w(a, b, c) * self.shifted(value, a - 1) for a in range(3)])
        @pl.loop(0, self.steps)
        def _(step):
            first, last, get, stacked = self.column_tools(r, w, step)
            f, l = (get(col_first), get(col_last))
            for k, (pieces, upper, lower) in enumerate((([(0, l)], q[0], q[2]), ([(2, f)], q[1], q[3]))):
                value = stacked(pieces)
                for part in range(2):
                    r.edge_cols[k, :, self.lane_slice(step, part)] = (
                        value[part] - upper * first[part] - lower * last[part]
                    )

    def edge_lines(self, r, w, rows):
        Z = self.depth
        for tier in range(self.tiers):
            here = pl.ds(8 * tier, 8)
            c = [self.beside(r, COS, part, tier) for part in range(2)]
            s = self.beside(r, SIN, 0, tier)
            for k, (b, source) in enumerate(((0, 1), (2, 0))):
                for z in range(Z):
                    out = None
                    for a in range(3):
                        if not 0 <= z + a - 1 < Z:
                            continue
                        w0, w1, w2 = (w(a, b, c_index) for c_index in range(3))
                        turn = (w2 - w0) * s
                        p, t = (rows[source, z + a - 1, part, here] for part in range(2))
                        term = [
                            (w1 + (w0 + w2) * c[0]) * p + turn * t,
                            (w1 + (w0 + w2) * c[1]) * t - turn * p,
                        ]
                        out = term if out is None else [x + v for x, v in zip(out, term)]
                    for part in range(2):
                        r.edge_rows[k, z, part, here] = out[part]

    def map_columns(self, r, w, cols, mapped, extra=None):
        total = lambda terms: sum(terms[1:], terms[0])
        at = [self.corners(r, cols[x]) for x in range(4)]
        fix = []
        for (c0, v0), (c1, v1) in (((1, at[0]), (2, at[1])), ((0, at[2]), (1, at[3]))):
            fix.append(
                [
                    total(
                        [
                            w(a, b, c0) * self.shifted(v0[y], a - 1) + w(a, b, c1) * self.shifted(v1[y], a - 1)
                            for a in range(3)
                        ]
                    )
                    for b, y in ((0, 1), (2, 0))
                ]
            )

        @pl.loop(0, self.steps)
        def _(step):
            first, last, get, stacked = self.column_tools(r, w, step)
            f, n, g, l = (get(cols.at[x]) for x in range(4))
            for k, pieces in enumerate(([(1, f), (2, n)], [(0, g), (1, l)])):
                value = stacked(pieces)
                for part in range(2):
                    here = (k, slice(None), self.lane_slice(step, part))
                    value_here = value[part] - fix[k][0] * first[part] - fix[k][1] * last[part]
                    if extra is not None:
                        value_here = value_here + extra(here)
                    mapped[here] = value_here

    def edge_field(self, r, masks, tier, step, z):
        here = pl.ds(8 * tier, 8)
        out = []
        for part in range(2):
            e0, e1 = (r.edge_rows[k, z, part, here] for k in range(2))
            x0, x1 = (self.beside(r, which, part, tier) for which in (FIRST, LAST))
            for side in range(2):
                y0, y1 = (self.along(r, which, step, side) for which in (FIRST, LAST))
                c0, c1 = (r.edge_cols[k, pl.ds(z, 1), self.lane_slice(step, side)] for k in range(2))
                out.append(e0 * y0 + e1 * y1 + x0 * c0 + x1 * c1)
        return self.combine(masks, *out)

    def circular_field(self, r, tier, step, field, flip, out=None):
        Z = self.depth
        value = [self.load(field, z, tier, step) for z in range(Z)]
        out = [None] * Z if out is None else out
        for a in range(3):
            factor = self.factor(r.stencil.at[a], tier, step)
            for z in range(Z):
                other = z + (1 - a if flip else a - 1)
                if 0 <= other < Z:
                    term = self.times(factor, value[other], flip)
                    out[z] = term if out[z] is None else [o + t for o, t in zip(out[z], term)]
        return out

    def turn_round(self, r, field, out, norm=None):
        def body(tier, step, masks, columns):
            for z, value in enumerate(self.circular_field(r, tier, step, field, False)):
                self.keep(out, z, tier, step, value)
                if norm is not None:
                    own = self.load(field, z, tier, step)
                    norm[...] += self.dot(masks, own, own)

        self.sweep(body)

    def build_stencil(self, r, w):
        def body(tier, step, masks, columns):
            row, lane, corner, special = masks
            here = pl.ds(8 * tier, 8)
            sx = self.beside(r, SIN, 0, tier)
            ys = self.along(r, SIN, step, 0)
            for side in range(2):
                cx = self.beside(r, COS, side, tier)
                cy = self.along(r, COS, step, 0)
                sy = jnp.broadcast_to(ys, (8, 128))
                cy = jnp.broadcast_to(cy, (8, 128))
                if side:
                    cy = jnp.where(row, cy, self.along(r, COS, step, 1))
                    sy = jnp.where(row, sy, -sy)
                for a in range(3):
                    real, imag = ([], [])
                    for b in range(3):
                        real.append(w(a, b, 1) + (w(a, b, 0) + w(a, b, 2)) * cx)
                        imag.append((w(a, b, 2) - w(a, b, 0)) * sx)
                    value = real[1] + (real[0] + real[2]) * cy - (imag[2] - imag[0]) * sy
                    cross = imag[1] + (imag[0] + imag[2]) * cy + (real[2] - real[0]) * sy
                    other = jnp.where(corner, real[1] - (real[0] + real[2]), value)
                    for k, item in enumerate((value, other, cross)):
                        r.stencil[a, side, k, here, self.lane_slice(step)] = item

        self.sweep(body)

    def build_blur(self, r):
        def body(tier, step, masks, columns):
            row, lane, corner, special = masks
            here = pl.ds(8 * tier, 8)
            wave = [
                r.wave_p[part, here, self.lane_slice(step, side)] for part in range(2) for side in range(2)
            ]
            value = self.combine(masks, wave[0], wave[1], wave[2], wave[3])
            for side in range(2):
                real, imag = (value[2 * side], value[2 * side + 1])
                other = jnp.where(corner, imag, real)
                cross = jnp.where(corner, 0.0, imag)
                for k, item in enumerate((real, other, cross)):
                    r.blur[side, k, here, self.lane_slice(step)] = item
                square = cross * cross
                r.gain[side, 0, here, self.lane_slice(step)] = real * real + square
                r.gain[side, 1, here, self.lane_slice(step)] = other * other + square

        self.sweep(body)

    def gained(self, r, tier, step, value):
        where = (pl.ds(8 * tier, 8), self.lane_slice(step))
        return [r.gain[(k // 2, k % 2) + where] * value[k] for k in range(4)]

    def dot(self, masks, left, right):
        corner = masks[2]
        total = sum(a * b for a, b in zip(left, right))
        return jnp.where(corner, 0.5 * total, total)


    def stencil_twice(self, r, w, cols, mapped, rows_m, cols_m, make, finish, inner, extra=None):
        def flipped(a, b, c):
            return w(2 - a, 2 - b, 2 - c)

        self.edges(r, w, cols.at[0], cols.at[3])
        self.clear(rows_m)

        def forward(tier, step, masks, columns):
            for z in range(self.depth):
                value = [m - e for m, e in zip(make(tier, step, z), self.edge_field(r, masks, tier, step, z))]
                self.keep(mapped, z, tier, step, value)
                self.frames(r, masks, tier, step, z, value, rows_m)

        self.sweep(forward)
        self.settle(rows_m)
        inner()
        self.map_columns(r, w, cols, cols_m, extra)
        self.edge_lines(r, flipped, rows_m)
        self.edges(r, flipped, cols_m.at[0], cols_m.at[1])

        def back(tier, step, masks, columns):
            out = [[-e for e in self.edge_field(r, masks, tier, step, z)] for z in range(self.depth)]
            finish(tier, step, masks, columns, self.circular_field(r, tier, step, mapped, True, out))

        self.sweep(back)

    def scalars_out(self, r, turn, count):
        lane = lax.broadcasted_iota(jnp.int32, (1, 128), 1)
        line = jnp.zeros((1, 128), jnp.float32)
        for k in range(count):
            whole = jnp.sum(jnp.sum(r.acc[k], 0, keepdims=True), -1, keepdims=True)
            line = jnp.where(lane == k, whole, line)
        r.line_part[turn] = line

    def scalars_in(self, r, turn, count):
        line = r.line_full[turn]
        return [jnp.broadcast_to(line[:, k : k + 1], (8, 128)) for k in range(count)]

    def run(self, r):
        Z = self.depth
        self.find_place()

        def w(a, b, c):
            return r.weights[a, b, c]

        barrier = pltpu.get_barrier_semaphore()

        for place in self.peers:
            pl.semaphore_signal(barrier, inc=1, device_id=place, device_id_type=MESH)

        def load(name):
            far = getattr(r, "far_" + name)
            far = far.at[self.me] if name == "frequencies" else far
            return pltpu.make_async_copy(far, getattr(r, name), r.loaded.at[r.inputs.index(name)])

        tables = [name for name in r.inputs if name.startswith("wave")]
        order = ["frequencies", "weights", "along", "point_spread"] + tables + ["measured", "upstream"]
        for name in order:
            load(name).start()
        load("frequencies").wait()
        for which in range(9):
            for part in range(2):
                r.across[which, part] = jnp.broadcast_to(
                    r.frequencies[part * self.bins : (part + 1) * self.bins, which : which + 1], (self.bins, 128)
                )
        load("along").wait()
        load("weights").wait()
        self.build_stencil(r, w)
        load("point_spread").wait()
        for name in tables:
            load(name).wait()
        self.point_spectra(r, r.point_spread[...])
        load("measured").wait()
        self.row_spectra(r, r.measured[0], r.sent_m)
        pl.semaphore_wait(barrier, self.nd - 1)
        self.point_start(r)
        self.spread_start(r, r.sent_m, r.got_m, 0)
        load("upstream").wait()
        self.row_spectra(r, r.upstream[0], r.sent_u)
        self.clear(r.rows_v0, r.rows_v1, r.rows_v2, r.rows_up, r.acc, r.taps)
        self.clear(r.cols_v0, r.cols_v1, r.cols_v2, r.cols_up)

        self.point_wait(r)
        self.column_spectra(r, r.got_p, r.wave_p)
        self.build_blur(r)
        self.spread_wait(r, r.sent_m, 0)
        self.spread_start(r, r.sent_u, r.got_u, 1, 0, self.cuts[0])
        self.column_spectra(r, r.got_m, r.wave)

        def start(tier, step, masks, columns):
            factor = self.factor(r.blur, tier, step)
            for z in range(Z):
                value = self.combine(masks, *self.load_wave(r.wave, z, tier, step))
                value = self.times(factor, value, True)
                self.keep(r.v0, z, tier, step, value)
                self.frames(r, masks, tier, step, z, value, r.rows_v0, columns)
            self.put_columns(r, 0, (0, 1), tier, step, columns)

        self.sweep(start)
        self.reduce_start(r, 0, [0, 1])
        self.settle(r.rows_v0)
        self.edge_lines(r, w, r.rows_v0)
        self.reduce_middle(r, 0, [0, 1])
        self.spread_start(r, r.sent_u, r.got_u, 1, self.cuts[0], self.cuts[1])
        self.turn_round(r, r.v0, r.m0, r.acc.at[0])
        self.reduce_end(r, 0, [0])
        self.unpack(r, 0, 0, r.cols_v0, False)
        self.spread_start(r, r.sent_u, r.got_u, 1, self.cuts[1], self.cuts[2])

        def inner_0():
            self.reduce_end(r, 0, [1])
            self.unpack(r, 0, 1, r.cols_v0, True)

        def first(tier, step, masks, columns, back):
            for z in range(Z):
                before = self.load(r.v0, z, tier, step)
                value = [g + b for g, b in zip(self.gained(r, tier, step, before), back[z])]
                self.keep(r.v1, z, tier, step, value)
                self.frames(r, masks, tier, step, z, value, r.rows_v1, columns)
                r.acc[1] += self.dot(masks, before, value)
                r.acc[2] += self.dot(masks, value, value)
            self.put_columns(r, 1, (0, 1), tier, step, columns)

        def plain(field):
            return lambda tier, step, z: self.load(field, z, tier, step)

        self.stencil_twice(
            r, w, r.cols_v0, r.m0, r.rows_m0, r.cols_m0, plain(r.m0), first, inner_0
        )
        self.reduce_start(r, 1, [0])
        self.scalars_out(r, 1, 3)
        self.reduce_start(r, 1, [1, 2])
        self.settle(r.rows_v1)
        self.edge_lines(r, w, r.rows_v1)
        self.reduce_middle(r, 1, [0, 1, 2])
        self.spread_start(r, r.sent_u, r.got_u, 1, self.cuts[2])
        self.turn_round(r, r.v1, r.m1)
        self.spread_wait(r, r.sent_u, 1)
        self.column_spectra(r, r.got_u, r.wave)

        def upper(tier, step, masks, columns):
            for z in range(Z):
                value = self.combine(masks, *self.load_wave(r.wave, z, tier, step))
                self.keep(r.up, z, tier, step, value)
                self.frames(r, masks, tier, step, z, value, r.rows_up, columns)
                r.acc[5] += self.dot(masks, value, self.load(r.v0, z, tier, step))
                r.acc[6] += self.dot(masks, value, self.load(r.v1, z, tier, step))
            self.put_columns(r, 2, (3, 4), tier, step, columns)

        self.clear(r.acc)
        self.sweep(upper)
        self.settle(r.rows_up)
        self.reduce_end(r, 1, [0])
        self.unpack(r, 1, 0, r.cols_v1, False)
        scalars = []

        def inner_1():
            self.reduce_end(r, 1, [1, 2])
            self.unpack(r, 1, 1, r.cols_v1, True)
            self.reduce_start(r, 2, [3, 4])
            scalars.extend(self.scalars_in(r, 1, 3))
            scalars.append(scalars[0] / scalars[1])

        def second(tier, step, masks, columns, back):
            for z in range(Z):
                before, value = (self.load(f, z, tier, step) for f in (r.v0, r.v1))
                after = [g + b for g, b in zip(self.gained(r, tier, step, value), back[z])]
                self.keep(r.v2, z, tier, step, after)
                self.frames(r, masks, tier, step, z, after, r.rows_v2, columns)
                step_0 = scalars[3]
                residual = [p - step_0 * q for p, q in zip(before, value)]
                image = [p - step_0 * q for p, q in zip(value, after)]
                for k, (p, q) in enumerate(
                    ((residual, residual), (residual, value), (residual, image), (image, value))
                ):
                    r.acc[k] += self.dot(masks, p, q)
            self.put_columns(r, 2, (0, 1), tier, step, columns)

        self.stencil_twice(
            r, w, r.cols_v1, r.m1, r.rows_m1, r.cols_m1, plain(r.m1), second, inner_1
        )
        norm_0, curve_0, image_0, step_0 = scalars
        self.scalars_out(r, 2, 7)
        self.reduce_start(r, 2, [2, 0, 1])
        self.settle(r.rows_v2)
        self.reduce_middle(r, 2, [3, 4, 2, 0, 1])
        self.turn_round(r, r.up, r.around)
        self.turn_round(r, r.v2, r.mw)
        self.reduce_end(r, 2, [3, 4])
        self.unpack(r, 2, 3, r.cols_up, False)
        self.unpack(r, 2, 4, r.cols_up, True)
        self.reduce_end(r, 2, [2, 0])
        self.unpack(r, 2, 0, r.cols_v2, False)

        norm_1, cross, inner, image_cross, unused, up_0, up_1 = self.scalars_in(r, 2, 7)
        up_residual = up_0 - step_0 * up_1
        ratio = norm_1 / norm_0
        curve_1 = inner + 2.0 * ratio * cross + ratio * ratio * curve_0
        step_1 = norm_1 / curve_1
        grad_step_1 = up_residual + ratio * up_0
        grad_curve_1 = -grad_step_1 * step_1 / curve_1
        grad_ratio = step_1 * up_0 + 2.0 * grad_curve_1 * (cross + ratio * curve_0)
        grad_norm = grad_step_1 / curve_1 + grad_ratio / norm_0
        grad_step_0 = (
            up_0 - step_1 * up_1 - 2.0 * grad_curve_1 * (image_cross + ratio * image_0) - 2.0 * grad_norm * cross
        )
        more = 1.0 + ratio
        g0 = grad_norm - grad_ratio * ratio / norm_0 + grad_step_0 / curve_0
        g1 = grad_curve_1 * more * more - 2.0 * grad_norm * step_0 - grad_step_0 * step_0 / curve_0
        g2 = -2.0 * grad_curve_1 * step_0 * more + grad_norm * step_0 * step_0
        g3 = grad_curve_1 * step_0 * step_0
        q0 = step_0 + step_1 * more
        q1 = -step_1 * step_0
        mix = (g1, 2.0 * g2, 2.0 * g3, q1)

        def mixed(*values):
            return sum(m * v for m, v in zip(mix[4 - len(values) :], values))

        def mix_columns(places):
            for x in places:
                for lane in range(self.lanes):
                    here = (x, slice(None), pl.ds(lane * 128, 128))
                    r.cols_w3[here] = mixed(r.cols_v2[here], r.cols_up[here])

        mix_columns((0, 3))
        for k in range(2):
            for part in range(2):
                for tier in range(self.tiers):
                    for z in range(Z):
                        here = (k, z, part, pl.ds(8 * tier, 8))
                        r.rows_w3[here] = mixed(r.rows_v2[here], r.rows_up[here])

        self.edge_lines(r, w, r.rows_w3)

        def inner_2():
            self.reduce_end(r, 2, [1])
            self.unpack(r, 2, 1, r.cols_v2, True)
            mix_columns((1, 2))

        def make(tier, step, z):
            values = [self.load(f, z, tier, step) for f in (r.v0, r.v1, r.v2, r.up)]
            self.keep(r.w3, z, tier, step, [mixed(*parts) for parts in zip(*values)])
            values = [self.load(f, z, tier, step) for f in (r.m0, r.m1, r.mw, r.around)]
            return [mixed(*parts) for parts in zip(*values)]

        def extra(here):
            return mix[0] * r.cols_m0[here] + mix[1] * r.cols_m1[here]

        scale = 1.0 / (self.rows * self.columns)

        def last(tier, step, masks, columns, back):
            factor = self.factor(r.blur, tier, step)
            here = pl.ds(8 * tier, 8)
            for z in range(Z):
                v0, v1, w3, up = (self.load(f, z, tier, step) for f in (r.v0, r.v1, r.w3, r.up))
                value = [
                    b + d + 2.0 * g0 * p + g1 * q + q0 * u
                    for b, d, p, q, u in zip(back[z], self.gained(r, tier, step, w3), v0, v1, up)
                ]
                value = self.separate(masks, self.times(factor, value))
                for part in range(2):
                    heavy = scale * self.beside(r, WEIGHT, part, tier)
                    for side in range(2):
                        r.wave[z, part, here, self.lane_slice(step, side)] = (
                            value[2 * part + side] * heavy * self.along(r, WEIGHT, step, side)
                        )

        self.stencil_twice(
            r, w, r.cols_w3, r.mw, r.rows_mw, r.cols_mw, make, last, inner_2, extra
        )
        self.column_values(r, r.wave, r.sent_o)
        middle = len(self.peers) // 2
        self.return_start(r, 0, middle)
        for k in range(2):
            for x in (0, 3):
                if k == 0:
                    r.cols_w3[x] = r.cols_w3[x] + self.blend(mix, r.cols_v0[x], r.cols_v1[x])
            r.rows_w3[k] = r.rows_w3[k] + self.blend(mix, r.rows_v0[k], r.rows_v1[k])
        self.tap_sums(r, 2.0 * g3)

        for place in self.peers:
            self.remote_to(r.tap_part, r.tap_slots.at[self.me], r.send_tap, r.recv_tap, place).start()
        self.return_start(r, middle, None)
        r.got_o[self.me] = r.sent_o[self.z, :, :, self.row_lanes(self.y)]
        r.tap_slots[self.me] = r.tap_part[...]
        others = pl.ds(0, self.nd - 1)
        self.arrived(r.got_o.at[others], r.recv_big.at[2])
        self.row_values(r, r.got_o, r.out)
        self.arrived(r.got_o.at[others], r.send_big.at[2])
        self.arrived(r.tap_slots.at[others], r.recv_tap)
        self.arrived(r.tap_slots.at[others], r.send_tap)
        lots = [r.tap_slots[k] for k in range(self.nd)]
        while len(lots) > 1:
            lots = [lots[k] + lots[k + 1] for k in range(0, len(lots) - 1, 2)] + lots[len(lots) // 2 * 2 :]
        line = jnp.broadcast_to(lots[0] / math.sqrt(self.depth * self.rows * self.columns), (8, 128))
        for a in range(3):
            for b in range(3):
                first = 9 * a + 3 * b
                turned = pltpu.roll(line, 128 - first, 1) if first else line
                r.tap_out[a, pl.ds(b, 1)] = turned[:1, :3]

    def blend(self, mix, one, two):
        return mix[0][:1, :1] * one + mix[1][:1, :1] * two

    def tap_sums(self, r, weight):
        Z = self.depth
        pairs = ((r.v0, r.mw, None), (r.w3, r.m0, None), (r.v1, r.m1, weight))

        def body(tier, step, masks, columns):
            corner = masks[2]
            sx = self.beside(r, SIN, 0, tier)
            gamma = [[None, None, None, None] for a in range(3)]
            for left, right, scale in pairs:
                x = [self.load(left, z, tier, step) for z in range(Z)]
                if scale is not None:
                    x = [[scale * item for item in value] for value in x]
                for z in range(Z):
                    m = self.load(right, z, tier, step)
                    for a in range(3):
                        if not 0 <= z + a - 1 < Z:
                            continue
                        v = x[z + a - 1]
                        for side in range(2):
                            vr, vi, mr, mi = (v[2 * side], v[2 * side + 1], m[2 * side], m[2 * side + 1])
                            p, q = (vr * mr, vi * mi)
                            terms = (jnp.where(corner, 0.5 * (p + q), p + q), jnp.where(corner, 0.5 * (p - q), p + q), vi * mr - vr * mi)
                            old = gamma[a][side]
                            gamma[a][side] = terms if old is None else [o + t for o, t in zip(old, terms)]
            for a in range(3):
                sums = [0.0] * 9
                for side in range(2):
                    cx = self.beside(r, COS, side, tier)
                    cy = jnp.broadcast_to(self.along(r, COS, step, 0), (8, 128))
                    sy = jnp.broadcast_to(self.along(r, SIN, step, 0), (8, 128))
                    if side:
                        cy = jnp.where(masks[0], cy, self.along(r, COS, step, 1))
                        sy = jnp.where(masks[0], sy, -sy)
                    near, far, turn = gamma[a][side]
                    items = (
                        near, near * cx, far * cy, far * cy * cx, near * sx * sy,
                        turn * sx, turn * sy, turn * cx * sy, turn * sx * cy,
                    )
                    sums = [s + item for s, item in zip(sums, items)]
                for k in range(9):
                    r.taps[9 * a + k] += sums[k]

        self.sweep(body)

        sides = (
            (r.rows_v0, r.cols_v0, r.rows_mw, r.cols_mw, None),
            (r.rows_w3, r.cols_w3, r.rows_m0, r.cols_m0, None),
            (r.rows_v1, r.cols_v1, r.rows_m1, r.cols_m1, weight),
        )
        zero = jnp.zeros((8, 128), jnp.float32)
        by_row = [[[zero] * 3 for k in range(2)] for a in range(3)]
        by_col = [[[zero] * 3 for k in range(2)] for a in range(3)]
        by_corner = [[[zero] * 2 for k in range(2)] for a in range(3)]
        for rows_x, cols_x, rows_m, cols_m, scale in sides:
            extra = 1.0 if scale is None else scale
            for tier in range(self.tiers):
                here = pl.ds(8 * tier, 8)
                heavy = self.beside(r, WEIGHT, 0, tier) * extra
                ca, cb = (self.beside(r, COS, part, tier) for part in range(2))
                s = self.beside(r, SIN, 0, tier)
                for k in range(2):
                    for z in range(Z):
                        ma, mb = (rows_m[k, z, part, here] for part in range(2))
                        for a in range(3):
                            if not 0 <= z + a - 1 < Z:
                                continue
                            xa, xb = (rows_x[1 - k, z + a - 1, part, here] for part in range(2))
                            p, q = (heavy * xa * ma, heavy * xb * mb)
                            terms = (p + q, p * ca + q * cb, heavy * s * (xa * mb - xb * ma))
                            by_row[a][k] = [o + t for o, t in zip(by_row[a][k], terms)]
            for k in range(2):
                col_x, col_m = (cols_x.at[0 if k else 3], cols_m.at[k])
                for step in range(self.steps):
                    (xc, xs), (mc, ms) = (
                        [ref[:, pl.ds(part * self.half + 128 * step, 128)] * (extra if ref is col_x else 1.0) for part in range(2)]
                        for ref in (col_x, col_m)
                    )
                    heavy = self.along(r, WEIGHT, step, 0)
                    cc, cs = (self.along(r, COS, step, part) for part in range(2))
                    s = self.along(r, SIN, step, 0)
                    for a in range(3):
                        xc_a, xs_a = (self.shifted(item, a - 1) for item in (xc, xs))
                        p, q = (heavy * xc_a * mc, heavy * xs_a * ms)
                        terms = (p + q, p * cc + q * cs, heavy * s * (xc_a * ms - xs_a * mc))
                        by_col[a][k] = [o + t for o, t in zip(by_col[a][k], terms)]
                at_x, at_m = (self.corners(r, ref[...]) for ref in (col_x, col_m))
                for a in range(3):
                    for edge in range(2):
                        term = extra * self.shifted(at_x[1 - edge], a - 1) * at_m[edge]
                        by_corner[a][edge][k] = by_corner[a][edge][k] + term

        lots = []
        for a in range(3):
            s = [r.taps[9 * a + k] for k in range(9)]
            for b in range(3):
                for c in range(3):
                    beta, gamma = (float(b - 1), float(c - 1))
                    if b == 1 and c == 1:
                        value = s[0]
                    elif b == 1:
                        value = s[1] - gamma * s[5]
                    elif c == 1:
                        value = s[2] - beta * s[6]
                    else:
                        value = s[3] - beta * gamma * s[4] - beta * s[7] - gamma * s[8]
                    value = value * (2.0 / (self.rows * self.columns))
                    if b != 1:
                        one, two, three = by_row[a][b // 2]
                        value = value - (one if c == 1 else two - gamma * three) * (1.0 / (128 * self.columns))
                    if c != 1:
                        one, two, three = by_col[a][c // 2]
                        value = value - (one if b == 1 else two - beta * three) * (1.0 / (self.rows * self.nd))
                    if b != 1 and c != 1:
                        value = value + by_corner[a][b // 2][c // 2] * (1.0 / (128 * self.nd))
                    lots.append(value)
        lane = lax.broadcasted_iota(jnp.int32, (1, 128), 1)
        line = jnp.zeros((1, 128), jnp.float32)
        for k, value in enumerate(lots):
            whole = jnp.sum(jnp.sum(value, 0, keepdims=True), -1, keepdims=True)
            line = jnp.where(lane == k, whole, line)
        r.tap_part[...] = line


class Refs:
    def __init__(self, names, refs):
        for name, ref in zip(names, refs):
            setattr(self, name, ref)


def spectral(measured, point_spread, stencil_weights, upstream):
    planes, row_count, columns = measured.shape
    plan = Spectral(lax.axis_size("gy"), lax.axis_size("gz"), planes, row_count, columns)
    waves = [jnp.asarray(part) for part in wave_rows(columns)]
    if plan.rows != columns:
        waves += [jnp.asarray(part) for part in wave_rows(plan.rows)]
    along = jnp.asarray(axis_values(plan.rows).reshape(9, 1, plan.rows))
    across = axis_values(columns).reshape(9, 2, plan.nd, plan.bins).transpose(2, 1, 3, 0)
    frequencies = np.zeros((plan.nd, 2 * plan.bins, 128), np.float32)
    frequencies[:, :, :9] = across.reshape(plan.nd, 2 * plan.bins, 9)
    scratch = plan.scratch()
    arrays = dict(weights=stencil_weights, measured=measured, point_spread=point_spread, upstream=upstream, along=along)
    arrays.update({"wave_%d" % k: part for k, part in enumerate(waves)})
    arrays["frequencies"] = jnp.asarray(frequencies)
    for name, array in arrays.items():
        shape = array.shape[1:] if name == "frequencies" else array.shape
        space = pltpu.SMEM if name == "weights" else pltpu.VMEM
        scratch[name] = space(shape, array.dtype)
    scratch["loaded"] = pltpu.SemaphoreType.DMA((len(arrays),))
    names = ["far_" + name for name in arrays] + ["out", "tap_out"] + list(scratch)

    def body(*refs):
        r = Refs(names, refs)
        r.tab_x = (r.wave_0, r.wave_1)
        r.tab_y = (r.wave_2, r.wave_3) if len(waves) > 2 else r.tab_x
        r.inputs = list(arrays)
        plan.run(r)

    out, taps = pl.pallas_call(
        body,
        out_shape=(
            jax.ShapeDtypeStruct(measured.shape, jnp.float32),
            jax.ShapeDtypeStruct((3, 3, 3), jnp.float32),
        ),
        in_specs=[HBM] * len(arrays),
        out_specs=(VMEM, VMEM),
        scratch_shapes=list(scratch.values()),
        compiler_params=pltpu.CompilerParams(
            collective_id=0, has_side_effects=True, vmem_limit_bytes=32 * 1024 * 1024
        ),
        name="spectral",
    )(
        *(pltpu.with_memory_space_constraint(array, pltpu.HBM) for array in arrays.values())
    )
    return (out, taps)


def solution(mesh):
    def program(measured, point_spread, stencil_weights, upstream):
        planes, row_count, columns = measured.shape
        fits = spectral_fits(mesh.shape["gy"], mesh.shape["gz"], planes, row_count, columns)
        chosen = spectral if fits else local
        return chosen(measured, point_spread, stencil_weights, upstream)

    return jax.shard_map(
        program,
        mesh=mesh,
        in_specs=(P("gz", "gy", None), P("gy", None), P(), P("gz", "gy", None)),
        out_specs=(P("gz", "gy", None), P()),
        check_vma=False,
    )
```

```python
import math

import jax
import jax.numpy as jnp
import numpy as np
from jax import lax
from jax.experimental import pallas as pl
from jax.experimental.pallas import tpu as pltpu
from jax.sharding import PartitionSpec as P

MESH = pl.DeviceIdType.MESH
SIDES = [(dy, dz) for dy in (-1, 0, 1) for dz in (-1, 0, 1) if (dy, dz) != (0, 0)]
VMEM = pl.BlockSpec(memory_space=pltpu.VMEM)
SMEM = pl.BlockSpec(memory_space=pltpu.SMEM)
HBM = pl.BlockSpec(memory_space=pltpu.HBM)


def moved(value, shift):
    if shift == 0:
        return value
    width = value.shape[1]
    lane = lax.broadcasted_iota(jnp.int32, value.shape, 1)
    edge = 0 if shift > 0 else width - 1
    return jnp.where(lane == edge, 0.0, pltpu.roll(value, shift % width, 1))


def regular_kernel(count_y, count_z, weights, volume, back, grown, mapped, shifted, send, receive):
    rows, columns = volume.shape
    y, z = (lax.axis_index("gy"), lax.axis_index("gz"))

    def there(dy, dz):
        return (y + dy >= 0) & (y + dy < count_y) & (z + dz >= 0) & (z + dz < count_z)

    barrier = pltpu.get_barrier_semaphore()
    for dy, dz in SIDES:

        @pl.when(there(dy, dz))
        def _():
            pl.semaphore_signal(barrier, inc=1, device_id=(y + dy, z + dz), device_id_type=MESH)

    def span(place, count):
        return 1 + jnp.where(place > 0, 1, 0) + jnp.where(place < count - 1, 1, 0)

    pl.semaphore_wait(barrier, span(y, count_y) * span(z, count_z) - 1)

    def copy(field, phase, number):
        dy, dz = SIDES[number]
        source = field.at[1, pl.ds(rows if dy > 0 else 8, 8 if dy else rows)]
        start = 8 if dy == 0 else 0 if dy > 0 else rows + 8
        return pltpu.make_async_remote_copy(
            src_ref=source,
            dst_ref=field.at[1 - dz, pl.ds(start, 8 if dy else rows)],
            send_sem=send.at[phase, number],
            recv_sem=receive.at[phase, number],
            device_id=(y + dy, z + dz),
            device_id_type=MESH,
        )

    def exchange(field, phase):
        for number, (dy, dz) in enumerate(SIDES):

            @pl.when(there(dy, dz))
            def _():
                copy(field, phase, number).start()

        for number, (dy, dz) in enumerate(SIDES):
            start = 8 if dy == 0 else 0 if dy > 0 else rows + 8

            @pl.when(jnp.logical_not(there(-dy, -dz)))
            def _():
                field[1 - dz, pl.ds(start, 8 if dy else rows)] = jnp.zeros(
                    (8 if dy else rows, columns), jnp.float32
                )

        for number, (dy, dz) in enumerate(SIDES):

            @pl.when(there(-dy, -dz))
            def _():
                copy(field, phase, number).wait_recv()

            @pl.when(there(dy, dz))
            def _():
                copy(field, phase, number).wait_send()

    def apply(field, flip, put):
        def weight(a, b, c):
            return weights[26 - (9 * a + 3 * b + c) if flip else 9 * a + 3 * b + c]

        @pl.loop(0, (rows + 16) // 8)
        def _(step):
            here = pl.ds(pl.multiple_of(step * 8, 8), 8)
            sums = [None] * 3
            for a in range(3):
                value = field[a, here]
                for c in range(3):
                    turned = moved(value, 1 - c)
                    for b in range(3):
                        term = weight(a, b, c) * turned
                        sums[b] = term if sums[b] is None else sums[b] + term
            for b in range(3):
                shifted[b, here] = sums[b]

        @pl.loop(0, rows // 8)
        def _(step):
            first = pl.multiple_of(step * 8, 8)
            around = pl.ds(first, 24)
            total = shifted[1, pl.ds(first + 8, 8)]
            total = total + shifted[0, around][7:15] + shifted[2, around][9:17]
            put(first, total)

    @pl.loop(0, rows // 8)
    def _(step):
        first = pl.multiple_of(step * 8, 8)
        grown[1, pl.ds(first + 8, 8)] = volume[pl.ds(first, 8)]

    exchange(grown, 0)

    def put_mapped(first, total):
        mapped[1, pl.ds(first + 8, 8)] = total

    apply(grown, False, put_mapped)
    exchange(mapped, 1)

    def put_back(first, total):
        back[pl.ds(first, 8)] = total

    apply(mapped, True, put_back)


def regular(volume, kernel):
    rows, columns = volume.shape[1:]
    count_y, count_z = (lax.axis_size("gy"), lax.axis_size("gz"))
    field = jax.ShapeDtypeStruct((3, rows + 16, columns), jnp.float32)

    def body(*refs):
        regular_kernel(count_y, count_z, *refs)

    back, grown, mapped = pl.pallas_call(
        body,
        out_shape=(jax.ShapeDtypeStruct((rows, columns), jnp.float32), field, field),
        in_specs=[SMEM, VMEM],
        out_specs=(VMEM, VMEM, VMEM),
        scratch_shapes=[
            pltpu.VMEM((3, rows + 16, columns), jnp.float32),
            pltpu.SemaphoreType.DMA((2, 8)),
            pltpu.SemaphoreType.DMA((2, 8)),
        ],
        cost_estimate=pl.CostEstimate(flops=120 * rows * columns, bytes_accessed=20 * rows * columns, transcendentals=0),
        compiler_params=pltpu.CompilerParams(collective_id=0, has_side_effects=True),
        name="regular",
    )(kernel.reshape(27), volume[0])
    return (back[None], grown, mapped)


def total_kernel(count_y, count_z, value, out, column, row, across, send, receive):
    y, z = (lax.axis_index("gy"), lax.axis_index("gz"))
    along_y = [(lax.rem(y + k, count_y), z) for k in range(1, count_y)]
    along_z = [(y, lax.rem(z + k, count_z)) for k in range(1, count_z)]
    barrier = pltpu.get_barrier_semaphore()
    for place in along_y + along_z:
        pl.semaphore_signal(barrier, inc=1, device_id=place, device_id_type=MESH)
    pl.semaphore_wait(barrier, count_y + count_z - 2)

    def gather(source, slots, places, base):
        copies = []
        for k, place in enumerate(places):
            copies.append(
                pltpu.make_async_remote_copy(
                    src_ref=source,
                    dst_ref=slots.at[k],
                    send_sem=send.at[base + k],
                    recv_sem=receive.at[base + k],
                    device_id=place,
                    device_id_type=MESH,
                )
            )
            copies[-1].start()
        for item in copies:
            item.wait()

    def ordered(own, slots, index, count):
        total = jnp.zeros_like(own)
        for j in range(count):
            term = own
            for k in range(1, count):
                term = jnp.where(lax.rem(index - j + count, count) == k, slots[k - 1], term)
            total = total + term
        return total

    gather(value, column, along_y, 0)
    across[...] = ordered(value[...], column, y, count_y)
    gather(across, row, along_z, count_y - 1)
    out[...] = ordered(across[...], row, z, count_z)


def total(values, collective):
    count_y, count_z = (lax.axis_size("gy"), lax.axis_size("gz"))
    count = values.shape[0]

    def body(*refs):
        total_kernel(count_y, count_z, *refs)

    block = jnp.broadcast_to(jnp.pad(values, (0, 128 - count))[None], (8, 128))
    copies = count_y + count_z - 2
    summed = pl.pallas_call(
        body,
        out_shape=jax.ShapeDtypeStruct((8, 128), jnp.float32),
        in_specs=[VMEM],
        out_specs=VMEM,
        scratch_shapes=[
            pltpu.VMEM((count_y - 1, 8, 128), jnp.float32),
            pltpu.VMEM((count_z - 1, 8, 128), jnp.float32),
            pltpu.VMEM((8, 128), jnp.float32),
            pltpu.SemaphoreType.DMA((copies,)),
            pltpu.SemaphoreType.DMA((copies,)),
        ],
        compiler_params=pltpu.CompilerParams(collective_id=collective, has_side_effects=True),
        name="total",
    )(block)
    return summed[0, :count]


def correlate_kernel(scalars, grown_0, grown_1, grown_2, grown_up, mapped_0, mapped_1, mapped_2, mapped_up, out):
    rows = grown_0.shape[1] - 16
    columns = grown_0.shape[2]
    c_up, c_zero, c_one, c_two, d_zero, d_one, s_zero, s_grad, s_direction = (scalars[k] for k in range(9))
    out[...] = jnp.zeros_like(out)

    @pl.loop(0, rows // 8)
    def _(step):
        first = pl.multiple_of(step * 8, 8)
        here = pl.ds(first + 8, 8)
        zero, one = (mapped_0[1, here], mapped_1[1, here])
        grad = c_up * mapped_up[1, here] + c_zero * zero + c_one * one + c_two * mapped_2[1, here]
        values = (
            s_zero * zero + s_grad * grad,
            s_grad * zero,
            s_direction * (d_zero * zero + d_one * one),
        )
        turned = [[moved(value, c - 1) for value in values] for c in range(3)]
        for a in range(3):
            around = pl.ds(first, 24)
            full_0, full_1 = (grown_0[a, around], grown_1[a, around])
            full_grad = c_up * grown_up[a, around] + c_zero * full_0 + c_one * full_1 + c_two * grown_2[a, around]
            full_direction = d_zero * full_0 + d_one * full_1
            for b in range(3):
                fields = [item[7 + b : 15 + b] for item in (full_0, full_grad, full_direction)]
                for c in range(3):
                    product = turned[c][0] * fields[0] + turned[c][1] * fields[1] + turned[c][2] * fields[2]
                    folded = product[:, :128]
                    for part in range(1, columns // 128):
                        folded = folded + product[:, 128 * part : 128 * part + 128]
                    out[9 * a + 3 * b + c] += folded


def correlate(scalars, *fields):
    return pl.pallas_call(
        correlate_kernel,
        out_shape=jax.ShapeDtypeStruct((27, 8, 128), jnp.float32),
        in_specs=[SMEM] + [VMEM] * 8,
        out_specs=VMEM,
        cost_estimate=pl.CostEstimate(flops=40000000, bytes_accessed=8000000, transcendentals=0),
        name="correlate",
    )(scalars, *fields).sum((1, 2))


def contract(form, left, right):
    return jnp.einsum(form, left, right, precision=lax.Precision.HIGH)


def wave_tables(length, groups):
    half = length // 2
    bins = half // groups
    pair = groups // 2
    shape = (half, pair, 2, bins)
    place = lax.broadcasted_iota(jnp.int32, shape, 0)
    part = lax.broadcasted_iota(jnp.int32, shape, 2)
    slot = lax.broadcasted_iota(jnp.int32, shape, 1) * bins + lax.broadcasted_iota(jnp.int32, shape, 3)
    tables = []
    for odd in range(2):
        frequency = 2 * slot + odd
        steps = place * frequency + part * (length // 4)
        if not odd:
            steps = jnp.where((slot == 0) & (part == 1), place * half, steps)
        angle = (steps % length).astype(jnp.float32) * (2.0 * math.pi / length)
        tables.append(jnp.cos(angle).reshape(half, pair, 2 * bins))
    return tables


def combine(raw, on_row, on_lane):
    even, odd = raw
    a, b, c, d = (
        jnp.concatenate([piece[:, part, :, :, side] for piece in (even, odd)], 0)
        for part, side in ((0, 0), (0, 1), (1, 0), (1, 1))
    )
    special = on_row | on_lane
    plus_real = jnp.where(special, a, a - d)
    plus_imaginary = jnp.where(on_row, b, jnp.where(on_lane, c, b + c))
    minus_real = jnp.where(on_row, c, jnp.where(on_lane, b, a + d))
    minus_imaginary = jnp.where(special, d, b - c)
    return (jnp.stack([plus_real, minus_real]), jnp.stack([plus_imaginary, minus_imaginary]))


def separate(spectrum, on_row, on_lane):
    (plus_real, minus_real), (plus_imaginary, minus_imaginary) = spectrum
    special = on_row | on_lane
    a = jnp.where(special, plus_real, plus_real + minus_real)
    d = jnp.where(special, minus_imaginary, minus_real - plus_real)
    b = jnp.where(on_row, plus_imaginary, jnp.where(on_lane, minus_real, plus_imaginary + minus_imaginary))
    c = jnp.where(on_row, minus_real, jnp.where(on_lane, plus_imaginary, plus_imaginary - minus_imaginary))
    scale = jnp.where(on_row & on_lane, 1.0, 2.0)
    a, b, c, d = (value * scale for value in (a, b, c, d))
    whole = jnp.stack([jnp.stack([a, b], 3), jnp.stack([c, d], 3)], 1)
    pair = whole.shape[0] // 2
    return (whole[:pair], whole[pair:])


def times(left, right, corner, conjugate=False):
    (a, b), (c, d) = (left, right)
    cross = b * d
    sign = -1.0 if conjugate else 1.0
    real = jnp.where(corner, a * c, a * c - sign * cross)
    imaginary = jnp.where(corner, cross, sign * a * d + b * c)
    return (real, imaginary)


def linear(*terms):
    total_real = total_imaginary = 0.0
    for scale, (real, imaginary) in terms:
        scale_real, scale_imaginary = scale if isinstance(scale, tuple) else (scale, scale)
        total_real = total_real + scale_real * real
        total_imaginary = total_imaginary + scale_imaginary * imaginary
    return (total_real, total_imaginary)


def local(measured, point_spread, stencil_weights, upstream):
    planes, row_count, columns = measured.shape
    groups = lax.axis_size("gy")
    rows = row_count * groups
    cells = planes * rows * columns * lax.axis_size("gz")
    bins = columns // 2 // groups
    even_x, odd_x = wave_tables(columns, groups)
    even_y, odd_y = (even_x, odd_x) if rows == columns else wave_tables(rows, groups)
    y_bins = rows // 2 // groups
    spectral = (groups, y_bins, 1, bins)
    on_row = (lax.broadcasted_iota(jnp.int32, spectral, 0) == 0) & (
        lax.broadcasted_iota(jnp.int32, spectral, 1) == 0
    )
    on_lane = (lax.broadcasted_iota(jnp.int32, spectral, 3) == 0) & (lax.axis_index("gy") == 0)
    corner = on_row & on_lane

    def forward(volumes):
        count = volumes.shape[0]
        low, high = (volumes[:, :, : columns // 2], volumes[:, :, columns // 2 :])
        sent = jnp.concatenate(
            [contract("vrj,jdl->drvl", low + high, even_x), contract("vrj,jdl->drvl", low - high, odd_x)], 0
        )
        arrived = lax.all_to_all(
            sent.reshape(groups, row_count, count * 2 * bins), "gy", split_axis=0, concat_axis=0, tiled=True
        )
        arrived = arrived.reshape(rows, count * 2 * bins)
        low, high = (arrived[: rows // 2], arrived[rows // 2 :])
        raw = [
            contract("jds,jl->dsl", table, value).reshape(groups // 2, 2, y_bins, count, 2, bins)
            for table, value in ((even_y, low + high), (odd_y, low - high))
        ]
        return combine(raw, on_row, on_lane)

    def inverse(spectrum):
        count = spectrum[0].shape[3]
        pieces = separate(spectrum, on_row, on_lane)
        one, two = (
            contract("jds,dsl->jl", table, piece.reshape(groups // 2, 2 * y_bins, count * 2 * bins))
            for table, piece in ((even_y, pieces[0]), (odd_y, pieces[1]))
        )
        sent = jnp.concatenate([one + two, one - two], 0).reshape(groups, row_count, count * 2 * bins)
        arrived = lax.all_to_all(sent, "gy", split_axis=0, concat_axis=0, tiled=True)
        arrived = arrived.reshape(groups, row_count, count, 2 * bins)
        one = contract("drvl,jdl->vrj", arrived[: groups // 2], even_x)
        two = contract("drvl,jdl->vrj", arrived[groups // 2 :], odd_x)
        return jnp.concatenate([one + two, one - two], 2) / float(rows * columns)

    def pick(spectrum, start, count):
        return tuple(lax.slice_in_dim(part, start, start + count, axis=3) for part in spectrum)

    def join(*spectra):
        return tuple(jnp.concatenate(parts, 3) for parts in zip(*spectra))

    spectra = forward(jnp.concatenate([point_spread[None], measured], 0))
    transfer = pick(spectra, 0, 1)
    squares = (transfer[0] ** 2, transfer[1] ** 2)
    gain = (
        jnp.where(corner, squares[0], squares[0] + squares[1]),
        jnp.where(corner, squares[1], squares[0] + squares[1]),
    )
    spectrum_0 = times(pick(spectra, 1, planes), transfer, corner, True)
    blurred_0 = linear((gain, spectrum_0))
    pair = inverse(join(spectrum_0, blurred_0))
    vector_0 = pair[:planes]
    back_0, grown_0, mapped_0 = regular(vector_0, stencil_weights)
    back_up, grown_up, mapped_up = regular(upstream, stencil_weights)
    vector_1 = pair[planes:] + back_0
    spectrum_1 = linear((1.0, blurred_0), (1.0, forward(back_0)))
    blurred_1 = linear((gain, spectrum_1))
    early = forward(jnp.concatenate([upstream, back_up], 0))
    back_1, grown_1, mapped_1 = regular(vector_1, stencil_weights)
    vector_2 = inverse(blurred_1) + back_1
    norm_0, curve_0, image_0, up_0, up_1 = total(
        jnp.stack(
            [
                jnp.sum(vector_0 * vector_0),
                jnp.sum(vector_0 * vector_1),
                jnp.sum(vector_1 * vector_1),
                jnp.sum(upstream * vector_0),
                jnp.sum(upstream * vector_1),
            ]
        ),
        1,
    )
    step_0 = norm_0 / curve_0
    residual = vector_0 - step_0 * vector_1
    residual_image = vector_1 - step_0 * vector_2
    norm_1, cross, inner, up_residual, image_cross = total(
        jnp.stack(
            [
                jnp.sum(residual * residual),
                jnp.sum(residual * vector_1),
                jnp.sum(residual * residual_image),
                jnp.sum(upstream * residual),
                jnp.sum(residual_image * vector_1),
            ]
        ),
        2,
    )
    back_2, grown_2, mapped_2 = regular(vector_2, stencil_weights)
    late = forward(jnp.concatenate([back_1, back_2], 0))
    ratio = norm_1 / norm_0
    curve_1 = inner + 2.0 * ratio * cross + ratio * ratio * curve_0
    step_1 = norm_1 / curve_1
    grad_step_1 = up_residual + ratio * up_0
    grad_curve_1 = -grad_step_1 * step_1 / curve_1
    grad_ratio = step_1 * up_0 + 2.0 * grad_curve_1 * (cross + ratio * curve_0)
    known_image = step_1 * up_1 + 2.0 * grad_curve_1 * (image_cross + ratio * image_0)
    grad_norm = grad_step_1 / curve_1 + grad_ratio / norm_0
    grad_step_0 = up_0 - known_image - 2.0 * grad_norm * cross
    grad_curve_0 = -grad_step_0 * step_0 / curve_0
    grad_norm_0 = -grad_ratio * ratio / norm_0 + grad_step_0 / curve_0

    spectrum_2 = linear((1.0, linear((gain, spectrum_1))), (1.0, pick(late, 0, planes)))
    spectrum_up = pick(early, 0, planes)
    residual_terms = ((1.0, spectrum_0), (-step_0, spectrum_1))
    direction_image = linear((1.0 + ratio, spectrum_1), (-step_0, spectrum_2))
    grad_direction = linear((step_1, spectrum_up), (2.0 * grad_curve_1, direction_image))
    grad_residual = linear((1.0, grad_direction), (2.0 * grad_norm, linear(*residual_terms)))
    grad_back = linear(
        (step_1, pick(early, planes, planes)),
        (2.0 * grad_curve_1 * (1.0 + ratio) - 2.0 * grad_norm * step_0, pick(late, 0, planes)),
        (-2.0 * grad_curve_1 * step_0, pick(late, planes, planes)),
        (2.0 * grad_norm, linear((1.0, spectrum_1), (-1.0, blurred_0))),
    )
    grad_right = linear(
        (step_0, spectrum_up),
        (ratio, grad_direction),
        (2.0 * grad_curve_0, spectrum_1),
        (2.0 * grad_norm_0, spectrum_0),
        (1.0, grad_residual),
        (-step_0, linear((gain, grad_residual), (1.0, grad_back))),
    )
    grad_measured = inverse(times(grad_right, transfer, corner))

    terms = correlate(
        jnp.stack(
            [
                step_1,
                2.0 * grad_norm,
                2.0 * grad_curve_1 * (1.0 + ratio) - 2.0 * grad_norm * step_0,
                -2.0 * grad_curve_1 * step_0,
                1.0 + ratio,
                -step_0,
                2.0 * grad_curve_0,
                -step_0,
                2.0 * grad_curve_1,
            ]
        ),
        grown_0, grown_1, grown_2, grown_up, mapped_0, mapped_1, mapped_2, mapped_up,
    )
    grad_stencil = total(terms, 3).reshape(3, 3, 3) / math.sqrt(cells)
    return (grad_measured, grad_stencil)


def spectral_fits(mesh_y, mesh_z, planes, row_count, columns):
    devices, rows, depth = (mesh_y * mesh_z, row_count * mesh_y, planes * mesh_z)
    if columns % (16 * devices) or row_count % 128 or rows % 512 or planes != 1 or mesh_z % 2:
        return False
    tiles = 2 * depth // 8 * (rows // 128)
    return depth == 4 and mesh_y % 4 == 0 and tiles % (2 * mesh_z) == 0


def wave_rows(length):
    half, quarter = (length // 2, length // 4)
    place = np.arange(half)[None, :]
    tables = []
    for odd in range(2):
        frequency = 2 * np.arange(quarter)[:, None] + odd
        angle = (place * frequency % length) * (2.0 * np.pi / length)
        cosine, sine = (np.cos(angle), np.sin(angle))
        if not odd:
            sine[0] = np.cos(np.pi * place[0])
        tables += [cosine, sine]
    table = np.stack(tables)
    high = table.astype(jnp.bfloat16)
    low = (table - high.astype(np.float64)).astype(jnp.bfloat16)
    return (high, low)


def basis(length, place):
    half = length // 2
    frequency = np.concatenate([np.arange(0, half, 2), np.arange(1, half, 2)])
    angle = frequency * place % length * (2.0 * np.pi / length)
    cosine, sine = (np.cos(angle), np.sin(angle))
    sine[0] = np.cos(np.pi * place)
    return (cosine, sine)


def axis_values(length):
    cosine, sine = basis(length, 1)
    pure = sine.copy()
    pure[0] = 0.0
    other = cosine.copy()
    other[0] = -1.0
    weight = np.full(length // 2, 2.0)
    weight[0] = 1.0
    values = [(cosine, other), (pure, pure), basis(length, 0), basis(length, length - 1), (weight, weight)]
    for place in (0, 1, length - 2, length - 1):
        values.append(tuple(weight * part / length for part in basis(length, place)))
    return np.stack([np.stack(pair) for pair in values]).astype(np.float32)


COS, SIN, FIRST, LAST, WEIGHT, AT = range(6)


def split(value):
    high = value.astype(jnp.bfloat16)
    return (high, (value - high.astype(jnp.float32)).astype(jnp.bfloat16))


def product(left, right, contracting):
    numbers = (contracting, ((), ()))

    def one(a, b):
        return lax.dot_general(a, b, numbers, preferred_element_type=jnp.float32)

    return one(left[0], right[0]) + (one(left[0], right[1]) + one(left[1], right[0]))


class Spectral:
    def __init__(self, count_y, count_z, planes, row_count, columns):
        self.ny, self.nz = (count_y, count_z)
        self.nd = count_y * count_z
        self.depth = planes * count_z
        self.row_count = row_count
        self.rows = row_count * count_y
        self.columns = columns
        self.bins = columns // 2 // self.nd
        self.half = self.rows // 2
        self.steps = self.half // 128
        self.tiers = self.bins // 8
        self.lanes = self.rows // 128
        self.tiles = 2 * self.depth // 8 * self.lanes
        self.share = self.tiles // (2 * self.nz)

    def place_of(self, index):
        return (lax.rem(index, self.ny), lax.div(index, self.ny))

    def find_place(self):
        self.y, self.z = (lax.axis_index("gy"), lax.axis_index("gz"))
        self.me = self.z * self.ny + self.y

        def turned(place, count):
            moved = [place + k for k in range(count)]
            return [jnp.where(item >= count, item - count, item) for item in moved]

        ys, zs = (turned(self.y, self.ny), turned(self.z, self.nz))
        far = sorted(range(self.ny), key=lambda k: -min(k, self.ny - k))
        self.cuts = (self.nd // 16, self.nd // 2, self.nd * 7 // 8)
        self.peers = [(ys[a], zs[b]) for a in far for b in reversed(range(self.nz)) if a or b]

    def remote_to(self, source, target, send, receive, place):
        return pltpu.make_async_remote_copy(
            src_ref=source, dst_ref=target, send_sem=send, recv_sem=receive, device_id=place, device_id_type=MESH
        )

    def scratch(self):
        Z, bins, half, nd = (self.depth, self.bins, self.half, self.nd)
        packed = (Z, 2, bins, self.rows)
        field = (Z, 4, bins, half)
        edge = (2, Z, 2, bins, 128)
        F = jnp.float32
        D = pltpu.SemaphoreType.DMA
        others = nd - 1
        names = dict(
            sent_m=pltpu.VMEM((nd, 2, bins, 128 * (self.row_count // 128)), F),
            sent_u=pltpu.VMEM((nd, 2, bins, self.row_count), F),
            sent_p=pltpu.VMEM((self.ny, 2, bins, self.row_count), F),
            got_m=pltpu.VMEM(packed, F),
            got_u=pltpu.VMEM(packed, F),
            got_p=pltpu.VMEM((2, bins, self.rows), F),
            wave=pltpu.VMEM(packed, F),
            wave_p=pltpu.VMEM((2, bins, self.rows), F),
            v0=pltpu.VMEM(field, F),
            v1=pltpu.VMEM(field, F),
            v2=pltpu.VMEM(field, F),
            up=pltpu.VMEM(field, F),
            w3=pltpu.VMEM(field, F),
            m0=pltpu.VMEM(field, F),
            m1=pltpu.VMEM(field, F),
            mw=pltpu.VMEM(field, F),
            stencil=pltpu.VMEM((3, 2, 3, bins, half), F),
            blur=pltpu.VMEM((2, 3, bins, half), F),
            gain=pltpu.VMEM((2, 2, bins, half), F),
            across=pltpu.VMEM((9, 2, bins, 128), F),
            rows_v0=pltpu.VMEM(edge, F),
            rows_v1=pltpu.VMEM(edge, F),
            rows_v2=pltpu.VMEM(edge, F),
            rows_up=pltpu.VMEM(edge, F),
            rows_w3=pltpu.VMEM(edge, F),
            rows_m0=pltpu.VMEM(edge, F),
            rows_m1=pltpu.VMEM(edge, F),
            rows_mw=pltpu.VMEM(edge, F),
            edge_rows=pltpu.VMEM(edge, F),
            cols_v0=pltpu.VMEM((4, 8, self.rows), F),
            cols_v1=pltpu.VMEM((4, 8, self.rows), F),
            cols_v2=pltpu.VMEM((4, 8, self.rows), F),
            cols_up=pltpu.VMEM((4, 8, self.rows), F),
            cols_w3=pltpu.VMEM((4, 8, self.rows), F),
            cols_m0=pltpu.VMEM((2, 8, self.rows), F),
            cols_m1=pltpu.VMEM((2, 8, self.rows), F),
            cols_mw=pltpu.VMEM((2, 8, self.rows), F),
            edge_cols=pltpu.VMEM((2, 8, self.rows), F),
            part=pltpu.VMEM((3, 5, self.tiles, 8, 128), F),
            slots=pltpu.VMEM((3, 5, others, self.share, 8, 128), F),
            sums=pltpu.VMEM((3, 5, self.share, 8, 128), F),
            full=pltpu.VMEM((3, 5, self.tiles, 8, 128), F),
            line_part=pltpu.VMEM((3, 1, 128), F),
            line_slots=pltpu.VMEM((3, others, 1, 128), F),
            line_sums=pltpu.VMEM((3, 1, 128), F),
            line_full=pltpu.VMEM((3, 1, 128), F),
            around=pltpu.VMEM(field, F),
            acc=pltpu.VMEM((8, 8, 128), F),
            turned=pltpu.VMEM((2, 4, half, half // 2), jnp.bfloat16),
            taps=pltpu.VMEM((27, 8, 128), F),
            tap_part=pltpu.VMEM((1, 128), F),
            tap_slots=pltpu.VMEM((nd, 1, 128), F),
            sent_o=pltpu.VMEM(packed, F),
            got_o=pltpu.VMEM((nd, 2, bins, self.row_count), F),
            send_big=D((4,)),
            recv_big=D((4,)),
            send_p=D,
            recv_p=D,
            send_part=D((2, 5)),
            recv_part=D((2, 5)),
            send_full=D((2, 5)),
            recv_full=D((2, 5)),
            send_tap=D,
            recv_tap=D,
        )
        return names


    def remote(self, source, target, send, receive, peer):
        return pltpu.make_async_remote_copy(
            src_ref=source, dst_ref=target, send_sem=send, recv_sem=receive,
            device_id=self.place_of(peer), device_id_type=MESH,
        )

    def arrived(self, shape, semaphore):
        self.remote(shape, shape, semaphore, semaphore, self.me).wait_recv()

    def row_lanes(self, y):
        return pl.ds(pl.multiple_of(y * self.row_count, 128), self.row_count)

    def spread_start(self, r, sent, got, lot, first=0, end=None):
        here = got.at[self.z, :, :, self.row_lanes(self.y)]
        for y, z in self.peers[first:end]:
            self.remote_to(sent.at[z * self.ny + y], here, r.send_big.at[lot], r.recv_big.at[lot], (y, z)).start()
        if first == 0:
            here[...] = sent[self.me]

    def spread_wait(self, r, sent, lot):
        others = sent.at[pl.ds(0, self.nd - 1)]
        self.arrived(others, r.recv_big.at[lot])
        self.arrived(others, r.send_big.at[lot])

    def point_start(self, r):
        here = r.got_p.at[:, :, self.row_lanes(self.y)]

        @pl.loop(1, self.ny)
        def _(k):
            peer = lax.rem(self.y + k, self.ny)
            self.remote(r.sent_p.at[peer], here, r.send_p, r.recv_p, self.z * self.ny + peer).start()

        here[...] = r.sent_p[self.y]

    def point_wait(self, r):
        others = r.sent_p.at[pl.ds(0, self.ny - 1)]
        self.arrived(others, r.recv_p)
        self.arrived(others, r.send_p)

    def return_start(self, r, first, end):
        for y, z in self.peers[first:end]:
            self.remote_to(
                r.sent_o.at[z, :, :, self.row_lanes(y)], r.got_o.at[self.me], r.send_big.at[2], r.recv_big.at[2], (y, z)
            ).start()

    def owner(self, kind, number):
        if kind == 2:
            number = self.nz
        return lax.rem(number, self.nz) * self.ny + self.ny // 2 - 1 + 2 * lax.div(number, self.nz)

    def owned(self, kind):
        low = self.ny // 2 - 1
        if kind == 2:
            return self.me == self.owner(2, 0)
        return (self.y == low) | (self.y == low + 2)

    def owners(self, kind):
        return 1 if kind == 2 else 2 * self.nz

    def mine(self, kind):
        return 0 if kind == 2 else jnp.where(self.y == self.ny // 2 - 1, 0, self.nz) + self.z

    def width(self, kind):
        return 1 if kind == 2 else self.share

    def lot(self, r, name, turn, kind, number, count=1):
        if kind == 2:
            return getattr(r, "line_" + name).at[turn]
        return getattr(r, name).at[turn, kind, pl.ds(number * self.share, count * self.share)]

    def slot(self, r, turn, kind, first, count=1):
        if kind == 2:
            return r.line_slots.at[turn, pl.ds(first, count)]
        return r.slots.at[turn, kind, pl.ds(first, count)]

    def reduce_start(self, r, turn, kinds):
        for kind in kinds:
            send, receive = (r.send_part.at[turn % 2, kind], r.recv_part.at[turn % 2, kind])

            @pl.loop(0, self.owners(kind))
            def _(number):
                owner = self.owner(kind, number)

                @pl.when(owner != self.me)
                def _():
                    place = lax.rem(self.me - owner + self.nd, self.nd) - 1
                    self.remote(
                        self.lot(r, "part", turn, kind, number), self.slot(r, turn, kind, place).at[0], send, receive, owner
                    ).start()

    def reduce_middle(self, r, turn, kinds):
        others = self.nd - 1
        for kind in kinds:
            send, receive = (r.send_full.at[turn % 2, kind], r.recv_full.at[turn % 2, kind])

            @pl.when(self.owned(kind))
            def _():
                number = self.mine(kind)
                self.arrived(self.slot(r, turn, kind, 0, others), r.recv_part.at[turn % 2, kind])
                lots = [self.lot(r, "part", turn, kind, number)[...]]
                lots += [self.slot(r, turn, kind, k)[0] for k in range(others)]
                while len(lots) > 1:
                    lots = [lots[k] + lots[k + 1] for k in range(0, len(lots) - 1, 2)] + lots[len(lots) // 2 * 2 :]
                sums = self.lot(r, "sums", turn, kind, 0)
                sums[...] = lots[0]
                full = self.lot(r, "full", turn, kind, number)
                for place in self.peers:
                    self.remote_to(sums, full, send, receive, place).start()
                full[...] = lots[0]

    def reduce_end(self, r, turn, kinds):
        for kind in kinds:
            count = self.owners(kind)

            def finish(count):
                if count:
                    self.arrived(self.lot(r, "full", turn, kind, 0, count), r.recv_full.at[turn % 2, kind])
                    self.arrived(self.lot(r, "part", turn, kind, 0, count), r.send_part.at[turn % 2, kind])

            @pl.when(self.owned(kind))
            def _():
                finish(count - 1)
                self.arrived(self.slot(r, turn, kind, 0, self.nd - 1), r.send_full.at[turn % 2, kind])

            @pl.when(jnp.logical_not(self.owned(kind)))
            def _():
                finish(count)


    def row_spectra(self, r, source, sent):
        half = self.columns // 2
        low, high = (source[:, :half], source[:, half:])
        per = self.nd // 2
        for odd, value in enumerate((low + high, low - high)):
            value = split(value)
            for part in range(2):
                table = (r.tab_x[0][2 * odd + part], r.tab_x[1][2 * odd + part])
                sent[pl.ds(odd * per, per), part] = product(table, value, ((1,), (1,))).reshape(
                    per, self.bins, self.row_count
                )

    def point_spectra(self, r, source):
        half = self.columns // 2
        low, high = (source[:, :half], source[:, half:])
        odd = lax.div(2 * self.z, self.nz)
        sign = 1.0 - 2.0 * odd.astype(jnp.float32)
        value = split(low + sign * high)
        block = self.ny * self.bins
        start = pl.multiple_of(lax.rem(self.z, self.nz // 2) * block, block)
        for part in range(2):
            table = tuple(half_table[2 * odd + part, pl.ds(start, block)] for half_table in r.tab_x)
            r.sent_p[:, part] = product(table, value, ((1,), (1,))).reshape(self.ny, self.bins, self.row_count)

    def turn_tables(self, r):
        for k in range(2):
            for part in range(4):
                r.turned[k, part] = r.tab_y[k][part].astype(jnp.float32).T.astype(jnp.bfloat16)

    def column_spectra(self, r, got, wave, turned=True):
        count = math.prod(got.shape[:-1])
        value = got[...].reshape(count, self.rows)
        low, high = (value[:, : self.half], value[:, self.half :])
        quarter = self.half // 2
        for odd, value in enumerate((low + high, low - high)):
            value = split(value)
            for part in range(2):
                tables = (r.turned.at[0], r.turned.at[1]) if turned else r.tab_y
                table = (tables[0][2 * odd + part], tables[1][2 * odd + part])
                wave[..., pl.ds(part * self.half + odd * quarter, quarter)] = product(
                    value, table, ((1,), (0 if turned else 1,))
                ).reshape(got.shape[:-1] + (quarter,))

    def column_values(self, r, wave, target):
        count = math.prod(wave.shape[:-1])
        value = wave[...].reshape(count, self.rows)
        quarter = self.half // 2
        even, odd = (
            sum(
                product(
                    split(value[:, part * self.half + k * quarter : part * self.half + (k + 1) * quarter]),
                    (r.tab_y[0][2 * k + part], r.tab_y[1][2 * k + part]),
                    ((1,), (0,)),
                )
                for part in range(2)
            )
            for k in range(2)
        )
        shape = wave.shape[:-1] + (self.half,)
        target[..., : self.half] = (even + odd).reshape(shape)
        target[..., self.half :] = (even - odd).reshape(shape)

    def row_values(self, r, got, out):
        per = self.nd // 2
        sides = []
        for k in range(2):
            side = 0.0
            for part in range(2):
                value = got[pl.ds(k * per, per), part].reshape(per * self.bins, self.row_count)
                side = side + product(
                    split(value.T), (r.tab_x[0][2 * k + part], r.tab_x[1][2 * k + part]), ((1,), (0,))
                )
            sides.append(side)
        half = self.columns // 2
        out[0, :, :half] = sides[0] + sides[1]
        out[0, :, half:] = sides[0] - sides[1]


    def masks(self, tier, step):
        shape = (8, 128)
        row = (lax.broadcasted_iota(jnp.int32, shape, 0) == 0) & (self.me == 0)
        lane = lax.broadcasted_iota(jnp.int32, shape, 1) + 128 * step == 0
        if tier:
            row = row & False
        return (row, lane, row & lane, row | lane)

    def combine(self, masks, ac, as_, bc, bs):
        row, lane, corner, special = masks
        pr = jnp.where(special, ac, ac - bs)
        pi = jnp.where(corner, as_, jnp.where(row, -as_, jnp.where(lane, -bc, -(as_ + bc))))
        mr = jnp.where(row, bc, jnp.where(lane, as_, ac + bs))
        mi = jnp.where(corner, bs, jnp.where(special, -bs, as_ - bc))
        return [pr, pi, mr, mi]

    def separate(self, masks, field):
        row, lane, corner, special = masks
        pr, pi, mr, mi = field
        ac = jnp.where(special, pr, 0.5 * (pr + mr))
        as_ = jnp.where(corner, pi, jnp.where(row, -pi, jnp.where(lane, mr, 0.5 * (mi - pi))))
        bc = jnp.where(row, mr, jnp.where(lane, -pi, -0.5 * (pi + mi)))
        bs = jnp.where(corner, mi, jnp.where(special, -mi, 0.5 * (mr - pr)))
        return (ac, as_, bc, bs)

    def lane_slice(self, step, part=0):
        return pl.ds(pl.multiple_of(part * self.half + step * 128, 128), 128)

    def along(self, r, which, step, part):
        return r.along[which, :, self.lane_slice(step, part)]

    def beside(self, r, which, part, tier):
        return r.across[which, part, pl.ds(8 * tier, 8)]

    def load(self, field, z, tier, step):
        return [field[z, k, pl.ds(8 * tier, 8), self.lane_slice(step)] for k in range(4)]

    def keep(self, field, z, tier, step, values):
        for k in range(4):
            field[z, k, pl.ds(8 * tier, 8), self.lane_slice(step)] = values[k]

    def load_wave(self, wave, z, tier, step):
        return [
            wave[z, part, pl.ds(8 * tier, 8), self.lane_slice(step, side)]
            for part in range(2)
            for side in range(2)
        ]

    def times(self, factor, value, conjugate=False):
        out = []
        for side in range(2):
            real, other, cross = factor[side]
            a, b = (value[2 * side], value[2 * side + 1])
            if conjugate:
                out += [real * a + cross * b, other * b - cross * a]
            else:
                out += [real * a - cross * b, other * b + cross * a]
        return out

    def factor(self, array, tier, step):
        where = (pl.ds(8 * tier, 8), self.lane_slice(step))
        return [[array[(side, k) + where] for k in range(3)] for side in range(2)]

    def sweep(self, body):
        @pl.loop(0, self.steps)
        def _(step):
            columns = {}
            for tier in range(self.tiers):
                body(tier, step, self.masks(tier, step), columns)

    def frames(self, r, masks, tier, step, z, value, rows, columns=None):
        ac, as_, bc, bs = self.separate(masks, value)
        here = pl.ds(8 * tier, 8)
        for k, which in enumerate((AT, AT + 3)):
            c, s = (self.along(r, which, step, 0), self.along(r, which, step, 1))
            rows[k, z, 0, here] += ac * c + as_ * s
            rows[k, z, 1, here] += bc * c + bs * s
        if columns is None:
            return
        for x in range(4):
            a, b = (self.beside(r, AT + x, 0, tier), self.beside(r, AT + x, 1, tier))
            for side, (p, q) in enumerate(((ac, bc), (as_, bs))):
                term = a * p + b * q
                key = (x, z, side)
                columns[key] = term if key not in columns else columns[key] + term

    def put_columns(self, r, turn, kinds, tier, step, columns):
        if tier < self.tiers - 1:
            return
        for (x, z, side), value in columns.items():
            index = x // 2 * self.depth + z
            kind = kinds[0] if x in (0, 3) else kinds[1]
            tile = index // 8 * self.lanes + side * self.steps + step
            r.part[turn, kind, tile, pl.ds(index % 8, 1)] = jnp.sum(value, 0, keepdims=True)

    def clear(self, *refs):
        for ref in refs:
            ref[...] = jnp.zeros(ref.shape, jnp.float32)

    def settle(self, rows):
        for k in range(2):
            rows[k] = jnp.broadcast_to(jnp.sum(rows[k], -1, keepdims=True), rows.shape[1:])

    def unpack(self, r, turn, kind, cols, inner):
        Z = self.depth
        for x in (1, 2) if inner else (0, 3):
            first = x // 2 * Z
            for lane in range(self.lanes):
                cols[x, pl.ds(0, Z), pl.ds(lane * 128, 128)] = r.full[
                    turn, kind, first // 8 * self.lanes + lane, pl.ds(first % 8, Z)
                ]

    def shifted(self, value, by):
        if by == 0:
            return value
        value = pltpu.roll(value, 7 if by > 0 else 1, 0)
        sub = lax.broadcasted_iota(jnp.int32, value.shape, 0)
        return jnp.where(sub < self.depth, value, 0.0)

    def corners(self, r, col):
        out = []
        for which in (AT, AT + 3):
            weight = jnp.concatenate([r.along[which, :, :]], 0)
            out.append(jnp.broadcast_to(jnp.sum(col * weight, -1, keepdims=True), (8, 128)))
        return out

    def column_tools(self, r, w, step):
        c = [self.along(r, COS, step, part) for part in range(2)]
        s = self.along(r, SIN, step, 0)
        first = [self.along(r, FIRST, step, part) for part in range(2)]
        last = [self.along(r, LAST, step, part) for part in range(2)]

        def get(col):
            return [col[:, self.lane_slice(step, part)] for part in range(2)]

        def line(a, c_index, col):
            w0, w1, w2 = (w(a, b, c_index) for b in range(3))
            turn = (w2 - w0) * s
            return [
                (w1 + (w0 + w2) * c[0]) * col[0] + turn * col[1],
                (w1 + (w0 + w2) * c[1]) * col[1] - turn * col[0],
            ]

        def stacked(pieces):
            out = None
            for a in range(3):
                for c_index, col in pieces:
                    term = [self.shifted(part, a - 1) for part in line(a, c_index, col)]
                    out = term if out is None else [p + t for p, t in zip(out, term)]
            return out

        return (first, last, get, stacked)

    def edges(self, r, w, col_first, col_last):
        Z = self.depth
        k_first, k_last = (self.corners(r, col_first[...]), self.corners(r, col_last[...]))
        total = lambda terms: sum(terms[1:], terms[0])
        q = {}
        for name, b, c, value in ((0, 0, 0, k_last[1]), (1, 0, 2, k_first[1]), (2, 2, 0, k_last[0]), (3, 2, 2, k_first[0])):
            q[name] = total([w(a, b, c) * self.shifted(value, a - 1) for a in range(3)])
        @pl.loop(0, self.steps, unroll=True)
        def _(step):
            first, last, get, stacked = self.column_tools(r, w, step)
            f, l = (get(col_first), get(col_last))
            for k, (pieces, upper, lower) in enumerate((([(0, l)], q[0], q[2]), ([(2, f)], q[1], q[3]))):
                value = stacked(pieces)
                for part in range(2):
                    r.edge_cols[k, :, self.lane_slice(step, part)] = (
                        value[part] - upper * first[part] - lower * last[part]
                    )

    def edge_lines(self, r, w, rows):
        Z = self.depth
        for tier in range(self.tiers):
            here = pl.ds(8 * tier, 8)
            c = [self.beside(r, COS, part, tier) for part in range(2)]
            s = self.beside(r, SIN, 0, tier)
            for k, (b, source) in enumerate(((0, 1), (2, 0))):
                for z in range(Z):
                    out = None
                    for a in range(3):
                        if not 0 <= z + a - 1 < Z:
                            continue
                        w0, w1, w2 = (w(a, b, c_index) for c_index in range(3))
                        turn = (w2 - w0) * s
                        p, t = (rows[source, z + a - 1, part, here] for part in range(2))
                        term = [
                            (w1 + (w0 + w2) * c[0]) * p + turn * t,
                            (w1 + (w0 + w2) * c[1]) * t - turn * p,
                        ]
                        out = term if out is None else [x + v for x, v in zip(out, term)]
                    for part in range(2):
                        r.edge_rows[k, z, part, here] = out[part]

    def map_columns(self, r, w, cols, mapped, extra=None):
        total = lambda terms: sum(terms[1:], terms[0])
        at = [self.corners(r, cols[x]) for x in range(4)]
        fix = []
        for (c0, v0), (c1, v1) in (((1, at[0]), (2, at[1])), ((0, at[2]), (1, at[3]))):
            fix.append(
                [
                    total(
                        [
                            w(a, b, c0) * self.shifted(v0[y], a - 1) + w(a, b, c1) * self.shifted(v1[y], a - 1)
                            for a in range(3)
                        ]
                    )
                    for b, y in ((0, 1), (2, 0))
                ]
            )

        @pl.loop(0, self.steps, unroll=True)
        def _(step):
            first, last, get, stacked = self.column_tools(r, w, step)
            f, n, g, l = (get(cols.at[x]) for x in range(4))
            for k, pieces in enumerate(([(1, f), (2, n)], [(0, g), (1, l)])):
                value = stacked(pieces)
                for part in range(2):
                    here = (k, slice(None), self.lane_slice(step, part))
                    value_here = value[part] - fix[k][0] * first[part] - fix[k][1] * last[part]
                    if extra is not None:
                        value_here = value_here + extra(here)
                    mapped[here] = value_here

    def edge_field(self, r, masks, tier, step, z):
        here = pl.ds(8 * tier, 8)
        out = []
        for part in range(2):
            e0, e1 = (r.edge_rows[k, z, part, here] for k in range(2))
            x0, x1 = (self.beside(r, which, part, tier) for which in (FIRST, LAST))
            for side in range(2):
                y0, y1 = (self.along(r, which, step, side) for which in (FIRST, LAST))
                c0, c1 = (r.edge_cols[k, pl.ds(z, 1), self.lane_slice(step, side)] for k in range(2))
                out.append(e0 * y0 + e1 * y1 + x0 * c0 + x1 * c1)
        return self.combine(masks, *out)

    def circular_field(self, r, tier, step, field, flip, out=None):
        Z = self.depth
        value = [self.load(field, z, tier, step) for z in range(Z)]
        out = [None] * Z if out is None else out
        for a in range(3):
            factor = self.factor(r.stencil.at[a], tier, step)
            for z in range(Z):
                other = z + (1 - a if flip else a - 1)
                if 0 <= other < Z:
                    term = self.times(factor, value[other], flip)
                    out[z] = term if out[z] is None else [o + t for o, t in zip(out[z], term)]
        return out

    def turn_round(self, r, field, out, norm=None):
        def body(tier, step, masks, columns):
            for z, value in enumerate(self.circular_field(r, tier, step, field, False)):
                self.keep(out, z, tier, step, value)
                if norm is not None:
                    own = self.load(field, z, tier, step)
                    norm[...] += self.dot(masks, own, own)

        self.sweep(body)

    def build_stencil(self, r, w):
        def body(tier, step, masks, columns):
            row, lane, corner, special = masks
            here = pl.ds(8 * tier, 8)
            sx = self.beside(r, SIN, 0, tier)
            ys = self.along(r, SIN, step, 0)
            for side in range(2):
                cx = self.beside(r, COS, side, tier)
                cy = self.along(r, COS, step, 0)
                sy = jnp.broadcast_to(ys, (8, 128))
                cy = jnp.broadcast_to(cy, (8, 128))
                if side:
                    cy = jnp.where(row, cy, self.along(r, COS, step, 1))
                    sy = jnp.where(row, sy, -sy)
                for a in range(3):
                    real, imag = ([], [])
                    for b in range(3):
                        real.append(w(a, b, 1) + (w(a, b, 0) + w(a, b, 2)) * cx)
                        imag.append((w(a, b, 2) - w(a, b, 0)) * sx)
                    value = real[1] + (real[0] + real[2]) * cy - (imag[2] - imag[0]) * sy
                    cross = imag[1] + (imag[0] + imag[2]) * cy + (real[2] - real[0]) * sy
                    other = jnp.where(corner, real[1] - (real[0] + real[2]), value)
                    for k, item in enumerate((value, other, cross)):
                        r.stencil[a, side, k, here, self.lane_slice(step)] = item

        self.sweep(body)

    def build_blur(self, r):
        def body(tier, step, masks, columns):
            row, lane, corner, special = masks
            here = pl.ds(8 * tier, 8)
            wave = [
                r.wave_p[part, here, self.lane_slice(step, side)] for part in range(2) for side in range(2)
            ]
            value = self.combine(masks, wave[0], wave[1], wave[2], wave[3])
            for side in range(2):
                real, imag = (value[2 * side], value[2 * side + 1])
                other = jnp.where(corner, imag, real)
                cross = jnp.where(corner, 0.0, imag)
                for k, item in enumerate((real, other, cross)):
                    r.blur[side, k, here, self.lane_slice(step)] = item
                square = cross * cross
                r.gain[side, 0, here, self.lane_slice(step)] = real * real + square
                r.gain[side, 1, here, self.lane_slice(step)] = other * other + square

        self.sweep(body)

    def gained(self, r, tier, step, value):
        where = (pl.ds(8 * tier, 8), self.lane_slice(step))
        return [r.gain[(k // 2, k % 2) + where] * value[k] for k in range(4)]

    def dot(self, masks, left, right):
        corner = masks[2]
        total = sum(a * b for a, b in zip(left, right))
        return jnp.where(corner, 0.5 * total, total)


    def stencil_twice(self, r, w, cols, mapped, rows_m, cols_m, make, finish, inner, extra=None):
        def flipped(a, b, c):
            return w(2 - a, 2 - b, 2 - c)

        self.edges(r, w, cols.at[0], cols.at[3])
        self.clear(rows_m)

        def forward(tier, step, masks, columns):
            for z in range(self.depth):
                value = [m - e for m, e in zip(make(tier, step, z), self.edge_field(r, masks, tier, step, z))]
                self.keep(mapped, z, tier, step, value)
                self.frames(r, masks, tier, step, z, value, rows_m)

        self.sweep(forward)
        self.settle(rows_m)
        inner()
        self.map_columns(r, w, cols, cols_m, extra)
        self.edge_lines(r, flipped, rows_m)
        self.edges(r, flipped, cols_m.at[0], cols_m.at[1])

        def back(tier, step, masks, columns):
            out = [[-e for e in self.edge_field(r, masks, tier, step, z)] for z in range(self.depth)]
            finish(tier, step, masks, columns, self.circular_field(r, tier, step, mapped, True, out))

        self.sweep(back)

    def scalars_out(self, r, turn, count):
        lane = lax.broadcasted_iota(jnp.int32, (1, 128), 1)
        line = jnp.zeros((1, 128), jnp.float32)
        for k in range(count):
            whole = jnp.sum(jnp.sum(r.acc[k], 0, keepdims=True), -1, keepdims=True)
            line = jnp.where(lane == k, whole, line)
        r.line_part[turn] = line

    def scalars_in(self, r, turn, count):
        line = r.line_full[turn]
        return [jnp.broadcast_to(line[:, k : k + 1], (8, 128)) for k in range(count)]

    def run(self, r):
        Z = self.depth
        self.find_place()

        def w(a, b, c):
            return r.weights[a, b, c]

        barrier = pltpu.get_barrier_semaphore()

        for place in self.peers:
            pl.semaphore_signal(barrier, inc=1, device_id=place, device_id_type=MESH)

        def load(name):
            far = getattr(r, "far_" + name)
            far = far.at[self.me] if name == "frequencies" else far
            return pltpu.make_async_copy(far, getattr(r, name), r.loaded.at[r.inputs.index(name)])

        tables = [name for name in r.inputs if name.startswith("wave")]
        order = ["frequencies", "weights", "along", "point_spread"] + tables + ["measured", "upstream"]
        for name in order:
            load(name).start()
        load("frequencies").wait()
        for which in range(9):
            for part in range(2):
                r.across[which, part] = jnp.broadcast_to(
                    r.frequencies[part * self.bins : (part + 1) * self.bins, which : which + 1], (self.bins, 128)
                )
        load("along").wait()
        load("weights").wait()
        self.build_stencil(r, w)
        load("point_spread").wait()
        for name in tables:
            load(name).wait()
        self.point_spectra(r, r.point_spread[...])
        load("measured").wait()
        self.row_spectra(r, r.measured[0], r.sent_m)
        pl.semaphore_wait(barrier, self.nd - 1)
        self.point_start(r)
        self.spread_start(r, r.sent_m, r.got_m, 0)
        load("upstream").wait()
        self.row_spectra(r, r.upstream[0], r.sent_u)
        self.clear(r.rows_v0, r.rows_v1, r.rows_v2, r.rows_up, r.acc, r.taps)
        self.clear(r.cols_v0, r.cols_v1, r.cols_v2, r.cols_up)

        self.point_wait(r)
        self.column_spectra(r, r.got_p, r.wave_p, False)
        self.build_blur(r)
        self.turn_tables(r)
        self.spread_wait(r, r.sent_m, 0)
        self.spread_start(r, r.sent_u, r.got_u, 1, 0, self.cuts[0])
        self.column_spectra(r, r.got_m, r.wave)

        def start(tier, step, masks, columns):
            factor = self.factor(r.blur, tier, step)
            for z in range(Z):
                value = self.combine(masks, *self.load_wave(r.wave, z, tier, step))
                value = self.times(factor, value, True)
                self.keep(r.v0, z, tier, step, value)
                self.frames(r, masks, tier, step, z, value, r.rows_v0, columns)
            self.put_columns(r, 0, (0, 1), tier, step, columns)

        self.sweep(start)
        self.reduce_start(r, 0, [0, 1])
        self.settle(r.rows_v0)
        self.edge_lines(r, w, r.rows_v0)
        self.reduce_middle(r, 0, [0, 1])
        self.spread_start(r, r.sent_u, r.got_u, 1, self.cuts[0], self.cuts[1])
        self.turn_round(r, r.v0, r.m0, r.acc.at[0])
        self.reduce_end(r, 0, [0])
        self.unpack(r, 0, 0, r.cols_v0, False)
        self.spread_start(r, r.sent_u, r.got_u, 1, self.cuts[1], self.cuts[2])

        def inner_0():
            self.reduce_end(r, 0, [1])
            self.unpack(r, 0, 1, r.cols_v0, True)

        def first(tier, step, masks, columns, back):
            for z in range(Z):
                before = self.load(r.v0, z, tier, step)
                value = [g + b for g, b in zip(self.gained(r, tier, step, before), back[z])]
                self.keep(r.v1, z, tier, step, value)
                self.frames(r, masks, tier, step, z, value, r.rows_v1, columns)
                r.acc[1] += self.dot(masks, before, value)
                r.acc[2] += self.dot(masks, value, value)
            self.put_columns(r, 1, (0, 1), tier, step, columns)

        def plain(field):
            return lambda tier, step, z: self.load(field, z, tier, step)

        self.stencil_twice(
            r, w, r.cols_v0, r.m0, r.rows_m0, r.cols_m0, plain(r.m0), first, inner_0
        )
        self.reduce_start(r, 1, [0])
        self.scalars_out(r, 1, 3)
        self.reduce_start(r, 1, [1, 2])
        self.settle(r.rows_v1)
        self.edge_lines(r, w, r.rows_v1)
        self.reduce_middle(r, 1, [0, 1, 2])
        self.spread_start(r, r.sent_u, r.got_u, 1, self.cuts[2])
        self.turn_round(r, r.v1, r.m1)
        self.spread_wait(r, r.sent_u, 1)
        self.column_spectra(r, r.got_u, r.wave)

        def upper(tier, step, masks, columns):
            for z in range(Z):
                value = self.combine(masks, *self.load_wave(r.wave, z, tier, step))
                self.keep(r.up, z, tier, step, value)
                self.frames(r, masks, tier, step, z, value, r.rows_up, columns)
                r.acc[5] += self.dot(masks, value, self.load(r.v0, z, tier, step))
                r.acc[6] += self.dot(masks, value, self.load(r.v1, z, tier, step))
            self.put_columns(r, 2, (3, 4), tier, step, columns)

        self.clear(r.acc)
        self.sweep(upper)
        self.settle(r.rows_up)
        self.reduce_end(r, 1, [0])
        self.unpack(r, 1, 0, r.cols_v1, False)
        scalars = []

        def inner_1():
            self.reduce_end(r, 1, [1, 2])
            self.unpack(r, 1, 1, r.cols_v1, True)
            self.reduce_start(r, 2, [3, 4])
            scalars.extend(self.scalars_in(r, 1, 3))
            scalars.append(scalars[0] / scalars[1])

        def second(tier, step, masks, columns, back):
            for z in range(Z):
                before, value = (self.load(f, z, tier, step) for f in (r.v0, r.v1))
                after = [g + b for g, b in zip(self.gained(r, tier, step, value), back[z])]
                self.keep(r.v2, z, tier, step, after)
                self.frames(r, masks, tier, step, z, after, r.rows_v2, columns)
                step_0 = scalars[3]
                residual = [p - step_0 * q for p, q in zip(before, value)]
                image = [p - step_0 * q for p, q in zip(value, after)]
                for k, (p, q) in enumerate(
                    ((residual, residual), (residual, value), (residual, image), (image, value))
                ):
                    r.acc[k] += self.dot(masks, p, q)
            self.put_columns(r, 2, (0, 1), tier, step, columns)

        self.stencil_twice(
            r, w, r.cols_v1, r.m1, r.rows_m1, r.cols_m1, plain(r.m1), second, inner_1
        )
        norm_0, curve_0, image_0, step_0 = scalars
        self.scalars_out(r, 2, 7)
        self.reduce_start(r, 2, [2, 0, 1])
        self.settle(r.rows_v2)
        self.reduce_middle(r, 2, [3, 4, 2, 0, 1])
        self.turn_round(r, r.up, r.around)
        self.turn_round(r, r.v2, r.mw)
        self.reduce_end(r, 2, [3, 4])
        self.unpack(r, 2, 3, r.cols_up, False)
        self.unpack(r, 2, 4, r.cols_up, True)
        self.reduce_end(r, 2, [2, 0])
        self.unpack(r, 2, 0, r.cols_v2, False)

        norm_1, cross, inner, image_cross, unused, up_0, up_1 = self.scalars_in(r, 2, 7)
        up_residual = up_0 - step_0 * up_1
        ratio = norm_1 / norm_0
        curve_1 = inner + 2.0 * ratio * cross + ratio * ratio * curve_0
        step_1 = norm_1 / curve_1
        grad_step_1 = up_residual + ratio * up_0
        grad_curve_1 = -grad_step_1 * step_1 / curve_1
        grad_ratio = step_1 * up_0 + 2.0 * grad_curve_1 * (cross + ratio * curve_0)
        grad_norm = grad_step_1 / curve_1 + grad_ratio / norm_0
        grad_step_0 = (
            up_0 - step_1 * up_1 - 2.0 * grad_curve_1 * (image_cross + ratio * image_0) - 2.0 * grad_norm * cross
        )
        more = 1.0 + ratio
        g0 = grad_norm - grad_ratio * ratio / norm_0 + grad_step_0 / curve_0
        g1 = grad_curve_1 * more * more - 2.0 * grad_norm * step_0 - grad_step_0 * step_0 / curve_0
        g2 = -2.0 * grad_curve_1 * step_0 * more + grad_norm * step_0 * step_0
        g3 = grad_curve_1 * step_0 * step_0
        q0 = step_0 + step_1 * more
        q1 = -step_1 * step_0
        mix = (g1, 2.0 * g2, 2.0 * g3, q1)

        def mixed(*values):
            return sum(m * v for m, v in zip(mix[4 - len(values) :], values))

        def mix_columns(places):
            for x in places:
                for lane in range(self.lanes):
                    here = (x, slice(None), pl.ds(lane * 128, 128))
                    r.cols_w3[here] = mixed(r.cols_v2[here], r.cols_up[here])

        mix_columns((0, 3))
        for k in range(2):
            for part in range(2):
                for tier in range(self.tiers):
                    for z in range(Z):
                        here = (k, z, part, pl.ds(8 * tier, 8))
                        r.rows_w3[here] = mixed(r.rows_v2[here], r.rows_up[here])

        self.edge_lines(r, w, r.rows_w3)

        def inner_2():
            self.reduce_end(r, 2, [1])
            self.unpack(r, 2, 1, r.cols_v2, True)
            mix_columns((1, 2))

        def make(tier, step, z):
            values = [self.load(f, z, tier, step) for f in (r.v0, r.v1, r.v2, r.up)]
            self.keep(r.w3, z, tier, step, [mixed(*parts) for parts in zip(*values)])
            values = [self.load(f, z, tier, step) for f in (r.m0, r.m1, r.mw, r.around)]
            return [mixed(*parts) for parts in zip(*values)]

        def extra(here):
            return mix[0] * r.cols_m0[here] + mix[1] * r.cols_m1[here]

        scale = 1.0 / (self.rows * self.columns)

        def last(tier, step, masks, columns, back):
            factor = self.factor(r.blur, tier, step)
            here = pl.ds(8 * tier, 8)
            for z in range(Z):
                v0, v1, w3, up = (self.load(f, z, tier, step) for f in (r.v0, r.v1, r.w3, r.up))
                value = [
                    b + d + 2.0 * g0 * p + g1 * q + q0 * u
                    for b, d, p, q, u in zip(back[z], self.gained(r, tier, step, w3), v0, v1, up)
                ]
                value = self.separate(masks, self.times(factor, value))
                for part in range(2):
                    heavy = scale * self.beside(r, WEIGHT, part, tier)
                    for side in range(2):
                        r.wave[z, part, here, self.lane_slice(step, side)] = (
                            value[2 * part + side] * heavy * self.along(r, WEIGHT, step, side)
                        )

        self.stencil_twice(
            r, w, r.cols_w3, r.mw, r.rows_mw, r.cols_mw, make, last, inner_2, extra
        )
        self.column_values(r, r.wave, r.sent_o)
        middle = len(self.peers) // 2
        self.return_start(r, 0, middle)
        for k in range(2):
            for x in (0, 3):
                if k == 0:
                    r.cols_w3[x] = r.cols_w3[x] + self.blend(mix, r.cols_v0[x], r.cols_v1[x])
            r.rows_w3[k] = r.rows_w3[k] + self.blend(mix, r.rows_v0[k], r.rows_v1[k])
        self.tap_sums(r, 2.0 * g3)

        for place in self.peers:
            self.remote_to(r.tap_part, r.tap_slots.at[self.me], r.send_tap, r.recv_tap, place).start()
        self.return_start(r, middle, None)
        r.got_o[self.me] = r.sent_o[self.z, :, :, self.row_lanes(self.y)]
        r.tap_slots[self.me] = r.tap_part[...]
        others = pl.ds(0, self.nd - 1)
        self.arrived(r.got_o.at[others], r.recv_big.at[2])
        self.row_values(r, r.got_o, r.out)
        self.arrived(r.got_o.at[others], r.send_big.at[2])
        self.arrived(r.tap_slots.at[others], r.recv_tap)
        self.arrived(r.tap_slots.at[others], r.send_tap)
        lots = [r.tap_slots[k] for k in range(self.nd)]
        while len(lots) > 1:
            lots = [lots[k] + lots[k + 1] for k in range(0, len(lots) - 1, 2)] + lots[len(lots) // 2 * 2 :]
        line = jnp.broadcast_to(lots[0] / math.sqrt(self.depth * self.rows * self.columns), (8, 128))
        for a in range(3):
            for b in range(3):
                first = 9 * a + 3 * b
                turned = pltpu.roll(line, 128 - first, 1) if first else line
                r.tap_out[a, pl.ds(b, 1)] = turned[:1, :3]

    def blend(self, mix, one, two):
        return mix[0][:1, :1] * one + mix[1][:1, :1] * two

    def tap_sums(self, r, weight):
        Z = self.depth
        pairs = ((r.v0, r.mw, None), (r.w3, r.m0, None), (r.v1, r.m1, weight))

        def body(tier, step, masks, columns):
            corner = masks[2]
            sx = self.beside(r, SIN, 0, tier)
            gamma = [[None, None, None, None] for a in range(3)]
            for left, right, scale in pairs:
                x = [self.load(left, z, tier, step) for z in range(Z)]
                if scale is not None:
                    x = [[scale * item for item in value] for value in x]
                for z in range(Z):
                    m = self.load(right, z, tier, step)
                    for a in range(3):
                        if not 0 <= z + a - 1 < Z:
                            continue
                        v = x[z + a - 1]
                        for side in range(2):
                            vr, vi, mr, mi = (v[2 * side], v[2 * side + 1], m[2 * side], m[2 * side + 1])
                            p, q = (vr * mr, vi * mi)
                            terms = (jnp.where(corner, 0.5 * (p + q), p + q), jnp.where(corner, 0.5 * (p - q), p + q), vi * mr - vr * mi)
                            old = gamma[a][side]
                            gamma[a][side] = terms if old is None else [o + t for o, t in zip(old, terms)]
            for a in range(3):
                sums = [0.0] * 9
                for side in range(2):
                    cx = self.beside(r, COS, side, tier)
                    cy = jnp.broadcast_to(self.along(r, COS, step, 0), (8, 128))
                    sy = jnp.broadcast_to(self.along(r, SIN, step, 0), (8, 128))
                    if side:
                        cy = jnp.where(masks[0], cy, self.along(r, COS, step, 1))
                        sy = jnp.where(masks[0], sy, -sy)
                    near, far, turn = gamma[a][side]
                    items = (
                        near, near * cx, far * cy, far * cy * cx, near * sx * sy,
                        turn * sx, turn * sy, turn * cx * sy, turn * sx * cy,
                    )
                    sums = [s + item for s, item in zip(sums, items)]
                for k in range(9):
                    r.taps[9 * a + k] += sums[k]

        self.sweep(body)

        sides = (
            (r.rows_v0, r.cols_v0, r.rows_mw, r.cols_mw, None),
            (r.rows_w3, r.cols_w3, r.rows_m0, r.cols_m0, None),
            (r.rows_v1, r.cols_v1, r.rows_m1, r.cols_m1, weight),
        )
        zero = jnp.zeros((8, 128), jnp.float32)
        by_row = [[[zero] * 3 for k in range(2)] for a in range(3)]
        by_col = [[[zero] * 3 for k in range(2)] for a in range(3)]
        by_corner = [[[zero] * 2 for k in range(2)] for a in range(3)]
        for rows_x, cols_x, rows_m, cols_m, scale in sides:
            extra = 1.0 if scale is None else scale
            for tier in range(self.tiers):
                here = pl.ds(8 * tier, 8)
                heavy = self.beside(r, WEIGHT, 0, tier) * extra
                ca, cb = (self.beside(r, COS, part, tier) for part in range(2))
                s = self.beside(r, SIN, 0, tier)
                for k in range(2):
                    for z in range(Z):
                        ma, mb = (rows_m[k, z, part, here] for part in range(2))
                        for a in range(3):
                            if not 0 <= z + a - 1 < Z:
                                continue
                            xa, xb = (rows_x[1 - k, z + a - 1, part, here] for part in range(2))
                            p, q = (heavy * xa * ma, heavy * xb * mb)
                            terms = (p + q, p * ca + q * cb, heavy * s * (xa * mb - xb * ma))
                            by_row[a][k] = [o + t for o, t in zip(by_row[a][k], terms)]
            for k in range(2):
                col_x, col_m = (cols_x.at[0 if k else 3], cols_m.at[k])
                for step in range(self.steps):
                    (xc, xs), (mc, ms) = (
                        [ref[:, pl.ds(part * self.half + 128 * step, 128)] * (extra if ref is col_x else 1.0) for part in range(2)]
                        for ref in (col_x, col_m)
                    )
                    heavy = self.along(r, WEIGHT, step, 0)
                    cc, cs = (self.along(r, COS, step, part) for part in range(2))
                    s = self.along(r, SIN, step, 0)
                    for a in range(3):
                        xc_a, xs_a = (self.shifted(item, a - 1) for item in (xc, xs))
                        p, q = (heavy * xc_a * mc, heavy * xs_a * ms)
                        terms = (p + q, p * cc + q * cs, heavy * s * (xc_a * ms - xs_a * mc))
                        by_col[a][k] = [o + t for o, t in zip(by_col[a][k], terms)]
                at_x, at_m = (self.corners(r, ref[...]) for ref in (col_x, col_m))
                for a in range(3):
                    for edge in range(2):
                        term = extra * self.shifted(at_x[1 - edge], a - 1) * at_m[edge]
                        by_corner[a][edge][k] = by_corner[a][edge][k] + term

        lots = []
        for a in range(3):
            s = [r.taps[9 * a + k] for k in range(9)]
            for b in range(3):
                for c in range(3):
                    beta, gamma = (float(b - 1), float(c - 1))
                    if b == 1 and c == 1:
                        value = s[0]
                    elif b == 1:
                        value = s[1] - gamma * s[5]
                    elif c == 1:
                        value = s[2] - beta * s[6]
                    else:
                        value = s[3] - beta * gamma * s[4] - beta * s[7] - gamma * s[8]
                    value = value * (2.0 / (self.rows * self.columns))
                    if b != 1:
                        one, two, three = by_row[a][b // 2]
                        value = value - (one if c == 1 else two - gamma * three) * (1.0 / (128 * self.columns))
                    if c != 1:
                        one, two, three = by_col[a][c // 2]
                        value = value - (one if b == 1 else two - beta * three) * (1.0 / (self.rows * self.nd))
                    if b != 1 and c != 1:
                        value = value + by_corner[a][b // 2][c // 2] * (1.0 / (128 * self.nd))
                    lots.append(value)
        lane = lax.broadcasted_iota(jnp.int32, (1, 128), 1)
        line = jnp.zeros((1, 128), jnp.float32)
        for k, value in enumerate(lots):
            whole = jnp.sum(jnp.sum(value, 0, keepdims=True), -1, keepdims=True)
            line = jnp.where(lane == k, whole, line)
        r.tap_part[...] = line


class Refs:
    def __init__(self, names, refs):
        for name, ref in zip(names, refs):
            setattr(self, name, ref)


def spectral(measured, point_spread, stencil_weights, upstream):
    planes, row_count, columns = measured.shape
    plan = Spectral(lax.axis_size("gy"), lax.axis_size("gz"), planes, row_count, columns)
    waves = [jnp.asarray(part) for part in wave_rows(columns)]
    if plan.rows != columns:
        waves += [jnp.asarray(part) for part in wave_rows(plan.rows)]
    along = jnp.asarray(axis_values(plan.rows).reshape(9, 1, plan.rows))
    across = axis_values(columns).reshape(9, 2, plan.nd, plan.bins).transpose(2, 1, 3, 0)
    frequencies = np.zeros((plan.nd, 2 * plan.bins, 128), np.float32)
    frequencies[:, :, :9] = across.reshape(plan.nd, 2 * plan.bins, 9)
    scratch = plan.scratch()
    arrays = dict(weights=stencil_weights, measured=measured, point_spread=point_spread, upstream=upstream, along=along)
    arrays.update({"wave_%d" % k: part for k, part in enumerate(waves)})
    arrays["frequencies"] = jnp.asarray(frequencies)
    for name, array in arrays.items():
        shape = array.shape[1:] if name == "frequencies" else array.shape
        space = pltpu.SMEM if name == "weights" else pltpu.VMEM
        scratch[name] = space(shape, array.dtype)
    scratch["loaded"] = pltpu.SemaphoreType.DMA((len(arrays),))
    names = ["far_" + name for name in arrays] + ["out", "tap_out"] + list(scratch)

    def body(*refs):
        r = Refs(names, refs)
        r.tab_x = (r.wave_0, r.wave_1)
        r.tab_y = (r.wave_2, r.wave_3) if len(waves) > 2 else r.tab_x
        r.inputs = list(arrays)
        plan.run(r)

    out, taps = pl.pallas_call(
        body,
        out_shape=(
            jax.ShapeDtypeStruct(measured.shape, jnp.float32),
            jax.ShapeDtypeStruct((3, 3, 3), jnp.float32),
        ),
        in_specs=[HBM] * len(arrays),
        out_specs=(VMEM, VMEM),
        scratch_shapes=list(scratch.values()),
        compiler_params=pltpu.CompilerParams(
            collective_id=0, has_side_effects=True, vmem_limit_bytes=32 * 1024 * 1024
        ),
        name="spectral",
    )(
        *(pltpu.with_memory_space_constraint(array, pltpu.HBM) for array in arrays.values())
    )
    return (out, taps)


def solution(mesh):
    def program(measured, point_spread, stencil_weights, upstream):
        planes, row_count, columns = measured.shape
        fits = spectral_fits(mesh.shape["gy"], mesh.shape["gz"], planes, row_count, columns)
        chosen = spectral if fits else local
        return chosen(measured, point_spread, stencil_weights, upstream)

    return jax.shard_map(
        program,
        mesh=mesh,
        in_specs=(P("gz", "gy", None), P("gy", None), P(), P("gz", "gy", None)),
        out_specs=(P("gz", "gy", None), P()),
        check_vma=False,
    )
```

```python
import math

import jax
import jax.numpy as jnp
import numpy as np
from jax import lax
from jax.experimental import pallas as pl
from jax.experimental.pallas import tpu as pltpu
from jax.sharding import PartitionSpec as P

MESH = pl.DeviceIdType.MESH
SIDES = [(dy, dz) for dy in (-1, 0, 1) for dz in (-1, 0, 1) if (dy, dz) != (0, 0)]
VMEM = pl.BlockSpec(memory_space=pltpu.VMEM)
SMEM = pl.BlockSpec(memory_space=pltpu.SMEM)
HBM = pl.BlockSpec(memory_space=pltpu.HBM)


def moved(value, shift):
    if shift == 0:
        return value
    width = value.shape[1]
    lane = lax.broadcasted_iota(jnp.int32, value.shape, 1)
    edge = 0 if shift > 0 else width - 1
    return jnp.where(lane == edge, 0.0, pltpu.roll(value, shift % width, 1))


def regular_kernel(count_y, count_z, weights, volume, back, grown, mapped, shifted, send, receive):
    rows, columns = volume.shape
    y, z = (lax.axis_index("gy"), lax.axis_index("gz"))

    def there(dy, dz):
        return (y + dy >= 0) & (y + dy < count_y) & (z + dz >= 0) & (z + dz < count_z)

    barrier = pltpu.get_barrier_semaphore()
    for dy, dz in SIDES:

        @pl.when(there(dy, dz))
        def _():
            pl.semaphore_signal(barrier, inc=1, device_id=(y + dy, z + dz), device_id_type=MESH)

    def span(place, count):
        return 1 + jnp.where(place > 0, 1, 0) + jnp.where(place < count - 1, 1, 0)

    pl.semaphore_wait(barrier, span(y, count_y) * span(z, count_z) - 1)

    def copy(field, phase, number):
        dy, dz = SIDES[number]
        source = field.at[1, pl.ds(rows if dy > 0 else 8, 8 if dy else rows)]
        start = 8 if dy == 0 else 0 if dy > 0 else rows + 8
        return pltpu.make_async_remote_copy(
            src_ref=source,
            dst_ref=field.at[1 - dz, pl.ds(start, 8 if dy else rows)],
            send_sem=send.at[phase, number],
            recv_sem=receive.at[phase, number],
            device_id=(y + dy, z + dz),
            device_id_type=MESH,
        )

    def exchange(field, phase):
        for number, (dy, dz) in enumerate(SIDES):

            @pl.when(there(dy, dz))
            def _():
                copy(field, phase, number).start()

        for number, (dy, dz) in enumerate(SIDES):
            start = 8 if dy == 0 else 0 if dy > 0 else rows + 8

            @pl.when(jnp.logical_not(there(-dy, -dz)))
            def _():
                field[1 - dz, pl.ds(start, 8 if dy else rows)] = jnp.zeros(
                    (8 if dy else rows, columns), jnp.float32
                )

        for number, (dy, dz) in enumerate(SIDES):

            @pl.when(there(-dy, -dz))
            def _():
                copy(field, phase, number).wait_recv()

            @pl.when(there(dy, dz))
            def _():
                copy(field, phase, number).wait_send()

    def apply(field, flip, put):
        def weight(a, b, c):
            return weights[26 - (9 * a + 3 * b + c) if flip else 9 * a + 3 * b + c]

        @pl.loop(0, (rows + 16) // 8)
        def _(step):
            here = pl.ds(pl.multiple_of(step * 8, 8), 8)
            sums = [None] * 3
            for a in range(3):
                value = field[a, here]
                for c in range(3):
                    turned = moved(value, 1 - c)
                    for b in range(3):
                        term = weight(a, b, c) * turned
                        sums[b] = term if sums[b] is None else sums[b] + term
            for b in range(3):
                shifted[b, here] = sums[b]

        @pl.loop(0, rows // 8)
        def _(step):
            first = pl.multiple_of(step * 8, 8)
            around = pl.ds(first, 24)
            total = shifted[1, pl.ds(first + 8, 8)]
            total = total + shifted[0, around][7:15] + shifted[2, around][9:17]
            put(first, total)

    @pl.loop(0, rows // 8)
    def _(step):
        first = pl.multiple_of(step * 8, 8)
        grown[1, pl.ds(first + 8, 8)] = volume[pl.ds(first, 8)]

    exchange(grown, 0)

    def put_mapped(first, total):
        mapped[1, pl.ds(first + 8, 8)] = total

    apply(grown, False, put_mapped)
    exchange(mapped, 1)

    def put_back(first, total):
        back[pl.ds(first, 8)] = total

    apply(mapped, True, put_back)


def regular(volume, kernel):
    rows, columns = volume.shape[1:]
    count_y, count_z = (lax.axis_size("gy"), lax.axis_size("gz"))
    field = jax.ShapeDtypeStruct((3, rows + 16, columns), jnp.float32)

    def body(*refs):
        regular_kernel(count_y, count_z, *refs)

    back, grown, mapped = pl.pallas_call(
        body,
        out_shape=(jax.ShapeDtypeStruct((rows, columns), jnp.float32), field, field),
        in_specs=[SMEM, VMEM],
        out_specs=(VMEM, VMEM, VMEM),
        scratch_shapes=[
            pltpu.VMEM((3, rows + 16, columns), jnp.float32),
            pltpu.SemaphoreType.DMA((2, 8)),
            pltpu.SemaphoreType.DMA((2, 8)),
        ],
        cost_estimate=pl.CostEstimate(flops=120 * rows * columns, bytes_accessed=20 * rows * columns, transcendentals=0),
        compiler_params=pltpu.CompilerParams(collective_id=0, has_side_effects=True),
        name="regular",
    )(kernel.reshape(27), volume[0])
    return (back[None], grown, mapped)


def total_kernel(count_y, count_z, value, out, column, row, across, send, receive):
    y, z = (lax.axis_index("gy"), lax.axis_index("gz"))
    along_y = [(lax.rem(y + k, count_y), z) for k in range(1, count_y)]
    along_z = [(y, lax.rem(z + k, count_z)) for k in range(1, count_z)]
    barrier = pltpu.get_barrier_semaphore()
    for place in along_y + along_z:
        pl.semaphore_signal(barrier, inc=1, device_id=place, device_id_type=MESH)
    pl.semaphore_wait(barrier, count_y + count_z - 2)

    def gather(source, slots, places, base):
        copies = []
        for k, place in enumerate(places):
            copies.append(
                pltpu.make_async_remote_copy(
                    src_ref=source,
                    dst_ref=slots.at[k],
                    send_sem=send.at[base + k],
                    recv_sem=receive.at[base + k],
                    device_id=place,
                    device_id_type=MESH,
                )
            )
            copies[-1].start()
        for item in copies:
            item.wait()

    def ordered(own, slots, index, count):
        total = jnp.zeros_like(own)
        for j in range(count):
            term = own
            for k in range(1, count):
                term = jnp.where(lax.rem(index - j + count, count) == k, slots[k - 1], term)
            total = total + term
        return total

    gather(value, column, along_y, 0)
    across[...] = ordered(value[...], column, y, count_y)
    gather(across, row, along_z, count_y - 1)
    out[...] = ordered(across[...], row, z, count_z)


def total(values, collective):
    count_y, count_z = (lax.axis_size("gy"), lax.axis_size("gz"))
    count = values.shape[0]

    def body(*refs):
        total_kernel(count_y, count_z, *refs)

    block = jnp.broadcast_to(jnp.pad(values, (0, 128 - count))[None], (8, 128))
    copies = count_y + count_z - 2
    summed = pl.pallas_call(
        body,
        out_shape=jax.ShapeDtypeStruct((8, 128), jnp.float32),
        in_specs=[VMEM],
        out_specs=VMEM,
        scratch_shapes=[
            pltpu.VMEM((count_y - 1, 8, 128), jnp.float32),
            pltpu.VMEM((count_z - 1, 8, 128), jnp.float32),
            pltpu.VMEM((8, 128), jnp.float32),
            pltpu.SemaphoreType.DMA((copies,)),
            pltpu.SemaphoreType.DMA((copies,)),
        ],
        compiler_params=pltpu.CompilerParams(collective_id=collective, has_side_effects=True),
        name="total",
    )(block)
    return summed[0, :count]


def correlate_kernel(scalars, grown_0, grown_1, grown_2, grown_up, mapped_0, mapped_1, mapped_2, mapped_up, out):
    rows = grown_0.shape[1] - 16
    columns = grown_0.shape[2]
    c_up, c_zero, c_one, c_two, d_zero, d_one, s_zero, s_grad, s_direction = (scalars[k] for k in range(9))
    out[...] = jnp.zeros_like(out)

    @pl.loop(0, rows // 8)
    def _(step):
        first = pl.multiple_of(step * 8, 8)
        here = pl.ds(first + 8, 8)
        zero, one = (mapped_0[1, here], mapped_1[1, here])
        grad = c_up * mapped_up[1, here] + c_zero * zero + c_one * one + c_two * mapped_2[1, here]
        values = (
            s_zero * zero + s_grad * grad,
            s_grad * zero,
            s_direction * (d_zero * zero + d_one * one),
        )
        turned = [[moved(value, c - 1) for value in values] for c in range(3)]
        for a in range(3):
            around = pl.ds(first, 24)
            full_0, full_1 = (grown_0[a, around], grown_1[a, around])
            full_grad = c_up * grown_up[a, around] + c_zero * full_0 + c_one * full_1 + c_two * grown_2[a, around]
            full_direction = d_zero * full_0 + d_one * full_1
            for b in range(3):
                fields = [item[7 + b : 15 + b] for item in (full_0, full_grad, full_direction)]
                for c in range(3):
                    product = turned[c][0] * fields[0] + turned[c][1] * fields[1] + turned[c][2] * fields[2]
                    folded = product[:, :128]
                    for part in range(1, columns // 128):
                        folded = folded + product[:, 128 * part : 128 * part + 128]
                    out[9 * a + 3 * b + c] += folded


def correlate(scalars, *fields):
    return pl.pallas_call(
        correlate_kernel,
        out_shape=jax.ShapeDtypeStruct((27, 8, 128), jnp.float32),
        in_specs=[SMEM] + [VMEM] * 8,
        out_specs=VMEM,
        cost_estimate=pl.CostEstimate(flops=40000000, bytes_accessed=8000000, transcendentals=0),
        name="correlate",
    )(scalars, *fields).sum((1, 2))


def contract(form, left, right):
    return jnp.einsum(form, left, right, precision=lax.Precision.HIGH)


def wave_tables(length, groups):
    half = length // 2
    bins = half // groups
    pair = groups // 2
    shape = (half, pair, 2, bins)
    place = lax.broadcasted_iota(jnp.int32, shape, 0)
    part = lax.broadcasted_iota(jnp.int32, shape, 2)
    slot = lax.broadcasted_iota(jnp.int32, shape, 1) * bins + lax.broadcasted_iota(jnp.int32, shape, 3)
    tables = []
    for odd in range(2):
        frequency = 2 * slot + odd
        steps = place * frequency + part * (length // 4)
        if not odd:
            steps = jnp.where((slot == 0) & (part == 1), place * half, steps)
        angle = (steps % length).astype(jnp.float32) * (2.0 * math.pi / length)
        tables.append(jnp.cos(angle).reshape(half, pair, 2 * bins))
    return tables


def combine(raw, on_row, on_lane):
    even, odd = raw
    a, b, c, d = (
        jnp.concatenate([piece[:, part, :, :, side] for piece in (even, odd)], 0)
        for part, side in ((0, 0), (0, 1), (1, 0), (1, 1))
    )
    special = on_row | on_lane
    plus_real = jnp.where(special, a, a - d)
    plus_imaginary = jnp.where(on_row, b, jnp.where(on_lane, c, b + c))
    minus_real = jnp.where(on_row, c, jnp.where(on_lane, b, a + d))
    minus_imaginary = jnp.where(special, d, b - c)
    return (jnp.stack([plus_real, minus_real]), jnp.stack([plus_imaginary, minus_imaginary]))


def separate(spectrum, on_row, on_lane):
    (plus_real, minus_real), (plus_imaginary, minus_imaginary) = spectrum
    special = on_row | on_lane
    a = jnp.where(special, plus_real, plus_real + minus_real)
    d = jnp.where(special, minus_imaginary, minus_real - plus_real)
    b = jnp.where(on_row, plus_imaginary, jnp.where(on_lane, minus_real, plus_imaginary + minus_imaginary))
    c = jnp.where(on_row, minus_real, jnp.where(on_lane, plus_imaginary, plus_imaginary - minus_imaginary))
    scale = jnp.where(on_row & on_lane, 1.0, 2.0)
    a, b, c, d = (value * scale for value in (a, b, c, d))
    whole = jnp.stack([jnp.stack([a, b], 3), jnp.stack([c, d], 3)], 1)
    pair = whole.shape[0] // 2
    return (whole[:pair], whole[pair:])


def times(left, right, corner, conjugate=False):
    (a, b), (c, d) = (left, right)
    cross = b * d
    sign = -1.0 if conjugate else 1.0
    real = jnp.where(corner, a * c, a * c - sign * cross)
    imaginary = jnp.where(corner, cross, sign * a * d + b * c)
    return (real, imaginary)


def linear(*terms):
    total_real = total_imaginary = 0.0
    for scale, (real, imaginary) in terms:
        scale_real, scale_imaginary = scale if isinstance(scale, tuple) else (scale, scale)
        total_real = total_real + scale_real * real
        total_imaginary = total_imaginary + scale_imaginary * imaginary
    return (total_real, total_imaginary)


def local(measured, point_spread, stencil_weights, upstream):
    planes, row_count, columns = measured.shape
    groups = lax.axis_size("gy")
    rows = row_count * groups
    cells = planes * rows * columns * lax.axis_size("gz")
    bins = columns // 2 // groups
    even_x, odd_x = wave_tables(columns, groups)
    even_y, odd_y = (even_x, odd_x) if rows == columns else wave_tables(rows, groups)
    y_bins = rows // 2 // groups
    spectral = (groups, y_bins, 1, bins)
    on_row = (lax.broadcasted_iota(jnp.int32, spectral, 0) == 0) & (
        lax.broadcasted_iota(jnp.int32, spectral, 1) == 0
    )
    on_lane = (lax.broadcasted_iota(jnp.int32, spectral, 3) == 0) & (lax.axis_index("gy") == 0)
    corner = on_row & on_lane

    def forward(volumes):
        count = volumes.shape[0]
        low, high = (volumes[:, :, : columns // 2], volumes[:, :, columns // 2 :])
        sent = jnp.concatenate(
            [contract("vrj,jdl->drvl", low + high, even_x), contract("vrj,jdl->drvl", low - high, odd_x)], 0
        )
        arrived = lax.all_to_all(
            sent.reshape(groups, row_count, count * 2 * bins), "gy", split_axis=0, concat_axis=0, tiled=True
        )
        arrived = arrived.reshape(rows, count * 2 * bins)
        low, high = (arrived[: rows // 2], arrived[rows // 2 :])
        raw = [
            contract("jds,jl->dsl", table, value).reshape(groups // 2, 2, y_bins, count, 2, bins)
            for table, value in ((even_y, low + high), (odd_y, low - high))
        ]
        return combine(raw, on_row, on_lane)

    def inverse(spectrum):
        count = spectrum[0].shape[3]
        pieces = separate(spectrum, on_row, on_lane)
        one, two = (
            contract("jds,dsl->jl", table, piece.reshape(groups // 2, 2 * y_bins, count * 2 * bins))
            for table, piece in ((even_y, pieces[0]), (odd_y, pieces[1]))
        )
        sent = jnp.concatenate([one + two, one - two], 0).reshape(groups, row_count, count * 2 * bins)
        arrived = lax.all_to_all(sent, "gy", split_axis=0, concat_axis=0, tiled=True)
        arrived = arrived.reshape(groups, row_count, count, 2 * bins)
        one = contract("drvl,jdl->vrj", arrived[: groups // 2], even_x)
        two = contract("drvl,jdl->vrj", arrived[groups // 2 :], odd_x)
        return jnp.concatenate([one + two, one - two], 2) / float(rows * columns)

    def pick(spectrum, start, count):
        return tuple(lax.slice_in_dim(part, start, start + count, axis=3) for part in spectrum)

    def join(*spectra):
        return tuple(jnp.concatenate(parts, 3) for parts in zip(*spectra))

    spectra = forward(jnp.concatenate([point_spread[None], measured], 0))
    transfer = pick(spectra, 0, 1)
    squares = (transfer[0] ** 2, transfer[1] ** 2)
    gain = (
        jnp.where(corner, squares[0], squares[0] + squares[1]),
        jnp.where(corner, squares[1], squares[0] + squares[1]),
    )
    spectrum_0 = times(pick(spectra, 1, planes), transfer, corner, True)
    blurred_0 = linear((gain, spectrum_0))
    pair = inverse(join(spectrum_0, blurred_0))
    vector_0 = pair[:planes]
    back_0, grown_0, mapped_0 = regular(vector_0, stencil_weights)
    back_up, grown_up, mapped_up = regular(upstream, stencil_weights)
    vector_1 = pair[planes:] + back_0
    spectrum_1 = linear((1.0, blurred_0), (1.0, forward(back_0)))
    blurred_1 = linear((gain, spectrum_1))
    early = forward(jnp.concatenate([upstream, back_up], 0))
    back_1, grown_1, mapped_1 = regular(vector_1, stencil_weights)
    vector_2 = inverse(blurred_1) + back_1
    norm_0, curve_0, image_0, up_0, up_1 = total(
        jnp.stack(
            [
                jnp.sum(vector_0 * vector_0),
                jnp.sum(vector_0 * vector_1),
                jnp.sum(vector_1 * vector_1),
                jnp.sum(upstream * vector_0),
                jnp.sum(upstream * vector_1),
            ]
        ),
        1,
    )
    step_0 = norm_0 / curve_0
    residual = vector_0 - step_0 * vector_1
    residual_image = vector_1 - step_0 * vector_2
    norm_1, cross, inner, up_residual, image_cross = total(
        jnp.stack(
            [
                jnp.sum(residual * residual),
                jnp.sum(residual * vector_1),
                jnp.sum(residual * residual_image),
                jnp.sum(upstream * residual),
                jnp.sum(residual_image * vector_1),
            ]
        ),
        2,
    )
    back_2, grown_2, mapped_2 = regular(vector_2, stencil_weights)
    late = forward(jnp.concatenate([back_1, back_2], 0))
    ratio = norm_1 / norm_0
    curve_1 = inner + 2.0 * ratio * cross + ratio * ratio * curve_0
    step_1 = norm_1 / curve_1
    grad_step_1 = up_residual + ratio * up_0
    grad_curve_1 = -grad_step_1 * step_1 / curve_1
    grad_ratio = step_1 * up_0 + 2.0 * grad_curve_1 * (cross + ratio * curve_0)
    known_image = step_1 * up_1 + 2.0 * grad_curve_1 * (image_cross + ratio * image_0)
    grad_norm = grad_step_1 / curve_1 + grad_ratio / norm_0
    grad_step_0 = up_0 - known_image - 2.0 * grad_norm * cross
    grad_curve_0 = -grad_step_0 * step_0 / curve_0
    grad_norm_0 = -grad_ratio * ratio / norm_0 + grad_step_0 / curve_0

    spectrum_2 = linear((1.0, linear((gain, spectrum_1))), (1.0, pick(late, 0, planes)))
    spectrum_up = pick(early, 0, planes)
    residual_terms = ((1.0, spectrum_0), (-step_0, spectrum_1))
    direction_image = linear((1.0 + ratio, spectrum_1), (-step_0, spectrum_2))
    grad_direction = linear((step_1, spectrum_up), (2.0 * grad_curve_1, direction_image))
    grad_residual = linear((1.0, grad_direction), (2.0 * grad_norm, linear(*residual_terms)))
    grad_back = linear(
        (step_1, pick(early, planes, planes)),
        (2.0 * grad_curve_1 * (1.0 + ratio) - 2.0 * grad_norm * step_0, pick(late, 0, planes)),
        (-2.0 * grad_curve_1 * step_0, pick(late, planes, planes)),
        (2.0 * grad_norm, linear((1.0, spectrum_1), (-1.0, blurred_0))),
    )
    grad_right = linear(
        (step_0, spectrum_up),
        (ratio, grad_direction),
        (2.0 * grad_curve_0, spectrum_1),
        (2.0 * grad_norm_0, spectrum_0),
        (1.0, grad_residual),
        (-step_0, linear((gain, grad_residual), (1.0, grad_back))),
    )
    grad_measured = inverse(times(grad_right, transfer, corner))

    terms = correlate(
        jnp.stack(
            [
                step_1,
                2.0 * grad_norm,
                2.0 * grad_curve_1 * (1.0 + ratio) - 2.0 * grad_norm * step_0,
                -2.0 * grad_curve_1 * step_0,
                1.0 + ratio,
                -step_0,
                2.0 * grad_curve_0,
                -step_0,
                2.0 * grad_curve_1,
            ]
        ),
        grown_0, grown_1, grown_2, grown_up, mapped_0, mapped_1, mapped_2, mapped_up,
    )
    grad_stencil = total(terms, 3).reshape(3, 3, 3) / math.sqrt(cells)
    return (grad_measured, grad_stencil)


def spectral_fits(mesh_y, mesh_z, planes, row_count, columns):
    devices, rows, depth = (mesh_y * mesh_z, row_count * mesh_y, planes * mesh_z)
    if columns % (16 * devices) or row_count % 128 or rows % 512 or planes != 1 or mesh_z % 2:
        return False
    tiles = 2 * depth // 8 * (rows // 128)
    return depth == 4 and mesh_y % 4 == 0 and tiles % (2 * mesh_z) == 0


def wave_rows(length):
    half, quarter = (length // 2, length // 4)
    place = np.arange(half)[None, :]
    tables = []
    for odd in range(2):
        frequency = 2 * np.arange(quarter)[:, None] + odd
        angle = (place * frequency % length) * (2.0 * np.pi / length)
        cosine, sine = (np.cos(angle), np.sin(angle))
        if not odd:
            sine[0] = np.cos(np.pi * place[0])
        tables += [cosine, sine]
    table = np.stack(tables)
    high = table.astype(jnp.bfloat16)
    low = (table - high.astype(np.float64)).astype(jnp.bfloat16)
    return (high, low)


def basis(length, place):
    half = length // 2
    frequency = np.concatenate([np.arange(0, half, 2), np.arange(1, half, 2)])
    angle = frequency * place % length * (2.0 * np.pi / length)
    cosine, sine = (np.cos(angle), np.sin(angle))
    sine[0] = np.cos(np.pi * place)
    return (cosine, sine)


def axis_values(length):
    cosine, sine = basis(length, 1)
    pure = sine.copy()
    pure[0] = 0.0
    other = cosine.copy()
    other[0] = -1.0
    weight = np.full(length // 2, 2.0)
    weight[0] = 1.0
    values = [(cosine, other), (pure, pure), basis(length, 0), basis(length, length - 1), (weight, weight)]
    for place in (0, 1, length - 2, length - 1):
        values.append(tuple(weight * part / length for part in basis(length, place)))
    return np.stack([np.stack(pair) for pair in values]).astype(np.float32)


COS, SIN, FIRST, LAST, WEIGHT, AT = range(6)


def split(value):
    high = value.astype(jnp.bfloat16)
    return (high, (value - high.astype(jnp.float32)).astype(jnp.bfloat16))


def product(left, right, contracting):
    numbers = (contracting, ((), ()))

    def one(a, b):
        return lax.dot_general(a, b, numbers, preferred_element_type=jnp.float32)

    return one(left[0], right[0]) + (one(left[0], right[1]) + one(left[1], right[0]))


class Spectral:
    def __init__(self, count_y, count_z, planes, row_count, columns):
        self.ny, self.nz = (count_y, count_z)
        self.nd = count_y * count_z
        self.depth = planes * count_z
        self.row_count = row_count
        self.rows = row_count * count_y
        self.columns = columns
        self.bins = columns // 2 // self.nd
        self.half = self.rows // 2
        self.steps = self.half // 128
        self.tiers = self.bins // 8
        self.lanes = self.rows // 128
        self.tiles = 2 * self.depth // 8 * self.lanes
        self.share = self.tiles // (2 * self.nz)

    def place_of(self, index):
        return (lax.rem(index, self.ny), lax.div(index, self.ny))

    def find_place(self):
        self.y, self.z = (lax.axis_index("gy"), lax.axis_index("gz"))
        self.me = self.z * self.ny + self.y

        def turned(place, count):
            moved = [place + k for k in range(count)]
            return [jnp.where(item >= count, item - count, item) for item in moved]

        ys, zs = (turned(self.y, self.ny), turned(self.z, self.nz))
        far = sorted(range(self.ny), key=lambda k: -min(k, self.ny - k))
        self.cuts = (self.nd // 16, self.nd * 9 // 16, self.nd * 7 // 8)
        self.peers = [(ys[a], zs[b]) for a in far for b in reversed(range(self.nz)) if a or b]

    def remote_to(self, source, target, send, receive, place):
        return pltpu.make_async_remote_copy(
            src_ref=source, dst_ref=target, send_sem=send, recv_sem=receive, device_id=place, device_id_type=MESH
        )

    def scratch(self):
        Z, bins, half, nd = (self.depth, self.bins, self.half, self.nd)
        packed = (Z, 2, bins, self.rows)
        field = (Z, 4, bins, half)
        edge = (2, Z, 2, bins, 128)
        F = jnp.float32
        D = pltpu.SemaphoreType.DMA
        others = nd - 1
        names = dict(
            sent_m=pltpu.VMEM((nd, 2, bins, 128 * (self.row_count // 128)), F),
            sent_u=pltpu.VMEM((nd, 2, bins, self.row_count), F),
            sent_p=pltpu.VMEM((self.ny, 2, bins, self.row_count), F),
            got_m=pltpu.VMEM(packed, F),
            got_u=pltpu.VMEM(packed, F),
            got_p=pltpu.VMEM((2, bins, self.rows), F),
            wave=pltpu.VMEM(packed, F),
            wave_p=pltpu.VMEM((2, bins, self.rows), F),
            v0=pltpu.VMEM(field, F),
            v1=pltpu.VMEM(field, F),
            v2=pltpu.VMEM(field, F),
            up=pltpu.VMEM(field, F),
            w3=pltpu.VMEM(field, F),
            m0=pltpu.VMEM(field, F),
            m1=pltpu.VMEM(field, F),
            mw=pltpu.VMEM(field, F),
            stencil=pltpu.VMEM((3, 2, 3, bins, half), F),
            blur=pltpu.VMEM((2, 3, bins, half), F),
            gain=pltpu.VMEM((2, 2, bins, half), F),
            across=pltpu.VMEM((9, 2, bins, 128), F),
            rows_v0=pltpu.VMEM(edge, F),
            rows_v1=pltpu.VMEM(edge, F),
            rows_v2=pltpu.VMEM(edge, F),
            rows_up=pltpu.VMEM(edge, F),
            rows_w3=pltpu.VMEM(edge, F),
            rows_m0=pltpu.VMEM(edge, F),
            rows_m1=pltpu.VMEM(edge, F),
            rows_mw=pltpu.VMEM(edge, F),
            edge_rows=pltpu.VMEM(edge, F),
            cols_v0=pltpu.VMEM((4, 8, self.rows), F),
            cols_v1=pltpu.VMEM((4, 8, self.rows), F),
            cols_v2=pltpu.VMEM((4, 8, self.rows), F),
            cols_up=pltpu.VMEM((4, 8, self.rows), F),
            cols_w3=pltpu.VMEM((4, 8, self.rows), F),
            cols_m0=pltpu.VMEM((2, 8, self.rows), F),
            cols_m1=pltpu.VMEM((2, 8, self.rows), F),
            cols_mw=pltpu.VMEM((2, 8, self.rows), F),
            edge_cols=pltpu.VMEM((2, 8, self.rows), F),
            part=pltpu.VMEM((3, 5, self.tiles, 8, 128), F),
            slots=pltpu.VMEM((3, 5, others, self.share, 8, 128), F),
            sums=pltpu.VMEM((3, 5, self.share, 8, 128), F),
            full=pltpu.VMEM((3, 5, self.tiles, 8, 128), F),
            line_part=pltpu.VMEM((3, 1, 128), F),
            line_slots=pltpu.VMEM((3, others, 1, 128), F),
            line_sums=pltpu.VMEM((3, 1, 128), F),
            line_full=pltpu.VMEM((3, 1, 128), F),
            around=pltpu.VMEM(field, F),
            acc=pltpu.VMEM((8, 8, 128), F),
            turned=pltpu.VMEM((2, 4, half, half // 2), jnp.bfloat16),
            taps=pltpu.VMEM((27, 8, 128), F),
            tap_part=pltpu.VMEM((1, 128), F),
            tap_slots=pltpu.VMEM((nd, 1, 128), F),
            sent_o=pltpu.VMEM(packed, F),
            got_o=pltpu.VMEM((nd, 2, bins, self.row_count), F),
            send_big=D((4,)),
            recv_big=D((4,)),
            send_p=D,
            recv_p=D,
            send_part=D((2, 5)),
            recv_part=D((2, 5)),
            send_full=D((2, 5)),
            recv_full=D((2, 5)),
            send_tap=D,
            recv_tap=D,
        )
        return names


    def remote(self, source, target, send, receive, peer):
        return pltpu.make_async_remote_copy(
            src_ref=source, dst_ref=target, send_sem=send, recv_sem=receive,
            device_id=self.place_of(peer), device_id_type=MESH,
        )

    def arrived(self, shape, semaphore):
        self.remote(shape, shape, semaphore, semaphore, self.me).wait_recv()

    def row_lanes(self, y):
        return pl.ds(pl.multiple_of(y * self.row_count, 128), self.row_count)

    def spread_start(self, r, sent, got, lot, first=0, end=None):
        here = got.at[self.z, :, :, self.row_lanes(self.y)]
        for y, z in self.peers[first:end]:
            self.remote_to(sent.at[z * self.ny + y], here, r.send_big.at[lot], r.recv_big.at[lot], (y, z)).start()
        if first == 0:
            here[...] = sent[self.me]

    def spread_wait(self, r, sent, lot):
        others = sent.at[pl.ds(0, self.nd - 1)]
        self.arrived(others, r.recv_big.at[lot])
        self.arrived(others, r.send_big.at[lot])

    def point_start(self, r):
        here = r.got_p.at[:, :, self.row_lanes(self.y)]

        @pl.loop(1, self.ny)
        def _(k):
            peer = lax.rem(self.y + k, self.ny)
            self.remote(r.sent_p.at[peer], here, r.send_p, r.recv_p, self.z * self.ny + peer).start()

        here[...] = r.sent_p[self.y]

    def point_wait(self, r):
        others = r.sent_p.at[pl.ds(0, self.ny - 1)]
        self.arrived(others, r.recv_p)
        self.arrived(others, r.send_p)

    def return_start(self, r, first, end):
        for y, z in self.peers[first:end]:
            self.remote_to(
                r.sent_o.at[z, :, :, self.row_lanes(y)], r.got_o.at[self.me], r.send_big.at[2], r.recv_big.at[2], (y, z)
            ).start()

    def owner(self, kind, number):
        if kind == 2:
            number = self.nz
        return lax.rem(number, self.nz) * self.ny + self.ny // 2 - 1 + 2 * lax.div(number, self.nz)

    def owned(self, kind):
        low = self.ny // 2 - 1
        if kind == 2:
            return self.me == self.owner(2, 0)
        return (self.y == low) | (self.y == low + 2)

    def owners(self, kind):
        return 1 if kind == 2 else 2 * self.nz

    def mine(self, kind):
        return 0 if kind == 2 else jnp.where(self.y == self.ny // 2 - 1, 0, self.nz) + self.z

    def width(self, kind):
        return 1 if kind == 2 else self.share

    def lot(self, r, name, turn, kind, number, count=1):
        if kind == 2:
            return getattr(r, "line_" + name).at[turn]
        return getattr(r, name).at[turn, kind, pl.ds(number * self.share, count * self.share)]

    def slot(self, r, turn, kind, first, count=1):
        if kind == 2:
            return r.line_slots.at[turn, pl.ds(first, count)]
        return r.slots.at[turn, kind, pl.ds(first, count)]

    def reduce_start(self, r, turn, kinds):
        for kind in kinds:
            send, receive = (r.send_part.at[turn % 2, kind], r.recv_part.at[turn % 2, kind])

            @pl.loop(0, self.owners(kind))
            def _(number):
                owner = self.owner(kind, number)

                @pl.when(owner != self.me)
                def _():
                    place = lax.rem(self.me - owner + self.nd, self.nd) - 1
                    self.remote(
                        self.lot(r, "part", turn, kind, number), self.slot(r, turn, kind, place).at[0], send, receive, owner
                    ).start()

    def reduce_middle(self, r, turn, kinds):
        others = self.nd - 1
        for kind in kinds:
            send, receive = (r.send_full.at[turn % 2, kind], r.recv_full.at[turn % 2, kind])

            @pl.when(self.owned(kind))
            def _():
                number = self.mine(kind)
                self.arrived(self.slot(r, turn, kind, 0, others), r.recv_part.at[turn % 2, kind])
                lots = [self.lot(r, "part", turn, kind, number)[...]]
                lots += [self.slot(r, turn, kind, k)[0] for k in range(others)]
                while len(lots) > 1:
                    lots = [lots[k] + lots[k + 1] for k in range(0, len(lots) - 1, 2)] + lots[len(lots) // 2 * 2 :]
                sums = self.lot(r, "sums", turn, kind, 0)
                sums[...] = lots[0]
                full = self.lot(r, "full", turn, kind, number)
                for place in self.peers:
                    self.remote_to(sums, full, send, receive, place).start()
                full[...] = lots[0]

    def reduce_end(self, r, turn, kinds):
        for kind in kinds:
            count = self.owners(kind)

            def finish(count):
                if count:
                    self.arrived(self.lot(r, "full", turn, kind, 0, count), r.recv_full.at[turn % 2, kind])
                    self.arrived(self.lot(r, "part", turn, kind, 0, count), r.send_part.at[turn % 2, kind])

            @pl.when(self.owned(kind))
            def _():
                finish(count - 1)
                self.arrived(self.slot(r, turn, kind, 0, self.nd - 1), r.send_full.at[turn % 2, kind])

            @pl.when(jnp.logical_not(self.owned(kind)))
            def _():
                finish(count)


    def row_spectra(self, r, source, sent):
        half = self.columns // 2
        low, high = (source[:, :half], source[:, half:])
        per = self.nd // 2
        for odd, value in enumerate((low + high, low - high)):
            value = split(value)
            for part in range(2):
                table = (r.tab_x[0][2 * odd + part], r.tab_x[1][2 * odd + part])
                sent[pl.ds(odd * per, per), part] = product(table, value, ((1,), (1,))).reshape(
                    per, self.bins, self.row_count
                )

    def point_spectra(self, r, source):
        half = self.columns // 2
        low, high = (source[:, :half], source[:, half:])
        odd = lax.div(2 * self.z, self.nz)
        sign = 1.0 - 2.0 * odd.astype(jnp.float32)
        value = split(low + sign * high)
        block = self.ny * self.bins
        start = pl.multiple_of(lax.rem(self.z, self.nz // 2) * block, block)
        for part in range(2):
            table = tuple(half_table[2 * odd + part, pl.ds(start, block)] for half_table in r.tab_x)
            r.sent_p[:, part] = product(table, value, ((1,), (1,))).reshape(self.ny, self.bins, self.row_count)

    def turn_tables(self, r):
        for k in range(2):
            for part in range(4):
                r.turned[k, part] = r.tab_y[k][part].astype(jnp.float32).T.astype(jnp.bfloat16)

    def column_spectra(self, r, got, wave, turned=True):
        count = math.prod(got.shape[:-1])
        value = got[...].reshape(count, self.rows)
        low, high = (value[:, : self.half], value[:, self.half :])
        quarter = self.half // 2
        for odd, value in enumerate((low + high, low - high)):
            value = split(value)
            for part in range(2):
                tables = (r.turned.at[0], r.turned.at[1]) if turned else r.tab_y
                table = (tables[0][2 * odd + part], tables[1][2 * odd + part])
                wave[..., pl.ds(part * self.half + odd * quarter, quarter)] = product(
                    value, table, ((1,), (0 if turned else 1,))
                ).reshape(got.shape[:-1] + (quarter,))

    def column_values(self, r, wave, target):
        count = math.prod(wave.shape[:-1])
        value = wave[...].reshape(count, self.rows)
        quarter = self.half // 2
        even, odd = (
            sum(
                product(
                    split(value[:, part * self.half + k * quarter : part * self.half + (k + 1) * quarter]),
                    (r.tab_y[0][2 * k + part], r.tab_y[1][2 * k + part]),
                    ((1,), (0,)),
                )
                for part in range(2)
            )
            for k in range(2)
        )
        shape = wave.shape[:-1] + (self.half,)
        target[..., : self.half] = (even + odd).reshape(shape)
        target[..., self.half :] = (even - odd).reshape(shape)

    def row_values(self, r, got, out):
        per = self.nd // 2
        sides = []
        for k in range(2):
            side = 0.0
            for part in range(2):
                value = got[pl.ds(k * per, per), part].reshape(per * self.bins, self.row_count)
                side = side + product(
                    split(value), (r.tab_x[0][2 * k + part], r.tab_x[1][2 * k + part]), ((0,), (0,))
                )
            sides.append(side)
        half = self.columns // 2
        out[0, :, :half] = sides[0] + sides[1]
        out[0, :, half:] = sides[0] - sides[1]


    def masks(self, tier, step):
        shape = (8, 128)
        row = (lax.broadcasted_iota(jnp.int32, shape, 0) == 0) & (self.me == 0)
        lane = lax.broadcasted_iota(jnp.int32, shape, 1) + 128 * step == 0
        if tier:
            row = row & False
        return (row, lane, row & lane, row | lane)

    def combine(self, masks, ac, as_, bc, bs):
        row, lane, corner, special = masks
        pr = jnp.where(special, ac, ac - bs)
        pi = jnp.where(corner, as_, jnp.where(row, -as_, jnp.where(lane, -bc, -(as_ + bc))))
        mr = jnp.where(row, bc, jnp.where(lane, as_, ac + bs))
        mi = jnp.where(corner, bs, jnp.where(special, -bs, as_ - bc))
        return [pr, pi, mr, mi]

    def separate(self, masks, field):
        row, lane, corner, special = masks
        pr, pi, mr, mi = field
        ac = jnp.where(special, pr, 0.5 * (pr + mr))
        as_ = jnp.where(corner, pi, jnp.where(row, -pi, jnp.where(lane, mr, 0.5 * (mi - pi))))
        bc = jnp.where(row, mr, jnp.where(lane, -pi, -0.5 * (pi + mi)))
        bs = jnp.where(corner, mi, jnp.where(special, -mi, 0.5 * (mr - pr)))
        return (ac, as_, bc, bs)

    def lane_slice(self, step, part=0):
        return pl.ds(pl.multiple_of(part * self.half + step * 128, 128), 128)

    def along(self, r, which, step, part):
        return r.along[which, :, self.lane_slice(step, part)]

    def beside(self, r, which, part, tier):
        return r.across[which, part, pl.ds(8 * tier, 8)]

    def load(self, field, z, tier, step):
        return [field[z, k, pl.ds(8 * tier, 8), self.lane_slice(step)] for k in range(4)]

    def keep(self, field, z, tier, step, values):
        for k in range(4):
            field[z, k, pl.ds(8 * tier, 8), self.lane_slice(step)] = values[k]

    def load_wave(self, wave, z, tier, step):
        return [
            wave[z, part, pl.ds(8 * tier, 8), self.lane_slice(step, side)]
            for part in range(2)
            for side in range(2)
        ]

    def times(self, factor, value, conjugate=False):
        out = []
        for side in range(2):
            real, other, cross = factor[side]
            a, b = (value[2 * side], value[2 * side + 1])
            if conjugate:
                out += [real * a + cross * b, other * b - cross * a]
            else:
                out += [real * a - cross * b, other * b + cross * a]
        return out

    def factor(self, array, tier, step):
        where = (pl.ds(8 * tier, 8), self.lane_slice(step))
        return [[array[(side, k) + where] for k in range(3)] for side in range(2)]

    def sweep(self, body):
        @pl.loop(0, self.steps)
        def _(step):
            columns = {}
            for tier in range(self.tiers):
                body(tier, step, self.masks(tier, step), columns)

    def frames(self, r, masks, tier, step, z, value, rows, columns=None):
        ac, as_, bc, bs = self.separate(masks, value)
        here = pl.ds(8 * tier, 8)
        for k, which in enumerate((AT, AT + 3)):
            c, s = (self.along(r, which, step, 0), self.along(r, which, step, 1))
            rows[k, z, 0, here] += ac * c + as_ * s
            rows[k, z, 1, here] += bc * c + bs * s
        if columns is None:
            return
        for x in range(4):
            a, b = (self.beside(r, AT + x, 0, tier), self.beside(r, AT + x, 1, tier))
            for side, (p, q) in enumerate(((ac, bc), (as_, bs))):
                term = a * p + b * q
                key = (x, z, side)
                columns[key] = term if key not in columns else columns[key] + term

    def put_columns(self, r, turn, kinds, tier, step, columns):
        if tier < self.tiers - 1:
            return
        for (x, z, side), value in columns.items():
            index = x // 2 * self.depth + z
            kind = kinds[0] if x in (0, 3) else kinds[1]
            tile = index // 8 * self.lanes + side * self.steps + step
            r.part[turn, kind, tile, pl.ds(index % 8, 1)] = jnp.sum(value, 0, keepdims=True)

    def clear(self, *refs):
        for ref in refs:
            ref[...] = jnp.zeros(ref.shape, jnp.float32)

    def settle(self, rows):
        for k in range(2):
            rows[k] = jnp.broadcast_to(jnp.sum(rows[k], -1, keepdims=True), rows.shape[1:])

    def unpack(self, r, turn, kind, cols, inner):
        Z = self.depth
        for x in (1, 2) if inner else (0, 3):
            first = x // 2 * Z
            for lane in range(self.lanes):
                cols[x, pl.ds(0, Z), pl.ds(lane * 128, 128)] = r.full[
                    turn, kind, first // 8 * self.lanes + lane, pl.ds(first % 8, Z)
                ]

    def shifted(self, value, by):
        if by == 0:
            return value
        value = pltpu.roll(value, 7 if by > 0 else 1, 0)
        sub = lax.broadcasted_iota(jnp.int32, value.shape, 0)
        return jnp.where(sub < self.depth, value, 0.0)

    def corners(self, r, col):
        out = []
        for which in (AT, AT + 3):
            weight = jnp.concatenate([r.along[which, :, :]], 0)
            out.append(jnp.broadcast_to(jnp.sum(col * weight, -1, keepdims=True), (8, 128)))
        return out

    def column_tools(self, r, w, step):
        c = [self.along(r, COS, step, part) for part in range(2)]
        s = self.along(r, SIN, step, 0)
        first = [self.along(r, FIRST, step, part) for part in range(2)]
        last = [self.along(r, LAST, step, part) for part in range(2)]

        def get(col):
            return [col[:, self.lane_slice(step, part)] for part in range(2)]

        def line(a, c_index, col):
            w0, w1, w2 = (w(a, b, c_index) for b in range(3))
            turn = (w2 - w0) * s
            return [
                (w1 + (w0 + w2) * c[0]) * col[0] + turn * col[1],
                (w1 + (w0 + w2) * c[1]) * col[1] - turn * col[0],
            ]

        def stacked(pieces):
            out = None
            for a in range(3):
                for c_index, col in pieces:
                    term = [self.shifted(part, a - 1) for part in line(a, c_index, col)]
                    out = term if out is None else [p + t for p, t in zip(out, term)]
            return out

        return (first, last, get, stacked)

    def edges(self, r, w, col_first, col_last):
        Z = self.depth
        k_first, k_last = (self.corners(r, col_first[...]), self.corners(r, col_last[...]))
        total = lambda terms: sum(terms[1:], terms[0])
        q = {}
        for name, b, c, value in ((0, 0, 0, k_last[1]), (1, 0, 2, k_first[1]), (2, 2, 0, k_last[0]), (3, 2, 2, k_first[0])):
            q[name] = total([w(a, b, c) * self.shifted(value, a - 1) for a in range(3)])
        @pl.loop(0, self.steps, unroll=True)
        def _(step):
            first, last, get, stacked = self.column_tools(r, w, step)
            f, l = (get(col_first), get(col_last))
            for k, (pieces, upper, lower) in enumerate((([(0, l)], q[0], q[2]), ([(2, f)], q[1], q[3]))):
                value = stacked(pieces)
                for part in range(2):
                    r.edge_cols[k, :, self.lane_slice(step, part)] = (
                        value[part] - upper * first[part] - lower * last[part]
                    )

    def edge_lines(self, r, w, rows):
        Z = self.depth
        for tier in range(self.tiers):
            here = pl.ds(8 * tier, 8)
            c = [self.beside(r, COS, part, tier) for part in range(2)]
            s = self.beside(r, SIN, 0, tier)
            for k, (b, source) in enumerate(((0, 1), (2, 0))):
                for z in range(Z):
                    out = None
                    for a in range(3):
                        if not 0 <= z + a - 1 < Z:
                            continue
                        w0, w1, w2 = (w(a, b, c_index) for c_index in range(3))
                        turn = (w2 - w0) * s
                        p, t = (rows[source, z + a - 1, part, here] for part in range(2))
                        term = [
                            (w1 + (w0 + w2) * c[0]) * p + turn * t,
                            (w1 + (w0 + w2) * c[1]) * t - turn * p,
                        ]
                        out = term if out is None else [x + v for x, v in zip(out, term)]
                    for part in range(2):
                        r.edge_rows[k, z, part, here] = out[part]

    def map_columns(self, r, w, cols, mapped, extra=None):
        total = lambda terms: sum(terms[1:], terms[0])
        at = [self.corners(r, cols[x]) for x in range(4)]
        fix = []
        for (c0, v0), (c1, v1) in (((1, at[0]), (2, at[1])), ((0, at[2]), (1, at[3]))):
            fix.append(
                [
                    total(
                        [
                            w(a, b, c0) * self.shifted(v0[y], a - 1) + w(a, b, c1) * self.shifted(v1[y], a - 1)
                            for a in range(3)
                        ]
                    )
                    for b, y in ((0, 1), (2, 0))
                ]
            )

        @pl.loop(0, self.steps, unroll=True)
        def _(step):
            first, last, get, stacked = self.column_tools(r, w, step)
            f, n, g, l = (get(cols.at[x]) for x in range(4))
            for k, pieces in enumerate(([(1, f), (2, n)], [(0, g), (1, l)])):
                value = stacked(pieces)
                for part in range(2):
                    here = (k, slice(None), self.lane_slice(step, part))
                    value_here = value[part] - fix[k][0] * first[part] - fix[k][1] * last[part]
                    if extra is not None:
                        value_here = value_here + extra(here)
                    mapped[here] = value_here

    def edge_field(self, r, masks, tier, step, z):
        here = pl.ds(8 * tier, 8)
        out = []
        for part in range(2):
            e0, e1 = (r.edge_rows[k, z, part, here] for k in range(2))
            x0, x1 = (self.beside(r, which, part, tier) for which in (FIRST, LAST))
            for side in range(2):
                y0, y1 = (self.along(r, which, step, side) for which in (FIRST, LAST))
                c0, c1 = (r.edge_cols[k, pl.ds(z, 1), self.lane_slice(step, side)] for k in range(2))
                out.append(e0 * y0 + e1 * y1 + x0 * c0 + x1 * c1)
        return self.combine(masks, *out)

    def circular_field(self, r, tier, step, field, flip, out=None):
        Z = self.depth
        value = [self.load(field, z, tier, step) for z in range(Z)]
        out = [None] * Z if out is None else out
        for a in range(3):
            factor = self.factor(r.stencil.at[a], tier, step)
            for z in range(Z):
                other = z + (1 - a if flip else a - 1)
                if 0 <= other < Z:
                    term = self.times(factor, value[other], flip)
                    out[z] = term if out[z] is None else [o + t for o, t in zip(out[z], term)]
        return out

    def turn_round(self, r, field, out, norm=None):
        def body(tier, step, masks, columns):
            for z, value in enumerate(self.circular_field(r, tier, step, field, False)):
                self.keep(out, z, tier, step, value)
                if norm is not None:
                    own = self.load(field, z, tier, step)
                    norm[...] += self.dot(masks, own, own)

        self.sweep(body)

    def build_stencil(self, r, w):
        def body(tier, step, masks, columns):
            row, lane, corner, special = masks
            here = pl.ds(8 * tier, 8)
            sx = self.beside(r, SIN, 0, tier)
            ys = self.along(r, SIN, step, 0)
            for side in range(2):
                cx = self.beside(r, COS, side, tier)
                cy = self.along(r, COS, step, 0)
                sy = jnp.broadcast_to(ys, (8, 128))
                cy = jnp.broadcast_to(cy, (8, 128))
                if side:
                    cy = jnp.where(row, cy, self.along(r, COS, step, 1))
                    sy = jnp.where(row, sy, -sy)
                for a in range(3):
                    real, imag = ([], [])
                    for b in range(3):
                        real.append(w(a, b, 1) + (w(a, b, 0) + w(a, b, 2)) * cx)
                        imag.append((w(a, b, 2) - w(a, b, 0)) * sx)
                    value = real[1] + (real[0] + real[2]) * cy - (imag[2] - imag[0]) * sy
                    cross = imag[1] + (imag[0] + imag[2]) * cy + (real[2] - real[0]) * sy
                    other = jnp.where(corner, real[1] - (real[0] + real[2]), value)
                    for k, item in enumerate((value, other, cross)):
                        r.stencil[a, side, k, here, self.lane_slice(step)] = item

        self.sweep(body)

    def build_blur(self, r):
        def body(tier, step, masks, columns):
            row, lane, corner, special = masks
            here = pl.ds(8 * tier, 8)
            wave = [
                r.wave_p[part, here, self.lane_slice(step, side)] for part in range(2) for side in range(2)
            ]
            value = self.combine(masks, wave[0], wave[1], wave[2], wave[3])
            for side in range(2):
                real, imag = (value[2 * side], value[2 * side + 1])
                other = jnp.where(corner, imag, real)
                cross = jnp.where(corner, 0.0, imag)
                for k, item in enumerate((real, other, cross)):
                    r.blur[side, k, here, self.lane_slice(step)] = item
                square = cross * cross
                r.gain[side, 0, here, self.lane_slice(step)] = real * real + square
                r.gain[side, 1, here, self.lane_slice(step)] = other * other + square

        self.sweep(body)

    def gained(self, r, tier, step, value):
        where = (pl.ds(8 * tier, 8), self.lane_slice(step))
        return [r.gain[(k // 2, k % 2) + where] * value[k] for k in range(4)]

    def dot(self, masks, left, right):
        corner = masks[2]
        total = sum(a * b for a, b in zip(left, right))
        return jnp.where(corner, 0.5 * total, total)


    def stencil_twice(self, r, w, cols, mapped, rows_m, cols_m, make, finish, inner, extra=None):
        def flipped(a, b, c):
            return w(2 - a, 2 - b, 2 - c)

        self.edges(r, w, cols.at[0], cols.at[3])
        self.clear(rows_m)

        def forward(tier, step, masks, columns):
            for z in range(self.depth):
                value = [m - e for m, e in zip(make(tier, step, z), self.edge_field(r, masks, tier, step, z))]
                self.keep(mapped, z, tier, step, value)
                self.frames(r, masks, tier, step, z, value, rows_m)

        self.sweep(forward)
        self.settle(rows_m)
        inner()
        self.map_columns(r, w, cols, cols_m, extra)
        self.edge_lines(r, flipped, rows_m)
        self.edges(r, flipped, cols_m.at[0], cols_m.at[1])

        def back(tier, step, masks, columns):
            out = [[-e for e in self.edge_field(r, masks, tier, step, z)] for z in range(self.depth)]
            finish(tier, step, masks, columns, self.circular_field(r, tier, step, mapped, True, out))

        self.sweep(back)

    def scalars_out(self, r, turn, count):
        lane = lax.broadcasted_iota(jnp.int32, (1, 128), 1)
        line = jnp.zeros((1, 128), jnp.float32)
        for k in range(count):
            whole = jnp.sum(jnp.sum(r.acc[k], 0, keepdims=True), -1, keepdims=True)
            line = jnp.where(lane == k, whole, line)
        r.line_part[turn] = line

    def scalars_in(self, r, turn, count):
        line = r.line_full[turn]
        return [jnp.broadcast_to(line[:, k : k + 1], (8, 128)) for k in range(count)]

    def run(self, r):
        Z = self.depth
        self.find_place()

        def w(a, b, c):
            return r.weights[a, b, c]

        barrier = pltpu.get_barrier_semaphore()

        for place in self.peers:
            pl.semaphore_signal(barrier, inc=1, device_id=place, device_id_type=MESH)

        def load(name):
            far = getattr(r, "far_" + name)
            far = far.at[self.me] if name == "frequencies" else far
            return pltpu.make_async_copy(far, getattr(r, name), r.loaded.at[r.inputs.index(name)])

        tables = [name for name in r.inputs if name.startswith("wave")]
        order = ["frequencies", "weights", "along", "point_spread"] + tables + ["measured", "upstream"]
        for name in order:
            load(name).start()
        load("frequencies").wait()
        for which in range(9):
            for part in range(2):
                r.across[which, part] = jnp.broadcast_to(
                    r.frequencies[part * self.bins : (part + 1) * self.bins, which : which + 1], (self.bins, 128)
                )
        load("along").wait()
        load("weights").wait()
        self.build_stencil(r, w)
        load("point_spread").wait()
        for name in tables:
            load(name).wait()
        self.point_spectra(r, r.point_spread[...])
        load("measured").wait()
        self.row_spectra(r, r.measured[0], r.sent_m)
        pl.semaphore_wait(barrier, self.nd - 1)
        self.point_start(r)
        self.spread_start(r, r.sent_m, r.got_m, 0)
        load("upstream").wait()
        self.row_spectra(r, r.upstream[0], r.sent_u)
        self.clear(r.rows_v0, r.rows_v1, r.rows_v2, r.rows_up, r.acc, r.taps)
        self.clear(r.cols_v0, r.cols_v1, r.cols_v2, r.cols_up)

        self.point_wait(r)
        self.column_spectra(r, r.got_p, r.wave_p, False)
        self.build_blur(r)
        self.turn_tables(r)
        self.spread_wait(r, r.sent_m, 0)
        self.spread_start(r, r.sent_u, r.got_u, 1, 0, self.cuts[0])
        self.column_spectra(r, r.got_m, r.wave)

        def start(tier, step, masks, columns):
            factor = self.factor(r.blur, tier, step)
            for z in range(Z):
                value = self.combine(masks, *self.load_wave(r.wave, z, tier, step))
                value = self.times(factor, value, True)
                self.keep(r.v0, z, tier, step, value)
                self.frames(r, masks, tier, step, z, value, r.rows_v0, columns)
            self.put_columns(r, 0, (0, 1), tier, step, columns)

        self.sweep(start)
        self.reduce_start(r, 0, [0, 1])
        self.settle(r.rows_v0)
        self.edge_lines(r, w, r.rows_v0)
        self.reduce_middle(r, 0, [0, 1])
        self.spread_start(r, r.sent_u, r.got_u, 1, self.cuts[0], self.cuts[1])
        self.turn_round(r, r.v0, r.m0, r.acc.at[0])
        self.reduce_end(r, 0, [0])
        self.unpack(r, 0, 0, r.cols_v0, False)
        self.spread_start(r, r.sent_u, r.got_u, 1, self.cuts[1], self.cuts[2])

        def inner_0():
            self.reduce_end(r, 0, [1])
            self.unpack(r, 0, 1, r.cols_v0, True)

        def first(tier, step, masks, columns, back):
            for z in range(Z):
                before = self.load(r.v0, z, tier, step)
                value = [g + b for g, b in zip(self.gained(r, tier, step, before), back[z])]
                self.keep(r.v1, z, tier, step, value)
                self.frames(r, masks, tier, step, z, value, r.rows_v1, columns)
                r.acc[1] += self.dot(masks, before, value)
                r.acc[2] += self.dot(masks, value, value)
            self.put_columns(r, 1, (0, 1), tier, step, columns)

        def plain(field):
            return lambda tier, step, z: self.load(field, z, tier, step)

        self.stencil_twice(
            r, w, r.cols_v0, r.m0, r.rows_m0, r.cols_m0, plain(r.m0), first, inner_0
        )
        self.reduce_start(r, 1, [0])
        self.scalars_out(r, 1, 3)
        self.reduce_start(r, 1, [1, 2])
        self.settle(r.rows_v1)
        self.edge_lines(r, w, r.rows_v1)
        self.reduce_middle(r, 1, [0, 1, 2])
        self.spread_start(r, r.sent_u, r.got_u, 1, self.cuts[2])
        self.turn_round(r, r.v1, r.m1)
        self.spread_wait(r, r.sent_u, 1)
        self.column_spectra(r, r.got_u, r.wave)

        def upper(tier, step, masks, columns):
            for z in range(Z):
                value = self.combine(masks, *self.load_wave(r.wave, z, tier, step))
                self.keep(r.up, z, tier, step, value)
                self.frames(r, masks, tier, step, z, value, r.rows_up, columns)
                r.acc[5] += self.dot(masks, value, self.load(r.v0, z, tier, step))
                r.acc[6] += self.dot(masks, value, self.load(r.v1, z, tier, step))
            self.put_columns(r, 2, (3, 4), tier, step, columns)

        self.clear(r.acc)
        self.sweep(upper)
        self.settle(r.rows_up)
        self.reduce_end(r, 1, [0])
        self.unpack(r, 1, 0, r.cols_v1, False)
        scalars = []

        def inner_1():
            self.reduce_end(r, 1, [1, 2])
            self.unpack(r, 1, 1, r.cols_v1, True)
            self.reduce_start(r, 2, [3, 4])
            scalars.extend(self.scalars_in(r, 1, 3))
            scalars.append(scalars[0] / scalars[1])

        def second(tier, step, masks, columns, back):
            for z in range(Z):
                before, value = (self.load(f, z, tier, step) for f in (r.v0, r.v1))
                after = [g + b for g, b in zip(self.gained(r, tier, step, value), back[z])]
                self.keep(r.v2, z, tier, step, after)
                self.frames(r, masks, tier, step, z, after, r.rows_v2, columns)
                step_0 = scalars[3]
                residual = [p - step_0 * q for p, q in zip(before, value)]
                image = [p - step_0 * q for p, q in zip(value, after)]
                for k, (p, q) in enumerate(
                    ((residual, residual), (residual, value), (residual, image), (image, value))
                ):
                    r.acc[k] += self.dot(masks, p, q)
            self.put_columns(r, 2, (0, 1), tier, step, columns)

        self.stencil_twice(
            r, w, r.cols_v1, r.m1, r.rows_m1, r.cols_m1, plain(r.m1), second, inner_1
        )
        norm_0, curve_0, image_0, step_0 = scalars
        self.scalars_out(r, 2, 7)
        self.reduce_start(r, 2, [2, 0, 1])
        self.settle(r.rows_v2)
        self.reduce_middle(r, 2, [3, 4, 2, 0, 1])
        self.turn_round(r, r.up, r.around)
        self.turn_round(r, r.v2, r.mw)
        self.reduce_end(r, 2, [3, 4])
        self.unpack(r, 2, 3, r.cols_up, False)
        self.unpack(r, 2, 4, r.cols_up, True)
        self.reduce_end(r, 2, [2, 0])
        self.unpack(r, 2, 0, r.cols_v2, False)

        norm_1, cross, inner, image_cross, unused, up_0, up_1 = self.scalars_in(r, 2, 7)
        up_residual = up_0 - step_0 * up_1
        ratio = norm_1 / norm_0
        curve_1 = inner + 2.0 * ratio * cross + ratio * ratio * curve_0
        step_1 = norm_1 / curve_1
        grad_step_1 = up_residual + ratio * up_0
        grad_curve_1 = -grad_step_1 * step_1 / curve_1
        grad_ratio = step_1 * up_0 + 2.0 * grad_curve_1 * (cross + ratio * curve_0)
        grad_norm = grad_step_1 / curve_1 + grad_ratio / norm_0
        grad_step_0 = (
            up_0 - step_1 * up_1 - 2.0 * grad_curve_1 * (image_cross + ratio * image_0) - 2.0 * grad_norm * cross
        )
        more = 1.0 + ratio
        g0 = grad_norm - grad_ratio * ratio / norm_0 + grad_step_0 / curve_0
        g1 = grad_curve_1 * more * more - 2.0 * grad_norm * step_0 - grad_step_0 * step_0 / curve_0
        g2 = -2.0 * grad_curve_1 * step_0 * more + grad_norm * step_0 * step_0
        g3 = grad_curve_1 * step_0 * step_0
        q0 = step_0 + step_1 * more
        q1 = -step_1 * step_0
        mix = (g1, 2.0 * g2, 2.0 * g3, q1)

        def mixed(*values):
            return sum(m * v for m, v in zip(mix[4 - len(values) :], values))

        def mix_columns(places):
            for x in places:
                for lane in range(self.lanes):
                    here = (x, slice(None), pl.ds(lane * 128, 128))
                    r.cols_w3[here] = mixed(r.cols_v2[here], r.cols_up[here])

        mix_columns((0, 3))
        for k in range(2):
            for part in range(2):
                for tier in range(self.tiers):
                    for z in range(Z):
                        here = (k, z, part, pl.ds(8 * tier, 8))
                        r.rows_w3[here] = mixed(r.rows_v2[here], r.rows_up[here])

        self.edge_lines(r, w, r.rows_w3)

        def inner_2():
            self.reduce_end(r, 2, [1])
            self.unpack(r, 2, 1, r.cols_v2, True)
            mix_columns((1, 2))

        def make(tier, step, z):
            values = [self.load(f, z, tier, step) for f in (r.v0, r.v1, r.v2, r.up)]
            self.keep(r.w3, z, tier, step, [mixed(*parts) for parts in zip(*values)])
            values = [self.load(f, z, tier, step) for f in (r.m0, r.m1, r.mw, r.around)]
            return [mixed(*parts) for parts in zip(*values)]

        def extra(here):
            return mix[0] * r.cols_m0[here] + mix[1] * r.cols_m1[here]

        scale = 1.0 / (self.rows * self.columns)

        def last(tier, step, masks, columns, back):
            factor = self.factor(r.blur, tier, step)
            here = pl.ds(8 * tier, 8)
            for z in range(Z):
                v0, v1, w3, up = (self.load(f, z, tier, step) for f in (r.v0, r.v1, r.w3, r.up))
                value = [
                    b + d + 2.0 * g0 * p + g1 * q + q0 * u
                    for b, d, p, q, u in zip(back[z], self.gained(r, tier, step, w3), v0, v1, up)
                ]
                value = self.separate(masks, self.times(factor, value))
                for part in range(2):
                    heavy = scale * self.beside(r, WEIGHT, part, tier)
                    for side in range(2):
                        r.wave[z, part, here, self.lane_slice(step, side)] = (
                            value[2 * part + side] * heavy * self.along(r, WEIGHT, step, side)
                        )

        self.stencil_twice(
            r, w, r.cols_w3, r.mw, r.rows_mw, r.cols_mw, make, last, inner_2, extra
        )
        self.column_values(r, r.wave, r.sent_o)
        middle = len(self.peers) // 2
        self.return_start(r, 0, middle)
        for k in range(2):
            for x in (0, 3):
                if k == 0:
                    r.cols_w3[x] = r.cols_w3[x] + self.blend(mix, r.cols_v0[x], r.cols_v1[x])
            r.rows_w3[k] = r.rows_w3[k] + self.blend(mix, r.rows_v0[k], r.rows_v1[k])
        self.tap_sums(r, 2.0 * g3)

        for place in self.peers:
            self.remote_to(r.tap_part, r.tap_slots.at[self.me], r.send_tap, r.recv_tap, place).start()
        self.return_start(r, middle, None)
        r.got_o[self.me] = r.sent_o[self.z, :, :, self.row_lanes(self.y)]
        r.tap_slots[self.me] = r.tap_part[...]
        others = pl.ds(0, self.nd - 1)
        self.arrived(r.got_o.at[others], r.recv_big.at[2])
        self.row_values(r, r.got_o, r.out)
        self.arrived(r.got_o.at[others], r.send_big.at[2])
        self.arrived(r.tap_slots.at[others], r.recv_tap)
        self.arrived(r.tap_slots.at[others], r.send_tap)
        lots = [r.tap_slots[k] for k in range(self.nd)]
        while len(lots) > 1:
            lots = [lots[k] + lots[k + 1] for k in range(0, len(lots) - 1, 2)] + lots[len(lots) // 2 * 2 :]
        line = jnp.broadcast_to(lots[0] / math.sqrt(self.depth * self.rows * self.columns), (8, 128))
        for a in range(3):
            for b in range(3):
                first = 9 * a + 3 * b
                turned = pltpu.roll(line, 128 - first, 1) if first else line
                r.tap_out[a, pl.ds(b, 1)] = turned[:1, :3]

    def blend(self, mix, one, two):
        return mix[0][:1, :1] * one + mix[1][:1, :1] * two

    def tap_sums(self, r, weight):
        Z = self.depth
        pairs = ((r.v0, r.mw, None), (r.w3, r.m0, None), (r.v1, r.m1, weight))

        def body(tier, step, masks, columns):
            corner = masks[2]
            sx = self.beside(r, SIN, 0, tier)
            gamma = [[None, None, None, None] for a in range(3)]
            for left, right, scale in pairs:
                x = [self.load(left, z, tier, step) for z in range(Z)]
                if scale is not None:
                    x = [[scale * item for item in value] for value in x]
                for z in range(Z):
                    m = self.load(right, z, tier, step)
                    for a in range(3):
                        if not 0 <= z + a - 1 < Z:
                            continue
                        v = x[z + a - 1]
                        for side in range(2):
                            vr, vi, mr, mi = (v[2 * side], v[2 * side + 1], m[2 * side], m[2 * side + 1])
                            p, q = (vr * mr, vi * mi)
                            terms = (jnp.where(corner, 0.5 * (p + q), p + q), jnp.where(corner, 0.5 * (p - q), p + q), vi * mr - vr * mi)
                            old = gamma[a][side]
                            gamma[a][side] = terms if old is None else [o + t for o, t in zip(old, terms)]
            for a in range(3):
                sums = [0.0] * 9
                for side in range(2):
                    cx = self.beside(r, COS, side, tier)
                    cy = jnp.broadcast_to(self.along(r, COS, step, 0), (8, 128))
                    sy = jnp.broadcast_to(self.along(r, SIN, step, 0), (8, 128))
                    if side:
                        cy = jnp.where(masks[0], cy, self.along(r, COS, step, 1))
                        sy = jnp.where(masks[0], sy, -sy)
                    near, far, turn = gamma[a][side]
                    items = (
                        near, near * cx, far * cy, far * cy * cx, near * sx * sy,
                        turn * sx, turn * sy, turn * cx * sy, turn * sx * cy,
                    )
                    sums = [s + item for s, item in zip(sums, items)]
                for k in range(9):
                    r.taps[9 * a + k] += sums[k]

        self.sweep(body)

        sides = (
            (r.rows_v0, r.cols_v0, r.rows_mw, r.cols_mw, None),
            (r.rows_w3, r.cols_w3, r.rows_m0, r.cols_m0, None),
            (r.rows_v1, r.cols_v1, r.rows_m1, r.cols_m1, weight),
        )
        zero = jnp.zeros((8, 128), jnp.float32)
        by_row = [[[zero] * 3 for k in range(2)] for a in range(3)]
        by_col = [[[zero] * 3 for k in range(2)] for a in range(3)]
        by_corner = [[[zero] * 2 for k in range(2)] for a in range(3)]
        for rows_x, cols_x, rows_m, cols_m, scale in sides:
            extra = 1.0 if scale is None else scale
            for tier in range(self.tiers):
                here = pl.ds(8 * tier, 8)
                heavy = self.beside(r, WEIGHT, 0, tier) * extra
                ca, cb = (self.beside(r, COS, part, tier) for part in range(2))
                s = self.beside(r, SIN, 0, tier)
                for k in range(2):
                    for z in range(Z):
                        ma, mb = (rows_m[k, z, part, here] for part in range(2))
                        for a in range(3):
                            if not 0 <= z + a - 1 < Z:
                                continue
                            xa, xb = (rows_x[1 - k, z + a - 1, part, here] for part in range(2))
                            p, q = (heavy * xa * ma, heavy * xb * mb)
                            terms = (p + q, p * ca + q * cb, heavy * s * (xa * mb - xb * ma))
                            by_row[a][k] = [o + t for o, t in zip(by_row[a][k], terms)]
            for k in range(2):
                col_x, col_m = (cols_x.at[0 if k else 3], cols_m.at[k])
                for step in range(self.steps):
                    (xc, xs), (mc, ms) = (
                        [ref[:, pl.ds(part * self.half + 128 * step, 128)] * (extra if ref is col_x else 1.0) for part in range(2)]
                        for ref in (col_x, col_m)
                    )
                    heavy = self.along(r, WEIGHT, step, 0)
                    cc, cs = (self.along(r, COS, step, part) for part in range(2))
                    s = self.along(r, SIN, step, 0)
                    for a in range(3):
                        xc_a, xs_a = (self.shifted(item, a - 1) for item in (xc, xs))
                        p, q = (heavy * xc_a * mc, heavy * xs_a * ms)
                        terms = (p + q, p * cc + q * cs, heavy * s * (xc_a * ms - xs_a * mc))
                        by_col[a][k] = [o + t for o, t in zip(by_col[a][k], terms)]
                at_x, at_m = (self.corners(r, ref[...]) for ref in (col_x, col_m))
                for a in range(3):
                    for edge in range(2):
                        term = extra * self.shifted(at_x[1 - edge], a - 1) * at_m[edge]
                        by_corner[a][edge][k] = by_corner[a][edge][k] + term

        lots = []
        for a in range(3):
            s = [r.taps[9 * a + k] for k in range(9)]
            for b in range(3):
                for c in range(3):
                    beta, gamma = (float(b - 1), float(c - 1))
                    if b == 1 and c == 1:
                        value = s[0]
                    elif b == 1:
                        value = s[1] - gamma * s[5]
                    elif c == 1:
                        value = s[2] - beta * s[6]
                    else:
                        value = s[3] - beta * gamma * s[4] - beta * s[7] - gamma * s[8]
                    value = value * (2.0 / (self.rows * self.columns))
                    if b != 1:
                        one, two, three = by_row[a][b // 2]
                        value = value - (one if c == 1 else two - gamma * three) * (1.0 / (128 * self.columns))
                    if c != 1:
                        one, two, three = by_col[a][c // 2]
                        value = value - (one if b == 1 else two - beta * three) * (1.0 / (self.rows * self.nd))
                    if b != 1 and c != 1:
                        value = value + by_corner[a][b // 2][c // 2] * (1.0 / (128 * self.nd))
                    lots.append(value)
        lane = lax.broadcasted_iota(jnp.int32, (1, 128), 1)
        line = jnp.zeros((1, 128), jnp.float32)
        for k, value in enumerate(lots):
            whole = jnp.sum(jnp.sum(value, 0, keepdims=True), -1, keepdims=True)
            line = jnp.where(lane == k, whole, line)
        r.tap_part[...] = line


class Refs:
    def __init__(self, names, refs):
        for name, ref in zip(names, refs):
            setattr(self, name, ref)


def spectral(measured, point_spread, stencil_weights, upstream):
    planes, row_count, columns = measured.shape
    plan = Spectral(lax.axis_size("gy"), lax.axis_size("gz"), planes, row_count, columns)
    waves = [jnp.asarray(part) for part in wave_rows(columns)]
    if plan.rows != columns:
        waves += [jnp.asarray(part) for part in wave_rows(plan.rows)]
    along = jnp.asarray(axis_values(plan.rows).reshape(9, 1, plan.rows))
    across = axis_values(columns).reshape(9, 2, plan.nd, plan.bins).transpose(2, 1, 3, 0)
    frequencies = np.zeros((plan.nd, 2 * plan.bins, 128), np.float32)
    frequencies[:, :, :9] = across.reshape(plan.nd, 2 * plan.bins, 9)
    scratch = plan.scratch()
    arrays = dict(weights=stencil_weights, measured=measured, point_spread=point_spread, upstream=upstream, along=along)
    arrays.update({"wave_%d" % k: part for k, part in enumerate(waves)})
    arrays["frequencies"] = jnp.asarray(frequencies)
    for name, array in arrays.items():
        shape = array.shape[1:] if name == "frequencies" else array.shape
        space = pltpu.SMEM if name == "weights" else pltpu.VMEM
        scratch[name] = space(shape, array.dtype)
    scratch["loaded"] = pltpu.SemaphoreType.DMA((len(arrays),))
    names = ["far_" + name for name in arrays] + ["out", "tap_out"] + list(scratch)

    def body(*refs):
        r = Refs(names, refs)
        r.tab_x = (r.wave_0, r.wave_1)
        r.tab_y = (r.wave_2, r.wave_3) if len(waves) > 2 else r.tab_x
        r.inputs = list(arrays)
        plan.run(r)

    out, taps = pl.pallas_call(
        body,
        out_shape=(
            jax.ShapeDtypeStruct(measured.shape, jnp.float32),
            jax.ShapeDtypeStruct((3, 3, 3), jnp.float32),
        ),
        in_specs=[HBM] * len(arrays),
        out_specs=(VMEM, VMEM),
        scratch_shapes=list(scratch.values()),
        compiler_params=pltpu.CompilerParams(
            collective_id=0, has_side_effects=True, vmem_limit_bytes=32 * 1024 * 1024
        ),
        name="spectral",
    )(
        *(pltpu.with_memory_space_constraint(array, pltpu.HBM) for array in arrays.values())
    )
    return (out, taps)


def solution(mesh):
    def program(measured, point_spread, stencil_weights, upstream):
        planes, row_count, columns = measured.shape
        fits = spectral_fits(mesh.shape["gy"], mesh.shape["gz"], planes, row_count, columns)
        chosen = spectral if fits else local
        return chosen(measured, point_spread, stencil_weights, upstream)

    return jax.shard_map(
        program,
        mesh=mesh,
        in_specs=(P("gz", "gy", None), P("gy", None), P(), P("gz", "gy", None)),
        out_specs=(P("gz", "gy", None), P()),
        check_vma=False,
    )
```
